32 devices in a mesh: dp: 2 (over x), tp: 16 (over z, y, core).
Axes of the slice: x: 2, y: 2, z: 4, core: 2. Of those that a mesh axis runs over, the one named last changes fastest.
Arguments:
- x_in: bfloat16 [8192, 4096], P(('dp', 'tp')), parts along dimension 0
- grad_out: bfloat16 [8192, 4096], P(('dp', 'tp')), parts along dimension 0
- positions: int32 [8192], P('dp'), parts along dimension 0
- norm_gain: float32 [4096], replicated
- w_query: bfloat16 [4096, 4096], P(None, 'tp')
- w_key: bfloat16 [4096, 1024], replicated
- w_value: bfloat16 [4096, 1024], replicated
- w_out: bfloat16 [4096, 4096], P('tp')
Outputs:
- output 1: bfloat16 [8192, 4096], P(('dp', 'tp')), parts along dimension 0
- output 2: bfloat16 [8192, 4096], P(('dp', 'tp')), parts along dimension 0
- output 3: bfloat16 [8192, 4096], P('dp', 'tp'), parts along dimension 0
- output 4: float32 [8192, 2048], P('dp', 'tp'), parts along dimension 0
- output 5: float32 [8192, 2048], P('dp', 'tp'), parts along dimension 0
- output 6: bfloat16 [8192, 4096], P(('dp', 'tp')), parts along dimension 0
- output 7: float32 [8192], P('dp'), parts along dimension 0
There are 2 independent parts. The reference program is written for one: setup_inputs(seed, part) draws one part's arguments, and reference() takes and returns one part's arrays. A program takes and returns all parts, laid end to end along the dimension named above; an argument that names none is the same for every part.
All inputs are finite; a program needn't handle non-finite values.
Results may differ from the reference program's by a relative error of at most 0.0199236.
Values are sent between devices in bfloat16 or wider.
A program may use at most 1 GiB of HBM per device.

```python
import functools
import jax
import jax.numpy as jnp
from jax import lax

D_MODEL = 4096
Q_HEADS = 32
KV_HEADS = 8
HEAD_DIM = 128
TP_SIZE = 16
SEQ_LEN = 4096
QUERY_BLOCK = 128
NUM_DOCS = 4
KV_REPEAT = TP_SIZE // KV_HEADS
GROUP_SIZE = Q_HEADS // KV_HEADS
SCORE_SCALE = HEAD_DIM ** -0.5
ROPE_THETA = 1000000.0
NORM_EPS = 1e-05


def draw_positions(pos_key):
    starts = jax.random.randint(pos_key, (NUM_DOCS - 1,), 1, SEQ_LEN)
    tok_idx = jnp.arange(SEQ_LEN, dtype=jnp.int32)
    doc_start = jnp.max(jnp.where(starts[None, :] <= tok_idx[:, None], starts[None, :], 0), axis=1)
    return (tok_idx - doc_start).astype(jnp.int32)


def setup_inputs(seed: int = 0, part: int = 0) -> dict:
    root_key = jax.random.key(seed)
    shared_key, part_root = jax.random.split(root_key)
    part_key = jax.random.fold_in(part_root, part)
    key_x, key_dy, key_pos = jax.random.split(part_key, 3)
    key_g, key_q, key_k, key_v, key_o = jax.random.split(shared_key, 5)
    q_width = Q_HEADS * HEAD_DIM
    kv_width = KV_HEADS * HEAD_DIM
    in_scale = D_MODEL ** -0.5
    x_in = 0.25 * jax.random.normal(key_x, (SEQ_LEN, D_MODEL), jnp.float32)
    grad_out = jax.random.normal(key_dy, (SEQ_LEN, D_MODEL), jnp.float32)
    positions = draw_positions(key_pos)
    norm_gain = jax.random.uniform(key_g, (D_MODEL,), jnp.float32, 0.5, 1.5)
    w_query = jax.random.normal(key_q, (D_MODEL, q_width), jnp.float32) * in_scale
    w_key = jax.random.normal(key_k, (D_MODEL, kv_width), jnp.float32) * in_scale
    w_value = jax.random.normal(key_v, (D_MODEL, kv_width), jnp.float32) * in_scale
    w_out = jax.random.normal(key_o, (q_width, D_MODEL), jnp.float32) * (2.0 * q_width ** -0.5)
    return {'x_in': x_in.astype(jnp.bfloat16), 'grad_out': grad_out.astype(jnp.bfloat16), 'positions': positions, 'norm_gain': norm_gain, 'w_query': w_query.astype(jnp.bfloat16), 'w_key': w_key.astype(jnp.bfloat16), 'w_value': w_value.astype(jnp.bfloat16), 'w_out': w_out.astype(jnp.bfloat16)}


def apply_rope(tensor, cos_t, sin_t):
    half_dim = HEAD_DIM // 2
    t_f32 = tensor.astype(jnp.float32)
    lead_half = t_f32[..., :half_dim]
    tail_half = t_f32[..., half_dim:]
    return jnp.concatenate([lead_half * cos_t - tail_half * sin_t, tail_half * cos_t + lead_half * sin_t], axis=-1).astype(jnp.bfloat16)


def forward_one(x_f32, norm_gain, w_query, w_key_f32, w_value_f32, w_out, positions):
    inv_rms = lax.rsqrt(jnp.mean(x_f32 * x_f32, axis=-1, keepdims=True) + NORM_EPS)
    hidden = (x_f32 * inv_rms * norm_gain).astype(jnp.bfloat16)
    hidden_f32 = hidden.astype(jnp.float32)
    query_proj = jnp.dot(hidden, w_query, preferred_element_type=jnp.float32).astype(jnp.bfloat16)
    key_proj = jnp.dot(hidden_f32, w_key_f32, preferred_element_type=jnp.float32).astype(jnp.bfloat16)
    value_proj = jnp.dot(hidden_f32, w_value_f32, preferred_element_type=jnp.float32).astype(jnp.bfloat16)
    exponents = jnp.arange(0, HEAD_DIM, 2, dtype=jnp.float32) / HEAD_DIM
    angles = positions.astype(jnp.float32)[:, None] * jnp.power(ROPE_THETA, -exponents)[None, :]
    cos_t = jnp.cos(angles)
    sin_t = jnp.sin(angles)
    q_rot = apply_rope(query_proj.reshape(SEQ_LEN, KV_HEADS, GROUP_SIZE, HEAD_DIM), cos_t[:, None, None, :], sin_t[:, None, None, :])
    k_rot = apply_rope(key_proj.reshape(SEQ_LEN, KV_HEADS, HEAD_DIM), cos_t[:, None, :], sin_t[:, None, :])
    key_f32 = k_rot.astype(jnp.float32)
    value_f32 = value_proj.reshape(SEQ_LEN, KV_HEADS, HEAD_DIM).astype(jnp.float32)
    col_idx = jnp.arange(SEQ_LEN, dtype=jnp.int32)
    key_doc = positions - col_idx

    def one_block(blk_item):
        q_blk, q_pos, row_idx = blk_item
        scores = jnp.einsum('qkgd,skd->kgqs', q_blk.astype(jnp.float32), key_f32) * SCORE_SCALE
        keep_mask = (col_idx[None, :] <= row_idx[:, None]) & (key_doc[None, :] == (q_pos - row_idx)[:, None])
        scores = jnp.where(keep_mask, scores, -1e30)
        prob_blk = jax.nn.softmax(scores, axis=-1).astype(jnp.bfloat16).astype(jnp.float32)
        return jnp.einsum('kgqs,skd->qkgd', prob_blk, value_f32).astype(jnp.bfloat16)

    num_blk = SEQ_LEN // QUERY_BLOCK
    blk_out = lax.map(jax.checkpoint(one_block), (q_rot.reshape(num_blk, QUERY_BLOCK, KV_HEADS, GROUP_SIZE, HEAD_DIM), positions.reshape(num_blk, QUERY_BLOCK), col_idx.reshape(num_blk, QUERY_BLOCK)))
    attn_flat = blk_out.reshape(SEQ_LEN, Q_HEADS * HEAD_DIM)
    attn_mix = jnp.dot(attn_flat, w_out, preferred_element_type=jnp.float32)
    return (x_f32 + attn_mix).astype(jnp.bfloat16)


def reference(x_in, grad_out, positions, norm_gain, w_query, w_key, w_value, w_out):
    x_f32 = x_in.astype(jnp.float32)
    forward = functools.partial(forward_one, positions=positions)
    result, pull_back = jax.vjp(forward, x_f32, norm_gain, w_query, w_key.astype(jnp.float32), w_value.astype(jnp.float32), w_out)
    d_x, d_gain, d_wq, d_wk, d_wv, d_wo = pull_back(grad_out)
    copy_shape = (D_MODEL, KV_HEADS, KV_REPEAT, HEAD_DIM)
    grad_wk = jnp.broadcast_to(d_wk.reshape(D_MODEL, KV_HEADS, 1, HEAD_DIM), copy_shape).reshape(D_MODEL, TP_SIZE * HEAD_DIM)
    grad_wv = jnp.broadcast_to(d_wv.reshape(D_MODEL, KV_HEADS, 1, HEAD_DIM), copy_shape).reshape(D_MODEL, TP_SIZE * HEAD_DIM)
    return (result, d_x.astype(jnp.bfloat16), d_wq, grad_wk, grad_wv, d_wo, d_gain)
```

```python
import functools
import jax
import jax.numpy as jnp
from jax import lax
from jax.experimental import pallas as pl
from jax.experimental.pallas import tpu as pltpu
from jax.sharding import PartitionSpec as P

HEAD_DIM = 128
SCORE_SCALE = HEAD_DIM ** -0.5
SCALE_LOG2E = SCORE_SCALE * 1.4426950408889634
ROPE_THETA = 1000000.0
NORM_EPS = 1e-05
MASKED = -1e30
Y_SIZE = 2
CORE_SIZE = 2
NATURAL = (((1,), (0,)), ((), ()))
ROWS_OF_BOTH = (((0,), (0,)), ((), ()))
COLS_OF_BOTH = (((1,), (1,)), ((), ()))


def dot_f32(lhs, rhs, dims=NATURAL):
    return lax.dot_general(lhs, rhs, dims, preferred_element_type=jnp.float32)


def rope_tables(positions):
    exponents = jnp.arange(0, HEAD_DIM, 2, dtype=jnp.float32) / HEAD_DIM
    angles = jnp.power(ROPE_THETA, -exponents)[:, None] * positions.astype(jnp.float32)[None, :]
    return jnp.cos(angles), jnp.sin(angles)


def rotate_rows(t_f32, cos_t, sin_t):
    lead_half, tail_half = t_f32[:HEAD_DIM // 2], t_f32[HEAD_DIM // 2:]
    return jnp.concatenate([lead_half * cos_t - tail_half * sin_t, tail_half * cos_t + lead_half * sin_t], axis=0).astype(jnp.bfloat16)


def unrotate_cols(t_f32, cos_t, sin_t):
    lead_half, tail_half = t_f32[:, :HEAD_DIM // 2], t_f32[:, HEAD_DIM // 2:]
    return jnp.concatenate([lead_half * cos_t + tail_half * sin_t, tail_half * cos_t - lead_half * sin_t], axis=1).astype(jnp.bfloat16)


def norm_forward(x_f32, norm_gain):
    inv_rms = lax.rsqrt(jnp.mean(x_f32 * x_f32, axis=-1, keepdims=True) + NORM_EPS)
    x_hat = x_f32 * inv_rms
    return (x_hat * norm_gain).astype(jnp.bfloat16), x_hat, inv_rms


def norm_backward(d_hidden, x_hat, inv_rms, norm_gain):
    d_f32 = d_hidden.astype(jnp.float32)
    d_gain = jnp.sum(d_f32 * x_hat, axis=0)
    scaled = d_f32 * norm_gain
    d_input = inv_rms * (scaled - x_hat * jnp.mean(scaled * x_hat, axis=-1, keepdims=True))
    return d_input, d_gain


def block_token(y_ref, b, bq):
    return pl.multiple_of((b // 2) * (4 * bq) + y_ref[0] * (2 * bq) + (b % 2) * bq, bq)


def key_range(pos_ref, start, bq, bk):
    lo_first, lo_last = start - pos_ref[start], start + bq - 1 - pos_ref[start + bq - 1]
    return lo_first // bk, (start + bq - 1) // bk + 1, (lo_last + bk - 1) // bk, (start + 1) // bk


def tile_lanes(row, heads):
    return jnp.concatenate([row] * heads, axis=1)


def row_bounds(lo_ref, start, bq, heads):
    tok = start + lax.broadcasted_iota(jnp.int32, (1, bq), 1)
    return tile_lanes(tok, heads), tile_lanes(lo_ref[:, pl.ds(start, bq)], heads)


def keep_mask(key_start, bk, t_row, lo_row):
    key_idx = key_start + lax.broadcasted_iota(jnp.int32, (bk, t_row.shape[1]), 0)
    return (key_idx <= t_row) & (key_idx >= lo_row)


def head_columns(block, h):
    return block[:, h * HEAD_DIM:(h + 1) * HEAD_DIM]


def rotated_queries(q_ref, cos_ref, sin_ref, start, bq, heads):
    cos_t, sin_t = cos_ref[:, pl.ds(start, bq)], sin_ref[:, pl.ds(start, bq)]
    return [rotate_rows(head_columns(q_ref, h).T.astype(jnp.float32), cos_t, sin_t) for h in range(heads)]


def visit_keys(bounds, step):
    first, end, inner_first, inner_end = bounds

    def visit(j, carry):
        inner = (j >= inner_first) & (j < inner_end)

        @pl.when(inner)
        def _():
            step(j, False)

        @pl.when(jnp.logical_not(inner))
        def _():
            step(j, True)

        return carry

    lax.fori_loop(first, end, visit, 0)


def fwd_kernel(heads, bk, y_ref, pos_ref, q_ref, kv_ref, cos_ref, sin_ref, lo_ref, o_ref, lse_ref, k_s, vt_s, qt_s, m_s, l_s, acc_s):
    b = pl.program_id(0)
    bq = q_ref.shape[0]
    seq = kv_ref.shape[0]

    @pl.when(b == 0)
    def _():
        def prepare(s, carry):
            rows = pl.ds(pl.multiple_of(s * bk, bk), bk)
            k_s[rows, :] = rotate_rows(kv_ref[rows, :HEAD_DIM].T.astype(jnp.float32), cos_ref[:, rows], sin_ref[:, rows]).T
            vt_s[:, rows] = kv_ref[rows, HEAD_DIM:].T
            return carry

        lax.fori_loop(0, seq // bk, prepare, 0)

    start = block_token(y_ref, b, bq)
    t_row, lo_row = row_bounds(lo_ref, start, bq, heads)
    qt_s[...] = jnp.concatenate(rotated_queries(q_ref, cos_ref, sin_ref, start, bq, heads), axis=1)
    m_s[...] = jnp.full_like(m_s, MASKED)
    l_s[...] = jnp.zeros_like(l_s)
    acc_s[...] = jnp.zeros_like(acc_s)

    def step(j, masked):
        key_start = pl.multiple_of(j * bk, bk)
        keys = pl.ds(key_start, bk)
        scores = dot_f32(k_s[keys, :], qt_s[...])
        if masked:
            scores = jnp.where(keep_mask(key_start, bk, t_row, lo_row), scores, MASKED)
        m_old = m_s[...]
        m_new = jnp.maximum(m_old, jnp.max(scores, axis=0, keepdims=True))
        probs = jnp.exp2(scores * SCALE_LOG2E - m_new * SCALE_LOG2E)
        alpha = jnp.exp2((m_old - m_new) * SCALE_LOG2E)
        m_s[...] = m_new
        l_s[...] = l_s[...] * alpha + jnp.sum(probs, axis=0, keepdims=True)
        acc_s[...] = acc_s[...] * alpha + dot_f32(vt_s[:, keys], probs.astype(jnp.bfloat16))

    visit_keys(key_range(pos_ref, start, bq, bk), step)
    out_t = (acc_s[...] / l_s[...]).astype(jnp.bfloat16)
    for h in range(heads):
        o_ref[:, h * HEAD_DIM:(h + 1) * HEAD_DIM] = out_t[:, h * bq:(h + 1) * bq].T
    lse_ref[0] = m_s[...] * SCALE_LOG2E + jnp.log2(l_s[...])


def bwd_kernel(heads, bk, y_ref, pos_ref, q_ref, do_ref, o_ref, kv_ref, cos_ref, sin_ref, lo_ref, lse_ref, dq_ref, dkv_ref, k_s, kt_s, q_s, qt_s, do_s, dot_s, dqt_s):
    b = pl.program_id(0)
    bq = q_ref.shape[0]
    seq = kv_ref.shape[0]

    @pl.when(b == 0)
    def _():
        def prepare(s, carry):
            rows = pl.ds(pl.multiple_of(s * bk, bk), bk)
            dkv_ref[rows, :] = jnp.zeros((bk, 2 * HEAD_DIM), jnp.float32)
            k_rot_t = rotate_rows(kv_ref[rows, :HEAD_DIM].T.astype(jnp.float32), cos_ref[:, rows], sin_ref[:, rows])
            kt_s[:, rows] = k_rot_t
            k_s[rows, :] = k_rot_t.T
            return carry

        lax.fori_loop(0, seq // bk, prepare, 0)

    start = block_token(y_ref, b, bq)
    t_row, lo_row = row_bounds(lo_ref, start, bq, heads)
    deltas = []
    for h, q_rot_t in enumerate(rotated_queries(q_ref, cos_ref, sin_ref, start, bq, heads)):
        lanes = slice(h * bq, (h + 1) * bq)
        qt_s[:, lanes] = q_rot_t
        q_s[lanes, :] = q_rot_t.T
        do_head = head_columns(do_ref, h)
        do_s[lanes, :] = do_head
        do_t = do_head.T
        dot_s[:, lanes] = do_t
        deltas.append(jnp.sum(do_t.astype(jnp.float32) * head_columns(o_ref, h).T.astype(jnp.float32), axis=0, keepdims=True))
    delta = jnp.concatenate(deltas, axis=1)
    lse = lse_ref[0]
    dqt_s[...] = jnp.zeros_like(dqt_s)

    def step(j, masked):
        key_start = pl.multiple_of(j * bk, bk)
        keys = pl.ds(key_start, bk)
        scores = dot_f32(k_s[keys, :], qt_s[...])
        probs = jnp.exp2(scores * SCALE_LOG2E - lse)
        if masked:
            probs = jnp.where(keep_mask(key_start, bk, t_row, lo_row), probs, 0.0)
        d_probs = dot_f32(kv_ref[keys, HEAD_DIM:], dot_s[...])
        d_scores = (probs * (d_probs - delta)).astype(jnp.bfloat16)
        dkv_ref[keys, HEAD_DIM:] += dot_f32(probs.astype(jnp.bfloat16), do_s[...])
        dkv_ref[keys, :HEAD_DIM] += dot_f32(d_scores, q_s[...]) * SCORE_SCALE
        dqt_s[...] += dot_f32(kt_s[:, keys], d_scores)

    visit_keys(key_range(pos_ref, start, bq, bk), step)
    cos_t, sin_t = cos_ref[:, pl.ds(start, bq)], sin_ref[:, pl.ds(start, bq)]
    for h in range(heads):
        dq_rot_t = (dqt_s[:, h * bq:(h + 1) * bq] * SCORE_SCALE).astype(jnp.bfloat16).astype(jnp.float32)
        dq_ref[:, h * HEAD_DIM:(h + 1) * HEAD_DIM] = rotate_rows(dq_rot_t, cos_t, -sin_t).T


def attention_specs(bq, heads, seq):
    row = pl.BlockSpec((bq, heads * HEAD_DIM), lambda b, *_: (b, 0))
    keys = pl.BlockSpec((seq, 2 * HEAD_DIM), lambda b, *_: (0, 0))
    table = pl.BlockSpec((HEAD_DIM // 2, seq), lambda b, *_: (0, 0))
    bound = pl.BlockSpec((1, seq), lambda b, *_: (0, 0))
    vec = pl.BlockSpec((1, 1, heads * bq), lambda b, *_: (b, 0, 0))
    return row, keys, table, bound, vec


def attend(y_one, positions, qkv, kv_all, cos_t, sin_t, lo_all, heads, bq, bk):
    rows, seq = qkv.shape[0], kv_all.shape[0]
    row, keys, table, bound, vec = attention_specs(bq, heads, seq)
    lanes, width = heads * bq, heads * HEAD_DIM
    return pl.pallas_call(
        functools.partial(fwd_kernel, heads, bk),
        out_shape=(jax.ShapeDtypeStruct((rows, width), jnp.bfloat16), jax.ShapeDtypeStruct((rows // bq, 1, lanes), jnp.float32)),
        grid_spec=pltpu.PrefetchScalarGridSpec(
            num_scalar_prefetch=2, grid=(rows // bq,),
            in_specs=[row, keys, table, table, bound], out_specs=(row, vec),
            scratch_shapes=[pltpu.VMEM((seq, HEAD_DIM), jnp.bfloat16), pltpu.VMEM((HEAD_DIM, seq), jnp.bfloat16), pltpu.VMEM((HEAD_DIM, lanes), jnp.bfloat16),
                            pltpu.VMEM((1, lanes), jnp.float32), pltpu.VMEM((1, lanes), jnp.float32), pltpu.VMEM((HEAD_DIM, lanes), jnp.float32)]),
        compiler_params=pltpu.CompilerParams(dimension_semantics=('arbitrary',), vmem_limit_bytes=48 << 20),
        cost_estimate=pl.CostEstimate(flops=4 * rows * heads * seq * HEAD_DIM, bytes_accessed=4 * rows * width + 4 * seq * HEAD_DIM, transcendentals=rows * heads * seq // 2),
        name='attend_fwd',
    )(y_one, positions, qkv, kv_all, cos_t, sin_t, lo_all)


def attend_backward(y_one, positions, qkv, d_o, o_own, kv_all, cos_t, sin_t, lo_all, lse, heads, bq, bk):
    rows, seq = qkv.shape[0], kv_all.shape[0]
    row, keys, table, bound, vec = attention_specs(bq, heads, seq)
    lanes, width = heads * bq, heads * HEAD_DIM
    return pl.pallas_call(
        functools.partial(bwd_kernel, heads, bk),
        out_shape=(jax.ShapeDtypeStruct((rows, width), jnp.bfloat16), jax.ShapeDtypeStruct((seq, 2 * HEAD_DIM), jnp.float32)),
        grid_spec=pltpu.PrefetchScalarGridSpec(
            num_scalar_prefetch=2, grid=(rows // bq,),
            in_specs=[row, row, row, keys, table, table, bound, vec], out_specs=(row, keys),
            scratch_shapes=[pltpu.VMEM((seq, HEAD_DIM), jnp.bfloat16), pltpu.VMEM((HEAD_DIM, seq), jnp.bfloat16),
                            pltpu.VMEM((lanes, HEAD_DIM), jnp.bfloat16), pltpu.VMEM((HEAD_DIM, lanes), jnp.bfloat16),
                            pltpu.VMEM((lanes, HEAD_DIM), jnp.bfloat16), pltpu.VMEM((HEAD_DIM, lanes), jnp.bfloat16), pltpu.VMEM((HEAD_DIM, lanes), jnp.float32)]),
        compiler_params=pltpu.CompilerParams(dimension_semantics=('arbitrary',), vmem_limit_bytes=56 << 20),
        cost_estimate=pl.CostEstimate(flops=10 * rows * heads * seq * HEAD_DIM, bytes_accessed=8 * rows * width + 12 * seq * HEAD_DIM, transcendentals=rows * heads * seq // 2),
        name='attend_bwd',
    )(y_one, positions, qkv, d_o, o_own, kv_all, cos_t, sin_t, lo_all, lse)


def solution(mesh):
    tp_size = mesh.shape['tp']
    quad = Y_SIZE * CORE_SIZE
    z_size = tp_size // quad

    def member(z, y, c):
        return (z * Y_SIZE + y) * CORE_SIZE + c

    every = [(z, y, c) for z in range(z_size) for y in range(Y_SIZE) for c in range(CORE_SIZE)]
    half_groups = [[member(z, y, c) for z in range(z_size) for c in range(CORE_SIZE)] for y in range(Y_SIZE)]
    line_groups = [[member(z, y, c) for z in range(z_size)] for y in range(Y_SIZE) for c in range(CORE_SIZE)]
    core_perm = [(member(z, y, c), member(z, y, 1 - c)) for z, y, c in every]
    y_perm = [(member(z, y, c), member(z, 1 - y, c)) for z, y, c in every]
    same_head_perm = [(member(z, y, c), member(z, 1 - y, 1 - c)) for z, y, c in every]

    def swap_core(val):
        return lax.ppermute(val, 'tp', core_perm)

    def swap_y(val):
        return lax.ppermute(val, 'tp', y_perm)

    def swap_same_head(val):
        return lax.ppermute(val, 'tp', same_head_perm)

    def sum_over_tp(val):
        val = val + swap_core(val)
        val = val + swap_y(val)
        stride = 1
        while stride < z_size:
            val = val + lax.ppermute(val, 'tp', [(member(z, y, c), member(z ^ stride, y, c)) for z, y, c in every])
            stride *= 2
        return val

    def device_step(x_blk, dy_blk, pos_all, norm_gain, wq_loc, wk_all, wv_all, wo_loc):
        seq_len = pos_all.shape[0]
        blk_rows = seq_len // tp_size
        half_rows = seq_len // Y_SIZE
        idx = lax.axis_index('tp')
        z_idx, y_idx, c_idx = idx // quad, (idx // CORE_SIZE) % Y_SIZE, idx % CORE_SIZE
        on_core0 = c_idx == 0
        on_y0 = y_idx == 0
        pair = wq_loc.shape[1]
        kv_own = Y_SIZE * z_idx + (y_idx ^ c_idx)
        kv_other = kv_own ^ 1

        def my_half(arr):
            parts = arr.reshape((z_size, Y_SIZE, 2 * blk_rows) + arr.shape[1:])
            return lax.dynamic_index_in_dim(parts, y_idx, 1, keepdims=False).reshape((half_rows,) + arr.shape[1:])

        def my_core_rows(arr):
            parts = arr.reshape(z_size, CORE_SIZE, blk_rows, arr.shape[1])
            return lax.dynamic_index_in_dim(parts, c_idx, 1, keepdims=False).reshape(z_size * blk_rows, arr.shape[1])

        def select(first, second):
            return jnp.where(on_core0, first, second)

        x_f32 = x_blk.astype(jnp.float32)
        hidden, x_hat, inv_rms = norm_forward(x_f32, norm_gain)
        h_half = lax.all_gather(hidden, 'tp', axis=0, tiled=True, axis_index_groups=half_groups)
        dy_gate, _ = lax.optimization_barrier((dy_blk, hidden))
        dy_half = lax.all_gather(dy_gate, 'tp', axis=0, tiled=True, axis_index_groups=half_groups)

        def four_slots(w_own):
            w_core = swap_core(w_own)
            w_y = swap_y(w_own)
            w_both = swap_core(w_y)
            return [select(w_own, w_y), select(w_core, w_both), select(w_both, w_core), select(w_y, w_own)]

        def kv_columns(head):
            return [lax.dynamic_slice_in_dim(w, head * HEAD_DIM, HEAD_DIM, axis=1) for w in (wk_all, wv_all)]

        q_slots = four_slots(wq_loc)
        w_in = jnp.concatenate(q_slots[:2] + kv_columns(kv_own) + q_slots[2:] + kv_columns(kv_other), axis=1)
        own_cols = 2 * pair + 2 * HEAD_DIM
        w_mix = jnp.concatenate(four_slots(wo_loc), axis=0)
        heads = 2 * pair // HEAD_DIM
        bq, bk = blk_rows, 2 * blk_rows
        lo_all = (lax.iota(jnp.int32, seq_len) - pos_all)[None, :]
        cos_t, sin_t = rope_tables(pos_all)
        y_one = y_idx.reshape(1)
        h_half, w_in, w_mix, cos_t, sin_t, lo_all = lax.optimization_barrier((h_half, w_in, w_mix, cos_t, sin_t, lo_all))

        qkv = dot_f32(h_half, w_in[:, :own_cols]).astype(jnp.bfloat16)
        kv_mine = qkv[:, 2 * pair:]
        kv_theirs = swap_same_head(kv_mine)
        lines = (z_size, 1, 2 * blk_rows, 2 * HEAD_DIM)
        kv_all = jnp.concatenate([jnp.where(on_y0, kv_mine, kv_theirs).reshape(lines), jnp.where(on_y0, kv_theirs, kv_mine).reshape(lines)], axis=1).reshape(seq_len, 2 * HEAD_DIM)
        o_own, lse = attend(y_one, pos_all, qkv, kv_all, cos_t, sin_t, lo_all, heads, bq, bk)
        o_all = jnp.concatenate([o_own, swap_core(o_own)], axis=1)
        mix_part = dot_f32(my_core_rows(o_all), w_mix).astype(jnp.bfloat16)
        mix_rows = lax.psum_scatter(mix_part, 'tp', scatter_dimension=0, tiled=True, axis_index_groups=line_groups)
        result = (x_f32 + mix_rows.astype(jnp.float32)).astype(jnp.bfloat16)

        o_send = select(o_all[:, 3 * pair:], o_all[:, :pair])
        o_keep = select(o_all[:, :pair], o_all[:, 3 * pair:])
        dy_half, mix_part = lax.optimization_barrier((dy_half, mix_part))
        d_o = dot_f32(dy_half, w_mix[:2 * pair], COLS_OF_BOTH).astype(jnp.bfloat16)
        dwo_send = dot_f32(o_send, dy_half, ROWS_OF_BOTH)
        dwo_theirs = swap_y(dwo_send)
        d_wo = (dot_f32(o_keep, dy_half, ROWS_OF_BOTH) + dwo_theirs).astype(jnp.bfloat16)
        d_o, dwo_send = lax.optimization_barrier((d_o, dwo_send))
        dq_raw, dkv_all = attend_backward(y_one, pos_all, qkv, d_o, o_own, kv_all, cos_t, sin_t, lo_all, lse, heads, bq, bk)

        dkv_parts = dkv_all.reshape(z_size, Y_SIZE, 2 * blk_rows, 2 * HEAD_DIM)
        dkv_send = lax.dynamic_index_in_dim(dkv_parts, 1 - y_idx, 1, keepdims=False).reshape(half_rows, 2 * HEAD_DIM)
        dkv_mine = my_half(dkv_all) + swap_same_head(dkv_send)
        cos_half, sin_half = my_half(cos_t.T), my_half(sin_t.T)
        dk_raw = unrotate_cols(dkv_mine[:, :HEAD_DIM].astype(jnp.bfloat16).astype(jnp.float32), cos_half, sin_half)
        d_own = jnp.concatenate([dq_raw, dk_raw, dkv_mine[:, HEAD_DIM:].astype(jnp.bfloat16)], axis=1)
        d_all = jnp.concatenate([d_own, swap_core(d_own)], axis=1)

        dh_part = dot_f32(my_core_rows(d_all), w_in, COLS_OF_BOTH).astype(jnp.bfloat16)
        dh_rows = lax.psum_scatter(dh_part, 'tp', scatter_dimension=0, tiled=True, axis_index_groups=line_groups)

        dh_part, d_late = lax.optimization_barrier((dh_part, d_all))
        q_first, q_last = d_late[:, :pair], d_late[:, own_cols + pair:own_cols + 2 * pair]
        dk_own, dv_own = d_late[:, 2 * pair:2 * pair + HEAD_DIM], d_late[:, 2 * pair + HEAD_DIM:own_cols]
        dk_other, dv_other = d_late[:, own_cols + 2 * pair:own_cols + 2 * pair + HEAD_DIM], d_late[:, own_cols + 2 * pair + HEAD_DIM:]
        send_cols = jnp.concatenate([select(q_last, q_first), select(dk_other, dv_own)], axis=1)
        keep_cols = jnp.concatenate([select(q_first, q_last), select(dk_own, dv_other)], axis=1)
        dw_keep, dw_theirs = lax.optimization_barrier((dot_f32(h_half, keep_cols, ROWS_OF_BOTH), swap_y(dot_f32(h_half, send_cols, ROWS_OF_BOTH))))
        dw_mine = dw_keep + dw_theirs
        d_wq = dw_mine[:, :pair].astype(jnp.bfloat16)
        kv_mine_sum = dw_mine[:, pair:]
        kv_other_sum = swap_core(kv_mine_sum)
        d_wk = select(kv_mine_sum, kv_other_sum)
        d_wv = select(kv_other_sum, kv_mine_sum)

        d_input, dg_part = norm_backward(dh_rows, x_hat, inv_rms, norm_gain)
        grad_x = (dy_blk.astype(jnp.float32) + d_input).astype(jnp.bfloat16)
        d_gain = sum_over_tp(dg_part)
        return result, grad_x, d_wq, d_wk, d_wv, d_wo, d_gain

    specs_in = (P(('dp', 'tp'), None), P(('dp', 'tp'), None), P('dp'), P(), P(None, 'tp'), P(), P(), P('tp', None))
    specs_out = (P(('dp', 'tp'), None), P(('dp', 'tp'), None), P('dp', 'tp'), P('dp', 'tp'), P('dp', 'tp'), P(('dp', 'tp'), None), P('dp'))
    return jax.shard_map(device_step, mesh=mesh, in_specs=specs_in, out_specs=specs_out, check_vma=False)
```

```python
import functools
import jax
import jax.numpy as jnp
from jax import lax
from jax.experimental import pallas as pl
from jax.experimental.pallas import tpu as pltpu
from jax.sharding import PartitionSpec as P

HEAD_DIM = 128
SCORE_SCALE = HEAD_DIM ** -0.5
SCALE_LOG2E = SCORE_SCALE * 1.4426950408889634
ROPE_THETA = 1000000.0
NORM_EPS = 1e-05
MASKED = -1e30
Y_SIZE = 2
CORE_SIZE = 2
NATURAL = (((1,), (0,)), ((), ()))
ROWS_OF_BOTH = (((0,), (0,)), ((), ()))
COLS_OF_BOTH = (((1,), (1,)), ((), ()))


def dot_f32(lhs, rhs, dims=NATURAL):
    return lax.dot_general(lhs, rhs, dims, preferred_element_type=jnp.float32)


def rope_tables(positions):
    exponents = jnp.arange(0, HEAD_DIM, 2, dtype=jnp.float32) / HEAD_DIM
    angles = jnp.power(ROPE_THETA, -exponents)[:, None] * positions.astype(jnp.float32)[None, :]
    return jnp.cos(angles), jnp.sin(angles)


def rotate_rows(t_f32, cos_t, sin_t):
    lead_half, tail_half = t_f32[:HEAD_DIM // 2], t_f32[HEAD_DIM // 2:]
    return jnp.concatenate([lead_half * cos_t - tail_half * sin_t, tail_half * cos_t + lead_half * sin_t], axis=0).astype(jnp.bfloat16)


def unrotate_cols(t_f32, cos_t, sin_t):
    lead_half, tail_half = t_f32[:, :HEAD_DIM // 2], t_f32[:, HEAD_DIM // 2:]
    return jnp.concatenate([lead_half * cos_t + tail_half * sin_t, tail_half * cos_t - lead_half * sin_t], axis=1).astype(jnp.bfloat16)


def norm_forward(x_f32, norm_gain):
    inv_rms = lax.rsqrt(jnp.mean(x_f32 * x_f32, axis=-1, keepdims=True) + NORM_EPS)
    x_hat = x_f32 * inv_rms
    return (x_hat * norm_gain).astype(jnp.bfloat16), x_hat, inv_rms


def norm_backward(d_hidden, x_hat, inv_rms, norm_gain):
    d_f32 = d_hidden.astype(jnp.float32)
    d_gain = jnp.sum(d_f32 * x_hat, axis=0)
    scaled = d_f32 * norm_gain
    d_input = inv_rms * (scaled - x_hat * jnp.mean(scaled * x_hat, axis=-1, keepdims=True))
    return d_input, d_gain


def block_token(y_ref, b, bq):
    return pl.multiple_of((b // 2) * (4 * bq) + y_ref[0] * (2 * bq) + (b % 2) * bq, bq)


def key_range(pos_ref, start, bq, bk):
    lo_first, lo_last = start - pos_ref[start], start + bq - 1 - pos_ref[start + bq - 1]
    return lo_first // bk, (start + bq - 1) // bk + 1, (lo_last + bk - 1) // bk, (start + 1) // bk


def tile_lanes(row, heads):
    return jnp.concatenate([row] * heads, axis=1)


def row_bounds(lo_ref, start, bq, heads):
    tok = start + lax.broadcasted_iota(jnp.int32, (1, bq), 1)
    return tile_lanes(tok, heads), tile_lanes(lo_ref[:, pl.ds(start, bq)], heads)


def keep_mask(key_start, bk, t_row, lo_row):
    key_idx = key_start + lax.broadcasted_iota(jnp.int32, (bk, t_row.shape[1]), 0)
    return (key_idx <= t_row) & (key_idx >= lo_row)


def head_columns(block, h):
    return block[:, h * HEAD_DIM:(h + 1) * HEAD_DIM]


def rotated_queries(q_ref, cos_ref, sin_ref, start, bq, heads):
    cos_t, sin_t = cos_ref[:, pl.ds(start, bq)], sin_ref[:, pl.ds(start, bq)]
    return [rotate_rows(head_columns(q_ref, h).T.astype(jnp.float32), cos_t, sin_t) for h in range(heads)]


def visit_keys(bounds, step):
    first, end, inner_first, inner_end = bounds

    def visit(j, carry):
        inner = (j >= inner_first) & (j < inner_end)

        @pl.when(inner)
        def _():
            step(j, False)

        @pl.when(jnp.logical_not(inner))
        def _():
            step(j, True)

        return carry

    lax.fori_loop(first, end, visit, 0)


def fwd_kernel(heads, bk, y_ref, pos_ref, q_ref, kv_ref, cos_ref, sin_ref, lo_ref, o_ref, lse_ref, k_s, vt_s, qt_s, m_s, l_s, acc_s):
    b = pl.program_id(0)
    bq = q_ref.shape[0]
    seq = kv_ref.shape[0]

    @pl.when(b == 0)
    def _():
        def prepare(s, carry):
            rows = pl.ds(pl.multiple_of(s * bk, bk), bk)
            k_s[rows, :] = rotate_rows(kv_ref[rows, :HEAD_DIM].T.astype(jnp.float32), cos_ref[:, rows], sin_ref[:, rows]).T
            vt_s[:, rows] = kv_ref[rows, HEAD_DIM:].T
            return carry

        lax.fori_loop(0, seq // bk, prepare, 0)

    start = block_token(y_ref, b, bq)
    t_row, lo_row = row_bounds(lo_ref, start, bq, heads)
    qt_s[...] = jnp.concatenate(rotated_queries(q_ref, cos_ref, sin_ref, start, bq, heads), axis=1)
    m_s[...] = jnp.full_like(m_s, MASKED)
    l_s[...] = jnp.zeros_like(l_s)
    acc_s[...] = jnp.zeros_like(acc_s)

    def step(j, masked):
        key_start = pl.multiple_of(j * bk, bk)
        keys = pl.ds(key_start, bk)
        scores = dot_f32(k_s[keys, :], qt_s[...])
        if masked:
            scores = jnp.where(keep_mask(key_start, bk, t_row, lo_row), scores, MASKED)
        m_old = m_s[...]
        m_new = jnp.maximum(m_old, jnp.max(scores, axis=0, keepdims=True))
        probs = jnp.exp2(scores * SCALE_LOG2E - m_new * SCALE_LOG2E)
        alpha = jnp.exp2((m_old - m_new) * SCALE_LOG2E)
        m_s[...] = m_new
        l_s[...] = l_s[...] * alpha + jnp.sum(probs, axis=0, keepdims=True)
        acc_s[...] = acc_s[...] * alpha + dot_f32(vt_s[:, keys], probs.astype(jnp.bfloat16))

    visit_keys(key_range(pos_ref, start, bq, bk), step)
    out_t = (acc_s[...] / l_s[...]).astype(jnp.bfloat16)
    for h in range(heads):
        o_ref[:, h * HEAD_DIM:(h + 1) * HEAD_DIM] = out_t[:, h * bq:(h + 1) * bq].T
    lse_ref[0] = m_s[...] * SCALE_LOG2E + jnp.log2(l_s[...])


def bwd_kernel(heads, bk, y_ref, pos_ref, q_ref, do_ref, o_ref, kv_ref, cos_ref, sin_ref, lo_ref, lse_ref, dq_ref, dkv_ref, k_s, kt_s, q_s, qt_s, do_s, dot_s, dqt_s):
    b = pl.program_id(0)
    bq = q_ref.shape[0]
    seq = kv_ref.shape[0]

    @pl.when(b == 0)
    def _():
        def prepare(s, carry):
            rows = pl.ds(pl.multiple_of(s * bk, bk), bk)
            dkv_ref[s % 2, pl.ds(pl.multiple_of((s // 2) * bk, bk), bk), :] = jnp.zeros((bk, 2 * HEAD_DIM), jnp.float32)
            k_rot_t = rotate_rows(kv_ref[rows, :HEAD_DIM].T.astype(jnp.float32), cos_ref[:, rows], sin_ref[:, rows])
            kt_s[:, rows] = k_rot_t
            k_s[rows, :] = k_rot_t.T
            return carry

        lax.fori_loop(0, seq // bk, prepare, 0)

    start = block_token(y_ref, b, bq)
    t_row, lo_row = row_bounds(lo_ref, start, bq, heads)
    deltas = []
    for h, q_rot_t in enumerate(rotated_queries(q_ref, cos_ref, sin_ref, start, bq, heads)):
        lanes = slice(h * bq, (h + 1) * bq)
        qt_s[:, lanes] = q_rot_t
        q_s[lanes, :] = q_rot_t.T
        do_head = head_columns(do_ref, h)
        do_s[lanes, :] = do_head
        do_t = do_head.T
        dot_s[:, lanes] = do_t
        deltas.append(jnp.sum(do_t.astype(jnp.float32) * head_columns(o_ref, h).T.astype(jnp.float32), axis=0, keepdims=True))
    delta = jnp.concatenate(deltas, axis=1)
    lse = lse_ref[0]
    dqt_s[...] = jnp.zeros_like(dqt_s)

    def step(j, masked):
        key_start = pl.multiple_of(j * bk, bk)
        keys = pl.ds(key_start, bk)
        scores = dot_f32(k_s[keys, :], qt_s[...])
        probs = jnp.exp2(scores * SCALE_LOG2E - lse)
        if masked:
            probs = jnp.where(keep_mask(key_start, bk, t_row, lo_row), probs, 0.0)
        d_probs = dot_f32(kv_ref[keys, HEAD_DIM:], dot_s[...])
        d_scores = (probs * (d_probs - delta)).astype(jnp.bfloat16)
        side, rows = (j % 2) ^ y_ref[0], pl.ds(pl.multiple_of((j // 2) * bk, bk), bk)
        dkv_ref[side, rows, HEAD_DIM:] += dot_f32(probs.astype(jnp.bfloat16), do_s[...])
        dkv_ref[side, rows, :HEAD_DIM] += dot_f32(d_scores, q_s[...]) * SCORE_SCALE
        dqt_s[...] += dot_f32(kt_s[:, keys], d_scores)

    visit_keys(key_range(pos_ref, start, bq, bk), step)
    cos_t, sin_t = cos_ref[:, pl.ds(start, bq)], sin_ref[:, pl.ds(start, bq)]
    for h in range(heads):
        dq_rot_t = (dqt_s[:, h * bq:(h + 1) * bq] * SCORE_SCALE).astype(jnp.bfloat16).astype(jnp.float32)
        dq_ref[:, h * HEAD_DIM:(h + 1) * HEAD_DIM] = rotate_rows(dq_rot_t, cos_t, -sin_t).T


def attention_specs(bq, heads, seq):
    row = pl.BlockSpec((bq, heads * HEAD_DIM), lambda b, *_: (b, 0))
    keys = pl.BlockSpec((seq, 2 * HEAD_DIM), lambda b, *_: (0, 0))
    table = pl.BlockSpec((HEAD_DIM // 2, seq), lambda b, *_: (0, 0))
    bound = pl.BlockSpec((1, seq), lambda b, *_: (0, 0))
    vec = pl.BlockSpec((1, 1, heads * bq), lambda b, *_: (b, 0, 0))
    return row, keys, table, bound, vec


def attend(y_one, positions, qkv, kv_all, cos_t, sin_t, lo_all, heads, bq, bk):
    rows, seq = qkv.shape[0], kv_all.shape[0]
    row, keys, table, bound, vec = attention_specs(bq, heads, seq)
    lanes, width = heads * bq, heads * HEAD_DIM
    return pl.pallas_call(
        functools.partial(fwd_kernel, heads, bk),
        out_shape=(jax.ShapeDtypeStruct((rows, width), jnp.bfloat16), jax.ShapeDtypeStruct((rows // bq, 1, lanes), jnp.float32)),
        grid_spec=pltpu.PrefetchScalarGridSpec(
            num_scalar_prefetch=2, grid=(rows // bq,),
            in_specs=[row, keys, table, table, bound], out_specs=(row, vec),
            scratch_shapes=[pltpu.VMEM((seq, HEAD_DIM), jnp.bfloat16), pltpu.VMEM((HEAD_DIM, seq), jnp.bfloat16), pltpu.VMEM((HEAD_DIM, lanes), jnp.bfloat16),
                            pltpu.VMEM((1, lanes), jnp.float32), pltpu.VMEM((1, lanes), jnp.float32), pltpu.VMEM((HEAD_DIM, lanes), jnp.float32)]),
        compiler_params=pltpu.CompilerParams(dimension_semantics=('arbitrary',), vmem_limit_bytes=48 << 20),
        cost_estimate=pl.CostEstimate(flops=4 * rows * heads * seq * HEAD_DIM, bytes_accessed=4 * rows * width + 4 * seq * HEAD_DIM, transcendentals=rows * heads * seq // 2),
        name='attend_fwd',
    )(y_one, positions, qkv, kv_all, cos_t, sin_t, lo_all)


def attend_backward(y_one, positions, qkv, d_o, o_own, kv_all, cos_t, sin_t, lo_all, lse, heads, bq, bk):
    rows, seq = qkv.shape[0], kv_all.shape[0]
    row, keys, table, bound, vec = attention_specs(bq, heads, seq)
    lanes, width = heads * bq, heads * HEAD_DIM
    return pl.pallas_call(
        functools.partial(bwd_kernel, heads, bk),
        out_shape=(jax.ShapeDtypeStruct((rows, width), jnp.bfloat16), jax.ShapeDtypeStruct((2, rows, 2 * HEAD_DIM), jnp.float32)),
        grid_spec=pltpu.PrefetchScalarGridSpec(
            num_scalar_prefetch=2, grid=(rows // bq,),
            in_specs=[row, row, row, keys, table, table, bound, vec], out_specs=(row, pl.BlockSpec((2, rows, 2 * HEAD_DIM), lambda b, *_: (0, 0, 0))),
            scratch_shapes=[pltpu.VMEM((seq, HEAD_DIM), jnp.bfloat16), pltpu.VMEM((HEAD_DIM, seq), jnp.bfloat16),
                            pltpu.VMEM((lanes, HEAD_DIM), jnp.bfloat16), pltpu.VMEM((HEAD_DIM, lanes), jnp.bfloat16),
                            pltpu.VMEM((lanes, HEAD_DIM), jnp.bfloat16), pltpu.VMEM((HEAD_DIM, lanes), jnp.bfloat16), pltpu.VMEM((HEAD_DIM, lanes), jnp.float32)]),
        compiler_params=pltpu.CompilerParams(dimension_semantics=('arbitrary',), vmem_limit_bytes=56 << 20),
        cost_estimate=pl.CostEstimate(flops=10 * rows * heads * seq * HEAD_DIM, bytes_accessed=8 * rows * width + 12 * seq * HEAD_DIM, transcendentals=rows * heads * seq // 2),
        name='attend_bwd',
    )(y_one, positions, qkv, d_o, o_own, kv_all, cos_t, sin_t, lo_all, lse)


def solution(mesh):
    tp_size = mesh.shape['tp']
    quad = Y_SIZE * CORE_SIZE
    z_size = tp_size // quad

    def member(z, y, c):
        return (z * Y_SIZE + y) * CORE_SIZE + c

    every = [(z, y, c) for z in range(z_size) for y in range(Y_SIZE) for c in range(CORE_SIZE)]
    half_groups = [[member(z, y, c) for z in range(z_size) for c in range(CORE_SIZE)] for y in range(Y_SIZE)]
    line_groups = [[member(z, y, c) for z in range(z_size)] for y in range(Y_SIZE) for c in range(CORE_SIZE)]
    core_perm = [(member(z, y, c), member(z, y, 1 - c)) for z, y, c in every]
    y_perm = [(member(z, y, c), member(z, 1 - y, c)) for z, y, c in every]
    same_head_perm = [(member(z, y, c), member(z, 1 - y, 1 - c)) for z, y, c in every]

    def swap_core(val):
        return lax.ppermute(val, 'tp', core_perm)

    def swap_y(val):
        return lax.ppermute(val, 'tp', y_perm)

    def swap_same_head(val):
        return lax.ppermute(val, 'tp', same_head_perm)

    def sum_over_tp(val):
        val = val + swap_core(val)
        val = val + swap_y(val)
        stride = 1
        while stride < z_size:
            val = val + lax.ppermute(val, 'tp', [(member(z, y, c), member(z ^ stride, y, c)) for z, y, c in every])
            stride *= 2
        return val

    def device_step(x_blk, dy_blk, pos_all, norm_gain, wq_loc, wk_all, wv_all, wo_loc):
        seq_len = pos_all.shape[0]
        blk_rows = seq_len // tp_size
        half_rows = seq_len // Y_SIZE
        idx = lax.axis_index('tp')
        z_idx, y_idx, c_idx = idx // quad, (idx // CORE_SIZE) % Y_SIZE, idx % CORE_SIZE
        on_core0 = c_idx == 0
        on_y0 = y_idx == 0
        pair = wq_loc.shape[1]
        kv_own = Y_SIZE * z_idx + (y_idx ^ c_idx)
        kv_other = kv_own ^ 1

        def my_half(arr):
            parts = arr.reshape((z_size, Y_SIZE, 2 * blk_rows) + arr.shape[1:])
            return lax.dynamic_index_in_dim(parts, y_idx, 1, keepdims=False).reshape((half_rows,) + arr.shape[1:])

        def my_core_rows(arr):
            parts = arr.reshape(z_size, CORE_SIZE, blk_rows, arr.shape[1])
            return lax.dynamic_index_in_dim(parts, c_idx, 1, keepdims=False).reshape(z_size * blk_rows, arr.shape[1])

        def select(first, second):
            return jnp.where(on_core0, first, second)

        x_f32 = x_blk.astype(jnp.float32)
        hidden, x_hat, inv_rms = norm_forward(x_f32, norm_gain)
        h_half = lax.all_gather(hidden, 'tp', axis=0, tiled=True, axis_index_groups=half_groups)
        dy_gate, _ = lax.optimization_barrier((dy_blk, hidden))
        dy_half = lax.all_gather(dy_gate, 'tp', axis=0, tiled=True, axis_index_groups=half_groups)

        def four_slots(w_own):
            w_core = swap_core(w_own)
            w_y = swap_y(w_own)
            w_both = swap_core(w_y)
            return [select(w_own, w_y), select(w_core, w_both), select(w_both, w_core), select(w_y, w_own)]

        def kv_columns(head):
            return [lax.dynamic_slice_in_dim(w, head * HEAD_DIM, HEAD_DIM, axis=1) for w in (wk_all, wv_all)]

        q_slots = four_slots(wq_loc)
        w_in = jnp.concatenate(q_slots[:2] + kv_columns(kv_own) + q_slots[2:] + kv_columns(kv_other), axis=1)
        own_cols = 2 * pair + 2 * HEAD_DIM
        w_mix = jnp.concatenate(four_slots(wo_loc), axis=0)
        heads = 2 * pair // HEAD_DIM
        bq, bk = blk_rows, 2 * blk_rows
        lo_all = (lax.iota(jnp.int32, seq_len) - pos_all)[None, :]
        cos_t, sin_t = rope_tables(pos_all)
        y_one = y_idx.reshape(1)
        h_half, w_in, w_mix, cos_t, sin_t, lo_all = lax.optimization_barrier((h_half, w_in, w_mix, cos_t, sin_t, lo_all))

        qkv = dot_f32(h_half, w_in[:, :own_cols]).astype(jnp.bfloat16)
        kv_mine = qkv[:, 2 * pair:]
        kv_theirs = swap_same_head(kv_mine)
        lines = (z_size, 1, 2 * blk_rows, 2 * HEAD_DIM)
        kv_all = jnp.concatenate([jnp.where(on_y0, kv_mine, kv_theirs).reshape(lines), jnp.where(on_y0, kv_theirs, kv_mine).reshape(lines)], axis=1).reshape(seq_len, 2 * HEAD_DIM)
        o_own, lse = attend(y_one, pos_all, qkv, kv_all, cos_t, sin_t, lo_all, heads, bq, bk)
        o_all = jnp.concatenate([o_own, swap_core(o_own)], axis=1)
        mix_part = dot_f32(my_core_rows(o_all), w_mix).astype(jnp.bfloat16)
        mix_rows = lax.psum_scatter(mix_part, 'tp', scatter_dimension=0, tiled=True, axis_index_groups=line_groups)
        result = (x_f32 + mix_rows.astype(jnp.float32)).astype(jnp.bfloat16)

        def pair_sides(own, partner):
            first, last = own[:, :pair], partner[:, pair:2 * pair]
            return select(first, last), select(last, first)

        o_keep, o_send = pair_sides(o_own, o_all[:, 2 * pair:])
        dy_half, mix_part = lax.optimization_barrier((dy_half, mix_part))
        d_o = dot_f32(dy_half, w_mix[:2 * pair], COLS_OF_BOTH).astype(jnp.bfloat16)
        half_cols = dy_half.shape[1] // 2
        dwo_send_a = dot_f32(o_send, dy_half[:, :half_cols], ROWS_OF_BOTH)
        dwo_send_b = dot_f32(o_send, dy_half[:, half_cols:], ROWS_OF_BOTH)
        dwo_theirs_a = swap_y(dwo_send_a)
        d_o, dwo_send_a, dwo_send_b = lax.optimization_barrier((d_o, dwo_send_a, dwo_send_b))
        dq_own, dkv_sides = attend_backward(y_one, pos_all, qkv, d_o, o_own, kv_all, cos_t, sin_t, lo_all, lse, heads, bq, bk)
        dkv_theirs = swap_same_head(dkv_sides[1])
        dq_partner = swap_core(dq_own)

        dwo_send_b, dkv_theirs = lax.optimization_barrier((dwo_send_b, dkv_theirs))
        dwo_theirs_b = swap_y(dwo_send_b)
        dkv_mine = dkv_sides[0] + dkv_theirs
        cos_half, sin_half = my_half(cos_t.T), my_half(sin_t.T)
        dk_raw = unrotate_cols(dkv_mine[:, :HEAD_DIM].astype(jnp.bfloat16).astype(jnp.float32), cos_half, sin_half)
        dkv_own = jnp.concatenate([dk_raw, dkv_mine[:, HEAD_DIM:].astype(jnp.bfloat16)], axis=1)
        dkv_partner = swap_core(dkv_own)

        d_rows = jnp.concatenate([my_core_rows(part) for part in (dq_own, dkv_own, dq_partner, dkv_partner)], axis=1)
        dh_part = dot_f32(d_rows, w_in, COLS_OF_BOTH).astype(jnp.bfloat16)
        dh_rows = lax.psum_scatter(dh_part, 'tp', scatter_dimension=0, tiled=True, axis_index_groups=line_groups)

        dh_part, dq_own, dkv_own = lax.optimization_barrier((dh_part, dq_own, dkv_own))
        q_keep, q_send = pair_sides(dq_own, dq_partner)
        kv_keep = select(dkv_own[:, :HEAD_DIM], dkv_partner[:, HEAD_DIM:])
        kv_send = select(dkv_partner[:, :HEAD_DIM], dkv_own[:, HEAD_DIM:])
        dwkv_theirs = swap_y(dot_f32(h_half, kv_send, ROWS_OF_BOTH))
        dwq_theirs = swap_y(dot_f32(h_half, q_send, ROWS_OF_BOTH))
        dwo_keep = dot_f32(o_keep, dy_half, ROWS_OF_BOTH)
        dwkv_keep = dot_f32(h_half, kv_keep, ROWS_OF_BOTH)
        dwq_keep = dot_f32(h_half, q_keep, ROWS_OF_BOTH)
        dwo_keep, dwo_theirs_a, dwo_theirs_b = lax.optimization_barrier((dwo_keep, dwo_theirs_a, dwo_theirs_b))
        d_wo = jnp.concatenate([dwo_keep[:, :half_cols] + dwo_theirs_a, dwo_keep[:, half_cols:] + dwo_theirs_b], axis=1).astype(jnp.bfloat16)
        dwkv_keep, dwkv_theirs = lax.optimization_barrier((dwkv_keep, dwkv_theirs))
        kv_mine_sum = dwkv_keep + dwkv_theirs
        kv_other_sum = swap_core(kv_mine_sum)
        d_wk = select(kv_mine_sum, kv_other_sum)
        d_wv = select(kv_other_sum, kv_mine_sum)
        dwq_keep, dwq_theirs, d_wk = lax.optimization_barrier((dwq_keep, dwq_theirs, d_wk))
        d_wq = (dwq_keep + dwq_theirs).astype(jnp.bfloat16)

        d_input, dg_part = norm_backward(dh_rows, x_hat, inv_rms, norm_gain)
        grad_x = (dy_blk.astype(jnp.float32) + d_input).astype(jnp.bfloat16)
        d_gain = sum_over_tp(dg_part)
        return result, grad_x, d_wq, d_wk, d_wv, d_wo, d_gain

    specs_in = (P(('dp', 'tp'), None), P(('dp', 'tp'), None), P('dp'), P(), P(None, 'tp'), P(), P(), P('tp', None))
    specs_out = (P(('dp', 'tp'), None), P(('dp', 'tp'), None), P('dp', 'tp'), P('dp', 'tp'), P('dp', 'tp'), P(('dp', 'tp'), None), P('dp'))
    return jax.shard_map(device_step, mesh=mesh, in_specs=specs_in, out_specs=specs_out, check_vma=False)
```

```python
import functools
import jax
import jax.numpy as jnp
from jax import lax
from jax.experimental import pallas as pl
from jax.experimental.pallas import tpu as pltpu
from jax.sharding import PartitionSpec as P

HEAD_DIM = 128
SCORE_SCALE = HEAD_DIM ** -0.5
SCALE_LOG2E = SCORE_SCALE * 1.4426950408889634
ROPE_THETA = 1000000.0
NORM_EPS = 1e-05
MASKED = -1e30
Z_SIZE = 4
Y_SIZE = 2
CORE_SIZE = 2
SLOTS = Z_SIZE * CORE_SIZE
DO_ORDER = (0, 2, 1, 3)
NATURAL = (((1,), (0,)), ((), ()))
COLS_OF_BOTH = (((1,), (1,)), ((), ()))


def dot_f32(lhs, rhs, dims=NATURAL):
    return lax.dot_general(lhs, rhs, dims, preferred_element_type=jnp.float32)


def rope_tables(positions):
    exponents = jnp.arange(0, HEAD_DIM, 2, dtype=jnp.float32) / HEAD_DIM
    angles = jnp.power(ROPE_THETA, -exponents)[:, None] * positions.astype(jnp.float32)[None, :]
    return jnp.cos(angles), jnp.sin(angles)


def rotate_rows(t_f32, cos_t, sin_t):
    lead_half, tail_half = t_f32[:HEAD_DIM // 2], t_f32[HEAD_DIM // 2:]
    return jnp.concatenate([lead_half * cos_t - tail_half * sin_t, tail_half * cos_t + lead_half * sin_t], axis=0).astype(jnp.bfloat16)


def norm_forward(x_f32, norm_gain):
    inv_rms = lax.rsqrt(jnp.mean(x_f32 * x_f32, axis=-1, keepdims=True) + NORM_EPS)
    x_hat = x_f32 * inv_rms
    return (x_hat * norm_gain).astype(jnp.bfloat16), x_hat, inv_rms


def norm_backward(d_hidden, x_hat, inv_rms, norm_gain):
    d_f32 = d_hidden.astype(jnp.float32)
    d_gain = jnp.sum(d_f32 * x_hat, axis=0)
    scaled = d_f32 * norm_gain
    d_input = inv_rms * (scaled - x_hat * jnp.mean(scaled * x_hat, axis=-1, keepdims=True))
    return d_input, d_gain


def slot_of(where_ref, z, c):
    return 2 * lax.rem(where_ref[0] - z + Z_SIZE, Z_SIZE) + (where_ref[2] ^ c)


def slot_of_other(where_ref, z, c):
    return 2 * lax.rem(where_ref[0] - z + Z_SIZE, Z_SIZE) + (1 - (where_ref[2] ^ c))


def do_slot_of(where_ref, z, c):
    s = lax.rem(where_ref[0] - z + Z_SIZE, Z_SIZE)
    return 2 * (s // 2 + 2 * (s % 2)) + (where_ref[2] ^ c)


def block_token(where_ref, b, bq):
    return pl.multiple_of((b // 2) * (4 * bq) + where_ref[1] * (2 * bq) + (b % 2) * bq, bq)


def key_range(pos_ref, start, bq, bk):
    lo_first, lo_last = start - pos_ref[start], start + bq - 1 - pos_ref[start + bq - 1]
    return lo_first // bk, (start + bq - 1) // bk + 1, (lo_last + bk - 1) // bk, (start + 1) // bk


def tile_lanes(row, heads):
    return jnp.concatenate([row] * heads, axis=1)


def row_bounds(lo_ref, start, bq, heads):
    tok = start + lax.broadcasted_iota(jnp.int32, (1, bq), 1)
    return tile_lanes(tok, heads), tile_lanes(lo_ref[:, pl.ds(start, bq)], heads)


def keep_mask(key_start, bk, t_row, lo_row):
    key_idx = key_start + lax.broadcasted_iota(jnp.int32, (bk, t_row.shape[1]), 0)
    return (key_idx <= t_row) & (key_idx >= lo_row)


def head_columns(block, h):
    return block[:, h * HEAD_DIM:(h + 1) * HEAD_DIM]


def rotated_queries(q_blk, cos_ref, sin_ref, start, bq, heads):
    cos_t, sin_t = cos_ref[:, pl.ds(start, bq)], sin_ref[:, pl.ds(start, bq)]
    return [rotate_rows(head_columns(q_blk, h).T.astype(jnp.float32), cos_t, sin_t) for h in range(heads)]


def visit_keys(bounds, step):
    first, end, inner_first, inner_end = bounds

    def visit(j, carry):
        inner = (j >= inner_first) & (j < inner_end)

        @pl.when(inner)
        def _():
            step(j, False)

        @pl.when(jnp.logical_not(inner))
        def _():
            step(j, True)

        return carry

    lax.fori_loop(first, end, visit, 0)


def for_key_blocks(where_ref, mine_ref, theirs_ref, count, bq, store):
    def visit(n, carry):
        z, y, c = n // 4, (n // 2) % 2, n % 2
        block = jnp.where(y == where_ref[1], mine_ref[slot_of(where_ref, z, c)], theirs_ref[slot_of_other(where_ref, z, c)])
        store(pl.ds(pl.multiple_of(n * bq, bq), bq), block)
        return carry

    lax.fori_loop(0, count, visit, 0)


def fwd_kernel(heads, bk, where_ref, pos_ref, q_ref, kv_ref, kv_other_ref, cos_ref, sin_ref, lo_ref, o_ref, lse_ref, k_s, vt_s, qt_s, m_s, l_s, acc_s):
    b = pl.program_id(0)
    bq = q_ref.shape[1]
    seq = k_s.shape[0]

    @pl.when(b == 0)
    def _():
        def store(rows, block):
            k_s[rows, :] = rotate_rows(block[:, :HEAD_DIM].T.astype(jnp.float32), cos_ref[:, rows], sin_ref[:, rows]).T
            vt_s[:, rows] = block[:, HEAD_DIM:].T

        for_key_blocks(where_ref, kv_ref, kv_other_ref, seq // bq, bq, store)

    start = block_token(where_ref, b, bq)
    t_row, lo_row = row_bounds(lo_ref, start, bq, heads)
    q_blk = q_ref[slot_of(where_ref, b // 2, b % 2)]
    qt_s[...] = jnp.concatenate(rotated_queries(q_blk, cos_ref, sin_ref, start, bq, heads), axis=1)
    m_s[...] = jnp.full_like(m_s, MASKED)
    l_s[...] = jnp.zeros_like(l_s)
    acc_s[...] = jnp.zeros_like(acc_s)

    def step(j, masked):
        key_start = pl.multiple_of(j * bk, bk)
        keys = pl.ds(key_start, bk)
        scores = dot_f32(k_s[keys, :], qt_s[...])
        if masked:
            scores = jnp.where(keep_mask(key_start, bk, t_row, lo_row), scores, MASKED)
        m_old = m_s[...]
        m_new = jnp.maximum(m_old, jnp.max(scores, axis=0, keepdims=True))
        probs = jnp.exp2(scores * SCALE_LOG2E - m_new * SCALE_LOG2E)
        alpha = jnp.exp2((m_old - m_new) * SCALE_LOG2E)
        m_s[...] = m_new
        l_s[...] = l_s[...] * alpha + jnp.sum(probs, axis=0, keepdims=True)
        acc_s[...] = acc_s[...] * alpha + dot_f32(vt_s[:, keys], probs.astype(jnp.bfloat16))

    visit_keys(key_range(pos_ref, start, bq, bk), step)
    out_t = (acc_s[...] / l_s[...]).astype(jnp.bfloat16)
    for h in range(heads):
        o_ref[0, :, h * HEAD_DIM:(h + 1) * HEAD_DIM] = out_t[:, h * bq:(h + 1) * bq].T
    lse_ref[0] = m_s[...] * SCALE_LOG2E + jnp.log2(l_s[...])


def bwd_kernel(heads, bk, z_first, top, where_ref, pos_ref, q_ref, do_ref, o_ref, kv_ref, kv_other_ref, cos_ref, sin_ref, lo_ref, lse_ref, *rest):
    if top:
        dq_ref, mine_ref, send_ref, part_ref, k_s, kt_s, v_s, q_s, qt_s, do_s, dot_s, dqt_s, acc_s = rest
    else:
        part_ref, _, dq_ref, mine_ref, send_ref, k_s, kt_s, v_s, q_s, qt_s, do_s, dot_s, dqt_s, acc_s = rest
    step_idx = pl.program_id(0)
    b = step_idx + 2 * z_first
    bq = q_ref.shape[1]
    seq = k_s.shape[0]

    @pl.when(step_idx == 0)
    def _():
        def store(rows, block):
            acc_s[rows, :] = jnp.zeros((bq, 2 * HEAD_DIM), jnp.float32) if top else part_ref[rows, :]
            k_rot_t = rotate_rows(block[:, :HEAD_DIM].T.astype(jnp.float32), cos_ref[:, rows], sin_ref[:, rows])
            kt_s[:, rows] = k_rot_t
            k_s[rows, :] = k_rot_t.T
            v_s[rows, :] = block[:, HEAD_DIM:]

        for_key_blocks(where_ref, kv_ref, kv_other_ref, seq // bq, bq, store)

    start = block_token(where_ref, b, bq)
    slot, do_slot = slot_of(where_ref, b // 2, b % 2), do_slot_of(where_ref, b // 2, b % 2)
    t_row, lo_row = row_bounds(lo_ref, start, bq, heads)
    q_blk, do_blk, o_blk = q_ref[slot], do_ref[do_slot], o_ref[slot]
    deltas = []
    for h, q_rot_t in enumerate(rotated_queries(q_blk, cos_ref, sin_ref, start, bq, heads)):
        lanes = slice(h * bq, (h + 1) * bq)
        qt_s[:, lanes] = q_rot_t
        q_s[lanes, :] = q_rot_t.T
        do_head = head_columns(do_blk, h)
        do_s[lanes, :] = do_head
        do_t = do_head.T
        dot_s[:, lanes] = do_t
        deltas.append(jnp.sum(do_t.astype(jnp.float32) * head_columns(o_blk, h).T.astype(jnp.float32), axis=0, keepdims=True))
    delta = jnp.concatenate(deltas, axis=1)
    lse = lse_ref[0]
    dqt_s[...] = jnp.zeros_like(dqt_s)

    def step(j, masked):
        key_start = pl.multiple_of(j * bk, bk)
        keys = pl.ds(key_start, bk)
        scores = dot_f32(k_s[keys, :], qt_s[...])
        probs = jnp.exp2(scores * SCALE_LOG2E - lse)
        if masked:
            probs = jnp.where(keep_mask(key_start, bk, t_row, lo_row), probs, 0.0)
        d_probs = dot_f32(v_s[keys, :], dot_s[...])
        d_scores = (probs * (d_probs - delta)).astype(jnp.bfloat16)
        acc_s[keys, HEAD_DIM:] += dot_f32(probs.astype(jnp.bfloat16), do_s[...])
        acc_s[keys, :HEAD_DIM] += dot_f32(d_scores, q_s[...]) * SCORE_SCALE
        dqt_s[...] += dot_f32(kt_s[:, keys], d_scores)

    visit_keys(key_range(pos_ref, start, bq, bk), step)
    cos_t, sin_t = cos_ref[:, pl.ds(start, bq)], sin_ref[:, pl.ds(start, bq)]
    for h in range(heads):
        dq_rot_t = (dqt_s[:, h * bq:(h + 1) * bq] * SCORE_SCALE).astype(jnp.bfloat16).astype(jnp.float32)
        dq_ref[0, :, h * HEAD_DIM:(h + 1) * HEAD_DIM] = rotate_rows(dq_rot_t, cos_t, -sin_t).T

    @pl.when(step_idx == pl.num_programs(0) - 1)
    def _():
        def hand_over(y, mine):
            for z in range(Z_SIZE // 2):
                for c in range(CORE_SIZE):
                    rows = (((z_first + z) * 2 + y) * 2 + c) * bq
                    e = where_ref[2] ^ c
                    if mine:
                        mine_ref[z, e] = acc_s[rows:rows + bq, :]
                    else:
                        send_ref[z, 1 - e] = acc_s[rows:rows + bq, :]

        for y in range(Y_SIZE):
            pl.when(where_ref[1] == y)(functools.partial(hand_over, y, True))
            pl.when(where_ref[1] != y)(functools.partial(hand_over, y, False))
        if top:
            part_ref[...] = acc_s[:part_ref.shape[0], :]


def token_grads_kernel(count, *refs):
    blocks, lhs_ref, out_refs, lhs_t = refs[:count], refs[count], refs[count + 1:-1], refs[-1]
    rows = lhs_ref.shape[1]

    @pl.when(pl.program_id(0) == 0)
    def _():
        for n in range(count):
            lhs_t[:, n * rows:(n + 1) * rows] = lhs_ref[n].T

    total = sum(dot_f32(lhs_t[:, n * rows:(n + 1) * rows], blocks[n][...]) for n in range(count))
    start = 0
    for ref in out_refs:
        if ref.shape[0] == blocks[0].shape[1]:
            size = ref.shape[1]
            ref[...] = total[start:start + size, :].T.astype(ref.dtype)
        else:
            size = ref.shape[0]
            ref[...] = total[start:start + size, :].astype(ref.dtype)
        start += size


def token_grads(blocks, lhs, outs, tile=512):
    rows, model = blocks[0].shape
    width = lhs.shape[2]
    specs = [pl.BlockSpec((tile, shape[1]), lambda i: (i, 0)) if shape[0] == model else pl.BlockSpec((shape[0], tile), lambda i: (0, i)) for shape, _ in outs]
    return pl.pallas_call(
        functools.partial(token_grads_kernel, len(blocks)),
        out_shape=[jax.ShapeDtypeStruct(*out) for out in outs], grid=(model // tile,),
        in_specs=[pl.BlockSpec((rows, tile), lambda i: (0, i)) for _ in blocks] + [pl.BlockSpec(lhs.shape, lambda i: (0, 0, 0))], out_specs=specs,
        scratch_shapes=[pltpu.VMEM((width, len(blocks) * rows), jnp.bfloat16)],
        compiler_params=pltpu.CompilerParams(dimension_semantics=('arbitrary',), vmem_limit_bytes=48 << 20),
        cost_estimate=pl.CostEstimate(flops=2 * len(blocks) * rows * model * width, bytes_accessed=2 * len(blocks) * rows * model, transcendentals=0),
    )(*blocks, lhs)


def finish_kernel(where_ref, mine_low, other_low, mine_top, other_top, cos_ref, sin_ref, out_ref):
    cores, _ = mine_low.shape[1:3]
    for z in range(Z_SIZE):
        mine, other = (mine_low, other_low) if z < Z_SIZE // 2 else (mine_top, other_top)
        slot = lax.rem(where_ref[0] - z + Z_SIZE, Z_SIZE)
        for e in range(cores):
            total = mine[z % (Z_SIZE // 2), e] + other[z % (Z_SIZE // 2), e]
            dk = total[:, :HEAD_DIM].astype(jnp.bfloat16).astype(jnp.float32)
            out_ref[slot, e, :, :HEAD_DIM] = (dk * cos_ref[z, e] + pltpu.roll(dk, HEAD_DIM // 2, 1) * sin_ref[z, e]).astype(jnp.bfloat16)
            out_ref[slot, e, :, HEAD_DIM:] = total[:, HEAD_DIM:].astype(jnp.bfloat16)


def finish_key_grads(where, *operands):
    cores, bq, width = operands[0].shape[1:]
    return pl.pallas_call(
        finish_kernel, out_shape=jax.ShapeDtypeStruct((Z_SIZE, cores, bq, width), jnp.bfloat16),
        grid_spec=pltpu.PrefetchScalarGridSpec(num_scalar_prefetch=1, grid=(1,), in_specs=[full_spec(arr.shape) for arr in operands], out_specs=full_spec((Z_SIZE, cores, bq, width))),
        compiler_params=pltpu.CompilerParams(dimension_semantics=('arbitrary',), vmem_limit_bytes=32 << 20),
        cost_estimate=pl.CostEstimate(flops=1000000, bytes_accessed=8000000, transcendentals=0),
    )(where, *operands)


def full_spec(shape):
    return pl.BlockSpec(shape, lambda b, *_: (0,) * len(shape))


def attend(where, positions, q_slots, kv_slots, kv_other, cos_t, sin_t, lo_all, bk):
    slots, bq, width = q_slots.shape
    seq = positions.shape[0]
    heads = width // HEAD_DIM
    lanes = heads * bq
    operands = (q_slots, kv_slots, kv_other, cos_t, sin_t, lo_all)
    return pl.pallas_call(
        functools.partial(fwd_kernel, heads, bk),
        out_shape=(jax.ShapeDtypeStruct(q_slots.shape, jnp.bfloat16), jax.ShapeDtypeStruct((slots, 1, lanes), jnp.float32)),
        grid_spec=pltpu.PrefetchScalarGridSpec(
            num_scalar_prefetch=2, grid=(slots,),
            in_specs=[full_spec(arr.shape) for arr in operands],
            out_specs=(pl.BlockSpec((1, bq, width), lambda b, where_ref, _: (slot_of(where_ref, b // 2, b % 2), 0, 0)),
                       pl.BlockSpec((1, 1, lanes), lambda b, *_: (b, 0, 0))),
            scratch_shapes=[pltpu.VMEM((seq, HEAD_DIM), jnp.bfloat16), pltpu.VMEM((HEAD_DIM, seq), jnp.bfloat16), pltpu.VMEM((HEAD_DIM, lanes), jnp.bfloat16),
                            pltpu.VMEM((1, lanes), jnp.float32), pltpu.VMEM((1, lanes), jnp.float32), pltpu.VMEM((HEAD_DIM, lanes), jnp.float32)]),
        compiler_params=pltpu.CompilerParams(dimension_semantics=('arbitrary',), vmem_limit_bytes=48 << 20),
        cost_estimate=pl.CostEstimate(flops=4 * slots * bq * heads * seq * HEAD_DIM, bytes_accessed=4 * slots * bq * width + 8 * seq * HEAD_DIM, transcendentals=slots * bq * heads * seq // 2),
        name='attend_fwd',
    )(where, positions, *operands)


def attend_backward(where, positions, q_slots, do_slots, o_slots, kv_slots, kv_other, cos_t, sin_t, lo_all, lse, bk, partial):
    top = partial is None
    slots, bq, width = q_slots.shape
    seq = positions.shape[0] // (1 if top else 2)
    heads = width // HEAD_DIM
    lanes = heads * bq
    z_first = Z_SIZE // 2 if top else 0
    operands = [q_slots, do_slots, o_slots, kv_slots, kv_other, cos_t, sin_t, lo_all]
    in_specs = [full_spec(arr.shape) for arr in operands] + [pl.BlockSpec((1, 1, lanes), lambda b, *_: (b + 2 * z_first, 0, 0))]
    operands.append(lse)
    dq_spec = pl.BlockSpec((1, bq, width), lambda b, where_ref, _: (slot_of(where_ref, z_first + b // 2, b % 2), 0, 0))
    final_shape = (Z_SIZE // 2, CORE_SIZE, bq, 2 * HEAD_DIM)
    out_shape = [jax.ShapeDtypeStruct(q_slots.shape, jnp.bfloat16)] + [jax.ShapeDtypeStruct(final_shape, jnp.float32)] * 2
    out_specs = [dq_spec] + [full_spec(final_shape)] * 2
    aliases = {}
    if top:
        part_shape = (positions.shape[0] // 2, 2 * HEAD_DIM)
        out_shape.append(jax.ShapeDtypeStruct(part_shape, jnp.float32))
        out_specs.append(full_spec(part_shape))
    else:
        part, dq_top = partial
        operands += [part, dq_top]
        in_specs += [full_spec(part.shape), pl.BlockSpec(memory_space=pl.ANY)]
        aliases = {2 + len(operands) - 1: 0}
    work = slots * bq * heads * seq * HEAD_DIM
    return pl.pallas_call(
        functools.partial(bwd_kernel, heads, bk, z_first, top),
        out_shape=out_shape,
        grid_spec=pltpu.PrefetchScalarGridSpec(
            num_scalar_prefetch=2, grid=(slots // 2,), in_specs=in_specs, out_specs=out_specs,
            scratch_shapes=[pltpu.VMEM((seq, HEAD_DIM), jnp.bfloat16), pltpu.VMEM((HEAD_DIM, seq), jnp.bfloat16), pltpu.VMEM((seq, HEAD_DIM), jnp.bfloat16),
                            pltpu.VMEM((lanes, HEAD_DIM), jnp.bfloat16), pltpu.VMEM((HEAD_DIM, lanes), jnp.bfloat16),
                            pltpu.VMEM((lanes, HEAD_DIM), jnp.bfloat16), pltpu.VMEM((HEAD_DIM, lanes), jnp.bfloat16), pltpu.VMEM((HEAD_DIM, lanes), jnp.float32),
                            pltpu.VMEM((seq, 2 * HEAD_DIM), jnp.float32)]),
        input_output_aliases=aliases,
        compiler_params=pltpu.CompilerParams(dimension_semantics=('arbitrary',), vmem_limit_bytes=58 << 20),
        cost_estimate=pl.CostEstimate(flops=(7 if top else 5) * work, bytes_accessed=8 * slots * bq * width + 24 * seq * HEAD_DIM, transcendentals=work // (2 * HEAD_DIM)),
        name='attend_bwd_top' if top else 'attend_bwd_low',
    )(where, positions, *operands)


def solution(mesh):
    def member(z, y, c):
        return (z * Y_SIZE + y) * CORE_SIZE + c

    every = [(z, y, c) for z in range(Z_SIZE) for y in range(Y_SIZE) for c in range(CORE_SIZE)]

    def permuter(target, senders=range(Z_SIZE)):
        pairs = [(member(*src), member(*target(*src))) for src in every if src[0] in senders]
        return lambda val: lax.ppermute(val, 'tp', pairs)

    swap_core = permuter(lambda z, y, c: (z, y, 1 - c))
    swap_y = permuter(lambda z, y, c: (z, 1 - y, c))
    swap_same_head = permuter(lambda z, y, c: (z, 1 - y, 1 - c))
    ring = permuter(lambda z, y, c: ((z + 1) % Z_SIZE, y, c))
    hops = range(1, Z_SIZE)
    gather_right = {k: permuter(lambda z, y, c: (z + 1, y, c), range(k - 1, Z_SIZE - 1)) for k in hops}
    gather_left = {k: permuter(lambda z, y, c: (z - 1, y, c), range(1, Z_SIZE - k + 1)) for k in hops}
    scatter_right = {k: permuter(lambda z, y, c: (z + 1, y, c), range(0, k)) for k in hops}
    scatter_left = {k: permuter(lambda z, y, c: (z - 1, y, c), range(Z_SIZE - k, Z_SIZE)) for k in hops}
    z_swaps = {k: permuter(lambda z, y, c, k=k: (z ^ k, y, c)) for k in (1, 2)}

    def after(val, *deps):
        return lax.optimization_barrier((val,) + deps)[0]

    def device_step(x_blk, dy_blk, pos_all, norm_gain, wq_loc, wk_all, wv_all, wo_loc):
        seq_len = pos_all.shape[0]
        bq = seq_len // (Z_SIZE * Y_SIZE * CORE_SIZE)
        bk = 2 * bq
        model = x_blk.shape[1]
        idx = lax.axis_index('tp')
        z_idx, y_idx, c_idx = idx // (Y_SIZE * CORE_SIZE), (idx // CORE_SIZE) % Y_SIZE, idx % CORE_SIZE
        where = jnp.stack([z_idx, y_idx, c_idx])
        on_core0 = c_idx == 0
        pair = wq_loc.shape[1]
        kv_own = Y_SIZE * z_idx + (y_idx ^ c_idx)

        def select(first, second):
            return jnp.where(on_core0, first, second)

        def flip_core(arr):
            return arr[:, ::-1]

        def slots(arrs):
            return jnp.concatenate([arr[None] for arr in arrs], axis=0)

        def interleave(own, partner):
            return [blk for both in zip(own, partner) for blk in both]

        x_f32 = x_blk.astype(jnp.float32)
        hidden, x_hat, inv_rms = norm_forward(x_f32, norm_gain)

        h_own = [hidden]
        for s in hops:
            h_own.append(ring(h_own[-1]))
        h_pair = []
        for blk in h_own:
            h_pair.append(swap_core(blk))

        def slot_order(w_own, w_core, w_y, w_both):
            return [select(w_own, w_y), select(w_core, w_both), select(w_both, w_core), select(w_y, w_own)]

        wq_y = swap_y(wq_loc)
        wq_core = swap_core(wq_loc)
        q_cols = slot_order(wq_loc, wq_core, wq_y, swap_core(wq_y))
        wo_y = swap_y(wo_loc)
        o_rows = (wo_loc, swap_core(wo_loc), wo_y, swap_core(wo_y))

        def kv_columns(head):
            return [lax.dynamic_slice_in_dim(w, head * HEAD_DIM, HEAD_DIM, axis=1) for w in (wk_all, wv_all)]

        w_q = jnp.concatenate(q_cols, axis=1)
        w_kv = lax.optimization_barrier(jnp.concatenate(kv_columns(kv_own) + kv_columns(kv_own ^ 1), axis=1))
        w_own = jnp.concatenate([w_q[:, :2 * pair], w_kv[:, :2 * HEAD_DIM]], axis=1)
        w_mix = jnp.concatenate(slot_order(*o_rows), axis=0)
        lo_all = (lax.iota(jnp.int32, seq_len) - pos_all)[None, :]
        cos_t, sin_t = rope_tables(pos_all)

        def my_tables(lead, tail):
            parts = jnp.concatenate([lead.T, tail.T], axis=1).reshape(Z_SIZE, Y_SIZE, CORE_SIZE, bq, HEAD_DIM)
            parts = lax.dynamic_index_in_dim(parts, y_idx, 1, keepdims=False)
            return select(parts, flip_core(parts))

        cos_my, sin_my = my_tables(cos_t, cos_t), my_tables(sin_t, -sin_t)

        qkv = []
        for s in range(Z_SIZE):
            qkv += [dot_f32(blk, w_own).astype(jnp.bfloat16) for blk in (h_own[s], h_pair[s])]
        kv_blocks = [blk[:, 2 * pair:] for blk in qkv]
        early = SLOTS - CORE_SIZE
        kv_other_early = swap_same_head(slots(kv_blocks[:early]))
        kv_other_late = swap_same_head(slots(kv_blocks[early:]))
        kv_other = jnp.concatenate([kv_other_early, kv_other_late], axis=0)
        q_slots, kv_slots = slots([blk[:, :2 * pair] for blk in qkv]), slots(kv_blocks)

        g_own = []
        for blk in h_own:
            g_own.append(swap_y(after(blk, kv_other_late)))

        right, left = {0: after(dy_blk, h_own[-1])}, {}
        left[0] = right[0]
        for k in hops:
            right[k] = gather_right[k](right[k - 1])
            left[k] = gather_left[k](left[k - 1])
            right[k], left[k] = lax.optimization_barrier((right[k], left[k]))
        dy_own = [dy_blk] + [jnp.where(z_idx >= s, right[s], left[Z_SIZE - s]) for s in hops]
        dy_pair = []
        for blk in dy_own:
            dy_pair.append(swap_core(blk))
        dy_slots = interleave([dy_own[s] for s in DO_ORDER], [dy_pair[s] for s in DO_ORDER])

        o_slots, lse = attend(where, pos_all, q_slots, kv_slots, kv_other, cos_t, sin_t, lo_all, bk)
        by_line = (Z_SIZE, CORE_SIZE, bq, -1)
        o_lines = o_slots.reshape(by_line)
        o_partner = swap_core(o_slots).reshape(by_line)
        o_mine = jnp.concatenate([o_lines[:, 0], o_partner[:, 1]], axis=-1)

        def pair_sides(own, partner):
            first, last = own[..., :pair], partner[..., pair:2 * pair]
            return select(first, last), select(last, first)

        def by_block(arr):
            return arr.reshape((SLOTS,) + arr.shape[2:])

        def dy_order(arr):
            return jnp.concatenate([arr[s:s + 1] for s in DO_ORDER], axis=0)

        o_sides = lax.optimization_barrier(by_block(jnp.concatenate(pair_sides(dy_order(o_lines), dy_order(flip_core(o_partner))), axis=-1)))
        mix_part = []
        for s in range(Z_SIZE):
            mix_part.append(lax.optimization_barrier(dot_f32(o_mine[s], w_mix).astype(jnp.bfloat16)))

        def plus(*parts):
            return sum(part.astype(jnp.float32) for part in parts)

        sum_right, sum_left = mix_part[1], mix_part[Z_SIZE - 1]
        for k in hops:
            if k > 1:
                sum_right, sum_left = lax.optimization_barrier((sum_right, sum_left))
                sum_right = plus(mix_part[k], sum_right).astype(jnp.bfloat16)
                sum_left = plus(mix_part[Z_SIZE - k], sum_left).astype(jnp.bfloat16)
            sum_right = scatter_right[k](sum_right)
            sum_left = scatter_left[k](sum_left)
        result = (x_f32 + plus(mix_part[0], sum_right, sum_left)).astype(jnp.bfloat16)

        do_blocks = []
        for s in DO_ORDER:
            do_blocks += [dot_f32(blk, w_mix[:2 * pair], COLS_OF_BOTH).astype(jnp.bfloat16) for blk in (dy_own[s], dy_pair[s])]
        do_slots = slots(do_blocks)
        keys = (q_slots, do_slots, o_slots, kv_slots, kv_other, cos_t, sin_t, lo_all, lse, bk)
        dq_top, mine_top, send_top, part = attend_backward(where, pos_all, *keys, None)
        other_top = swap_same_head(send_top)
        dq_slots, mine_low, send_low = attend_backward(where, pos_all, *keys, (part, dq_top))
        other_low = swap_same_head(send_low)
        dq_partner = flip_core(swap_core(dq_slots).reshape(by_line))
        g_pair = [swap_core(blk) for blk in lax.optimization_barrier((*g_own, dq_slots))[:Z_SIZE]]
        dq_lines = dq_slots.reshape(by_line)

        dkv_lines = finish_key_grads(where, mine_low, other_low, mine_top, other_top, cos_my, sin_my)
        dkv_partner = flip_core(swap_core(dkv_lines))

        dq_rows = jnp.concatenate([dq_lines[:, 0], dq_partner[:, 0]], axis=-1)
        dh_q = dot_f32(dq_rows.reshape(Z_SIZE * bq, -1), w_q, COLS_OF_BOTH).reshape(Z_SIZE, bq, model)
        dkv_rows = jnp.concatenate([dkv_lines[:, 0], dkv_partner[:, 0]], axis=-1)

        halves = [slice(0, model // 2), slice(model // 2, model)]

        def dh_part(s, cols):
            return dh_q[s, :, cols] + dot_f32(dkv_rows[s], w_kv[cols], COLS_OF_BOTH)

        dh_sum = [dh_part(1, cols).astype(jnp.bfloat16) for cols in halves]
        for s in hops:
            for n, cols in enumerate(halves):
                if s > 1:
                    dh_sum[n] = (dh_part(s, cols) + dh_sum[n].astype(jnp.float32)).astype(jnp.bfloat16)
                if s == hops[-1] and n == 0:
                    dh_sum[n], result = lax.optimization_barrier((dh_sum[n], result))
                dh_sum[n] = ring(dh_sum[n])
        dh_rows = jnp.concatenate([(dh_part(0, cols) + dh_sum[n].astype(jnp.float32)).astype(jnp.bfloat16) for n, cols in enumerate(halves)], axis=1)

        q_keep, q_send = pair_sides(dq_lines, dq_partner)
        kv_keep = select(dkv_lines[..., :HEAD_DIM], dkv_partner[..., HEAD_DIM:])
        kv_send = select(dkv_partner[..., :HEAD_DIM], dkv_lines[..., HEAD_DIM:])
        d_keep = by_block(jnp.concatenate([q_keep, kv_keep], axis=-1))
        d_send = by_block(jnp.concatenate([q_send, kv_send], axis=-1))
        d_theirs = swap_y(d_send)

        dwo_keep, dwo_send = token_grads(dy_slots, o_sides, [((pair, model), jnp.float32)] * 2)
        dwo_theirs = swap_y(dwo_send)
        d_wo = (dwo_keep + dwo_theirs).astype(jnp.bfloat16)

        d_wq, kv_mine_sum = token_grads(interleave(h_own, h_pair) + interleave(g_own, g_pair), jnp.concatenate([d_keep, d_theirs], axis=0),
                                        [((model, pair), jnp.bfloat16), ((model, HEAD_DIM), jnp.float32)])
        kv_other_sum = swap_core(kv_mine_sum)
        d_wk = select(kv_mine_sum, kv_other_sum)
        d_wv = select(kv_other_sum, kv_mine_sum)

        d_input, dg_part = norm_backward(dh_rows, x_hat, inv_rms, norm_gain)
        grad_x = (dy_blk.astype(jnp.float32) + d_input).astype(jnp.bfloat16)
        for swap in (swap_core, swap_y, z_swaps[1], z_swaps[2]):
            dg_part = dg_part + swap(dg_part)
        return result, grad_x, d_wq, d_wk, d_wv, d_wo, dg_part

    specs_in = (P(('dp', 'tp'), None), P(('dp', 'tp'), None), P('dp'), P(), P(None, 'tp'), P(), P(), P('tp', None))
    specs_out = (P(('dp', 'tp'), None), P(('dp', 'tp'), None), P('dp', 'tp'), P('dp', 'tp'), P('dp', 'tp'), P(('dp', 'tp'), None), P('dp'))
    return jax.shard_map(device_step, mesh=mesh, in_specs=specs_in, out_specs=specs_out, check_vma=False)
```

```python
import functools
import jax
import jax.numpy as jnp
from jax import lax
from jax.experimental import pallas as pl
from jax.experimental.pallas import tpu as pltpu
from jax.sharding import PartitionSpec as P

HEAD_DIM = 128
SCORE_SCALE = HEAD_DIM ** -0.5
SCALE_LOG2E = SCORE_SCALE * 1.4426950408889634
ROPE_THETA = 1000000.0
NORM_EPS = 1e-05
MASKED = -1e30
Z_SIZE = 4
Y_SIZE = 2
CORE_SIZE = 2
SLOTS = Z_SIZE * CORE_SIZE
DO_ORDER = (0, 2, 1, 3)
NATURAL = (((1,), (0,)), ((), ()))
COLS_OF_BOTH = (((1,), (1,)), ((), ()))


def dot_f32(lhs, rhs, dims=NATURAL):
    return lax.dot_general(lhs, rhs, dims, preferred_element_type=jnp.float32)


def rope_tables(positions):
    exponents = jnp.arange(0, HEAD_DIM, 2, dtype=jnp.float32) / HEAD_DIM
    angles = jnp.power(ROPE_THETA, -exponents)[:, None] * positions.astype(jnp.float32)[None, :]
    return jnp.cos(angles), jnp.sin(angles)


def rotate_rows(t_f32, cos_t, sin_t):
    lead_half, tail_half = t_f32[:HEAD_DIM // 2], t_f32[HEAD_DIM // 2:]
    return jnp.concatenate([lead_half * cos_t - tail_half * sin_t, tail_half * cos_t + lead_half * sin_t], axis=0).astype(jnp.bfloat16)


def norm_forward(x_f32, norm_gain):
    inv_rms = lax.rsqrt(jnp.mean(x_f32 * x_f32, axis=-1, keepdims=True) + NORM_EPS)
    x_hat = x_f32 * inv_rms
    return (x_hat * norm_gain).astype(jnp.bfloat16), x_hat, inv_rms


def norm_backward(d_hidden, x_hat, inv_rms, norm_gain):
    d_f32 = d_hidden.astype(jnp.float32)
    d_gain = jnp.sum(d_f32 * x_hat, axis=0)
    scaled = d_f32 * norm_gain
    d_input = inv_rms * (scaled - x_hat * jnp.mean(scaled * x_hat, axis=-1, keepdims=True))
    return d_input, d_gain


def slot_of(where_ref, z, c):
    return 2 * lax.rem(where_ref[0] - z + Z_SIZE, Z_SIZE) + (where_ref[2] ^ c)


def slot_of_other(where_ref, z, c):
    return 2 * lax.rem(where_ref[0] - z + Z_SIZE, Z_SIZE) + (1 - (where_ref[2] ^ c))


def do_slot_of(where_ref, z, c):
    s = lax.rem(where_ref[0] - z + Z_SIZE, Z_SIZE)
    return 2 * (s // 2 + 2 * (s % 2)) + (where_ref[2] ^ c)


def block_token(where_ref, b, bq):
    return pl.multiple_of((b // 2) * (4 * bq) + where_ref[1] * (2 * bq) + (b % 2) * bq, bq)


def key_range(pos_ref, start, bq, bk):
    lo_first, lo_last = start - pos_ref[start], start + bq - 1 - pos_ref[start + bq - 1]
    return lo_first // bk, (start + bq - 1) // bk + 1, (lo_last + bk - 1) // bk, (start + 1) // bk


def tile_lanes(row, heads):
    return jnp.concatenate([row] * heads, axis=1)


def row_bounds(lo_ref, start, bq, heads):
    tok = start + lax.broadcasted_iota(jnp.int32, (1, bq), 1)
    return tile_lanes(tok, heads), tile_lanes(lo_ref[:, pl.ds(start, bq)], heads)


def keep_mask(key_start, bk, t_row, lo_row):
    key_idx = key_start + lax.broadcasted_iota(jnp.int32, (bk, t_row.shape[1]), 0)
    return (key_idx <= t_row) & (key_idx >= lo_row)


def head_columns(block, h):
    return block[:, h * HEAD_DIM:(h + 1) * HEAD_DIM]


def rotated_queries(q_blk, cos_ref, sin_ref, start, bq, heads):
    cos_t, sin_t = cos_ref[:, pl.ds(start, bq)], sin_ref[:, pl.ds(start, bq)]
    return [rotate_rows(head_columns(q_blk, h).T.astype(jnp.float32), cos_t, sin_t) for h in range(heads)]


def visit_keys(bounds, step):
    first, end, inner_first, inner_end = bounds

    def visit(j, carry):
        inner = (j >= inner_first) & (j < inner_end)

        @pl.when(inner)
        def _():
            step(j, False)

        @pl.when(jnp.logical_not(inner))
        def _():
            step(j, True)

        return carry

    lax.fori_loop(first, end, visit, 0)


def for_key_blocks(where_ref, mine_ref, theirs_ref, count, bq, store):
    def visit(n, carry):
        z, y, c = n // 4, (n // 2) % 2, n % 2
        block = jnp.where(y == where_ref[1], mine_ref[slot_of(where_ref, z, c)], theirs_ref[slot_of_other(where_ref, z, c)])
        store(pl.ds(pl.multiple_of(n * bq, bq), bq), block)
        return carry

    lax.fori_loop(0, count, visit, 0)


def fwd_kernel(heads, bk, where_ref, pos_ref, q_ref, kv_ref, kv_other_ref, cos_ref, sin_ref, lo_ref, o_ref, lse_ref, k_s, vt_s, qt_s, m_s, l_s, acc_s):
    b = pl.program_id(0)
    bq = q_ref.shape[1]
    seq = k_s.shape[0]

    @pl.when(b == 0)
    def _():
        def store(rows, block):
            k_s[rows, :] = rotate_rows(block[:, :HEAD_DIM].T.astype(jnp.float32), cos_ref[:, rows], sin_ref[:, rows]).T
            vt_s[:, rows] = block[:, HEAD_DIM:].T

        for_key_blocks(where_ref, kv_ref, kv_other_ref, seq // bq, bq, store)

    start = block_token(where_ref, b, bq)
    t_row, lo_row = row_bounds(lo_ref, start, bq, heads)
    q_blk = q_ref[0]
    qt_s[...] = jnp.concatenate(rotated_queries(q_blk, cos_ref, sin_ref, start, bq, heads), axis=1)
    m_s[...] = jnp.full_like(m_s, MASKED)
    l_s[...] = jnp.zeros_like(l_s)
    acc_s[...] = jnp.zeros_like(acc_s)

    def step(j, masked):
        key_start = pl.multiple_of(j * bk, bk)
        keys = pl.ds(key_start, bk)
        scores = dot_f32(k_s[keys, :], qt_s[...])
        if masked:
            scores = jnp.where(keep_mask(key_start, bk, t_row, lo_row), scores, MASKED)
        m_old = m_s[...]
        m_new = jnp.maximum(m_old, jnp.max(scores, axis=0, keepdims=True))
        probs = jnp.exp2(scores * SCALE_LOG2E - m_new * SCALE_LOG2E)
        alpha = jnp.exp2((m_old - m_new) * SCALE_LOG2E)
        m_s[...] = m_new
        l_s[...] = l_s[...] * alpha + jnp.sum(probs, axis=0, keepdims=True)
        acc_s[...] = acc_s[...] * alpha + dot_f32(vt_s[:, keys], probs.astype(jnp.bfloat16))

    visit_keys(key_range(pos_ref, start, bq, bk), step)
    out_t = (acc_s[...] / l_s[...]).astype(jnp.bfloat16)
    for h in range(heads):
        o_ref[0, :, h * HEAD_DIM:(h + 1) * HEAD_DIM] = out_t[:, h * bq:(h + 1) * bq].T
    lse_ref[0] = m_s[...] * SCALE_LOG2E + jnp.log2(l_s[...])


def bwd_kernel(heads, bk, where_ref, pos_ref, q_ref, do_ref, o_ref, kv_ref, kv_other_ref, cos_ref, sin_ref, lo_ref, lse_ref, dq_ref, mine_ref, send_ref, k_s, kt_s, v_s, q_s, qt_s, do_s, dot_s, dqt_s, acc_s):
    b = pl.program_id(0)
    bq = q_ref.shape[1]
    seq = k_s.shape[0]

    @pl.when(b == 0)
    def _():
        def store(rows, block):
            acc_s[rows, :] = jnp.zeros((bq, 2 * HEAD_DIM), jnp.float32)
            k_rot_t = rotate_rows(block[:, :HEAD_DIM].T.astype(jnp.float32), cos_ref[:, rows], sin_ref[:, rows])
            kt_s[:, rows] = k_rot_t
            k_s[rows, :] = k_rot_t.T
            v_s[rows, :] = block[:, HEAD_DIM:]

        for_key_blocks(where_ref, kv_ref, kv_other_ref, seq // bq, bq, store)

    start = block_token(where_ref, b, bq)
    t_row, lo_row = row_bounds(lo_ref, start, bq, heads)
    q_blk, do_blk, o_blk = q_ref[0], do_ref[0], o_ref[0]
    deltas = []
    for h, q_rot_t in enumerate(rotated_queries(q_blk, cos_ref, sin_ref, start, bq, heads)):
        lanes = slice(h * bq, (h + 1) * bq)
        qt_s[:, lanes] = q_rot_t
        q_s[lanes, :] = q_rot_t.T
        do_head = head_columns(do_blk, h)
        do_s[lanes, :] = do_head
        do_t = do_head.T
        dot_s[:, lanes] = do_t
        deltas.append(jnp.sum(do_t.astype(jnp.float32) * head_columns(o_blk, h).T.astype(jnp.float32), axis=0, keepdims=True))
    delta = jnp.concatenate(deltas, axis=1)
    lse = lse_ref[0]
    dqt_s[...] = jnp.zeros_like(dqt_s)

    def step(j, masked):
        key_start = pl.multiple_of(j * bk, bk)
        keys = pl.ds(key_start, bk)
        scores = dot_f32(k_s[keys, :], qt_s[...])
        probs = jnp.exp2(scores * SCALE_LOG2E - lse)
        if masked:
            probs = jnp.where(keep_mask(key_start, bk, t_row, lo_row), probs, 0.0)
        d_probs = dot_f32(v_s[keys, :], dot_s[...])
        d_scores = (probs * (d_probs - delta)).astype(jnp.bfloat16)
        acc_s[keys, HEAD_DIM:] += dot_f32(probs.astype(jnp.bfloat16), do_s[...])
        acc_s[keys, :HEAD_DIM] += dot_f32(d_scores, q_s[...]) * SCORE_SCALE
        dqt_s[...] += dot_f32(kt_s[:, keys], d_scores)

    visit_keys(key_range(pos_ref, start, bq, bk), step)
    cos_t, sin_t = cos_ref[:, pl.ds(start, bq)], sin_ref[:, pl.ds(start, bq)]
    for h in range(heads):
        dq_rot_t = (dqt_s[:, h * bq:(h + 1) * bq] * SCORE_SCALE).astype(jnp.bfloat16).astype(jnp.float32)
        dq_ref[0, :, h * HEAD_DIM:(h + 1) * HEAD_DIM] = rotate_rows(dq_rot_t, cos_t, -sin_t).T

    @pl.when(b == pl.num_programs(0) - 1)
    def _():
        def hand_over(y, mine):
            for z in range(Z_SIZE):
                for c in range(CORE_SIZE):
                    rows = ((z * 2 + y) * 2 + c) * bq
                    e = where_ref[2] ^ c
                    if mine:
                        mine_ref[z, e] = acc_s[rows:rows + bq, :]
                    else:
                        send_ref[z, 1 - e] = acc_s[rows:rows + bq, :]

        for y in range(Y_SIZE):
            pl.when(where_ref[1] == y)(functools.partial(hand_over, y, True))
            pl.when(where_ref[1] != y)(functools.partial(hand_over, y, False))


def token_grads_kernel(count, *refs):
    blocks, lhs_ref, out_refs, lhs_t = refs[:count], refs[count], refs[count + 1:-1], refs[-1]
    rows = lhs_ref.shape[1]

    @pl.when(pl.program_id(0) == 0)
    def _():
        for n in range(count):
            lhs_t[:, n * rows:(n + 1) * rows] = lhs_ref[n].T

    total = sum(dot_f32(lhs_t[:, n * rows:(n + 1) * rows], blocks[n][...]) for n in range(count))
    start = 0
    for ref in out_refs:
        if ref.shape[0] == blocks[0].shape[1]:
            size = ref.shape[1]
            ref[...] = total[start:start + size, :].T.astype(ref.dtype)
        else:
            size = ref.shape[0]
            ref[...] = total[start:start + size, :].astype(ref.dtype)
        start += size


def token_grads(blocks, lhs, outs, tile=512):
    rows, model = blocks[0].shape
    width = lhs.shape[2]
    specs = [pl.BlockSpec((tile, shape[1]), lambda i: (i, 0)) if shape[0] == model else pl.BlockSpec((shape[0], tile), lambda i: (0, i)) for shape, _ in outs]
    return pl.pallas_call(
        functools.partial(token_grads_kernel, len(blocks)),
        out_shape=[jax.ShapeDtypeStruct(*out) for out in outs], grid=(model // tile,),
        in_specs=[pl.BlockSpec((rows, tile), lambda i: (0, i)) for _ in blocks] + [pl.BlockSpec(lhs.shape, lambda i: (0, 0, 0))], out_specs=specs,
        scratch_shapes=[pltpu.VMEM((width, len(blocks) * rows), jnp.bfloat16)],
        compiler_params=pltpu.CompilerParams(dimension_semantics=('arbitrary',), vmem_limit_bytes=48 << 20),
        cost_estimate=pl.CostEstimate(flops=2 * len(blocks) * rows * model * width, bytes_accessed=2 * len(blocks) * rows * model, transcendentals=0),
    )(*blocks, lhs)


def finish_kernel(where_ref, mine_ref, other_ref, cos_ref, sin_ref, out_ref):
    for z in range(Z_SIZE):
        slot = lax.rem(where_ref[0] - z + Z_SIZE, Z_SIZE)
        for e in range(CORE_SIZE):
            total = mine_ref[z, e] + other_ref[z, e]
            dk = total[:, :HEAD_DIM].astype(jnp.bfloat16).astype(jnp.float32)
            out_ref[slot, e, :, :HEAD_DIM] = (dk * cos_ref[z, e] + pltpu.roll(dk, HEAD_DIM // 2, 1) * sin_ref[z, e]).astype(jnp.bfloat16)
            out_ref[slot, e, :, HEAD_DIM:] = total[:, HEAD_DIM:].astype(jnp.bfloat16)


def finish_key_grads(where, *operands):
    return pl.pallas_call(
        finish_kernel, out_shape=jax.ShapeDtypeStruct(operands[0].shape, jnp.bfloat16),
        grid_spec=pltpu.PrefetchScalarGridSpec(num_scalar_prefetch=1, grid=(1,), in_specs=[full_spec(arr.shape) for arr in operands], out_specs=full_spec(operands[0].shape)),
        compiler_params=pltpu.CompilerParams(dimension_semantics=('arbitrary',), vmem_limit_bytes=32 << 20),
        cost_estimate=pl.CostEstimate(flops=1000000, bytes_accessed=8000000, transcendentals=0),
    )(where, *operands)


def full_spec(shape):
    return pl.BlockSpec(shape, lambda b, *_: (0,) * len(shape))


def slot_spec(bq, width, find):
    return pl.BlockSpec((1, bq, width), lambda b, where_ref, _: (find(where_ref, b // 2, b % 2), 0, 0))


def attend(where, positions, q_slots, kv_slots, kv_other, cos_t, sin_t, lo_all, bk):
    slots, bq, width = q_slots.shape
    seq = positions.shape[0]
    heads = width // HEAD_DIM
    lanes = heads * bq
    shared = (kv_slots, kv_other, cos_t, sin_t, lo_all)
    block = slot_spec(bq, width, slot_of)
    return pl.pallas_call(
        functools.partial(fwd_kernel, heads, bk),
        out_shape=(jax.ShapeDtypeStruct(q_slots.shape, jnp.bfloat16), jax.ShapeDtypeStruct((slots, 1, lanes), jnp.float32)),
        grid_spec=pltpu.PrefetchScalarGridSpec(
            num_scalar_prefetch=2, grid=(slots,), in_specs=[block] + [full_spec(arr.shape) for arr in shared],
            out_specs=(block, pl.BlockSpec((1, 1, lanes), lambda b, *_: (b, 0, 0))),
            scratch_shapes=[pltpu.VMEM((seq, HEAD_DIM), jnp.bfloat16), pltpu.VMEM((HEAD_DIM, seq), jnp.bfloat16), pltpu.VMEM((HEAD_DIM, lanes), jnp.bfloat16),
                            pltpu.VMEM((1, lanes), jnp.float32), pltpu.VMEM((1, lanes), jnp.float32), pltpu.VMEM((HEAD_DIM, lanes), jnp.float32)]),
        compiler_params=pltpu.CompilerParams(dimension_semantics=('arbitrary',), vmem_limit_bytes=48 << 20),
        cost_estimate=pl.CostEstimate(flops=4 * slots * bq * heads * seq * HEAD_DIM, bytes_accessed=4 * slots * bq * width + 8 * seq * HEAD_DIM, transcendentals=slots * bq * heads * seq // 2),
        name='attend_fwd',
    )(where, positions, q_slots, *shared)


def attend_backward(where, positions, q_slots, do_slots, o_slots, kv_slots, kv_other, cos_t, sin_t, lo_all, lse, bk):
    slots, bq, width = q_slots.shape
    seq = positions.shape[0]
    heads = width // HEAD_DIM
    lanes = heads * bq
    shared = (kv_slots, kv_other, cos_t, sin_t, lo_all)
    block = slot_spec(bq, width, slot_of)
    final_shape = (Z_SIZE, CORE_SIZE, bq, 2 * HEAD_DIM)
    return pl.pallas_call(
        functools.partial(bwd_kernel, heads, bk),
        out_shape=[jax.ShapeDtypeStruct(q_slots.shape, jnp.bfloat16)] + [jax.ShapeDtypeStruct(final_shape, jnp.float32)] * 2,
        grid_spec=pltpu.PrefetchScalarGridSpec(
            num_scalar_prefetch=2, grid=(slots,),
            in_specs=[block, slot_spec(bq, width, do_slot_of), block] + [full_spec(arr.shape) for arr in shared] + [pl.BlockSpec((1, 1, lanes), lambda b, *_: (b, 0, 0))],
            out_specs=[block, full_spec(final_shape), full_spec(final_shape)],
            scratch_shapes=[pltpu.VMEM((seq, HEAD_DIM), jnp.bfloat16), pltpu.VMEM((HEAD_DIM, seq), jnp.bfloat16), pltpu.VMEM((seq, HEAD_DIM), jnp.bfloat16),
                            pltpu.VMEM((lanes, HEAD_DIM), jnp.bfloat16), pltpu.VMEM((HEAD_DIM, lanes), jnp.bfloat16),
                            pltpu.VMEM((lanes, HEAD_DIM), jnp.bfloat16), pltpu.VMEM((HEAD_DIM, lanes), jnp.bfloat16), pltpu.VMEM((HEAD_DIM, lanes), jnp.float32),
                            pltpu.VMEM((seq, 2 * HEAD_DIM), jnp.float32)]),
        compiler_params=pltpu.CompilerParams(dimension_semantics=('arbitrary',), vmem_limit_bytes=58 << 20),
        cost_estimate=pl.CostEstimate(flops=10 * slots * bq * heads * seq * HEAD_DIM, bytes_accessed=8 * slots * bq * width + 24 * seq * HEAD_DIM, transcendentals=slots * bq * heads * seq // 2),
        name='attend_bwd',
    )(where, positions, q_slots, do_slots, o_slots, *shared, lse)


def solution(mesh):
    def member(z, y, c):
        return (z * Y_SIZE + y) * CORE_SIZE + c

    every = [(z, y, c) for z in range(Z_SIZE) for y in range(Y_SIZE) for c in range(CORE_SIZE)]

    def permuter(target, senders=range(Z_SIZE)):
        pairs = [(member(*src), member(*target(*src))) for src in every if src[0] in senders]
        return lambda val: lax.ppermute(val, 'tp', pairs)

    swap_core = permuter(lambda z, y, c: (z, y, 1 - c))
    swap_y = permuter(lambda z, y, c: (z, 1 - y, c))
    swap_same_head = permuter(lambda z, y, c: (z, 1 - y, 1 - c))
    ring = permuter(lambda z, y, c: ((z + 1) % Z_SIZE, y, c))
    ring_back = permuter(lambda z, y, c: ((z - 1) % Z_SIZE, y, c))
    hops = range(1, Z_SIZE)
    gather_right = {k: permuter(lambda z, y, c: (z + 1, y, c), range(k - 1, Z_SIZE - 1)) for k in hops}
    gather_left = {k: permuter(lambda z, y, c: (z - 1, y, c), range(1, Z_SIZE - k + 1)) for k in hops}
    scatter_right = {k: permuter(lambda z, y, c: (z + 1, y, c), range(0, k)) for k in hops}
    scatter_left = {k: permuter(lambda z, y, c: (z - 1, y, c), range(Z_SIZE - k, Z_SIZE)) for k in hops}
    z_swaps = {k: permuter(lambda z, y, c, k=k: (z ^ k, y, c)) for k in (1, 2)}

    def after(val, *deps):
        return lax.optimization_barrier((val,) + deps)[0]

    def device_step(x_blk, dy_blk, pos_all, norm_gain, wq_loc, wk_all, wv_all, wo_loc):
        seq_len = pos_all.shape[0]
        bq = seq_len // (Z_SIZE * Y_SIZE * CORE_SIZE)
        bk = 2 * bq
        model = x_blk.shape[1]
        idx = lax.axis_index('tp')
        z_idx, y_idx, c_idx = idx // (Y_SIZE * CORE_SIZE), (idx // CORE_SIZE) % Y_SIZE, idx % CORE_SIZE
        where = jnp.stack([z_idx, y_idx, c_idx])
        on_core0 = c_idx == 0
        pair = wq_loc.shape[1]
        kv_own = Y_SIZE * z_idx + (y_idx ^ c_idx)

        def select(first, second):
            return jnp.where(on_core0, first, second)

        def flip_core(arr):
            return arr[:, ::-1]

        def slots(arrs):
            return jnp.concatenate([arr[None] for arr in arrs], axis=0)

        def interleave(own, partner):
            return [blk for both in zip(own, partner) for blk in both]

        x_f32 = x_blk.astype(jnp.float32)
        hidden, x_hat, inv_rms = norm_forward(x_f32, norm_gain)

        h_own = [hidden]
        for s in hops:
            h_own.append(ring(h_own[-1]))
        h_pair = []
        for blk in h_own:
            h_pair.append(swap_core(blk))

        def slot_order(w_own, w_core, w_y, w_both):
            return [select(w_own, w_y), select(w_core, w_both), select(w_both, w_core), select(w_y, w_own)]

        wq_y = swap_y(wq_loc)
        wq_core = swap_core(wq_loc)
        q_cols = slot_order(wq_loc, wq_core, wq_y, swap_core(wq_y))
        wo_y = swap_y(wo_loc)
        o_rows = (wo_loc, swap_core(wo_loc), wo_y, swap_core(wo_y))

        def kv_columns(head):
            return [lax.dynamic_slice_in_dim(w, head * HEAD_DIM, HEAD_DIM, axis=1) for w in (wk_all, wv_all)]

        w_q = lax.optimization_barrier(jnp.concatenate(q_cols, axis=1))
        w_kv = lax.optimization_barrier(jnp.concatenate(kv_columns(kv_own) + kv_columns(kv_own ^ 1), axis=1))
        kv_next = lax.rem(kv_own + Y_SIZE, Y_SIZE * Z_SIZE)
        w_kv_next = lax.optimization_barrier(jnp.concatenate(kv_columns(kv_next) + kv_columns(kv_next ^ 1), axis=1))
        w_own = jnp.concatenate([w_q[:, :2 * pair], w_kv[:, :2 * HEAD_DIM]], axis=1)
        w_mix = jnp.concatenate(slot_order(*o_rows), axis=0)
        lo_all = (lax.iota(jnp.int32, seq_len) - pos_all)[None, :]
        cos_t, sin_t = rope_tables(pos_all)

        def my_tables(lead, tail):
            parts = jnp.concatenate([lead.T, tail.T], axis=1).reshape(Z_SIZE, Y_SIZE, CORE_SIZE, bq, HEAD_DIM)
            parts = lax.dynamic_index_in_dim(parts, y_idx, 1, keepdims=False)
            return select(parts, flip_core(parts))

        cos_my, sin_my = my_tables(cos_t, cos_t), my_tables(sin_t, -sin_t)

        qkv = []
        for s in range(Z_SIZE):
            qkv += [dot_f32(blk, w_own).astype(jnp.bfloat16) for blk in (h_own[s], h_pair[s])]
        kv_blocks = [blk[:, 2 * pair:] for blk in qkv]
        early = SLOTS - CORE_SIZE
        kv_other_early = swap_same_head(slots(kv_blocks[:early]))
        kv_other_late = swap_same_head(slots(kv_blocks[early:]))
        kv_other = jnp.concatenate([kv_other_early, kv_other_late], axis=0)
        q_slots, kv_slots = slots([blk[:, :2 * pair] for blk in qkv]), slots(kv_blocks)

        g_own = []
        for s, blk in enumerate(h_own):
            g_own.append(swap_y(after(blk, kv_other_late if s else wo_y)))

        right, left = {0: after(dy_blk, h_own[-1])}, {}
        left[0] = right[0]
        for k in hops:
            right[k] = gather_right[k](right[k - 1])
            left[k] = gather_left[k](left[k - 1])
            right[k], left[k] = lax.optimization_barrier((right[k], left[k]))
        dy_own = [dy_blk] + [jnp.where(z_idx >= s, right[s], left[Z_SIZE - s]) for s in hops]
        dy_pair = []
        for blk in dy_own:
            dy_pair.append(swap_core(blk))
        dy_slots = interleave([dy_own[s] for s in DO_ORDER], [dy_pair[s] for s in DO_ORDER])

        o_slots, lse = attend(where, pos_all, q_slots, kv_slots, kv_other, cos_t, sin_t, lo_all, bk)
        by_line = (Z_SIZE, CORE_SIZE, bq, -1)
        o_lines = o_slots.reshape(by_line)
        o_partner = swap_core(o_slots).reshape(by_line)
        o_mine = jnp.concatenate([o_lines[:, 0], o_partner[:, 1]], axis=-1)

        def pair_sides(own, partner):
            first, last = own[..., :pair], partner[..., pair:2 * pair]
            return select(first, last), select(last, first)

        def by_block(arr):
            return arr.reshape((SLOTS,) + arr.shape[2:])

        def dy_order(arr):
            return jnp.concatenate([arr[s:s + 1] for s in DO_ORDER], axis=0)

        o_sides = lax.optimization_barrier(by_block(jnp.concatenate(pair_sides(dy_order(o_lines), dy_order(flip_core(o_partner))), axis=-1)))
        mix_part = []
        for s in range(Z_SIZE):
            mix_part.append(lax.optimization_barrier(dot_f32(o_mine[s], w_mix).astype(jnp.bfloat16)))

        def plus(*parts):
            return sum(part.astype(jnp.float32) for part in parts)

        sum_right, sum_left = mix_part[1], mix_part[Z_SIZE - 1]
        for k in hops:
            if k > 1:
                sum_right, sum_left = lax.optimization_barrier((sum_right, sum_left))
                sum_right = plus(mix_part[k], sum_right).astype(jnp.bfloat16)
                sum_left = plus(mix_part[Z_SIZE - k], sum_left).astype(jnp.bfloat16)
            sum_right = scatter_right[k](sum_right)
            sum_left = scatter_left[k](sum_left)
        result = (x_f32 + plus(mix_part[0], sum_right, sum_left)).astype(jnp.bfloat16)

        do_blocks = []
        for s in DO_ORDER:
            do_blocks += [dot_f32(blk, w_mix[:2 * pair], COLS_OF_BOTH).astype(jnp.bfloat16) for blk in (dy_own[s], dy_pair[s])]
        do_slots = slots(do_blocks)
        dq_slots, dkv_mine, dkv_send = attend_backward(where, pos_all, q_slots, do_slots, o_slots, kv_slots, kv_other, cos_t, sin_t, lo_all, lse, bk)
        dkv_theirs = swap_same_head(dkv_send)
        dq_partner = flip_core(swap_core(dq_slots).reshape(by_line))
        dq_lines = dq_slots.reshape(by_line)
        dq_rows = jnp.concatenate([dq_lines[:, 0], dq_partner[:, 0]], axis=-1)
        halves = [slice(0, model // 2), slice(model // 2, model)]
        dh_sum = [dot_f32(dq_rows[1], w_q[cols], COLS_OF_BOTH).astype(jnp.bfloat16) for cols in halves]
        for n in range(2):
            dh_sum[n] = ring(dh_sum[n])

        dkv_lines = finish_key_grads(where, dkv_mine, dkv_theirs, cos_my, sin_my)
        dkv_partner = flip_core(swap_core(dkv_lines))
        dkv_rows = jnp.concatenate([dkv_lines[:, 0], dkv_partner[:, 0]], axis=-1)
        dkv_next = ring_back(dkv_rows[1])

        def dh_part(s, cols):
            return dot_f32(dq_rows[s], w_q[cols], COLS_OF_BOTH) + dot_f32(dkv_rows[s], w_kv[cols], COLS_OF_BOTH)

        for s in hops[1:]:
            for n, cols in enumerate(halves):
                dh_sum[n] = (dh_part(s, cols) + dh_sum[n].astype(jnp.float32)).astype(jnp.bfloat16)
                if s == hops[-1] and n == 0:
                    dh_sum[n], result = lax.optimization_barrier((dh_sum[n], result))
                dh_sum[n] = ring(dh_sum[n])
        dh_own = lax.optimization_barrier([dh_part(0, cols) + dot_f32(dkv_next, w_kv_next[cols], COLS_OF_BOTH) for cols in halves])
        dh_rows = jnp.concatenate([(own + part.astype(jnp.float32)).astype(jnp.bfloat16) for own, part in zip(dh_own, dh_sum)], axis=1)

        g_pair = [swap_core(blk) for blk in lax.optimization_barrier((*g_own, dq_slots))[:Z_SIZE]]
        q_keep, q_send = pair_sides(dq_lines, dq_partner)
        kv_keep = select(dkv_lines[..., :HEAD_DIM], dkv_partner[..., HEAD_DIM:])
        kv_send = select(dkv_partner[..., :HEAD_DIM], dkv_lines[..., HEAD_DIM:])
        d_keep = by_block(jnp.concatenate([q_keep, kv_keep], axis=-1))
        d_send = by_block(jnp.concatenate([q_send, kv_send], axis=-1))
        d_theirs = swap_y(d_send)

        dwo_keep, dwo_send = token_grads(dy_slots, o_sides, [((pair, model), jnp.float32)] * 2)
        theirs_first = swap_y(dwo_send[:, halves[0]])
        theirs_last = swap_y(dwo_send[:, halves[1]])
        d_wo = (dwo_keep + jnp.concatenate([theirs_first, theirs_last], axis=1)).astype(jnp.bfloat16)

        d_wq, kv_mine_sum = token_grads(interleave(h_own, h_pair) + interleave(g_own, g_pair), jnp.concatenate([d_keep, d_theirs], axis=0),
                                        [((model, pair), jnp.bfloat16), ((model, HEAD_DIM), jnp.float32)])
        kv_other_sum = swap_core(kv_mine_sum)
        d_wk = select(kv_mine_sum, kv_other_sum)
        d_wv = select(kv_other_sum, kv_mine_sum)

        d_input, dg_part = norm_backward(dh_rows, x_hat, inv_rms, norm_gain)
        grad_x = (dy_blk.astype(jnp.float32) + d_input).astype(jnp.bfloat16)
        for swap in (swap_core, swap_y, z_swaps[1], z_swaps[2]):
            dg_part = dg_part + swap(dg_part)
        return result, grad_x, d_wq, d_wk, d_wv, d_wo, dg_part

    specs_in = (P(('dp', 'tp'), None), P(('dp', 'tp'), None), P('dp'), P(), P(None, 'tp'), P(), P(), P('tp', None))
    specs_out = (P(('dp', 'tp'), None), P(('dp', 'tp'), None), P('dp', 'tp'), P('dp', 'tp'), P('dp', 'tp'), P(('dp', 'tp'), None), P('dp'))
    return jax.shard_map(device_step, mesh=mesh, in_specs=specs_in, out_specs=specs_out, check_vma=False)
```

```python
import functools
import jax
import jax.numpy as jnp
from jax import lax
from jax.experimental import pallas as pl
from jax.experimental.pallas import tpu as pltpu
from jax.sharding import PartitionSpec as P

HEAD_DIM = 128
SCORE_SCALE = HEAD_DIM ** -0.5
SCALE_LOG2E = SCORE_SCALE * 1.4426950408889634
ROPE_THETA = 1000000.0
NORM_EPS = 1e-05
MASKED = -1e30
Z_SIZE = 4
Y_SIZE = 2
CORE_SIZE = 2
SLOTS = Z_SIZE * CORE_SIZE
DO_ORDER = (0, 2, 1, 3)
EARLY, LATE = DO_ORDER[:2], DO_ORDER[2:]
NATURAL = (((1,), (0,)), ((), ()))
COLS_OF_BOTH = (((1,), (1,)), ((), ()))


def dot_f32(lhs, rhs, dims=NATURAL):
    return lax.dot_general(lhs, rhs, dims, preferred_element_type=jnp.float32)


def rope_tables(positions):
    exponents = jnp.arange(0, HEAD_DIM, 2, dtype=jnp.float32) / HEAD_DIM
    angles = jnp.power(ROPE_THETA, -exponents)[:, None] * positions.astype(jnp.float32)[None, :]
    return jnp.cos(angles), jnp.sin(angles)


def rotate_rows(t_f32, cos_t, sin_t):
    lead_half, tail_half = t_f32[:HEAD_DIM // 2], t_f32[HEAD_DIM // 2:]
    return jnp.concatenate([lead_half * cos_t - tail_half * sin_t, tail_half * cos_t + lead_half * sin_t], axis=0).astype(jnp.bfloat16)


def norm_forward(x_f32, norm_gain):
    inv_rms = lax.rsqrt(jnp.mean(x_f32 * x_f32, axis=-1, keepdims=True) + NORM_EPS)
    x_hat = x_f32 * inv_rms
    return (x_hat * norm_gain).astype(jnp.bfloat16), x_hat, inv_rms


def norm_backward(d_hidden, x_hat, inv_rms, norm_gain):
    d_f32 = d_hidden.astype(jnp.float32)
    d_gain = jnp.sum(d_f32 * x_hat, axis=0)
    scaled = d_f32 * norm_gain
    d_input = inv_rms * (scaled - x_hat * jnp.mean(scaled * x_hat, axis=-1, keepdims=True))
    return d_input, d_gain


def slot_of(where_ref, z, c):
    return 2 * lax.rem(where_ref[0] - z + Z_SIZE, Z_SIZE) + (where_ref[2] ^ c)


def slot_of_other(where_ref, z, c):
    return 2 * lax.rem(where_ref[0] - z + Z_SIZE, Z_SIZE) + (1 - (where_ref[2] ^ c))


def block_token(where_ref, b, bq):
    return pl.multiple_of((b // 2) * (4 * bq) + where_ref[1] * (2 * bq) + (b % 2) * bq, bq)


def key_range(pos_ref, start, bq, bk):
    lo_first, lo_last = start - pos_ref[start], start + bq - 1 - pos_ref[start + bq - 1]
    return lo_first // bk, (start + bq - 1) // bk + 1, (lo_last + bk - 1) // bk, (start + 1) // bk


def tile_lanes(row, heads):
    return jnp.concatenate([row] * heads, axis=1)


def row_bounds(lo_ref, start, bq, heads):
    tok = start + lax.broadcasted_iota(jnp.int32, (1, bq), 1)
    return tile_lanes(tok, heads), tile_lanes(lo_ref[:, pl.ds(start, bq)], heads)


def keep_mask(key_start, bk, t_row, lo_row):
    key_idx = key_start + lax.broadcasted_iota(jnp.int32, (bk, t_row.shape[1]), 0)
    return (key_idx <= t_row) & (key_idx >= lo_row)


def head_columns(block, h):
    return block[:, h * HEAD_DIM:(h + 1) * HEAD_DIM]


def rotated_queries(q_blk, cos_ref, sin_ref, start, bq, heads):
    cos_t, sin_t = cos_ref[:, pl.ds(start, bq)], sin_ref[:, pl.ds(start, bq)]
    return [rotate_rows(head_columns(q_blk, h).T.astype(jnp.float32), cos_t, sin_t) for h in range(heads)]


def visit_keys(bounds, step):
    first, end, inner_first, inner_end = bounds

    def visit(j, carry):
        inner = (j >= inner_first) & (j < inner_end)

        @pl.when(inner)
        def _():
            step(j, False)

        @pl.when(jnp.logical_not(inner))
        def _():
            step(j, True)

        return carry

    lax.fori_loop(first, end, visit, 0)


def for_key_blocks(where_ref, mine_ref, theirs_ref, count, bq, store):
    def visit(n, carry):
        z, y, c = n // 4, (n // 2) % 2, n % 2
        block = jnp.where(y == where_ref[1], mine_ref[slot_of(where_ref, z, c)], theirs_ref[slot_of_other(where_ref, z, c)])
        store(pl.ds(pl.multiple_of(n * bq, bq), bq), block)
        return carry

    lax.fori_loop(0, count, visit, 0)


def fwd_kernel(heads, bk, where_ref, pos_ref, q_ref, kv_ref, kv_other_ref, cos_ref, sin_ref, lo_ref, o_ref, lse_ref, k_s, vt_s, qt_s, m_s, l_s, acc_s):
    b = pl.program_id(0)
    bq = q_ref.shape[1]
    seq = k_s.shape[0]

    @pl.when(b == 0)
    def _():
        def store(rows, block):
            k_s[rows, :] = rotate_rows(block[:, :HEAD_DIM].T.astype(jnp.float32), cos_ref[:, rows], sin_ref[:, rows]).T
            vt_s[:, rows] = block[:, HEAD_DIM:].T

        for_key_blocks(where_ref, kv_ref, kv_other_ref, seq // bq, bq, store)

    start = block_token(where_ref, b, bq)
    t_row, lo_row = row_bounds(lo_ref, start, bq, heads)
    q_blk = q_ref[0]
    qt_s[...] = jnp.concatenate(rotated_queries(q_blk, cos_ref, sin_ref, start, bq, heads), axis=1)
    m_s[...] = jnp.full_like(m_s, MASKED)
    l_s[...] = jnp.zeros_like(l_s)
    acc_s[...] = jnp.zeros_like(acc_s)

    def step(j, masked):
        key_start = pl.multiple_of(j * bk, bk)
        keys = pl.ds(key_start, bk)
        scores = dot_f32(k_s[keys, :], qt_s[...])
        if masked:
            scores = jnp.where(keep_mask(key_start, bk, t_row, lo_row), scores, MASKED)
        m_old = m_s[...]
        m_new = jnp.maximum(m_old, jnp.max(scores, axis=0, keepdims=True))
        probs = jnp.exp2(scores * SCALE_LOG2E - m_new * SCALE_LOG2E)
        alpha = jnp.exp2((m_old - m_new) * SCALE_LOG2E)
        m_s[...] = m_new
        l_s[...] = l_s[...] * alpha + jnp.sum(probs, axis=0, keepdims=True)
        acc_s[...] = acc_s[...] * alpha + dot_f32(vt_s[:, keys], probs.astype(jnp.bfloat16))

    visit_keys(key_range(pos_ref, start, bq, bk), step)
    out_t = (acc_s[...] / l_s[...]).astype(jnp.bfloat16)
    for h in range(heads):
        o_ref[0, :, h * HEAD_DIM:(h + 1) * HEAD_DIM] = out_t[:, h * bq:(h + 1) * bq].T
    lse_ref[0] = m_s[...] * SCALE_LOG2E + jnp.log2(l_s[...])


def bwd_block(where_ref, step, slots):
    s = slots[0] + (slots[1] - slots[0]) * (step // 2)
    return lax.rem(where_ref[0] - s + Z_SIZE, Z_SIZE), where_ref[2] ^ (step % 2)


def bwd_kernel(heads, bk, slots, where_ref, pos_ref, q_ref, do_ref, o_ref, kv_ref, kv_other_ref, cos_ref, sin_ref, lo_ref, lse_ref, *refs):
    first = slots[0] == 0
    if first:
        dq_ref, part_ref, k_s, kt_s, v_s, q_s, qt_s, do_s, dot_s, dqt_s, acc_s = refs
    else:
        part_ref, dq_ref, mine_ref, send_ref, k_s, kt_s, v_s, q_s, qt_s, do_s, dot_s, dqt_s, acc_s = refs
    step_idx = pl.program_id(0)
    z_blk, c_blk = bwd_block(where_ref, step_idx, slots)
    b = 2 * z_blk + c_blk
    bq = q_ref.shape[1]
    seq = k_s.shape[0]

    @pl.when(step_idx == 0)
    def _():
        def store(rows, block):
            acc_s[rows, :] = jnp.zeros((bq, 2 * HEAD_DIM), jnp.float32) if first else part_ref[rows, :]
            k_rot_t = rotate_rows(block[:, :HEAD_DIM].T.astype(jnp.float32), cos_ref[:, rows], sin_ref[:, rows])
            kt_s[:, rows] = k_rot_t
            k_s[rows, :] = k_rot_t.T
            v_s[rows, :] = block[:, HEAD_DIM:]

        for_key_blocks(where_ref, kv_ref, kv_other_ref, seq // bq, bq, store)

    start = block_token(where_ref, b, bq)
    t_row, lo_row = row_bounds(lo_ref, start, bq, heads)
    q_blk, do_blk, o_blk = q_ref[0], do_ref[0], o_ref[0]
    deltas = []
    for h, q_rot_t in enumerate(rotated_queries(q_blk, cos_ref, sin_ref, start, bq, heads)):
        lanes = slice(h * bq, (h + 1) * bq)
        qt_s[:, lanes] = q_rot_t
        q_s[lanes, :] = q_rot_t.T
        do_head = head_columns(do_blk, h)
        do_s[lanes, :] = do_head
        do_t = do_head.T
        dot_s[:, lanes] = do_t
        deltas.append(jnp.sum(do_t.astype(jnp.float32) * head_columns(o_blk, h).T.astype(jnp.float32), axis=0, keepdims=True))
    delta = jnp.concatenate(deltas, axis=1)
    lse = lse_ref[0]
    dqt_s[...] = jnp.zeros_like(dqt_s)

    def step(j, masked):
        key_start = pl.multiple_of(j * bk, bk)
        keys = pl.ds(key_start, bk)
        scores = dot_f32(k_s[keys, :], qt_s[...])
        probs = jnp.exp2(scores * SCALE_LOG2E - lse)
        if masked:
            probs = jnp.where(keep_mask(key_start, bk, t_row, lo_row), probs, 0.0)
        d_probs = dot_f32(v_s[keys, :], dot_s[...])
        d_scores = (probs * (d_probs - delta)).astype(jnp.bfloat16)
        acc_s[keys, HEAD_DIM:] += dot_f32(probs.astype(jnp.bfloat16), do_s[...])
        acc_s[keys, :HEAD_DIM] += dot_f32(d_scores, q_s[...]) * SCORE_SCALE
        dqt_s[...] += dot_f32(kt_s[:, keys], d_scores)

    visit_keys(key_range(pos_ref, start, bq, bk), step)
    cos_t, sin_t = cos_ref[:, pl.ds(start, bq)], sin_ref[:, pl.ds(start, bq)]
    for h in range(heads):
        dq_rot_t = (dqt_s[:, h * bq:(h + 1) * bq] * SCORE_SCALE).astype(jnp.bfloat16).astype(jnp.float32)
        dq_ref[0, :, h * HEAD_DIM:(h + 1) * HEAD_DIM] = rotate_rows(dq_rot_t, cos_t, -sin_t).T

    @pl.when(step_idx == pl.num_programs(0) - 1)
    def _():
        if first:
            part_ref[...] = acc_s[...]
            return

        def hand_over(y, mine):
            for z in range(Z_SIZE):
                for c in range(CORE_SIZE):
                    rows = ((z * 2 + y) * 2 + c) * bq
                    e = where_ref[2] ^ c
                    if mine:
                        mine_ref[z, e] = acc_s[rows:rows + bq, :]
                    else:
                        send_ref[z, 1 - e] = acc_s[rows:rows + bq, :]

        for y in range(Y_SIZE):
            pl.when(where_ref[1] == y)(functools.partial(hand_over, y, True))
            pl.when(where_ref[1] != y)(functools.partial(hand_over, y, False))


def token_grads_kernel(count, *refs):
    blocks, lhs_ref, out_refs, lhs_t = refs[:count], refs[count], refs[count + 1:-1], refs[-1]
    rows = lhs_ref.shape[1]

    @pl.when(pl.program_id(0) == 0)
    def _():
        for n in range(count):
            lhs_t[:, n * rows:(n + 1) * rows] = lhs_ref[n].T

    total = sum(dot_f32(lhs_t[:, n * rows:(n + 1) * rows], blocks[n][...]) for n in range(count))
    start = 0
    for ref in out_refs:
        if ref.shape[0] == blocks[0].shape[1]:
            size = ref.shape[1]
            ref[...] = total[start:start + size, :].T.astype(ref.dtype)
        else:
            size = ref.shape[0]
            ref[...] = total[start:start + size, :].astype(ref.dtype)
        start += size


def token_grads(blocks, lhs, outs, tile=512):
    rows, model = blocks[0].shape
    width = lhs.shape[2]
    specs = [pl.BlockSpec((tile, shape[1]), lambda i: (i, 0)) if shape[0] == model else pl.BlockSpec((shape[0], tile), lambda i: (0, i)) for shape, _ in outs]
    return pl.pallas_call(
        functools.partial(token_grads_kernel, len(blocks)),
        out_shape=[jax.ShapeDtypeStruct(*out) for out in outs], grid=(model // tile,),
        in_specs=[pl.BlockSpec((rows, tile), lambda i: (0, i)) for _ in blocks] + [pl.BlockSpec(lhs.shape, lambda i: (0, 0, 0))], out_specs=specs,
        scratch_shapes=[pltpu.VMEM((width, len(blocks) * rows), jnp.bfloat16)],
        compiler_params=pltpu.CompilerParams(dimension_semantics=('arbitrary',), vmem_limit_bytes=48 << 20),
        cost_estimate=pl.CostEstimate(flops=2 * len(blocks) * rows * model * width, bytes_accessed=2 * len(blocks) * rows * model, transcendentals=0),
    )(*blocks, lhs)


def finish_kernel(where_ref, mine_ref, other_ref, cos_ref, sin_ref, out_ref):
    for z in range(Z_SIZE):
        slot = lax.rem(where_ref[0] - z + Z_SIZE, Z_SIZE)
        for e in range(CORE_SIZE):
            total = mine_ref[z, e] + other_ref[z, e]
            dk = total[:, :HEAD_DIM].astype(jnp.bfloat16).astype(jnp.float32)
            out_ref[slot, e, :, :HEAD_DIM] = (dk * cos_ref[z, e] + pltpu.roll(dk, HEAD_DIM // 2, 1) * sin_ref[z, e]).astype(jnp.bfloat16)
            out_ref[slot, e, :, HEAD_DIM:] = total[:, HEAD_DIM:].astype(jnp.bfloat16)


def finish_key_grads(where, *operands):
    return pl.pallas_call(
        finish_kernel, out_shape=jax.ShapeDtypeStruct(operands[0].shape, jnp.bfloat16),
        grid_spec=pltpu.PrefetchScalarGridSpec(num_scalar_prefetch=1, grid=(1,), in_specs=[full_spec(arr.shape) for arr in operands], out_specs=full_spec(operands[0].shape)),
        compiler_params=pltpu.CompilerParams(dimension_semantics=('arbitrary',), vmem_limit_bytes=32 << 20),
        cost_estimate=pl.CostEstimate(flops=1000000, bytes_accessed=8000000, transcendentals=0),
    )(where, *operands)


def full_spec(shape):
    return pl.BlockSpec(shape, lambda b, *_: (0,) * len(shape))


def slot_spec(bq, width, find):
    return pl.BlockSpec((1, bq, width), lambda b, where_ref, _: (find(where_ref, b // 2, b % 2), 0, 0))


def attend(where, positions, q_slots, kv_slots, kv_other, cos_t, sin_t, lo_all, bk):
    slots, bq, width = q_slots.shape
    seq = positions.shape[0]
    heads = width // HEAD_DIM
    lanes = heads * bq
    shared = (kv_slots, kv_other, cos_t, sin_t, lo_all)
    block = slot_spec(bq, width, slot_of)
    return pl.pallas_call(
        functools.partial(fwd_kernel, heads, bk),
        out_shape=(jax.ShapeDtypeStruct(q_slots.shape, jnp.bfloat16), jax.ShapeDtypeStruct((slots, 1, lanes), jnp.float32)),
        grid_spec=pltpu.PrefetchScalarGridSpec(
            num_scalar_prefetch=2, grid=(slots,), in_specs=[block] + [full_spec(arr.shape) for arr in shared],
            out_specs=(block, pl.BlockSpec((1, 1, lanes), lambda b, *_: (b, 0, 0))),
            scratch_shapes=[pltpu.VMEM((seq, HEAD_DIM), jnp.bfloat16), pltpu.VMEM((HEAD_DIM, seq), jnp.bfloat16), pltpu.VMEM((HEAD_DIM, lanes), jnp.bfloat16),
                            pltpu.VMEM((1, lanes), jnp.float32), pltpu.VMEM((1, lanes), jnp.float32), pltpu.VMEM((HEAD_DIM, lanes), jnp.float32)]),
        compiler_params=pltpu.CompilerParams(dimension_semantics=('arbitrary',), vmem_limit_bytes=48 << 20),
        cost_estimate=pl.CostEstimate(flops=4 * slots * bq * heads * seq * HEAD_DIM, bytes_accessed=4 * slots * bq * width + 8 * seq * HEAD_DIM, transcendentals=slots * bq * heads * seq // 2),
        name='attend_fwd',
    )(where, positions, q_slots, *shared)


def attend_backward(where, positions, q_slots, do_blocks, o_slots, kv_slots, kv_other, cos_t, sin_t, lo_all, lse, bk, slots, part=None):
    count, bq, width = do_blocks.shape
    seq = positions.shape[0]
    heads = width // HEAD_DIM
    lanes = heads * bq
    shared = (kv_slots, kv_other, cos_t, sin_t, lo_all)

    def slot_index(i, where_ref, _):
        return (2 * slots[0] + i % 2 + 2 * (slots[1] - slots[0]) * (i // 2), 0, 0)

    def lse_index(i, where_ref, _):
        z_blk, c_blk = bwd_block(where_ref, i, slots)
        return (2 * z_blk + c_blk, 0, 0)

    block = pl.BlockSpec((1, bq, width), slot_index)
    local = pl.BlockSpec((1, bq, width), lambda i, *_: (i, 0, 0))
    operands = [q_slots, do_blocks, o_slots, *shared, lse]
    in_specs = [block, local, block] + [full_spec(arr.shape) for arr in shared] + [pl.BlockSpec((1, 1, lanes), lse_index)]
    part_shape, final_shape = (seq, 2 * HEAD_DIM), (Z_SIZE, CORE_SIZE, bq, 2 * HEAD_DIM)
    grads = [part_shape] if part is None else [final_shape] * 2
    if part is not None:
        operands.append(part)
        in_specs.append(full_spec(part_shape))
    work = count * bq * heads * seq * HEAD_DIM
    return pl.pallas_call(
        functools.partial(bwd_kernel, heads, bk, slots),
        out_shape=[jax.ShapeDtypeStruct(do_blocks.shape, jnp.bfloat16)] + [jax.ShapeDtypeStruct(shape, jnp.float32) for shape in grads],
        grid_spec=pltpu.PrefetchScalarGridSpec(
            num_scalar_prefetch=2, grid=(count,), in_specs=in_specs, out_specs=[local] + [full_spec(shape) for shape in grads],
            scratch_shapes=[pltpu.VMEM((seq, HEAD_DIM), jnp.bfloat16), pltpu.VMEM((HEAD_DIM, seq), jnp.bfloat16), pltpu.VMEM((seq, HEAD_DIM), jnp.bfloat16),
                            pltpu.VMEM((lanes, HEAD_DIM), jnp.bfloat16), pltpu.VMEM((HEAD_DIM, lanes), jnp.bfloat16),
                            pltpu.VMEM((lanes, HEAD_DIM), jnp.bfloat16), pltpu.VMEM((HEAD_DIM, lanes), jnp.bfloat16), pltpu.VMEM((HEAD_DIM, lanes), jnp.float32),
                            pltpu.VMEM((seq, 2 * HEAD_DIM), jnp.float32)]),
        compiler_params=pltpu.CompilerParams(dimension_semantics=('arbitrary',), vmem_limit_bytes=58 << 20),
        cost_estimate=pl.CostEstimate(flops=10 * work, bytes_accessed=8 * count * bq * width + 24 * seq * HEAD_DIM, transcendentals=work // (2 * HEAD_DIM)),
        name='attend_bwd',
    )(where, positions, *operands)


def solution(mesh):
    def member(z, y, c):
        return (z * Y_SIZE + y) * CORE_SIZE + c

    every = [(z, y, c) for z in range(Z_SIZE) for y in range(Y_SIZE) for c in range(CORE_SIZE)]

    def permuter(target, senders=range(Z_SIZE)):
        pairs = [(member(*src), member(*target(*src))) for src in every if src[0] in senders]
        return lambda val: lax.ppermute(val, 'tp', pairs)

    swap_core = permuter(lambda z, y, c: (z, y, 1 - c))
    swap_y = permuter(lambda z, y, c: (z, 1 - y, c))
    swap_same_head = permuter(lambda z, y, c: (z, 1 - y, 1 - c))
    ring = permuter(lambda z, y, c: ((z + 1) % Z_SIZE, y, c))
    ring_back = permuter(lambda z, y, c: ((z - 1) % Z_SIZE, y, c))
    hops = range(1, Z_SIZE)
    gather_right = {k: permuter(lambda z, y, c: (z + 1, y, c), range(k - 1, Z_SIZE - 1)) for k in hops}
    gather_left = {k: permuter(lambda z, y, c: (z - 1, y, c), range(1, Z_SIZE - k + 1)) for k in hops}
    scatter_right = {k: permuter(lambda z, y, c: (z + 1, y, c), range(0, k)) for k in hops}
    scatter_left = {k: permuter(lambda z, y, c: (z - 1, y, c), range(Z_SIZE - k, Z_SIZE)) for k in hops}
    z_swaps = {k: permuter(lambda z, y, c, k=k: (z ^ k, y, c)) for k in (1, 2)}

    def after(val, *deps):
        return lax.optimization_barrier((val,) + deps)[0]

    def device_step(x_blk, dy_blk, pos_all, norm_gain, wq_loc, wk_all, wv_all, wo_loc):
        seq_len = pos_all.shape[0]
        bq = seq_len // (Z_SIZE * Y_SIZE * CORE_SIZE)
        bk = 2 * bq
        model = x_blk.shape[1]
        idx = lax.axis_index('tp')
        z_idx, y_idx, c_idx = idx // (Y_SIZE * CORE_SIZE), (idx // CORE_SIZE) % Y_SIZE, idx % CORE_SIZE
        where = jnp.stack([z_idx, y_idx, c_idx])
        on_core0 = c_idx == 0
        pair = wq_loc.shape[1]
        kv_own = Y_SIZE * z_idx + (y_idx ^ c_idx)

        def select(first, second):
            return jnp.where(on_core0, first, second)

        def flip_core(arr):
            return arr[:, ::-1]

        def slots(arrs):
            return jnp.concatenate([arr[None] for arr in arrs], axis=0)

        def interleave(own, partner):
            return [blk for both in zip(own, partner) for blk in both]

        x_f32 = x_blk.astype(jnp.float32)
        hidden, x_hat, inv_rms = norm_forward(x_f32, norm_gain)

        h_own = [hidden]
        for s in hops:
            h_own.append(ring(h_own[-1]))
        h_pair = []
        for blk in h_own:
            h_pair.append(swap_core(blk))

        def slot_order(w_own, w_core, w_y, w_both):
            return [select(w_own, w_y), select(w_core, w_both), select(w_both, w_core), select(w_y, w_own)]

        wq_y = swap_y(wq_loc)
        wq_core = swap_core(wq_loc)
        q_cols = slot_order(wq_loc, wq_core, wq_y, swap_core(wq_y))
        wo_y = swap_y(wo_loc)
        o_rows = (wo_loc, swap_core(wo_loc), wo_y, swap_core(wo_y))

        def kv_columns(head):
            return [lax.dynamic_slice_in_dim(w, head * HEAD_DIM, HEAD_DIM, axis=1) for w in (wk_all, wv_all)]

        w_q = lax.optimization_barrier(jnp.concatenate(q_cols, axis=1))
        w_kv = lax.optimization_barrier(jnp.concatenate(kv_columns(kv_own) + kv_columns(kv_own ^ 1), axis=1))
        kv_next = lax.rem(kv_own + Y_SIZE, Y_SIZE * Z_SIZE)
        w_kv_next = lax.optimization_barrier(jnp.concatenate(kv_columns(kv_next) + kv_columns(kv_next ^ 1), axis=1))
        w_own = jnp.concatenate([w_q[:, :2 * pair], w_kv[:, :2 * HEAD_DIM]], axis=1)
        w_mix = jnp.concatenate(slot_order(*o_rows), axis=0)
        lo_all = (lax.iota(jnp.int32, seq_len) - pos_all)[None, :]
        cos_t, sin_t = rope_tables(pos_all)

        def my_tables(lead, tail):
            parts = jnp.concatenate([lead.T, tail.T], axis=1).reshape(Z_SIZE, Y_SIZE, CORE_SIZE, bq, HEAD_DIM)
            parts = lax.dynamic_index_in_dim(parts, y_idx, 1, keepdims=False)
            return select(parts, flip_core(parts))

        cos_my, sin_my = my_tables(cos_t, cos_t), my_tables(sin_t, -sin_t)

        qkv = []
        for s in range(Z_SIZE):
            qkv += [dot_f32(blk, w_own).astype(jnp.bfloat16) for blk in (h_own[s], h_pair[s])]
        kv_blocks = [blk[:, 2 * pair:] for blk in qkv]
        early = SLOTS - CORE_SIZE
        kv_other_early = swap_same_head(slots(kv_blocks[:early]))
        kv_other_late = swap_same_head(slots(kv_blocks[early:]))
        kv_other = jnp.concatenate([kv_other_early, kv_other_late], axis=0)
        q_slots, kv_slots = slots([blk[:, :2 * pair] for blk in qkv]), slots(kv_blocks)

        g_own = []
        for s, blk in enumerate(h_own):
            g_own.append(swap_y(after(blk, kv_other_late) if s else blk))

        right, left = {0: after(dy_blk, h_own[-1])}, {}
        left[0] = right[0]
        for k in hops:
            right[k] = gather_right[k](right[k - 1])
            left[k] = gather_left[k](left[k - 1])
            right[k], left[k] = lax.optimization_barrier((right[k], left[k]))
        dy_own = [dy_blk] + [jnp.where(z_idx >= s, right[s], left[Z_SIZE - s]) for s in hops]
        dy_pair = []
        for blk in dy_own:
            dy_pair.append(swap_core(blk))
        dy_slots = interleave([dy_own[s] for s in DO_ORDER], [dy_pair[s] for s in DO_ORDER])

        o_slots, lse = attend(where, pos_all, q_slots, kv_slots, kv_other, cos_t, sin_t, lo_all, bk)
        by_line = (Z_SIZE, CORE_SIZE, bq, -1)
        o_lines = o_slots.reshape(by_line)
        o_partner = swap_core(o_slots).reshape(by_line)
        o_mine = jnp.concatenate([o_lines[:, 0], o_partner[:, 1]], axis=-1)

        def pair_sides(own, partner):
            first, last = own[..., :pair], partner[..., pair:2 * pair]
            return select(first, last), select(last, first)

        def by_block(arr):
            return arr.reshape((SLOTS,) + arr.shape[2:])

        def dy_order(arr):
            return jnp.concatenate([arr[s:s + 1] for s in DO_ORDER], axis=0)

        o_sides = lax.optimization_barrier(by_block(jnp.concatenate(pair_sides(dy_order(o_lines), dy_order(flip_core(o_partner))), axis=-1)))
        mix_part = []
        for s in range(Z_SIZE):
            mix_part.append(lax.optimization_barrier(dot_f32(o_mine[s], w_mix).astype(jnp.bfloat16)))

        def plus(*parts):
            return sum(part.astype(jnp.float32) for part in parts)

        sum_right, sum_left = mix_part[1], mix_part[Z_SIZE - 1]
        for k in hops:
            if k > 1:
                sum_right, sum_left = lax.optimization_barrier((sum_right, sum_left))
                sum_right = plus(mix_part[k], sum_right).astype(jnp.bfloat16)
                sum_left = plus(mix_part[Z_SIZE - k], sum_left).astype(jnp.bfloat16)
            sum_right = scatter_right[k](sum_right)
            sum_left = scatter_left[k](sum_left)
        result = (x_f32 + plus(mix_part[0], sum_right, sum_left)).astype(jnp.bfloat16)

        d_o = {}
        for s in DO_ORDER:
            d_o[s] = [dot_f32(blk, w_mix[:2 * pair], COLS_OF_BOTH).astype(jnp.bfloat16) for blk in (dy_own[s], dy_pair[s])]
        shared = (o_slots, kv_slots, kv_other, cos_t, sin_t, lo_all, lse, bk)
        dq_early, dkv_part = attend_backward(where, pos_all, q_slots, slots(d_o[EARLY[0]] + d_o[EARLY[1]]), *shared, EARLY)
        dq_early_partner = swap_core(dq_early)
        dq_late, dkv_mine, dkv_send = attend_backward(where, pos_all, q_slots, slots(d_o[LATE[0]] + d_o[LATE[1]]), *shared, LATE, dkv_part)
        dkv_theirs = swap_same_head(dkv_send)
        dq_late_partner = swap_core(dq_late)
        dq_own, dq_partner = {}, {}
        for group, own, partner in ((EARLY, dq_early, dq_early_partner), (LATE, dq_late, dq_late_partner)):
            for n, s in enumerate(group):
                dq_own[s], dq_partner[s] = own[2 * n:2 * n + 2], partner[2 * n:2 * n + 2][::-1]
        dq_rows = {s: jnp.concatenate([dq_own[s][0], dq_partner[s][0]], axis=-1) for s in DO_ORDER}
        halves = [slice(0, model // 2), slice(model // 2, model)]
        dh_sum = []
        for n, cols in enumerate(halves):
            dh_sum.append(dot_f32(dq_rows[1], w_q[cols], COLS_OF_BOTH).astype(jnp.bfloat16))
            dh_sum[n] = ring(dh_sum[n])

        dkv_lines = finish_key_grads(where, dkv_mine, dkv_theirs, cos_my, sin_my)
        dkv_partner = flip_core(swap_core(dkv_lines))
        dkv_rows = jnp.concatenate([dkv_lines[:, 0], dkv_partner[:, 0]], axis=-1)
        dkv_next = ring_back(dkv_rows[1])

        def dh_part(s, cols):
            return dot_f32(dq_rows[s], w_q[cols], COLS_OF_BOTH) + dot_f32(dkv_rows[s], w_kv[cols], COLS_OF_BOTH)

        for s in hops[1:]:
            for n, cols in enumerate(halves):
                dh_sum[n] = (dh_part(s, cols) + dh_sum[n].astype(jnp.float32)).astype(jnp.bfloat16)
                if s == hops[-1] and n == 0:
                    dh_sum[n], result = lax.optimization_barrier((dh_sum[n], result))
                dh_sum[n] = ring(dh_sum[n])
        dh_own = lax.optimization_barrier([dh_part(0, cols) + dot_f32(dkv_next, w_kv_next[cols], COLS_OF_BOTH) for cols in halves])
        dh_rows = jnp.concatenate([(own + part.astype(jnp.float32)).astype(jnp.bfloat16) for own, part in zip(dh_own, dh_sum)], axis=1)

        g_pair = [swap_core(blk) for blk in lax.optimization_barrier((*g_own, dq_late))[:Z_SIZE]]
        sides = [pair_sides(dq_own[s], dq_partner[s]) for s in DO_ORDER]
        q_keep, q_send = (jnp.concatenate([side[n][None] for side in sides], axis=0) for n in range(2))
        kv_keep = dy_order(select(dkv_lines[..., :HEAD_DIM], dkv_partner[..., HEAD_DIM:]))
        kv_send = dy_order(select(dkv_partner[..., :HEAD_DIM], dkv_lines[..., HEAD_DIM:]))
        d_keep = by_block(jnp.concatenate([q_keep, kv_keep], axis=-1))
        d_send = by_block(jnp.concatenate([q_send, kv_send], axis=-1))
        d_theirs = swap_y(d_send)

        dwo_keep, dwo_send = token_grads(dy_slots, o_sides, [((pair, model), jnp.float32)] * 2)
        theirs_first = swap_y(dwo_send[:, halves[0]])
        theirs_last = swap_y(dwo_send[:, halves[1]])
        d_wo = (dwo_keep + jnp.concatenate([theirs_first, theirs_last], axis=1)).astype(jnp.bfloat16)

        d_wq, kv_mine_sum = token_grads([blks[s] for mine, theirs in ((h_own, h_pair), (g_own, g_pair)) for s in DO_ORDER for blks in (mine, theirs)], jnp.concatenate([d_keep, d_theirs], axis=0),
                                        [((model, pair), jnp.bfloat16), ((model, HEAD_DIM), jnp.float32)])
        kv_other_sum = swap_core(kv_mine_sum)
        d_wk = select(kv_mine_sum, kv_other_sum)
        d_wv = select(kv_other_sum, kv_mine_sum)

        d_input, dg_part = norm_backward(dh_rows, x_hat, inv_rms, norm_gain)
        grad_x = (dy_blk.astype(jnp.float32) + d_input).astype(jnp.bfloat16)
        for swap in (swap_core, swap_y, z_swaps[1], z_swaps[2]):
            dg_part = dg_part + swap(dg_part)
        return result, grad_x, d_wq, d_wk, d_wv, d_wo, dg_part

    specs_in = (P(('dp', 'tp'), None), P(('dp', 'tp'), None), P('dp'), P(), P(None, 'tp'), P(), P(), P('tp', None))
    specs_out = (P(('dp', 'tp'), None), P(('dp', 'tp'), None), P('dp', 'tp'), P('dp', 'tp'), P('dp', 'tp'), P(('dp', 'tp'), None), P('dp'))
    return jax.shard_map(device_step, mesh=mesh, in_specs=specs_in, out_specs=specs_out, check_vma=False)
```

```python
import functools
import jax
import jax.numpy as jnp
from jax import lax
from jax.experimental import pallas as pl
from jax.experimental.pallas import tpu as pltpu
from jax.sharding import PartitionSpec as P

HEAD_DIM = 128
SCORE_SCALE = HEAD_DIM ** -0.5
SCALE_LOG2E = SCORE_SCALE * 1.4426950408889634
ROPE_THETA = 1000000.0
NORM_EPS = 1e-05
MASKED = -1e30
Z_SIZE = 4
Y_SIZE = 2
CORE_SIZE = 2
SLOTS = Z_SIZE * CORE_SIZE
NATURAL = (((1,), (0,)), ((), ()))
COLS_OF_BOTH = (((1,), (1,)), ((), ()))


def dot_f32(lhs, rhs, dims=NATURAL):
    return lax.dot_general(lhs, rhs, dims, preferred_element_type=jnp.float32)


def rope_tables(positions):
    exponents = jnp.arange(0, HEAD_DIM, 2, dtype=jnp.float32) / HEAD_DIM
    angles = jnp.power(ROPE_THETA, -exponents)[:, None] * positions.astype(jnp.float32)[None, :]
    return jnp.cos(angles), jnp.sin(angles)


def rotate_rows(t_f32, cos_t, sin_t):
    lead_half, tail_half = t_f32[:HEAD_DIM // 2], t_f32[HEAD_DIM // 2:]
    return jnp.concatenate([lead_half * cos_t - tail_half * sin_t, tail_half * cos_t + lead_half * sin_t], axis=0).astype(jnp.bfloat16)


def norm_forward(x_f32, norm_gain):
    inv_rms = lax.rsqrt(jnp.mean(x_f32 * x_f32, axis=-1, keepdims=True) + NORM_EPS)
    x_hat = x_f32 * inv_rms
    return (x_hat * norm_gain).astype(jnp.bfloat16), x_hat, inv_rms


def norm_backward(d_hidden, x_hat, inv_rms, norm_gain):
    d_f32 = d_hidden.astype(jnp.float32)
    d_gain = jnp.sum(d_f32 * x_hat, axis=0)
    scaled = d_f32 * norm_gain
    d_input = inv_rms * (scaled - x_hat * jnp.mean(scaled * x_hat, axis=-1, keepdims=True))
    return d_input, d_gain


def slot_of(where_ref, z, c):
    return 2 * lax.rem(where_ref[0] - z + Z_SIZE, Z_SIZE) + (where_ref[2] ^ c)


def slot_of_other(where_ref, z, c):
    return 2 * lax.rem(where_ref[0] - z + Z_SIZE, Z_SIZE) + (1 - (where_ref[2] ^ c))


def block_token(where_ref, b, bq):
    return pl.multiple_of((b // 2) * (4 * bq) + where_ref[1] * (2 * bq) + (b % 2) * bq, bq)


def key_range(pos_ref, start, bq, bk):
    lo_first, lo_last = start - pos_ref[start], start + bq - 1 - pos_ref[start + bq - 1]
    return lo_first // bk, (start + bq - 1) // bk + 1, (lo_last + bk - 1) // bk, (start + 1) // bk


def tile_lanes(row, heads):
    return jnp.concatenate([row] * heads, axis=1)


def row_bounds(lo_ref, start, bq, heads):
    tok = start + lax.broadcasted_iota(jnp.int32, (1, bq), 1)
    return tile_lanes(tok, heads), tile_lanes(lo_ref[:, pl.ds(start, bq)], heads)


def keep_mask(key_start, bk, t_row, lo_row):
    key_idx = key_start + lax.broadcasted_iota(jnp.int32, (bk, t_row.shape[1]), 0)
    return (key_idx <= t_row) & (key_idx >= lo_row)


def head_columns(block, h):
    return block[:, h * HEAD_DIM:(h + 1) * HEAD_DIM]


def rotated_queries(q_blk, cos_ref, sin_ref, start, bq, heads):
    cos_t, sin_t = cos_ref[:, pl.ds(start, bq)], sin_ref[:, pl.ds(start, bq)]
    return [rotate_rows(head_columns(q_blk, h).T.astype(jnp.float32), cos_t, sin_t) for h in range(heads)]


def visit_keys(bounds, step):
    first, end, inner_first, inner_end = bounds

    def visit(j, carry):
        inner = (j >= inner_first) & (j < inner_end)

        @pl.when(inner)
        def _():
            step(j, False)

        @pl.when(jnp.logical_not(inner))
        def _():
            step(j, True)

        return carry

    lax.fori_loop(first, end, visit, 0)


def for_key_blocks(where_ref, mine_ref, theirs_ref, count, bq, store):
    def visit(n, carry):
        z, y, c = n // 4, (n // 2) % 2, n % 2
        block = jnp.where(y == where_ref[1], mine_ref[slot_of(where_ref, z, c)], theirs_ref[slot_of_other(where_ref, z, c)])
        store(pl.ds(pl.multiple_of(n * bq, bq), bq), block)
        return carry

    lax.fori_loop(0, count, visit, 0)


def fwd_kernel(heads, bk, where_ref, pos_ref, q_ref, kv_ref, kv_other_ref, cos_ref, sin_ref, lo_ref, o_ref, lse_ref, k_s, vt_s, qt_s, m_s, l_s, acc_s):
    b = pl.program_id(0)
    bq = q_ref.shape[1]
    seq = k_s.shape[0]

    @pl.when(b == 0)
    def _():
        def store(rows, block):
            k_s[rows, :] = rotate_rows(block[:, :HEAD_DIM].T.astype(jnp.float32), cos_ref[:, rows], sin_ref[:, rows]).T
            vt_s[:, rows] = block[:, HEAD_DIM:].T

        for_key_blocks(where_ref, kv_ref, kv_other_ref, seq // bq, bq, store)

    start = block_token(where_ref, b, bq)
    t_row, lo_row = row_bounds(lo_ref, start, bq, heads)
    q_blk = q_ref[0]
    qt_s[...] = jnp.concatenate(rotated_queries(q_blk, cos_ref, sin_ref, start, bq, heads), axis=1)
    m_s[...] = jnp.full_like(m_s, MASKED)
    l_s[...] = jnp.zeros_like(l_s)
    acc_s[...] = jnp.zeros_like(acc_s)

    def step(j, masked):
        key_start = pl.multiple_of(j * bk, bk)
        keys = pl.ds(key_start, bk)
        scores = dot_f32(k_s[keys, :], qt_s[...])
        if masked:
            scores = jnp.where(keep_mask(key_start, bk, t_row, lo_row), scores, MASKED)
        m_old = m_s[...]
        m_new = jnp.maximum(m_old, jnp.max(scores, axis=0, keepdims=True))
        probs = jnp.exp2(scores * SCALE_LOG2E - m_new * SCALE_LOG2E)
        alpha = jnp.exp2((m_old - m_new) * SCALE_LOG2E)
        m_s[...] = m_new
        l_s[...] = l_s[...] * alpha + jnp.sum(probs, axis=0, keepdims=True)
        acc_s[...] = acc_s[...] * alpha + dot_f32(vt_s[:, keys], probs.astype(jnp.bfloat16))

    visit_keys(key_range(pos_ref, start, bq, bk), step)
    out_t = (acc_s[...] / l_s[...]).astype(jnp.bfloat16)
    for h in range(heads):
        o_ref[0, :, h * HEAD_DIM:(h + 1) * HEAD_DIM] = out_t[:, h * bq:(h + 1) * bq].T
    lse_ref[0] = m_s[...] * SCALE_LOG2E + jnp.log2(l_s[...])


def early_slot(where_ref, step):
    n = step // 2
    return jnp.where(n == 1, where_ref[3], n)


def late_slot(where_ref, step):
    return where_ref[4]


def bwd_block(where_ref, step, find):
    return lax.rem(where_ref[0] - find(where_ref, step) + Z_SIZE, Z_SIZE), where_ref[2] ^ (step % 2)


def bwd_kernel(heads, bk, find, where_ref, pos_ref, q_ref, do_ref, o_ref, kv_ref, kv_other_ref, cos_ref, sin_ref, lo_ref, lse_ref, *refs):
    first = find is early_slot
    if first:
        dq_ref, part_ref, k_s, kt_s, v_s, q_s, qt_s, do_s, dot_s, dqt_s, acc_s = refs
    else:
        part_ref, dq_ref, mine_ref, send_ref, k_s, kt_s, v_s, q_s, qt_s, do_s, dot_s, dqt_s, acc_s = refs
    step_idx = pl.program_id(0)
    z_blk, c_blk = bwd_block(where_ref, step_idx, find)
    b = 2 * z_blk + c_blk
    bq = q_ref.shape[1]
    seq = k_s.shape[0]

    @pl.when(step_idx == 0)
    def _():
        def store(rows, block):
            acc_s[rows, :] = jnp.zeros((bq, 2 * HEAD_DIM), jnp.float32) if first else part_ref[rows, :]
            k_rot_t = rotate_rows(block[:, :HEAD_DIM].T.astype(jnp.float32), cos_ref[:, rows], sin_ref[:, rows])
            kt_s[:, rows] = k_rot_t
            k_s[rows, :] = k_rot_t.T
            v_s[rows, :] = block[:, HEAD_DIM:]

        for_key_blocks(where_ref, kv_ref, kv_other_ref, seq // bq, bq, store)

    start = block_token(where_ref, b, bq)
    t_row, lo_row = row_bounds(lo_ref, start, bq, heads)
    q_blk, do_blk, o_blk = q_ref[0], do_ref[0], o_ref[0]
    deltas = []
    for h, q_rot_t in enumerate(rotated_queries(q_blk, cos_ref, sin_ref, start, bq, heads)):
        lanes = slice(h * bq, (h + 1) * bq)
        qt_s[:, lanes] = q_rot_t
        q_s[lanes, :] = q_rot_t.T
        do_head = head_columns(do_blk, h)
        do_s[lanes, :] = do_head
        do_t = do_head.T
        dot_s[:, lanes] = do_t
        deltas.append(jnp.sum(do_t.astype(jnp.float32) * head_columns(o_blk, h).T.astype(jnp.float32), axis=0, keepdims=True))
    delta = jnp.concatenate(deltas, axis=1)
    lse = lse_ref[0]
    dqt_s[...] = jnp.zeros_like(dqt_s)

    def step(j, masked):
        key_start = pl.multiple_of(j * bk, bk)
        keys = pl.ds(key_start, bk)
        scores = dot_f32(k_s[keys, :], qt_s[...])
        probs = jnp.exp2(scores * SCALE_LOG2E - lse)
        if masked:
            probs = jnp.where(keep_mask(key_start, bk, t_row, lo_row), probs, 0.0)
        d_probs = dot_f32(v_s[keys, :], dot_s[...])
        d_scores = (probs * (d_probs - delta)).astype(jnp.bfloat16)
        acc_s[keys, HEAD_DIM:] += dot_f32(probs.astype(jnp.bfloat16), do_s[...])
        acc_s[keys, :HEAD_DIM] += dot_f32(d_scores, q_s[...]) * SCORE_SCALE
        dqt_s[...] += dot_f32(kt_s[:, keys], d_scores)

    visit_keys(key_range(pos_ref, start, bq, bk), step)
    cos_t, sin_t = cos_ref[:, pl.ds(start, bq)], sin_ref[:, pl.ds(start, bq)]
    for h in range(heads):
        dq_rot_t = (dqt_s[:, h * bq:(h + 1) * bq] * SCORE_SCALE).astype(jnp.bfloat16).astype(jnp.float32)
        dq_ref[0, :, h * HEAD_DIM:(h + 1) * HEAD_DIM] = rotate_rows(dq_rot_t, cos_t, -sin_t).T

    @pl.when(step_idx == pl.num_programs(0) - 1)
    def _():
        if first:
            part_ref[...] = acc_s[...]
            return

        def hand_over(y, mine):
            for z in range(Z_SIZE):
                for c in range(CORE_SIZE):
                    rows = ((z * 2 + y) * 2 + c) * bq
                    e = where_ref[2] ^ c
                    if mine:
                        mine_ref[z, e] = acc_s[rows:rows + bq, :]
                    else:
                        send_ref[z, 1 - e] = acc_s[rows:rows + bq, :]

        for y in range(Y_SIZE):
            pl.when(where_ref[1] == y)(functools.partial(hand_over, y, True))
            pl.when(where_ref[1] != y)(functools.partial(hand_over, y, False))


def token_grads_kernel(count, *refs):
    blocks, lhs_ref, out_refs, lhs_t = refs[:count], refs[count], refs[count + 1:-1], refs[-1]
    rows = lhs_ref.shape[1]

    @pl.when(pl.program_id(0) == 0)
    def _():
        for n in range(count):
            lhs_t[:, n * rows:(n + 1) * rows] = lhs_ref[n].T

    total = sum(dot_f32(lhs_t[:, n * rows:(n + 1) * rows], blocks[n][...]) for n in range(count))
    start = 0
    for ref in out_refs:
        if ref.shape[0] == blocks[0].shape[1]:
            size = ref.shape[1]
            ref[...] = total[start:start + size, :].T.astype(ref.dtype)
        else:
            size = ref.shape[0]
            ref[...] = total[start:start + size, :].astype(ref.dtype)
        start += size


def token_grads(blocks, lhs, outs, tile=512):
    rows, model = blocks[0].shape
    width = lhs.shape[2]
    specs = [pl.BlockSpec((tile, shape[1]), lambda i: (i, 0)) if shape[0] == model else pl.BlockSpec((shape[0], tile), lambda i: (0, i)) for shape, _ in outs]
    return pl.pallas_call(
        functools.partial(token_grads_kernel, len(blocks)),
        out_shape=[jax.ShapeDtypeStruct(*out) for out in outs], grid=(model // tile,),
        in_specs=[pl.BlockSpec((rows, tile), lambda i: (0, i)) for _ in blocks] + [pl.BlockSpec(lhs.shape, lambda i: (0, 0, 0))], out_specs=specs,
        scratch_shapes=[pltpu.VMEM((width, len(blocks) * rows), jnp.bfloat16)],
        compiler_params=pltpu.CompilerParams(dimension_semantics=('arbitrary',), vmem_limit_bytes=48 << 20),
        cost_estimate=pl.CostEstimate(flops=2 * len(blocks) * rows * model * width, bytes_accessed=2 * len(blocks) * rows * model, transcendentals=0),
    )(*blocks, lhs)


def pair_add_kernel(a_ref, b_ref, c_ref, d_ref, ab_ref, cd_ref):
    for left, right, out in ((a_ref, b_ref, ab_ref), (c_ref, d_ref, cd_ref)):
        out[...] = (left[...].astype(jnp.float32) + right[...].astype(jnp.float32)).astype(jnp.bfloat16)


def pair_add(*operands):
    rows, model = operands[0].shape
    tile = model // 4
    spec = pl.BlockSpec((rows, tile), lambda i: (0, i))
    return pl.pallas_call(
        pair_add_kernel, out_shape=[jax.ShapeDtypeStruct((rows, model), jnp.bfloat16)] * 2, grid=(model // tile,), in_specs=[spec] * 4, out_specs=[spec] * 2,
        compiler_params=pltpu.CompilerParams(dimension_semantics=('arbitrary',), vmem_limit_bytes=32 << 20),
        cost_estimate=pl.CostEstimate(flops=4 * rows * model, bytes_accessed=12 * rows * model, transcendentals=0),
    )(*operands)


def finish_kernel(where_ref, mine_ref, other_ref, cos_ref, sin_ref, out_ref):
    for z in range(Z_SIZE):
        slot = lax.rem(where_ref[0] - z + Z_SIZE, Z_SIZE)
        for e in range(CORE_SIZE):
            total = mine_ref[z, e] + other_ref[z, e]
            dk = total[:, :HEAD_DIM].astype(jnp.bfloat16).astype(jnp.float32)
            out_ref[slot, e, :, :HEAD_DIM] = (dk * cos_ref[z, e] + pltpu.roll(dk, HEAD_DIM // 2, 1) * sin_ref[z, e]).astype(jnp.bfloat16)
            out_ref[slot, e, :, HEAD_DIM:] = total[:, HEAD_DIM:].astype(jnp.bfloat16)


def finish_key_grads(where, *operands):
    return pl.pallas_call(
        finish_kernel, out_shape=jax.ShapeDtypeStruct(operands[0].shape, jnp.bfloat16),
        grid_spec=pltpu.PrefetchScalarGridSpec(num_scalar_prefetch=1, grid=(1,), in_specs=[full_spec(arr.shape) for arr in operands], out_specs=full_spec(operands[0].shape)),
        compiler_params=pltpu.CompilerParams(dimension_semantics=('arbitrary',), vmem_limit_bytes=32 << 20),
        cost_estimate=pl.CostEstimate(flops=1000000, bytes_accessed=8000000, transcendentals=0),
    )(where, *operands)


def full_spec(shape):
    return pl.BlockSpec(shape, lambda b, *_: (0,) * len(shape))


def slot_spec(bq, width, find):
    return pl.BlockSpec((1, bq, width), lambda b, where_ref, _: (find(where_ref, b // 2, b % 2), 0, 0))


def attend(where, positions, q_slots, kv_slots, kv_other, cos_t, sin_t, lo_all, bk):
    slots, bq, width = q_slots.shape
    seq = positions.shape[0]
    heads = width // HEAD_DIM
    lanes = heads * bq
    shared = (kv_slots, kv_other, cos_t, sin_t, lo_all)
    block = slot_spec(bq, width, slot_of)
    return pl.pallas_call(
        functools.partial(fwd_kernel, heads, bk),
        out_shape=(jax.ShapeDtypeStruct(q_slots.shape, jnp.bfloat16), jax.ShapeDtypeStruct((slots, 1, lanes), jnp.float32)),
        grid_spec=pltpu.PrefetchScalarGridSpec(
            num_scalar_prefetch=2, grid=(slots,), in_specs=[block] + [full_spec(arr.shape) for arr in shared],
            out_specs=(block, pl.BlockSpec((1, 1, lanes), lambda b, *_: (b, 0, 0))),
            scratch_shapes=[pltpu.VMEM((seq, HEAD_DIM), jnp.bfloat16), pltpu.VMEM((HEAD_DIM, seq), jnp.bfloat16), pltpu.VMEM((HEAD_DIM, lanes), jnp.bfloat16),
                            pltpu.VMEM((1, lanes), jnp.float32), pltpu.VMEM((1, lanes), jnp.float32), pltpu.VMEM((HEAD_DIM, lanes), jnp.float32)]),
        compiler_params=pltpu.CompilerParams(dimension_semantics=('arbitrary',), vmem_limit_bytes=48 << 20),
        cost_estimate=pl.CostEstimate(flops=4 * slots * bq * heads * seq * HEAD_DIM, bytes_accessed=4 * slots * bq * width + 8 * seq * HEAD_DIM, transcendentals=slots * bq * heads * seq // 2),
        name='attend_fwd',
    )(where, positions, q_slots, *shared)


def attend_backward(where, positions, q_slots, do_blocks, o_slots, kv_slots, kv_other, cos_t, sin_t, lo_all, lse, bk, find, part=None):
    count, bq, width = do_blocks.shape
    seq = positions.shape[0]
    heads = width // HEAD_DIM
    lanes = heads * bq
    shared = (kv_slots, kv_other, cos_t, sin_t, lo_all)

    def slot_index(i, where_ref, _):
        return (2 * find(where_ref, i) + i % 2, 0, 0)

    def lse_index(i, where_ref, _):
        z_blk, c_blk = bwd_block(where_ref, i, find)
        return (2 * z_blk + c_blk, 0, 0)

    block = pl.BlockSpec((1, bq, width), slot_index)
    local = pl.BlockSpec((1, bq, width), lambda i, *_: (i, 0, 0))
    operands = [q_slots, do_blocks, o_slots, *shared, lse]
    in_specs = [block, local, block] + [full_spec(arr.shape) for arr in shared] + [pl.BlockSpec((1, 1, lanes), lse_index)]
    part_shape, final_shape = (seq, 2 * HEAD_DIM), (Z_SIZE, CORE_SIZE, bq, 2 * HEAD_DIM)
    grads = [part_shape] if part is None else [final_shape] * 2
    if part is not None:
        operands.append(part)
        in_specs.append(full_spec(part_shape))
    work = count * bq * heads * seq * HEAD_DIM
    return pl.pallas_call(
        functools.partial(bwd_kernel, heads, bk, find),
        out_shape=[jax.ShapeDtypeStruct(do_blocks.shape, jnp.bfloat16)] + [jax.ShapeDtypeStruct(shape, jnp.float32) for shape in grads],
        grid_spec=pltpu.PrefetchScalarGridSpec(
            num_scalar_prefetch=2, grid=(count,), in_specs=in_specs, out_specs=[local] + [full_spec(shape) for shape in grads],
            scratch_shapes=[pltpu.VMEM((seq, HEAD_DIM), jnp.bfloat16), pltpu.VMEM((HEAD_DIM, seq), jnp.bfloat16), pltpu.VMEM((seq, HEAD_DIM), jnp.bfloat16),
                            pltpu.VMEM((lanes, HEAD_DIM), jnp.bfloat16), pltpu.VMEM((HEAD_DIM, lanes), jnp.bfloat16),
                            pltpu.VMEM((lanes, HEAD_DIM), jnp.bfloat16), pltpu.VMEM((HEAD_DIM, lanes), jnp.bfloat16), pltpu.VMEM((HEAD_DIM, lanes), jnp.float32),
                            pltpu.VMEM((seq, 2 * HEAD_DIM), jnp.float32)]),
        compiler_params=pltpu.CompilerParams(dimension_semantics=('arbitrary',), vmem_limit_bytes=58 << 20),
        cost_estimate=pl.CostEstimate(flops=10 * work, bytes_accessed=8 * count * bq * width + 24 * seq * HEAD_DIM, transcendentals=work // (2 * HEAD_DIM)),
        name='attend_bwd',
    )(where, positions, *operands)


def solution(mesh):
    def member(z, y, c):
        return (z * Y_SIZE + y) * CORE_SIZE + c

    every = [(z, y, c) for z in range(Z_SIZE) for y in range(Y_SIZE) for c in range(CORE_SIZE)]

    def permuter(target, senders=range(Z_SIZE)):
        pairs = [(member(*src), member(*target(*src))) for src in every if src[0] in senders]
        return lambda val: lax.ppermute(val, 'tp', pairs)

    swap_core = permuter(lambda z, y, c: (z, y, 1 - c))
    swap_y = permuter(lambda z, y, c: (z, 1 - y, c))
    swap_same_head = permuter(lambda z, y, c: (z, 1 - y, 1 - c))
    ring = permuter(lambda z, y, c: ((z + 1) % Z_SIZE, y, c))
    ring_back = permuter(lambda z, y, c: ((z - 1) % Z_SIZE, y, c))
    hops = range(1, Z_SIZE)
    gather_right = {k: permuter(lambda z, y, c: (z + 1, y, c), range(k - 1, Z_SIZE - 1)) for k in hops}
    gather_left = {k: permuter(lambda z, y, c: (z - 1, y, c), range(1, Z_SIZE - k + 1)) for k in hops}
    scatter_right = {k: permuter(lambda z, y, c: (z + 1, y, c), range(0, k)) for k in hops}
    scatter_left = {k: permuter(lambda z, y, c: (z - 1, y, c), range(Z_SIZE - k, Z_SIZE)) for k in hops}
    z_swaps = {k: permuter(lambda z, y, c, k=k: (z ^ k, y, c)) for k in hops}

    def after(val, *deps):
        return lax.optimization_barrier((val,) + deps)[0]

    def device_step(x_blk, dy_blk, pos_all, norm_gain, wq_loc, wk_all, wv_all, wo_loc):
        seq_len = pos_all.shape[0]
        bq = seq_len // (Z_SIZE * Y_SIZE * CORE_SIZE)
        bk = 2 * bq
        model = x_blk.shape[1]
        idx = lax.axis_index('tp')
        z_idx, y_idx, c_idx = idx // (Y_SIZE * CORE_SIZE), (idx // CORE_SIZE) % Y_SIZE, idx % CORE_SIZE
        low_z = z_idx < Z_SIZE // 2
        where = jnp.stack([z_idx, y_idx, c_idx, jnp.where(low_z, 3, 1), jnp.where(low_z, 1, 3)])
        on_core0 = c_idx == 0
        pair = wq_loc.shape[1]
        kv_own = Y_SIZE * z_idx + (y_idx ^ c_idx)

        def select(first, second):
            return jnp.where(on_core0, first, second)

        def flip_core(arr):
            return arr[:, ::-1]

        def slots(arrs):
            return jnp.concatenate([arr[None] for arr in arrs], axis=0)

        def interleave(own, partner):
            return [blk for both in zip(own, partner) for blk in both]

        x_f32 = x_blk.astype(jnp.float32)
        hidden, x_hat, inv_rms = norm_forward(x_f32, norm_gain)

        h_own = [hidden]
        for s in hops:
            h_own.append(ring(h_own[-1]))
        h_pair = []
        for blk in h_own:
            h_pair.append(swap_core(blk))

        def slot_order(w_own, w_core, w_y, w_both):
            return [select(w_own, w_y), select(w_core, w_both), select(w_both, w_core), select(w_y, w_own)]

        wq_y = swap_y(wq_loc)
        wq_core = swap_core(wq_loc)
        q_cols = slot_order(wq_loc, wq_core, wq_y, swap_core(wq_y))
        wo_y = swap_y(wo_loc)
        o_rows = (wo_loc, swap_core(wo_loc), wo_y, swap_core(wo_y))

        def kv_columns(head):
            return [lax.dynamic_slice_in_dim(w, head * HEAD_DIM, HEAD_DIM, axis=1) for w in (wk_all, wv_all)]

        w_q = lax.optimization_barrier(jnp.concatenate(q_cols, axis=1))
        w_kv = lax.optimization_barrier(jnp.concatenate(kv_columns(kv_own) + kv_columns(kv_own ^ 1), axis=1))
        kv_next = lax.rem(kv_own + Y_SIZE, Y_SIZE * Z_SIZE)
        w_kv_next = lax.optimization_barrier(jnp.concatenate(kv_columns(kv_next) + kv_columns(kv_next ^ 1), axis=1))
        w_own = jnp.concatenate([w_q[:, :2 * pair], w_kv[:, :2 * HEAD_DIM]], axis=1)
        w_mix = jnp.concatenate(slot_order(*o_rows), axis=0)
        lo_all = (lax.iota(jnp.int32, seq_len) - pos_all)[None, :]
        cos_t, sin_t = rope_tables(pos_all)

        def my_tables(lead, tail):
            parts = jnp.concatenate([lead.T, tail.T], axis=1).reshape(Z_SIZE, Y_SIZE, CORE_SIZE, bq, HEAD_DIM)
            parts = lax.dynamic_index_in_dim(parts, y_idx, 1, keepdims=False)
            return select(parts, flip_core(parts))

        cos_my, sin_my = my_tables(cos_t, cos_t), my_tables(sin_t, -sin_t)

        qkv = []
        for s in range(Z_SIZE):
            qkv += [dot_f32(blk, w_own).astype(jnp.bfloat16) for blk in (h_own[s], h_pair[s])]
        kv_blocks = [blk[:, 2 * pair:] for blk in qkv]
        early = SLOTS - CORE_SIZE
        kv_other_early = swap_same_head(slots(kv_blocks[:early]))
        kv_other_late = swap_same_head(slots(kv_blocks[early:]))
        kv_other = jnp.concatenate([kv_other_early, kv_other_late], axis=0)
        q_slots, kv_slots = slots([blk[:, :2 * pair] for blk in qkv]), slots(kv_blocks)

        g_own = []
        for s, blk in enumerate(h_own):
            g_own.append(swap_y(after(blk, kv_other_late) if s else blk))

        right, left = {0: after(dy_blk, h_own[-1])}, {}
        left[0] = right[0]
        for k in hops:
            right[k] = gather_right[k](right[k - 1])
            left[k] = gather_left[k](left[k - 1])
            right[k], left[k] = lax.optimization_barrier((right[k], left[k]))

        def apart(*vals):
            return lax.optimization_barrier(vals)

        def choose(pred, first, second):
            return jnp.where(*apart(pred, first, second))

        def last_block(z, left_near, left_far, right_near, right_far):
            return jnp.where(z == 0, left_far, jnp.where(z == 3, right_far, jnp.where(z == 1, right_near, left_near)))

        dy_own = [dy_blk, choose(low_z, left[1], right[1]), choose(low_z, left[2], right[2]), last_block(*apart(z_idx, left[1], left[3], right[1], right[3]))]
        dy_pair = []
        for blk in dy_own:
            dy_pair.append(swap_core(blk))
        dy_slots = interleave(dy_own, dy_pair)

        def arrival(blocks):
            return [blocks[0], jnp.where(low_z, blocks[3], blocks[1]), blocks[2], jnp.where(low_z, blocks[1], blocks[3])]

        o_slots, lse = attend(where, pos_all, q_slots, kv_slots, kv_other, cos_t, sin_t, lo_all, bk)
        by_line = (Z_SIZE, CORE_SIZE, bq, -1)
        o_lines = o_slots.reshape(by_line)
        o_partner = swap_core(o_slots).reshape(by_line)
        o_mine = jnp.concatenate([o_lines[:, 0], o_partner[:, 1]], axis=-1)

        def pair_sides(own, partner):
            first, last = own[..., :pair], partner[..., pair:2 * pair]
            return select(first, last), select(last, first)

        def by_block(arr):
            return arr.reshape((SLOTS,) + arr.shape[2:])

        o_sides = jnp.concatenate(pair_sides(o_lines, flip_core(o_partner)), axis=-1)
        o_sides = lax.optimization_barrier(by_block(jnp.concatenate([blk[None] for blk in arrival(o_sides)], axis=0)))
        mix_part = []
        for s in range(Z_SIZE):
            mix_part.append(lax.optimization_barrier(dot_f32(o_mine[s], w_mix).astype(jnp.bfloat16)))

        def plus(*parts):
            return sum(part.astype(jnp.float32) for part in parts)

        sum_right, sum_left = mix_part[1], mix_part[Z_SIZE - 1]
        for k in hops:
            if k > 1:
                sum_right, sum_left = lax.optimization_barrier((sum_right, sum_left))
                sum_right, sum_left = pair_add(mix_part[k], sum_right, mix_part[Z_SIZE - k], sum_left)
            sum_right = scatter_right[k](sum_right)
            sum_left = scatter_left[k](sum_left)
        result = (x_f32 + plus(mix_part[0], sum_right, sum_left)).astype(jnp.bfloat16)

        d_o = []
        for n in range(Z_SIZE):
            d_o.append([dot_f32(blk, w_mix[:2 * pair], COLS_OF_BOTH).astype(jnp.bfloat16) for blk in (dy_own[n], dy_pair[n])])
        shared = (o_slots, kv_slots, kv_other, cos_t, sin_t, lo_all, lse, bk)
        dq_early, dkv_part = attend_backward(where, pos_all, q_slots, slots(d_o[0] + d_o[1] + d_o[2]), *shared, early_slot)
        dq_early_partner = swap_core(dq_early)
        early_own, early_partner = apart(dq_early, dq_early_partner)
        early_keep, early_send = pair_sides(early_own, early_partner.reshape(3, CORE_SIZE, bq, -1)[:, ::-1].reshape(early_own.shape))
        q_theirs = swap_y(early_send)
        dq_late, dkv_mine, dkv_send = attend_backward(where, pos_all, q_slots, slots(d_o[3]), *shared, late_slot, dkv_part)
        dkv_theirs = swap_same_head(dkv_send)
        dq_late_partner = swap_core(dq_late)

        def blocks_of(early, late):
            return [early[2 * n:2 * n + 2] for n in range(3)] + [late]

        dq_own, dq_partner = blocks_of(dq_early, dq_late), [blk[::-1] for blk in blocks_of(dq_early_partner, dq_late_partner)]
        dq_rows = arrival([jnp.concatenate([own[0], partner[0]], axis=-1) for own, partner in zip(dq_own, dq_partner)])
        halves = [slice(0, model // 2), slice(model // 2, model)]
        dh_sum = []
        for n, cols in enumerate(halves):
            dh_sum.append(dot_f32(dq_rows[1], w_q[cols], COLS_OF_BOTH).astype(jnp.bfloat16))
            dh_sum[n] = ring(dh_sum[n])

        dkv_lines = finish_key_grads(where, dkv_mine, dkv_theirs, cos_my, sin_my)
        dkv_partner = flip_core(swap_core(dkv_lines))
        dkv_rows = jnp.concatenate([dkv_lines[:, 0], dkv_partner[:, 0]], axis=-1)
        dkv_next = ring_back(dkv_rows[1])

        def dh_part(s, cols):
            return dot_f32(dq_rows[s], w_q[cols], COLS_OF_BOTH) + dot_f32(dkv_rows[s], w_kv[cols], COLS_OF_BOTH)

        for s in hops[1:]:
            for n, cols in enumerate(halves):
                dh_sum[n] = (dh_part(s, cols) + dh_sum[n].astype(jnp.float32)).astype(jnp.bfloat16)
                if s == hops[-1] and n == 0:
                    dh_sum[n], result = lax.optimization_barrier((dh_sum[n], result))
                dh_sum[n] = ring(dh_sum[n])
        dh_own = lax.optimization_barrier([dh_part(0, cols) + dot_f32(dkv_next, w_kv_next[cols], COLS_OF_BOTH) for cols in halves])
        dh_rows = jnp.concatenate([(own + part.astype(jnp.float32)).astype(jnp.bfloat16) for own, part in zip(dh_own, dh_sum)], axis=1)

        g_pair = [swap_core(blk) for blk in lax.optimization_barrier((*g_own, dq_late))[:Z_SIZE]]
        kv_keep = select(dkv_lines[..., :HEAD_DIM], dkv_partner[..., HEAD_DIM:])
        kv_send = select(dkv_partner[..., :HEAD_DIM], dkv_lines[..., HEAD_DIM:])
        kv_theirs = swap_y(kv_send)
        late_keep, late_send = pair_sides(dq_own[3], dq_partner[3])
        late_theirs = swap_y(late_send)

        def rows_of(q_blocks, kv_lines):
            q_lines = jnp.concatenate([blk[None] for blk in arrival(q_blocks)], axis=0)
            return by_block(jnp.concatenate([q_lines, kv_lines], axis=-1))

        d_keep = rows_of(blocks_of(early_keep, late_keep), kv_keep)
        d_theirs = rows_of(blocks_of(q_theirs, late_theirs), kv_theirs)

        dwo_keep, dwo_send = token_grads(dy_slots, o_sides, [((pair, model), jnp.float32)] * 2)
        theirs_first = swap_y(dwo_send[:, halves[0]])
        theirs_last = swap_y(dwo_send[:, halves[1]])

        d_wq, kv_mine_sum = token_grads([blks[s] for mine, theirs in ((h_own, h_pair), (g_own, g_pair)) for s in range(Z_SIZE) for blks in (mine, theirs)], jnp.concatenate([d_keep, d_theirs], axis=0),
                                        [((model, pair), jnp.bfloat16), ((model, HEAD_DIM), jnp.float32)])
        kv_other_sum = swap_core(kv_mine_sum)
        d_wk = select(kv_mine_sum, kv_other_sum)
        d_wv = select(kv_other_sum, kv_mine_sum)

        d_input, dg_part = norm_backward(dh_rows, x_hat, inv_rms, norm_gain)
        grad_x = (dy_blk.astype(jnp.float32) + d_input).astype(jnp.bfloat16)
        for near, far, both in ((swap_core, swap_y, swap_same_head), (z_swaps[1], z_swaps[2], z_swaps[3])):
            dg_part = (dg_part + near(dg_part)) + (far(dg_part) + both(dg_part))
            if near is swap_core:
                theirs_last = after(theirs_last, dg_part)
        d_wo = (dwo_keep + jnp.concatenate([theirs_first, theirs_last], axis=1)).astype(jnp.bfloat16)
        return result, grad_x, d_wq, d_wk, d_wv, d_wo, dg_part

    specs_in = (P(('dp', 'tp'), None), P(('dp', 'tp'), None), P('dp'), P(), P(None, 'tp'), P(), P(), P('tp', None))
    specs_out = (P(('dp', 'tp'), None), P(('dp', 'tp'), None), P('dp', 'tp'), P('dp', 'tp'), P('dp', 'tp'), P(('dp', 'tp'), None), P('dp'))
    return jax.shard_map(device_step, mesh=mesh, in_specs=specs_in, out_specs=specs_out, check_vma=False)
```

```python
import functools
import jax
import jax.numpy as jnp
from jax import lax
from jax.experimental import pallas as pl
from jax.experimental.pallas import tpu as pltpu
from jax.sharding import PartitionSpec as P

HEAD_DIM = 128
SCORE_SCALE = HEAD_DIM ** -0.5
SCALE_LOG2E = SCORE_SCALE * 1.4426950408889634
ROPE_THETA = 1000000.0
NORM_EPS = 1e-05
MASKED = -1e30
Z_SIZE = 4
Y_SIZE = 2
CORE_SIZE = 2
SLOTS = Z_SIZE * CORE_SIZE
EARLY, LATE = (1, 2), (0, 3)
NATURAL = (((1,), (0,)), ((), ()))
COLS_OF_BOTH = (((1,), (1,)), ((), ()))


def dot_f32(lhs, rhs, dims=NATURAL):
    return lax.dot_general(lhs, rhs, dims, preferred_element_type=jnp.float32)


def rope_tables(positions):
    exponents = jnp.arange(0, HEAD_DIM, 2, dtype=jnp.float32) / HEAD_DIM
    angles = jnp.power(ROPE_THETA, -exponents)[:, None] * positions.astype(jnp.float32)[None, :]
    return jnp.cos(angles), jnp.sin(angles)


def rotate_rows(t_f32, cos_t, sin_t):
    lead_half, tail_half = t_f32[:HEAD_DIM // 2], t_f32[HEAD_DIM // 2:]
    return jnp.concatenate([lead_half * cos_t - tail_half * sin_t, tail_half * cos_t + lead_half * sin_t], axis=0).astype(jnp.bfloat16)


def norm_forward(x_f32, norm_gain):
    inv_rms = lax.rsqrt(jnp.mean(x_f32 * x_f32, axis=-1, keepdims=True) + NORM_EPS)
    x_hat = x_f32 * inv_rms
    return (x_hat * norm_gain).astype(jnp.bfloat16), x_hat, inv_rms


def norm_backward(d_hidden, x_hat, inv_rms, norm_gain):
    d_f32 = d_hidden.astype(jnp.float32)
    d_gain = jnp.sum(d_f32 * x_hat, axis=0)
    scaled = d_f32 * norm_gain
    d_input = inv_rms * (scaled - x_hat * jnp.mean(scaled * x_hat, axis=-1, keepdims=True))
    return d_input, d_gain


def slot_of(where_ref, z, c):
    return 2 * lax.rem(where_ref[0] - z + Z_SIZE, Z_SIZE) + (where_ref[2] ^ c)


def slot_of_other(where_ref, z, c):
    return 2 * lax.rem(where_ref[0] - z + Z_SIZE, Z_SIZE) + (1 - (where_ref[2] ^ c))


def block_token(where_ref, b, bq):
    return pl.multiple_of((b // 2) * (4 * bq) + where_ref[1] * (2 * bq) + (b % 2) * bq, bq)


def key_range(pos_ref, start, bq, bk):
    lo_first, lo_last = start - pos_ref[start], start + bq - 1 - pos_ref[start + bq - 1]
    return lo_first // bk, (start + bq - 1) // bk + 1, (lo_last + bk - 1) // bk, (start + 1) // bk


def tile_lanes(row, heads):
    return jnp.concatenate([row] * heads, axis=1)


def row_bounds(lo_ref, start, bq, heads):
    tok = start + lax.broadcasted_iota(jnp.int32, (1, bq), 1)
    return tile_lanes(tok, heads), tile_lanes(lo_ref[:, pl.ds(start, bq)], heads)


def keep_mask(key_start, bk, t_row, lo_row):
    key_idx = key_start + lax.broadcasted_iota(jnp.int32, (bk, t_row.shape[1]), 0)
    return (key_idx <= t_row) & (key_idx >= lo_row)


def head_columns(block, h):
    return block[:, h * HEAD_DIM:(h + 1) * HEAD_DIM]


def rotated_queries(q_blk, cos_ref, sin_ref, start, bq, heads):
    cos_t, sin_t = cos_ref[:, pl.ds(start, bq)], sin_ref[:, pl.ds(start, bq)]
    return [rotate_rows(head_columns(q_blk, h).T.astype(jnp.float32), cos_t, sin_t) for h in range(heads)]


def visit_keys(bounds, step):
    first, end, inner_first, inner_end = bounds

    def visit(j, carry):
        inner = (j >= inner_first) & (j < inner_end)

        @pl.when(inner)
        def _():
            step(j, False)

        @pl.when(jnp.logical_not(inner))
        def _():
            step(j, True)

        return carry

    lax.fori_loop(first, end, visit, 0)


def for_key_blocks(where_ref, mine_ref, theirs_ref, count, bq, store):
    def visit(n, carry):
        z, y, c = n // 4, (n // 2) % 2, n % 2
        block = jnp.where(y == where_ref[1], mine_ref[slot_of(where_ref, z, c)], theirs_ref[slot_of_other(where_ref, z, c)])
        store(pl.ds(pl.multiple_of(n * bq, bq), bq), block)
        return carry

    lax.fori_loop(0, count, visit, 0)


def fwd_kernel(heads, bk, where_ref, pos_ref, q_ref, kv_ref, kv_other_ref, cos_ref, sin_ref, lo_ref, o_ref, lse_ref, k_s, vt_s, qt_s, m_s, l_s, acc_s):
    b = pl.program_id(0)
    bq = q_ref.shape[1]
    seq = k_s.shape[0]

    @pl.when(b == 0)
    def _():
        def store(rows, block):
            k_s[rows, :] = rotate_rows(block[:, :HEAD_DIM].T.astype(jnp.float32), cos_ref[:, rows], sin_ref[:, rows]).T
            vt_s[:, rows] = block[:, HEAD_DIM:].T

        for_key_blocks(where_ref, kv_ref, kv_other_ref, seq // bq, bq, store)

    start = block_token(where_ref, b, bq)
    t_row, lo_row = row_bounds(lo_ref, start, bq, heads)
    q_blk = q_ref[0]
    qt_s[...] = jnp.concatenate(rotated_queries(q_blk, cos_ref, sin_ref, start, bq, heads), axis=1)
    m_s[...] = jnp.full_like(m_s, MASKED)
    l_s[...] = jnp.zeros_like(l_s)
    acc_s[...] = jnp.zeros_like(acc_s)

    def step(j, masked):
        key_start = pl.multiple_of(j * bk, bk)
        keys = pl.ds(key_start, bk)
        scores = dot_f32(k_s[keys, :], qt_s[...])
        if masked:
            scores = jnp.where(keep_mask(key_start, bk, t_row, lo_row), scores, MASKED)
        m_old = m_s[...]
        m_new = jnp.maximum(m_old, jnp.max(scores, axis=0, keepdims=True))
        probs = jnp.exp2(scores * SCALE_LOG2E - m_new * SCALE_LOG2E)
        alpha = jnp.exp2((m_old - m_new) * SCALE_LOG2E)
        m_s[...] = m_new
        l_s[...] = l_s[...] * alpha + jnp.sum(probs, axis=0, keepdims=True)
        acc_s[...] = acc_s[...] * alpha + dot_f32(vt_s[:, keys], probs.astype(jnp.bfloat16))

    visit_keys(key_range(pos_ref, start, bq, bk), step)
    out_t = (acc_s[...] / l_s[...]).astype(jnp.bfloat16)
    for h in range(heads):
        o_ref[0, :, h * HEAD_DIM:(h + 1) * HEAD_DIM] = out_t[:, h * bq:(h + 1) * bq].T
    lse_ref[0] = m_s[...] * SCALE_LOG2E + jnp.log2(l_s[...])


def bwd_block(where_ref, step, rows):
    return rows[0] + (rows[1] - rows[0]) * (step // 2), where_ref[2] ^ (step % 2)


def bwd_kernel(heads, bk, rows_of_z, where_ref, pos_ref, q_ref, do_ref, o_ref, kv_ref, kv_other_ref, cos_ref, sin_ref, lo_ref, lse_ref, *refs):
    first = rows_of_z == EARLY
    if first:
        dq_ref, part_ref, k_s, kt_s, v_s, q_s, qt_s, do_s, dot_s, dqt_s, acc_s = refs
    else:
        part_ref, dq_ref, mine_ref, send_ref, k_s, kt_s, v_s, q_s, qt_s, do_s, dot_s, dqt_s, acc_s = refs
    step_idx = pl.program_id(0)
    z_blk, c_blk = bwd_block(where_ref, step_idx, rows_of_z)
    b = 2 * z_blk + c_blk
    bq = q_ref.shape[1]
    seq = k_s.shape[0]

    @pl.when(step_idx == 0)
    def _():
        def store(rows, block):
            acc_s[rows, :] = jnp.zeros((bq, 2 * HEAD_DIM), jnp.float32) if first else part_ref[rows, :]
            k_rot_t = rotate_rows(block[:, :HEAD_DIM].T.astype(jnp.float32), cos_ref[:, rows], sin_ref[:, rows])
            kt_s[:, rows] = k_rot_t
            k_s[rows, :] = k_rot_t.T
            v_s[rows, :] = block[:, HEAD_DIM:]

        for_key_blocks(where_ref, kv_ref, kv_other_ref, seq // bq, bq, store)

    start = block_token(where_ref, b, bq)
    t_row, lo_row = row_bounds(lo_ref, start, bq, heads)
    q_blk, do_blk, o_blk = q_ref[0], do_ref[0], o_ref[0]
    deltas = []
    for h, q_rot_t in enumerate(rotated_queries(q_blk, cos_ref, sin_ref, start, bq, heads)):
        lanes = slice(h * bq, (h + 1) * bq)
        qt_s[:, lanes] = q_rot_t
        q_s[lanes, :] = q_rot_t.T
        do_head = head_columns(do_blk, h)
        do_s[lanes, :] = do_head
        do_t = do_head.T
        dot_s[:, lanes] = do_t
        deltas.append(jnp.sum(do_t.astype(jnp.float32) * head_columns(o_blk, h).T.astype(jnp.float32), axis=0, keepdims=True))
    delta = jnp.concatenate(deltas, axis=1)
    lse = lse_ref[0]
    dqt_s[...] = jnp.zeros_like(dqt_s)

    def step(j, masked):
        key_start = pl.multiple_of(j * bk, bk)
        keys = pl.ds(key_start, bk)
        scores = dot_f32(k_s[keys, :], qt_s[...])
        probs = jnp.exp2(scores * SCALE_LOG2E - lse)
        if masked:
            probs = jnp.where(keep_mask(key_start, bk, t_row, lo_row), probs, 0.0)
        d_probs = dot_f32(v_s[keys, :], dot_s[...])
        d_scores = (probs * (d_probs - delta)).astype(jnp.bfloat16)
        acc_s[keys, HEAD_DIM:] += dot_f32(probs.astype(jnp.bfloat16), do_s[...])
        acc_s[keys, :HEAD_DIM] += dot_f32(d_scores, q_s[...]) * SCORE_SCALE
        dqt_s[...] += dot_f32(kt_s[:, keys], d_scores)

    visit_keys(key_range(pos_ref, start, bq, bk), step)
    cos_t, sin_t = cos_ref[:, pl.ds(start, bq)], sin_ref[:, pl.ds(start, bq)]
    for h in range(heads):
        dq_rot_t = (dqt_s[:, h * bq:(h + 1) * bq] * SCORE_SCALE).astype(jnp.bfloat16).astype(jnp.float32)
        dq_ref[0, :, h * HEAD_DIM:(h + 1) * HEAD_DIM] = rotate_rows(dq_rot_t, cos_t, -sin_t).T

    @pl.when(step_idx == pl.num_programs(0) - 1)
    def _():
        if first:
            part_ref[...] = acc_s[...]
            return

        def hand_over(y, mine):
            for z in range(Z_SIZE):
                for c in range(CORE_SIZE):
                    rows = ((z * 2 + y) * 2 + c) * bq
                    e = where_ref[2] ^ c
                    if mine:
                        mine_ref[z, e] = acc_s[rows:rows + bq, :]
                    else:
                        send_ref[z, 1 - e] = acc_s[rows:rows + bq, :]

        for y in range(Y_SIZE):
            pl.when(where_ref[1] == y)(functools.partial(hand_over, y, True))
            pl.when(where_ref[1] != y)(functools.partial(hand_over, y, False))


def token_grads_kernel(count, *refs):
    blocks, lhs_ref, out_refs, lhs_t = refs[:count], refs[count], refs[count + 1:-1], refs[-1]
    rows = lhs_ref.shape[1]

    @pl.when(pl.program_id(0) == 0)
    def _():
        for n in range(count):
            lhs_t[:, n * rows:(n + 1) * rows] = lhs_ref[n].T

    total = sum(dot_f32(lhs_t[:, n * rows:(n + 1) * rows], blocks[n][...]) for n in range(count))
    start = 0
    for ref in out_refs:
        if ref.shape[0] == blocks[0].shape[1]:
            size = ref.shape[1]
            ref[...] = total[start:start + size, :].T.astype(ref.dtype)
        else:
            size = ref.shape[0]
            ref[...] = total[start:start + size, :].astype(ref.dtype)
        start += size


def token_grads(blocks, lhs, outs, tile=512):
    rows, model = blocks[0].shape
    width = lhs.shape[2]
    specs = [pl.BlockSpec((tile, shape[1]), lambda i: (i, 0)) if shape[0] == model else pl.BlockSpec((shape[0], tile), lambda i: (0, i)) for shape, _ in outs]
    return pl.pallas_call(
        functools.partial(token_grads_kernel, len(blocks)),
        out_shape=[jax.ShapeDtypeStruct(*out) for out in outs], grid=(model // tile,),
        in_specs=[pl.BlockSpec((rows, tile), lambda i: (0, i)) for _ in blocks] + [pl.BlockSpec(lhs.shape, lambda i: (0, 0, 0))], out_specs=specs,
        scratch_shapes=[pltpu.VMEM((width, len(blocks) * rows), jnp.bfloat16)],
        compiler_params=pltpu.CompilerParams(dimension_semantics=('arbitrary',), vmem_limit_bytes=48 << 20),
        cost_estimate=pl.CostEstimate(flops=2 * len(blocks) * rows * model * width, bytes_accessed=2 * len(blocks) * rows * model, transcendentals=0),
    )(*blocks, lhs)


def pick_kernel(count, where_ref, *refs):
    sources, outs, sems = refs[:count * Z_SIZE], refs[count * Z_SIZE:-1], refs[-1]

    def copy(n, k):
        return pltpu.make_async_copy(sources[n * Z_SIZE + k], outs[n], sems.at[n])

    for n in range(count):
        for k in range(Z_SIZE):
            pl.when(where_ref[0] == k)(lambda n=n, k=k: copy(n, k).start())
    for n in range(count):
        copy(n, 0).wait()


def pick(where, *choices):
    shape = choices[0][0].shape
    return pl.pallas_call(
        functools.partial(pick_kernel, len(choices)), out_shape=[jax.ShapeDtypeStruct(shape, jnp.bfloat16)] * len(choices),
        grid_spec=pltpu.PrefetchScalarGridSpec(
            num_scalar_prefetch=1, grid=(1,), in_specs=[pl.BlockSpec(memory_space=pl.ANY)] * (len(choices) * Z_SIZE), out_specs=[full_spec(shape)] * len(choices),
            scratch_shapes=[pltpu.SemaphoreType.DMA((len(choices),))]),
        compiler_params=pltpu.CompilerParams(dimension_semantics=('arbitrary',), vmem_limit_bytes=32 << 20),
        cost_estimate=pl.CostEstimate(flops=1000000, bytes_accessed=8000000, transcendentals=0),
    )(where, *(arr for choice in choices for arr in choice))


def pair_add_kernel(a_ref, b_ref, c_ref, d_ref, ab_ref, cd_ref):
    for left, right, out in ((a_ref, b_ref, ab_ref), (c_ref, d_ref, cd_ref)):
        out[...] = (left[...].astype(jnp.float32) + right[...].astype(jnp.float32)).astype(jnp.bfloat16)


def pair_add(*operands):
    rows, model = operands[0].shape
    tile = model // 4
    spec = pl.BlockSpec((rows, tile), lambda i: (0, i))
    return pl.pallas_call(
        pair_add_kernel, out_shape=[jax.ShapeDtypeStruct((rows, model), jnp.bfloat16)] * 2, grid=(model // tile,), in_specs=[spec] * 4, out_specs=[spec] * 2,
        compiler_params=pltpu.CompilerParams(dimension_semantics=('arbitrary',), vmem_limit_bytes=32 << 20),
        cost_estimate=pl.CostEstimate(flops=4 * rows * model, bytes_accessed=12 * rows * model, transcendentals=0),
    )(*operands)


def finish_kernel(where_ref, mine_ref, other_ref, cos_ref, sin_ref, out_ref):
    for z in range(Z_SIZE):
        slot = lax.rem(where_ref[0] - z + Z_SIZE, Z_SIZE)
        for e in range(CORE_SIZE):
            total = mine_ref[z, e] + other_ref[z, e]
            dk = total[:, :HEAD_DIM].astype(jnp.bfloat16).astype(jnp.float32)
            out_ref[slot, e, :, :HEAD_DIM] = (dk * cos_ref[z, e] + pltpu.roll(dk, HEAD_DIM // 2, 1) * sin_ref[z, e]).astype(jnp.bfloat16)
            out_ref[slot, e, :, HEAD_DIM:] = total[:, HEAD_DIM:].astype(jnp.bfloat16)


def finish_key_grads(where, *operands):
    return pl.pallas_call(
        finish_kernel, out_shape=jax.ShapeDtypeStruct(operands[0].shape, jnp.bfloat16),
        grid_spec=pltpu.PrefetchScalarGridSpec(num_scalar_prefetch=1, grid=(1,), in_specs=[full_spec(arr.shape) for arr in operands], out_specs=full_spec(operands[0].shape)),
        compiler_params=pltpu.CompilerParams(dimension_semantics=('arbitrary',), vmem_limit_bytes=32 << 20),
        cost_estimate=pl.CostEstimate(flops=1000000, bytes_accessed=8000000, transcendentals=0),
    )(where, *operands)


def full_spec(shape):
    return pl.BlockSpec(shape, lambda b, *_: (0,) * len(shape))


def slot_spec(bq, width, find):
    return pl.BlockSpec((1, bq, width), lambda b, where_ref, _: (find(where_ref, b // 2, b % 2), 0, 0))


def attend(where, positions, q_slots, kv_slots, kv_other, cos_t, sin_t, lo_all, bk):
    slots, bq, width = q_slots.shape
    seq = positions.shape[0]
    heads = width // HEAD_DIM
    lanes = heads * bq
    shared = (kv_slots, kv_other, cos_t, sin_t, lo_all)
    block = slot_spec(bq, width, slot_of)
    return pl.pallas_call(
        functools.partial(fwd_kernel, heads, bk),
        out_shape=(jax.ShapeDtypeStruct(q_slots.shape, jnp.bfloat16), jax.ShapeDtypeStruct((slots, 1, lanes), jnp.float32)),
        grid_spec=pltpu.PrefetchScalarGridSpec(
            num_scalar_prefetch=2, grid=(slots,), in_specs=[block] + [full_spec(arr.shape) for arr in shared],
            out_specs=(block, pl.BlockSpec((1, 1, lanes), lambda b, *_: (b, 0, 0))),
            scratch_shapes=[pltpu.VMEM((seq, HEAD_DIM), jnp.bfloat16), pltpu.VMEM((HEAD_DIM, seq), jnp.bfloat16), pltpu.VMEM((HEAD_DIM, lanes), jnp.bfloat16),
                            pltpu.VMEM((1, lanes), jnp.float32), pltpu.VMEM((1, lanes), jnp.float32), pltpu.VMEM((HEAD_DIM, lanes), jnp.float32)]),
        compiler_params=pltpu.CompilerParams(dimension_semantics=('arbitrary',), vmem_limit_bytes=48 << 20),
        cost_estimate=pl.CostEstimate(flops=4 * slots * bq * heads * seq * HEAD_DIM, bytes_accessed=4 * slots * bq * width + 8 * seq * HEAD_DIM, transcendentals=slots * bq * heads * seq // 2),
        name='attend_fwd',
    )(where, positions, q_slots, *shared)


def attend_backward(where, positions, q_slots, do_blocks, o_slots, kv_slots, kv_other, cos_t, sin_t, lo_all, lse, bk, rows_of_z, part=None):
    count, bq, width = do_blocks.shape
    seq = positions.shape[0]
    heads = width // HEAD_DIM
    lanes = heads * bq
    shared = (kv_slots, kv_other, cos_t, sin_t, lo_all)

    def slot_index(i, where_ref, _):
        return (slot_of(where_ref, *bwd_block(where_ref, i, rows_of_z)), 0, 0)

    def lse_index(i, where_ref, _):
        z_blk, c_blk = bwd_block(where_ref, i, rows_of_z)
        return (2 * z_blk + c_blk, 0, 0)

    block = pl.BlockSpec((1, bq, width), slot_index)
    local = pl.BlockSpec((1, bq, width), lambda i, *_: (i, 0, 0))
    operands = [q_slots, do_blocks, o_slots, *shared, lse]
    in_specs = [block, local, block] + [full_spec(arr.shape) for arr in shared] + [pl.BlockSpec((1, 1, lanes), lse_index)]
    part_shape, final_shape = (seq, 2 * HEAD_DIM), (Z_SIZE, CORE_SIZE, bq, 2 * HEAD_DIM)
    grads = [part_shape] if part is None else [final_shape] * 2
    if part is not None:
        operands.append(part)
        in_specs.append(full_spec(part_shape))
    work = count * bq * heads * seq * HEAD_DIM
    return pl.pallas_call(
        functools.partial(bwd_kernel, heads, bk, rows_of_z),
        out_shape=[jax.ShapeDtypeStruct(do_blocks.shape, jnp.bfloat16)] + [jax.ShapeDtypeStruct(shape, jnp.float32) for shape in grads],
        grid_spec=pltpu.PrefetchScalarGridSpec(
            num_scalar_prefetch=2, grid=(count,), in_specs=in_specs, out_specs=[local] + [full_spec(shape) for shape in grads],
            scratch_shapes=[pltpu.VMEM((seq, HEAD_DIM), jnp.bfloat16), pltpu.VMEM((HEAD_DIM, seq), jnp.bfloat16), pltpu.VMEM((seq, HEAD_DIM), jnp.bfloat16),
                            pltpu.VMEM((lanes, HEAD_DIM), jnp.bfloat16), pltpu.VMEM((HEAD_DIM, lanes), jnp.bfloat16),
                            pltpu.VMEM((lanes, HEAD_DIM), jnp.bfloat16), pltpu.VMEM((HEAD_DIM, lanes), jnp.bfloat16), pltpu.VMEM((HEAD_DIM, lanes), jnp.float32),
                            pltpu.VMEM((seq, 2 * HEAD_DIM), jnp.float32)]),
        compiler_params=pltpu.CompilerParams(dimension_semantics=('arbitrary',), vmem_limit_bytes=58 << 20),
        cost_estimate=pl.CostEstimate(flops=10 * work, bytes_accessed=8 * count * bq * width + 24 * seq * HEAD_DIM, transcendentals=work // (2 * HEAD_DIM)),
        name='attend_bwd',
    )(where, positions, *operands)


def solution(mesh):
    def member(z, y, c):
        return (z * Y_SIZE + y) * CORE_SIZE + c

    every = [(z, y, c) for z in range(Z_SIZE) for y in range(Y_SIZE) for c in range(CORE_SIZE)]

    def permuter(target, senders=range(Z_SIZE)):
        pairs = [(member(*src), member(*target(*src))) for src in every if src[0] in senders]
        return lambda val: lax.ppermute(val, 'tp', pairs)

    swap_core = permuter(lambda z, y, c: (z, y, 1 - c))
    swap_y = permuter(lambda z, y, c: (z, 1 - y, c))
    swap_same_head = permuter(lambda z, y, c: (z, 1 - y, 1 - c))
    ring = permuter(lambda z, y, c: ((z + 1) % Z_SIZE, y, c))
    ring_back = permuter(lambda z, y, c: ((z - 1) % Z_SIZE, y, c))
    hops = range(1, Z_SIZE)
    gather_right = {k: permuter(lambda z, y, c: (z + 1, y, c), range(k - 1, Z_SIZE - 1)) for k in hops}
    gather_left = {k: permuter(lambda z, y, c: (z - 1, y, c), range(1, Z_SIZE - k + 1)) for k in hops}
    scatter_right = {k: permuter(lambda z, y, c: (z + 1, y, c), range(0, k)) for k in hops}
    scatter_left = {k: permuter(lambda z, y, c: (z - 1, y, c), range(Z_SIZE - k, Z_SIZE)) for k in hops}
    z_swaps = {k: permuter(lambda z, y, c, k=k: (z ^ k, y, c)) for k in hops}

    def after(val, *deps):
        return lax.optimization_barrier((val,) + deps)[0]

    def device_step(x_blk, dy_blk, pos_all, norm_gain, wq_loc, wk_all, wv_all, wo_loc):
        seq_len = pos_all.shape[0]
        bq = seq_len // (Z_SIZE * Y_SIZE * CORE_SIZE)
        bk = 2 * bq
        model = x_blk.shape[1]
        idx = lax.axis_index('tp')
        z_idx, y_idx, c_idx = idx // (Y_SIZE * CORE_SIZE), (idx // CORE_SIZE) % Y_SIZE, idx % CORE_SIZE
        where = jnp.stack([z_idx, y_idx, c_idx])
        on_core0 = c_idx == 0
        pair = wq_loc.shape[1]
        kv_own = Y_SIZE * z_idx + (y_idx ^ c_idx)

        def select(first, second):
            return jnp.where(on_core0, first, second)

        def flip_core(arr):
            return arr[:, ::-1]

        def slots(arrs):
            return jnp.concatenate([arr[None] for arr in arrs], axis=0)

        def interleave(own, partner):
            return [blk for both in zip(own, partner) for blk in both]

        x_f32 = x_blk.astype(jnp.float32)
        hidden, x_hat, inv_rms = norm_forward(x_f32, norm_gain)

        h_own = [hidden]
        for s in hops:
            h_own.append(ring(h_own[-1]))
        h_pair = []
        for blk in h_own:
            h_pair.append(swap_core(blk))

        def slot_order(w_own, w_core, w_y, w_both):
            return [select(w_own, w_y), select(w_core, w_both), select(w_both, w_core), select(w_y, w_own)]

        wq_y = swap_y(wq_loc)
        wq_core = swap_core(wq_loc)
        q_cols = slot_order(wq_loc, wq_core, wq_y, swap_core(wq_y))
        wo_y = swap_y(wo_loc)
        o_rows = (wo_loc, swap_core(wo_loc), wo_y, swap_core(wo_y))

        def kv_columns(head):
            return [lax.dynamic_slice_in_dim(w, head * HEAD_DIM, HEAD_DIM, axis=1) for w in (wk_all, wv_all)]

        w_q = lax.optimization_barrier(jnp.concatenate(q_cols, axis=1))
        w_kv = lax.optimization_barrier(jnp.concatenate(kv_columns(kv_own) + kv_columns(kv_own ^ 1), axis=1))
        kv_next = lax.rem(kv_own + Y_SIZE, Y_SIZE * Z_SIZE)
        w_kv_next = lax.optimization_barrier(jnp.concatenate(kv_columns(kv_next) + kv_columns(kv_next ^ 1), axis=1))
        w_own = jnp.concatenate([w_q[:, :2 * pair], w_kv[:, :2 * HEAD_DIM]], axis=1)
        w_mix = jnp.concatenate(slot_order(*o_rows), axis=0)
        lo_all = (lax.iota(jnp.int32, seq_len) - pos_all)[None, :]
        cos_t, sin_t = rope_tables(pos_all)

        def my_tables(lead, tail):
            parts = jnp.concatenate([lead.T, tail.T], axis=1).reshape(Z_SIZE, Y_SIZE, CORE_SIZE, bq, HEAD_DIM)
            parts = lax.dynamic_index_in_dim(parts, y_idx, 1, keepdims=False)
            return select(parts, flip_core(parts))

        cos_my, sin_my = my_tables(cos_t, cos_t), my_tables(sin_t, -sin_t)

        qkv = []
        for s in range(Z_SIZE):
            qkv += [dot_f32(blk, w_own).astype(jnp.bfloat16) for blk in (h_own[s], h_pair[s])]
        kv_blocks = [blk[:, 2 * pair:] for blk in qkv]
        early = SLOTS - CORE_SIZE
        kv_other_early = swap_same_head(slots(kv_blocks[:early]))
        kv_other_late = swap_same_head(slots(kv_blocks[early:]))
        kv_other = jnp.concatenate([kv_other_early, kv_other_late], axis=0)
        q_slots, kv_slots = slots([blk[:, :2 * pair] for blk in qkv]), slots(kv_blocks)

        g_own = []
        for s, blk in enumerate(h_own):
            g_own.append(swap_y(after(blk, kv_other_late) if s else blk))

        right, left = {0: after(dy_blk, h_own[-1])}, {}
        left[0] = right[0]
        for k in hops:
            right[k] = gather_right[k](right[k - 1])
            left[k] = gather_left[k](left[k - 1])
            right[k], left[k] = lax.optimization_barrier((right[k], left[k]))
        dy_one, dy_two = pick(where, (left[1], dy_blk, right[1], right[2]), (left[2], left[1], dy_blk, right[1]))
        dy_zero, dy_three = pick(where, (dy_blk, right[1], right[2], right[3]), (left[3], left[2], left[1], dy_blk))
        dy_own = [dy_zero, dy_one, dy_two, dy_three]
        dy_pair = []
        for blk in dy_own:
            dy_pair.append(swap_core(blk))
        dy_slots = interleave(dy_own, dy_pair)

        def mirrored(lines):
            return jnp.concatenate([lax.dynamic_slice_in_dim(lines, lax.rem(z_idx - s + Z_SIZE, Z_SIZE), 1, axis=0) for s in range(Z_SIZE)], axis=0)

        o_slots, lse = attend(where, pos_all, q_slots, kv_slots, kv_other, cos_t, sin_t, lo_all, bk)
        by_line = (Z_SIZE, CORE_SIZE, bq, -1)
        o_lines = o_slots.reshape(by_line)
        o_partner = swap_core(o_slots).reshape(by_line)
        o_mine = jnp.concatenate([o_lines[:, 0], o_partner[:, 1]], axis=-1)

        def pair_sides(own, partner):
            first, last = own[..., :pair], partner[..., pair:2 * pair]
            return select(first, last), select(last, first)

        def by_block(arr):
            return arr.reshape((SLOTS,) + arr.shape[2:])

        o_sides = jnp.concatenate(pair_sides(o_lines, flip_core(o_partner)), axis=-1)
        o_sides = lax.optimization_barrier(by_block(mirrored(o_sides)))
        mix_part = []
        for s in range(Z_SIZE):
            mix_part.append(lax.optimization_barrier(dot_f32(o_mine[s], w_mix).astype(jnp.bfloat16)))

        def plus(*parts):
            return sum(part.astype(jnp.float32) for part in parts)

        sum_right, sum_left = mix_part[1], mix_part[Z_SIZE - 1]
        for k in hops:
            if k > 1:
                sum_right, sum_left = lax.optimization_barrier((sum_right, sum_left))
                sum_right, sum_left = pair_add(mix_part[k], sum_right, mix_part[Z_SIZE - k], sum_left)
            sum_right = scatter_right[k](sum_right)
            sum_left = scatter_left[k](sum_left)
        result = (x_f32 + plus(mix_part[0], sum_right, sum_left)).astype(jnp.bfloat16)

        d_o = []
        for n in range(Z_SIZE):
            d_o.append([dot_f32(blk, w_mix[:2 * pair], COLS_OF_BOTH).astype(jnp.bfloat16) for blk in (dy_own[n], dy_pair[n])])
        shared = (o_slots, kv_slots, kv_other, cos_t, sin_t, lo_all, lse, bk)
        dq_early, dkv_part = attend_backward(where, pos_all, q_slots, slots(d_o[1] + d_o[2]), *shared, EARLY)
        dq_early_partner = swap_core(dq_early)
        early_own, early_partner = lax.optimization_barrier((dq_early, dq_early_partner))
        early_keep, early_send = pair_sides(early_own, early_partner.reshape(2, CORE_SIZE, bq, -1)[:, ::-1].reshape(early_own.shape))
        early_theirs = swap_y(early_send)
        dq_late, dkv_mine, dkv_send = attend_backward(where, pos_all, q_slots, slots(d_o[0] + d_o[3]), *shared, LATE, dkv_part)
        dkv_theirs = swap_same_head(dkv_send)
        dq_late_partner = swap_core(dq_late)

        late_partner = dq_late_partner.reshape(2, CORE_SIZE, bq, -1)[:, ::-1].reshape(dq_late.shape)
        late_keep, late_send = pair_sides(dq_late, late_partner)

        def natural(early, late):
            return jnp.concatenate([late[:2], early, late[2:]], axis=0).reshape((Z_SIZE, CORE_SIZE) + early.shape[1:])

        q_rows = jnp.concatenate([natural(dq_early, dq_late)[:, 0], natural(early_partner, dq_late_partner)[:, 1]], axis=-1)
        dq_rows = [lax.dynamic_index_in_dim(q_rows, lax.rem(z_idx - s + Z_SIZE, Z_SIZE), 0, keepdims=False) for s in range(Z_SIZE)]
        halves = [slice(0, model // 2), slice(model // 2, model)]
        dh_sum = []
        for n, cols in enumerate(halves):
            dh_sum.append(dot_f32(dq_rows[1], w_q[cols], COLS_OF_BOTH).astype(jnp.bfloat16))
            dh_sum[n] = ring(dh_sum[n])

        dkv_lines = finish_key_grads(where, dkv_mine, dkv_theirs, cos_my, sin_my)
        dkv_partner = flip_core(swap_core(dkv_lines))
        dkv_rows = jnp.concatenate([dkv_lines[:, 0], dkv_partner[:, 0]], axis=-1)
        dkv_next = ring_back(dkv_rows[1])

        def dh_part(s, cols):
            return dot_f32(dq_rows[s], w_q[cols], COLS_OF_BOTH) + dot_f32(dkv_rows[s], w_kv[cols], COLS_OF_BOTH)

        for s in hops[1:]:
            for n, cols in enumerate(halves):
                dh_sum[n] = (dh_part(s, cols) + dh_sum[n].astype(jnp.float32)).astype(jnp.bfloat16)
                if s == hops[-1] and n == 0:
                    dh_sum[n], result = lax.optimization_barrier((dh_sum[n], result))
                dh_sum[n] = ring(dh_sum[n])
        dh_own = lax.optimization_barrier([dh_part(0, cols) + dot_f32(dkv_next, w_kv_next[cols], COLS_OF_BOTH) for cols in halves])
        dh_rows = jnp.concatenate([(own + part.astype(jnp.float32)).astype(jnp.bfloat16) for own, part in zip(dh_own, dh_sum)], axis=1)

        g_pair = [swap_core(blk) for blk in lax.optimization_barrier((*g_own, dq_late))[:Z_SIZE]]
        kv_keep = select(dkv_lines[..., :HEAD_DIM], dkv_partner[..., HEAD_DIM:])
        kv_send = select(dkv_partner[..., :HEAD_DIM], dkv_lines[..., HEAD_DIM:])
        kv_theirs = swap_y(kv_send)
        late_theirs = swap_y(late_send)

        def rows_of(early, late, kv_lines):
            return by_block(jnp.concatenate([mirrored(natural(early, late)), kv_lines], axis=-1))

        d_keep = rows_of(early_keep, late_keep, kv_keep)
        d_theirs = rows_of(early_theirs, late_theirs, kv_theirs)

        dwo_keep, dwo_send = token_grads(dy_slots, o_sides, [((pair, model), jnp.float32)] * 2)
        theirs_first = swap_y(dwo_send[:, halves[0]])
        theirs_last = swap_y(dwo_send[:, halves[1]])

        d_wq, kv_mine_sum = token_grads([blks[s] for mine, theirs in ((h_own, h_pair), (g_own, g_pair)) for s in range(Z_SIZE) for blks in (mine, theirs)], jnp.concatenate([d_keep, d_theirs], axis=0),
                                        [((model, pair), jnp.bfloat16), ((model, HEAD_DIM), jnp.float32)])
        kv_other_sum = swap_core(kv_mine_sum)
        d_wk = select(kv_mine_sum, kv_other_sum)
        d_wv = select(kv_other_sum, kv_mine_sum)

        d_input, dg_part = norm_backward(dh_rows, x_hat, inv_rms, norm_gain)
        grad_x = (dy_blk.astype(jnp.float32) + d_input).astype(jnp.bfloat16)
        for near, far, both in ((swap_core, swap_y, swap_same_head), (z_swaps[1], z_swaps[2], z_swaps[3])):
            dg_part = (dg_part + near(dg_part)) + (far(dg_part) + both(dg_part))
            if near is swap_core:
                theirs_last = after(theirs_last, dg_part)
        d_wo = (dwo_keep + jnp.concatenate([theirs_first, theirs_last], axis=1)).astype(jnp.bfloat16)
        return result, grad_x, d_wq, d_wk, d_wv, d_wo, dg_part

    specs_in = (P(('dp', 'tp'), None), P(('dp', 'tp'), None), P('dp'), P(), P(None, 'tp'), P(), P(), P('tp', None))
    specs_out = (P(('dp', 'tp'), None), P(('dp', 'tp'), None), P('dp', 'tp'), P('dp', 'tp'), P('dp', 'tp'), P(('dp', 'tp'), None), P('dp'))
    return jax.shard_map(device_step, mesh=mesh, in_specs=specs_in, out_specs=specs_out, check_vma=False)
```

```python
import functools
import jax
import jax.numpy as jnp
from jax import lax
from jax.experimental import pallas as pl
from jax.experimental.pallas import tpu as pltpu
from jax.sharding import PartitionSpec as P

HEAD_DIM = 128
SCORE_SCALE = HEAD_DIM ** -0.5
SCALE_LOG2E = SCORE_SCALE * 1.4426950408889634
ROPE_THETA = 1000000.0
NORM_EPS = 1e-05
MASKED = -1e30
Z_SIZE = 4
Y_SIZE = 2
CORE_SIZE = 2
SLOTS = Z_SIZE * CORE_SIZE
EARLY, LATE = (1, 2), (0, 3)
FIRST_CALL = 6
NATURAL = (((1,), (0,)), ((), ()))
COLS_OF_BOTH = (((1,), (1,)), ((), ()))


def dot_f32(lhs, rhs, dims=NATURAL):
    return lax.dot_general(lhs, rhs, dims, preferred_element_type=jnp.float32)


def rope_tables(positions):
    exponents = jnp.arange(0, HEAD_DIM, 2, dtype=jnp.float32) / HEAD_DIM
    angles = jnp.power(ROPE_THETA, -exponents)[:, None] * positions.astype(jnp.float32)[None, :]
    return jnp.cos(angles), jnp.sin(angles)


def rotate_rows(t_f32, cos_t, sin_t):
    lead_half, tail_half = t_f32[:HEAD_DIM // 2], t_f32[HEAD_DIM // 2:]
    return jnp.concatenate([lead_half * cos_t - tail_half * sin_t, tail_half * cos_t + lead_half * sin_t], axis=0).astype(jnp.bfloat16)


def norm_forward(x_f32, norm_gain):
    inv_rms = lax.rsqrt(jnp.mean(x_f32 * x_f32, axis=-1, keepdims=True) + NORM_EPS)
    x_hat = x_f32 * inv_rms
    return (x_hat * norm_gain).astype(jnp.bfloat16), x_hat, inv_rms


def norm_backward(d_hidden, x_hat, inv_rms, norm_gain):
    d_f32 = d_hidden.astype(jnp.float32)
    d_gain = jnp.sum(d_f32 * x_hat, axis=0)
    scaled = d_f32 * norm_gain
    d_input = inv_rms * (scaled - x_hat * jnp.mean(scaled * x_hat, axis=-1, keepdims=True))
    return d_input, d_gain


def slot_of(where_ref, z, c):
    return 2 * lax.rem(where_ref[0] - z + Z_SIZE, Z_SIZE) + (where_ref[2] ^ c)


def slot_of_other(where_ref, z, c):
    return 2 * lax.rem(where_ref[0] - z + Z_SIZE, Z_SIZE) + (1 - (where_ref[2] ^ c))


def block_token(where_ref, b, bq):
    return pl.multiple_of((b // 2) * (4 * bq) + where_ref[1] * (2 * bq) + (b % 2) * bq, bq)


def key_range(pos_ref, start, bq, bk):
    lo_first, lo_last = start - pos_ref[start], start + bq - 1 - pos_ref[start + bq - 1]
    return lo_first // bk, (start + bq - 1) // bk + 1, (lo_last + bk - 1) // bk, (start + 1) // bk


def tile_lanes(row, heads):
    return jnp.concatenate([row] * heads, axis=1)


def row_bounds(lo_ref, start, bq, heads):
    tok = start + lax.broadcasted_iota(jnp.int32, (1, bq), 1)
    return tile_lanes(tok, heads), tile_lanes(lo_ref[:, pl.ds(start, bq)], heads)


def keep_mask(key_start, bk, t_row, lo_row):
    key_idx = key_start + lax.broadcasted_iota(jnp.int32, (bk, t_row.shape[1]), 0)
    return (key_idx <= t_row) & (key_idx >= lo_row)


def head_columns(block, h):
    return block[:, h * HEAD_DIM:(h + 1) * HEAD_DIM]


def rotated_queries(q_blk, cos_ref, sin_ref, start, bq, heads):
    cos_t, sin_t = cos_ref[:, pl.ds(start, bq)], sin_ref[:, pl.ds(start, bq)]
    return [rotate_rows(head_columns(q_blk, h).T.astype(jnp.float32), cos_t, sin_t) for h in range(heads)]


def visit_keys(bounds, step):
    first, end, inner_first, inner_end = bounds

    def visit(j, carry):
        inner = (j >= inner_first) & (j < inner_end)

        @pl.when(inner)
        def _():
            step(j, False)

        @pl.when(jnp.logical_not(inner))
        def _():
            step(j, True)

        return carry

    lax.fori_loop(first, end, visit, 0)


def for_key_blocks(where_ref, mine_ref, theirs_ref, count, bq, store):
    def visit(n, carry):
        z, y, c = n // 4, (n // 2) % 2, n % 2
        block = jnp.where(y == where_ref[1], mine_ref[slot_of(where_ref, z, c)], theirs_ref[slot_of_other(where_ref, z, c)])
        store(pl.ds(pl.multiple_of(n * bq, bq), bq), block)
        return carry

    lax.fori_loop(0, count, visit, 0)


def fwd_kernel(heads, bk, first_block, where_ref, pos_ref, q_ref, kv_ref, kv_other_ref, cos_ref, sin_ref, lo_ref, *refs):
    o_ref, lse_ref, k_s, vt_s, qt_s, m_s, l_s, acc_s = refs[-8:]
    step_idx = pl.program_id(0)
    b = step_idx + first_block
    bq = q_ref.shape[1]
    seq = k_s.shape[0]

    @pl.when(step_idx == 0)
    def _():
        def store(rows, block):
            k_s[rows, :] = rotate_rows(block[:, :HEAD_DIM].T.astype(jnp.float32), cos_ref[:, rows], sin_ref[:, rows]).T
            vt_s[:, rows] = block[:, HEAD_DIM:].T

        for_key_blocks(where_ref, kv_ref, kv_other_ref, seq // bq, bq, store)

    start = block_token(where_ref, b, bq)
    t_row, lo_row = row_bounds(lo_ref, start, bq, heads)
    q_blk = q_ref[0]
    qt_s[...] = jnp.concatenate(rotated_queries(q_blk, cos_ref, sin_ref, start, bq, heads), axis=1)
    m_s[...] = jnp.full_like(m_s, MASKED)
    l_s[...] = jnp.zeros_like(l_s)
    acc_s[...] = jnp.zeros_like(acc_s)

    def step(j, masked):
        key_start = pl.multiple_of(j * bk, bk)
        keys = pl.ds(key_start, bk)
        scores = dot_f32(k_s[keys, :], qt_s[...])
        if masked:
            scores = jnp.where(keep_mask(key_start, bk, t_row, lo_row), scores, MASKED)
        m_old = m_s[...]
        m_new = jnp.maximum(m_old, jnp.max(scores, axis=0, keepdims=True))
        probs = jnp.exp2(scores * SCALE_LOG2E - m_new * SCALE_LOG2E)
        alpha = jnp.exp2((m_old - m_new) * SCALE_LOG2E)
        m_s[...] = m_new
        l_s[...] = l_s[...] * alpha + jnp.sum(probs, axis=0, keepdims=True)
        acc_s[...] = acc_s[...] * alpha + dot_f32(vt_s[:, keys], probs.astype(jnp.bfloat16))

    visit_keys(key_range(pos_ref, start, bq, bk), step)
    out_t = (acc_s[...] / l_s[...]).astype(jnp.bfloat16)
    for h in range(heads):
        o_ref[0, :, h * HEAD_DIM:(h + 1) * HEAD_DIM] = out_t[:, h * bq:(h + 1) * bq].T
    lse_ref[0] = m_s[...] * SCALE_LOG2E + jnp.log2(l_s[...])


def bwd_block(where_ref, step, rows):
    return rows[0] + (rows[1] - rows[0]) * (step // 2), where_ref[2] ^ (step % 2)


def bwd_kernel(heads, bk, rows_of_z, where_ref, pos_ref, q_ref, do_ref, o_ref, kv_ref, kv_other_ref, cos_ref, sin_ref, lo_ref, lse_ref, *refs):
    first = rows_of_z == EARLY
    if first:
        dq_ref, part_ref, k_s, kt_s, v_s, qt_s, dot_s, dqt_s, acc_s = refs
    else:
        part_ref, dq_ref, mine_ref, send_ref, k_s, kt_s, v_s, qt_s, dot_s, dqt_s, acc_s = refs
    step_idx = pl.program_id(0)
    z_blk, c_blk = bwd_block(where_ref, step_idx, rows_of_z)
    b = 2 * z_blk + c_blk
    bq = q_ref.shape[1]
    seq = k_s.shape[0]

    @pl.when(step_idx == 0)
    def _():
        def store(rows, block):
            acc_s[:, rows] = jnp.zeros((2 * HEAD_DIM, bq), jnp.float32) if first else part_ref[:, rows]
            k_rot_t = rotate_rows(block[:, :HEAD_DIM].T.astype(jnp.float32), cos_ref[:, rows], sin_ref[:, rows])
            kt_s[:, rows] = k_rot_t
            k_s[rows, :] = k_rot_t.T
            v_s[rows, :] = block[:, HEAD_DIM:]

        for_key_blocks(where_ref, kv_ref, kv_other_ref, seq // bq, bq, store)

    start = block_token(where_ref, b, bq)
    t_row, lo_row = row_bounds(lo_ref, start, bq, heads)
    q_blk, do_blk, o_blk = q_ref[0], do_ref[0], o_ref[0]
    deltas = []
    for h, q_rot_t in enumerate(rotated_queries(q_blk, cos_ref, sin_ref, start, bq, heads)):
        lanes = slice(h * bq, (h + 1) * bq)
        qt_s[:, lanes] = q_rot_t
        do_t = head_columns(do_blk, h).T
        dot_s[:, lanes] = do_t
        deltas.append(jnp.sum(do_t.astype(jnp.float32) * head_columns(o_blk, h).T.astype(jnp.float32), axis=0, keepdims=True))
    delta = jnp.concatenate(deltas, axis=1)
    lse = lse_ref[0]
    dqt_s[...] = jnp.zeros_like(dqt_s)

    def step(j, masked):
        key_start = pl.multiple_of(j * bk, bk)
        keys = pl.ds(key_start, bk)
        scores = dot_f32(k_s[keys, :], qt_s[...])
        probs = jnp.exp2(scores * SCALE_LOG2E - lse)
        if masked:
            probs = jnp.where(keep_mask(key_start, bk, t_row, lo_row), probs, 0.0)
        d_probs = dot_f32(v_s[keys, :], dot_s[...])
        d_scores = (probs * (d_probs - delta)).astype(jnp.bfloat16)
        acc_s[HEAD_DIM:, keys] += dot_f32(dot_s[...], probs.astype(jnp.bfloat16), COLS_OF_BOTH)
        acc_s[:HEAD_DIM, keys] += dot_f32(qt_s[...], d_scores, COLS_OF_BOTH) * SCORE_SCALE
        dqt_s[...] += dot_f32(kt_s[:, keys], d_scores)

    visit_keys(key_range(pos_ref, start, bq, bk), step)
    cos_t, sin_t = cos_ref[:, pl.ds(start, bq)], sin_ref[:, pl.ds(start, bq)]
    for h in range(heads):
        dq_rot_t = (dqt_s[:, h * bq:(h + 1) * bq] * SCORE_SCALE).astype(jnp.bfloat16).astype(jnp.float32)
        dq_ref[0, :, h * HEAD_DIM:(h + 1) * HEAD_DIM] = rotate_rows(dq_rot_t, cos_t, -sin_t).T

    @pl.when(step_idx == pl.num_programs(0) - 1)
    def _():
        if first:
            part_ref[...] = acc_s[...]
            return

        def hand_over(y, mine):
            for z in range(Z_SIZE):
                for c in range(CORE_SIZE):
                    rows = ((z * 2 + y) * 2 + c) * bq
                    e = where_ref[2] ^ c
                    if mine:
                        mine_ref[z, e] = acc_s[:, rows:rows + bq].T
                    else:
                        send_ref[z, 1 - e] = acc_s[:, rows:rows + bq].T

        for y in range(Y_SIZE):
            pl.when(where_ref[1] == y)(functools.partial(hand_over, y, True))
            pl.when(where_ref[1] != y)(functools.partial(hand_over, y, False))


def token_grads_kernel(count, *refs):
    blocks, lhs_ref, out_refs, lhs_t = refs[:count], refs[count], refs[count + 1:-1], refs[-1]
    rows = lhs_ref.shape[1]

    @pl.when(pl.program_id(0) == 0)
    def _():
        for n in range(count):
            lhs_t[:, n * rows:(n + 1) * rows] = lhs_ref[n].T

    total = sum(dot_f32(lhs_t[:, n * rows:(n + 1) * rows], blocks[n][...]) for n in range(count))
    start = 0
    for ref in out_refs:
        if ref.shape[0] == blocks[0].shape[1]:
            size = ref.shape[1]
            ref[...] = total[start:start + size, :].T.astype(ref.dtype)
        else:
            size = ref.shape[0]
            ref[...] = total[start:start + size, :].astype(ref.dtype)
        start += size


def token_grads(blocks, lhs, outs, tile=512):
    rows, model = blocks[0].shape
    width = lhs.shape[2]
    specs = [pl.BlockSpec((tile, shape[1]), lambda i: (i, 0)) if shape[0] == model else pl.BlockSpec((shape[0], tile), lambda i: (0, i)) for shape, _ in outs]
    return pl.pallas_call(
        functools.partial(token_grads_kernel, len(blocks)),
        out_shape=[jax.ShapeDtypeStruct(*out) for out in outs], grid=(model // tile,),
        in_specs=[pl.BlockSpec((rows, tile), lambda i: (0, i)) for _ in blocks] + [pl.BlockSpec(lhs.shape, lambda i: (0, 0, 0))], out_specs=specs,
        scratch_shapes=[pltpu.VMEM((width, len(blocks) * rows), jnp.bfloat16)],
        compiler_params=pltpu.CompilerParams(dimension_semantics=('arbitrary',), vmem_limit_bytes=48 << 20),
        cost_estimate=pl.CostEstimate(flops=2 * len(blocks) * rows * model * width, bytes_accessed=2 * len(blocks) * rows * model, transcendentals=0),
    )(*blocks, lhs)


def pick_kernel(count, where_ref, *refs):
    sources, outs, sems = refs[:count * Z_SIZE], refs[count * Z_SIZE:-1], refs[-1]

    def copy(n, k):
        return pltpu.make_async_copy(sources[n * Z_SIZE + k], outs[n], sems.at[n])

    for n in range(count):
        for k in range(Z_SIZE):
            pl.when(where_ref[0] == k)(lambda n=n, k=k: copy(n, k).start())
    for n in range(count):
        copy(n, 0).wait()


def pick(where, *choices):
    shape = choices[0][0].shape
    return pl.pallas_call(
        functools.partial(pick_kernel, len(choices)), out_shape=[jax.ShapeDtypeStruct(shape, jnp.bfloat16)] * len(choices),
        grid_spec=pltpu.PrefetchScalarGridSpec(
            num_scalar_prefetch=1, grid=(1,), in_specs=[pl.BlockSpec(memory_space=pl.ANY)] * (len(choices) * Z_SIZE), out_specs=[full_spec(shape)] * len(choices),
            scratch_shapes=[pltpu.SemaphoreType.DMA((len(choices),))]),
        compiler_params=pltpu.CompilerParams(dimension_semantics=('arbitrary',), vmem_limit_bytes=32 << 20),
        cost_estimate=pl.CostEstimate(flops=1000000, bytes_accessed=8000000, transcendentals=0),
    )(where, *(arr for choice in choices for arr in choice))


def pair_add_kernel(a_ref, b_ref, c_ref, d_ref, ab_ref, cd_ref):
    for left, right, out in ((a_ref, b_ref, ab_ref), (c_ref, d_ref, cd_ref)):
        out[...] = (left[...].astype(jnp.float32) + right[...].astype(jnp.float32)).astype(jnp.bfloat16)


def pair_add(*operands):
    rows, model = operands[0].shape
    tile = model // 4
    spec = pl.BlockSpec((rows, tile), lambda i: (0, i))
    return pl.pallas_call(
        pair_add_kernel, out_shape=[jax.ShapeDtypeStruct((rows, model), jnp.bfloat16)] * 2, grid=(model // tile,), in_specs=[spec] * 4, out_specs=[spec] * 2,
        compiler_params=pltpu.CompilerParams(dimension_semantics=('arbitrary',), vmem_limit_bytes=32 << 20),
        cost_estimate=pl.CostEstimate(flops=4 * rows * model, bytes_accessed=12 * rows * model, transcendentals=0),
    )(*operands)


def finish_kernel(where_ref, mine_ref, other_ref, cos_ref, sin_ref, out_ref):
    for z in range(Z_SIZE):
        slot = lax.rem(where_ref[0] - z + Z_SIZE, Z_SIZE)
        for e in range(CORE_SIZE):
            total = mine_ref[z, e] + other_ref[z, e]
            dk = total[:, :HEAD_DIM].astype(jnp.bfloat16).astype(jnp.float32)
            out_ref[slot, e, :, :HEAD_DIM] = (dk * cos_ref[z, e] + pltpu.roll(dk, HEAD_DIM // 2, 1) * sin_ref[z, e]).astype(jnp.bfloat16)
            out_ref[slot, e, :, HEAD_DIM:] = total[:, HEAD_DIM:].astype(jnp.bfloat16)


def finish_key_grads(where, *operands):
    return pl.pallas_call(
        finish_kernel, out_shape=jax.ShapeDtypeStruct(operands[0].shape, jnp.bfloat16),
        grid_spec=pltpu.PrefetchScalarGridSpec(num_scalar_prefetch=1, grid=(1,), in_specs=[full_spec(arr.shape) for arr in operands], out_specs=full_spec(operands[0].shape)),
        compiler_params=pltpu.CompilerParams(dimension_semantics=('arbitrary',), vmem_limit_bytes=32 << 20),
        cost_estimate=pl.CostEstimate(flops=1000000, bytes_accessed=8000000, transcendentals=0),
    )(where, *operands)


def full_spec(shape):
    return pl.BlockSpec(shape, lambda b, *_: (0,) * len(shape))


def attend(where, positions, q_slots, kv_slots, kv_other, cos_t, sin_t, lo_all, bk, blocks, before=()):
    slots, bq, width = q_slots.shape
    seq = positions.shape[0]
    heads = width // HEAD_DIM
    lanes = heads * bq
    shared = (kv_slots, kv_other, cos_t, sin_t, lo_all)
    block = pl.BlockSpec((1, bq, width), lambda i, where_ref, _: (slot_of(where_ref, (i + blocks[0]) // 2, (i + blocks[0]) % 2), 0, 0))
    work = (blocks[1] - blocks[0]) * bq * heads * seq * HEAD_DIM
    return pl.pallas_call(
        functools.partial(fwd_kernel, heads, bk, blocks[0]),
        out_shape=(jax.ShapeDtypeStruct(q_slots.shape, jnp.bfloat16), jax.ShapeDtypeStruct((slots, 1, lanes), jnp.float32)),
        grid_spec=pltpu.PrefetchScalarGridSpec(
            num_scalar_prefetch=2, grid=(blocks[1] - blocks[0],),
            in_specs=[block] + [full_spec(arr.shape) for arr in shared] + [pl.BlockSpec(memory_space=pl.ANY)] * len(before),
            out_specs=(block, pl.BlockSpec((1, 1, lanes), lambda i, *_: (i + blocks[0], 0, 0))),
            scratch_shapes=[pltpu.VMEM((seq, HEAD_DIM), jnp.bfloat16), pltpu.VMEM((HEAD_DIM, seq), jnp.bfloat16), pltpu.VMEM((HEAD_DIM, lanes), jnp.bfloat16),
                            pltpu.VMEM((1, lanes), jnp.float32), pltpu.VMEM((1, lanes), jnp.float32), pltpu.VMEM((HEAD_DIM, lanes), jnp.float32)]),
        input_output_aliases={3 + len(shared) + n: n for n in range(len(before))},
        compiler_params=pltpu.CompilerParams(dimension_semantics=('arbitrary',), vmem_limit_bytes=48 << 20),
        cost_estimate=pl.CostEstimate(flops=4 * work, bytes_accessed=4 * slots * bq * width + 8 * seq * HEAD_DIM, transcendentals=work // (2 * HEAD_DIM)),
        name='attend_fwd',
    )(where, positions, q_slots, *shared, *before)


def attend_backward(where, positions, q_slots, do_blocks, o_slots, kv_slots, kv_other, cos_t, sin_t, lo_all, lse, bk, rows_of_z, part=None):
    count, bq, width = do_blocks.shape
    seq = positions.shape[0]
    heads = width // HEAD_DIM
    lanes = heads * bq
    shared = (kv_slots, kv_other, cos_t, sin_t, lo_all)

    def slot_index(i, where_ref, _):
        return (slot_of(where_ref, *bwd_block(where_ref, i, rows_of_z)), 0, 0)

    def lse_index(i, where_ref, _):
        z_blk, c_blk = bwd_block(where_ref, i, rows_of_z)
        return (2 * z_blk + c_blk, 0, 0)

    block = pl.BlockSpec((1, bq, width), slot_index)
    local = pl.BlockSpec((1, bq, width), lambda i, *_: (i, 0, 0))
    operands = [q_slots, do_blocks, o_slots, *shared, lse]
    in_specs = [block, local, block] + [full_spec(arr.shape) for arr in shared] + [pl.BlockSpec((1, 1, lanes), lse_index)]
    part_shape, final_shape = (2 * HEAD_DIM, seq), (Z_SIZE, CORE_SIZE, bq, 2 * HEAD_DIM)
    grads = [part_shape] if part is None else [final_shape] * 2
    if part is not None:
        operands.append(part)
        in_specs.append(full_spec(part_shape))
    work = count * bq * heads * seq * HEAD_DIM
    return pl.pallas_call(
        functools.partial(bwd_kernel, heads, bk, rows_of_z),
        out_shape=[jax.ShapeDtypeStruct(do_blocks.shape, jnp.bfloat16)] + [jax.ShapeDtypeStruct(shape, jnp.float32) for shape in grads],
        grid_spec=pltpu.PrefetchScalarGridSpec(
            num_scalar_prefetch=2, grid=(count,), in_specs=in_specs, out_specs=[local] + [full_spec(shape) for shape in grads],
            scratch_shapes=[pltpu.VMEM((seq, HEAD_DIM), jnp.bfloat16), pltpu.VMEM((HEAD_DIM, seq), jnp.bfloat16), pltpu.VMEM((seq, HEAD_DIM), jnp.bfloat16),
                            pltpu.VMEM((HEAD_DIM, lanes), jnp.bfloat16), pltpu.VMEM((HEAD_DIM, lanes), jnp.bfloat16), pltpu.VMEM((HEAD_DIM, lanes), jnp.float32),
                            pltpu.VMEM((2 * HEAD_DIM, seq), jnp.float32)]),
        compiler_params=pltpu.CompilerParams(dimension_semantics=('arbitrary',), vmem_limit_bytes=58 << 20),
        cost_estimate=pl.CostEstimate(flops=10 * work, bytes_accessed=8 * count * bq * width + 24 * seq * HEAD_DIM, transcendentals=work // (2 * HEAD_DIM)),
        name='attend_bwd',
    )(where, positions, *operands)


def solution(mesh):
    def member(z, y, c):
        return (z * Y_SIZE + y) * CORE_SIZE + c

    every = [(z, y, c) for z in range(Z_SIZE) for y in range(Y_SIZE) for c in range(CORE_SIZE)]

    def permuter(target, senders=range(Z_SIZE)):
        pairs = [(member(*src), member(*target(*src))) for src in every if src[0] in senders]
        return lambda val: lax.ppermute(val, 'tp', pairs)

    swap_core = permuter(lambda z, y, c: (z, y, 1 - c))
    swap_y = permuter(lambda z, y, c: (z, 1 - y, c))
    swap_same_head = permuter(lambda z, y, c: (z, 1 - y, 1 - c))
    ring = permuter(lambda z, y, c: ((z + 1) % Z_SIZE, y, c))
    ring_back = {k: permuter(lambda z, y, c, k=k: ((z - k) % Z_SIZE, y, c)) for k in (1, 2)}
    hops = range(1, Z_SIZE)
    gather_right = {k: permuter(lambda z, y, c: (z + 1, y, c), range(k - 1, Z_SIZE - 1)) for k in hops}
    gather_left = {k: permuter(lambda z, y, c: (z - 1, y, c), range(1, Z_SIZE - k + 1)) for k in hops}
    scatter_right = {k: permuter(lambda z, y, c: (z + 1, y, c), range(0, k)) for k in hops}
    scatter_left = {k: permuter(lambda z, y, c: (z - 1, y, c), range(Z_SIZE - k, Z_SIZE)) for k in hops}
    z_swaps = {k: permuter(lambda z, y, c, k=k: (z ^ k, y, c)) for k in hops}

    def after(val, *deps):
        return lax.optimization_barrier((val,) + deps)[0]

    def device_step(x_blk, dy_blk, pos_all, norm_gain, wq_loc, wk_all, wv_all, wo_loc):
        seq_len = pos_all.shape[0]
        bq = seq_len // (Z_SIZE * Y_SIZE * CORE_SIZE)
        bk = 2 * bq
        model = x_blk.shape[1]
        idx = lax.axis_index('tp')
        z_idx, y_idx, c_idx = idx // (Y_SIZE * CORE_SIZE), (idx // CORE_SIZE) % Y_SIZE, idx % CORE_SIZE
        where = jnp.stack([z_idx, y_idx, c_idx])
        on_core0 = c_idx == 0
        pair = wq_loc.shape[1]
        kv_own = Y_SIZE * z_idx + (y_idx ^ c_idx)

        def select(first, second):
            return jnp.where(on_core0, first, second)

        def flip_core(arr):
            return arr[:, ::-1]

        def slots(arrs):
            return jnp.concatenate([arr[None] for arr in arrs], axis=0)

        def interleave(own, partner):
            return [blk for both in zip(own, partner) for blk in both]

        x_f32 = x_blk.astype(jnp.float32)
        hidden, x_hat, inv_rms = norm_forward(x_f32, norm_gain)

        h_own = [hidden]
        for s in hops:
            h_own.append(ring(h_own[-1]))
        h_pair = []
        for blk in h_own:
            h_pair.append(swap_core(blk))

        def slot_order(w_own, w_core, w_y, w_both):
            return [select(w_own, w_y), select(w_core, w_both), select(w_both, w_core), select(w_y, w_own)]

        wq_y = swap_y(wq_loc)
        wq_core = swap_core(wq_loc)
        q_cols = slot_order(wq_loc, wq_core, wq_y, swap_core(wq_y))
        wo_y = swap_y(wo_loc)
        o_rows = (wo_loc, swap_core(wo_loc), wo_y, swap_core(wo_y))

        def kv_columns(head):
            return [lax.dynamic_slice_in_dim(w, head * HEAD_DIM, HEAD_DIM, axis=1) for w in (wk_all, wv_all)]

        w_q = lax.optimization_barrier(jnp.concatenate(q_cols, axis=1))
        w_kv = lax.optimization_barrier(jnp.concatenate(kv_columns(kv_own) + kv_columns(kv_own ^ 1), axis=1))
        kv_heads = [lax.rem(kv_own + k * Y_SIZE, Y_SIZE * Z_SIZE) for k in range(3)]
        w_kv_all = lax.optimization_barrier(jnp.concatenate([cols for head in kv_heads for h in (head, head ^ 1) for cols in kv_columns(h)], axis=1))
        w_own = jnp.concatenate([w_q[:, :2 * pair], w_kv[:, :2 * HEAD_DIM]], axis=1)
        w_mix = jnp.concatenate(slot_order(*o_rows), axis=0)
        lo_all = (lax.iota(jnp.int32, seq_len) - pos_all)[None, :]
        cos_t, sin_t = rope_tables(pos_all)

        def my_tables(lead, tail):
            parts = jnp.concatenate([lead.T, tail.T], axis=1).reshape(Z_SIZE, Y_SIZE, CORE_SIZE, bq, HEAD_DIM)
            parts = lax.dynamic_index_in_dim(parts, y_idx, 1, keepdims=False)
            return select(parts, flip_core(parts))

        cos_my, sin_my = my_tables(cos_t, cos_t), my_tables(sin_t, -sin_t)

        qkv = []
        for s in range(Z_SIZE):
            qkv += [dot_f32(blk, w_own).astype(jnp.bfloat16) for blk in (h_own[s], h_pair[s])]
        kv_blocks = [blk[:, 2 * pair:] for blk in qkv]
        early = SLOTS - CORE_SIZE
        kv_other_early = swap_same_head(slots(kv_blocks[:early]))
        kv_other_late = swap_same_head(slots(kv_blocks[early:]))
        kv_other = jnp.concatenate([kv_other_early, kv_other_late], axis=0)
        q_slots, kv_slots = slots([blk[:, :2 * pair] for blk in qkv]), slots(kv_blocks)

        g_own = []
        for s, blk in enumerate(h_own):
            g_own.append(swap_y(after(blk, kv_other_late) if s else blk))

        right, left = {0: after(dy_blk, h_own[-1])}, {}
        left[0] = right[0]
        for k in hops:
            right[k] = gather_right[k](right[k - 1])
            left[k] = gather_left[k](left[k - 1])
            right[k], left[k] = lax.optimization_barrier((right[k], left[k]))
        dy_one, dy_two = pick(where, (left[1], dy_blk, right[1], right[2]), (left[2], left[1], dy_blk, right[1]))
        dy_zero, dy_three = pick(where, (dy_blk, right[1], right[2], right[3]), (left[3], left[2], left[1], dy_blk))
        dy_own = [dy_zero, dy_one, dy_two, dy_three]
        dy_pair = []
        for blk in dy_own:
            dy_pair.append(swap_core(blk))
        dy_slots = interleave(dy_own, dy_pair)

        def mirrored(lines):
            return jnp.concatenate([lax.dynamic_slice_in_dim(lines, lax.rem(z_idx - s + Z_SIZE, Z_SIZE), 1, axis=0) for s in range(Z_SIZE)], axis=0)

        forward = functools.partial(attend, where, pos_all, q_slots, kv_slots, kv_other, cos_t, sin_t, lo_all, bk)
        before = forward((0, FIRST_CALL))
        o_slots, lse = forward((FIRST_CALL, SLOTS), before)
        by_line = (Z_SIZE, CORE_SIZE, bq, -1)
        o_lines = o_slots.reshape(by_line)
        o_partner = swap_core(o_slots).reshape(by_line)
        o_mine = jnp.concatenate([o_lines[:, 0], o_partner[:, 1]], axis=-1)

        def pair_sides(own, partner):
            first, last = own[..., :pair], partner[..., pair:2 * pair]
            return select(first, last), select(last, first)

        def by_block(arr):
            return arr.reshape((SLOTS,) + arr.shape[2:])

        o_sides = jnp.concatenate(pair_sides(o_lines, flip_core(o_partner)), axis=-1)
        o_sides = lax.optimization_barrier(by_block(mirrored(o_sides)))
        mix_part = []
        for s in range(Z_SIZE):
            mix_part.append(lax.optimization_barrier(dot_f32(o_mine[s], w_mix).astype(jnp.bfloat16)))

        def plus(*parts):
            return sum(part.astype(jnp.float32) for part in parts)

        sum_right, sum_left = mix_part[1], mix_part[Z_SIZE - 1]
        for k in hops:
            if k > 1:
                sum_right, sum_left = lax.optimization_barrier((sum_right, sum_left))
                sum_right, sum_left = pair_add(mix_part[k], sum_right, mix_part[Z_SIZE - k], sum_left)
            sum_right = scatter_right[k](sum_right)
            sum_left = scatter_left[k](sum_left)
        result = (x_f32 + plus(mix_part[0], sum_right, sum_left)).astype(jnp.bfloat16)

        d_o = []
        for n in range(Z_SIZE):
            d_o.append([dot_f32(blk, w_mix[:2 * pair], COLS_OF_BOTH).astype(jnp.bfloat16) for blk in (dy_own[n], dy_pair[n])])
        shared = (o_slots, kv_slots, kv_other, cos_t, sin_t, lo_all, lse, bk)
        dq_early, dkv_part = attend_backward(where, pos_all, q_slots, slots(d_o[1] + d_o[2]), *shared, EARLY)
        dq_early_partner = swap_core(dq_early)
        early_own, early_partner = lax.optimization_barrier((dq_early, dq_early_partner))
        early_keep, early_send = pair_sides(early_own, early_partner.reshape(2, CORE_SIZE, bq, -1)[:, ::-1].reshape(early_own.shape))
        early_theirs = swap_y(early_send)
        dq_late, dkv_mine, dkv_send = attend_backward(where, pos_all, q_slots, slots(d_o[0] + d_o[3]), *shared, LATE, dkv_part)
        dkv_theirs = swap_same_head(dkv_send)
        dq_late_partner = swap_core(dq_late)

        late_partner = dq_late_partner.reshape(2, CORE_SIZE, bq, -1)[:, ::-1].reshape(dq_late.shape)
        late_keep, late_send = pair_sides(dq_late, late_partner)

        def natural(early, late):
            return jnp.concatenate([late[:2], early, late[2:]], axis=0).reshape((Z_SIZE, CORE_SIZE) + early.shape[1:])

        q_rows = jnp.concatenate([natural(dq_early, dq_late)[:, 0], natural(early_partner, dq_late_partner)[:, 1]], axis=-1)
        dq_rows = [lax.dynamic_index_in_dim(q_rows, lax.rem(z_idx - s + Z_SIZE, Z_SIZE), 0, keepdims=False) for s in range(Z_SIZE)]
        halves = [slice(0, model // 2), slice(model // 2, model)]
        dh_sum = []
        for n, cols in enumerate(halves):
            dh_sum.append(dot_f32(dq_rows[1], w_q[cols], COLS_OF_BOTH).astype(jnp.bfloat16))
            dh_sum[n] = ring(dh_sum[n])

        dkv_lines = finish_key_grads(where, dkv_mine, dkv_theirs, cos_my, sin_my)
        dkv_partner = flip_core(swap_core(dkv_lines))
        dkv_rows = jnp.concatenate([dkv_lines[:, 0], dkv_partner[:, 0]], axis=-1)
        dkv_next = {}
        for k in ring_back:
            dkv_next[k] = ring_back[k](dkv_rows[k])

        def kv_part(rows, weights, cols):
            return dot_f32(rows, weights[cols], COLS_OF_BOTH)

        for s in hops[1:]:
            for n, cols in enumerate(halves):
                part = dot_f32(dq_rows[s], w_q[cols], COLS_OF_BOTH)
                if s == hops[-1]:
                    part = part + kv_part(dkv_rows[s], w_kv, cols)
                dh_sum[n] = (part + dh_sum[n].astype(jnp.float32)).astype(jnp.bfloat16)
                if s == hops[-1] and n == 0:
                    dh_sum[n], result = lax.optimization_barrier((dh_sum[n], result))
                dh_sum[n] = ring(dh_sum[n])
        kv_cols = jnp.concatenate([dkv_rows[0], dkv_next[1], dkv_next[2]], axis=1)
        dh_own = lax.optimization_barrier([dot_f32(dq_rows[0], w_q[cols], COLS_OF_BOTH) + kv_part(kv_cols, w_kv_all, cols) for cols in halves])
        dh_rows = jnp.concatenate([(own + part.astype(jnp.float32)).astype(jnp.bfloat16) for own, part in zip(dh_own, dh_sum)], axis=1)

        g_pair = [swap_core(blk) for blk in lax.optimization_barrier((*g_own, dq_late))[:Z_SIZE]]
        kv_keep = select(dkv_lines[..., :HEAD_DIM], dkv_partner[..., HEAD_DIM:])
        kv_send = select(dkv_partner[..., :HEAD_DIM], dkv_lines[..., HEAD_DIM:])
        kv_theirs = swap_y(kv_send)
        late_theirs = swap_y(late_send)

        def rows_of(early, late, kv_lines):
            return by_block(jnp.concatenate([mirrored(natural(early, late)), kv_lines], axis=-1))

        d_keep = rows_of(early_keep, late_keep, kv_keep)
        d_theirs = rows_of(early_theirs, late_theirs, kv_theirs)

        dwo_keep, dwo_send = token_grads(dy_slots, o_sides, [((pair, model), jnp.float32)] * 2)
        theirs_first = swap_y(dwo_send[:, halves[0]])
        theirs_last = swap_y(dwo_send[:, halves[1]])

        d_wq, kv_mine_sum = token_grads([blks[s] for mine, theirs in ((h_own, h_pair), (g_own, g_pair)) for s in range(Z_SIZE) for blks in (mine, theirs)], jnp.concatenate([d_keep, d_theirs], axis=0),
                                        [((model, pair), jnp.bfloat16), ((model, HEAD_DIM), jnp.float32)])
        kv_other_sum = swap_core(kv_mine_sum)
        d_wk = select(kv_mine_sum, kv_other_sum)
        d_wv = select(kv_other_sum, kv_mine_sum)

        d_input, dg_part = norm_backward(dh_rows, x_hat, inv_rms, norm_gain)
        grad_x = (dy_blk.astype(jnp.float32) + d_input).astype(jnp.bfloat16)
        for near, far, both in ((swap_core, swap_y, swap_same_head), (z_swaps[1], z_swaps[2], z_swaps[3])):
            dg_part = (dg_part + near(dg_part)) + (far(dg_part) + both(dg_part))
            if near is swap_core:
                theirs_last = after(theirs_last, dg_part)
        d_wo = (dwo_keep + jnp.concatenate([theirs_first, theirs_last], axis=1)).astype(jnp.bfloat16)
        return result, grad_x, d_wq, d_wk, d_wv, d_wo, dg_part

    specs_in = (P(('dp', 'tp'), None), P(('dp', 'tp'), None), P('dp'), P(), P(None, 'tp'), P(), P(), P('tp', None))
    specs_out = (P(('dp', 'tp'), None), P(('dp', 'tp'), None), P('dp', 'tp'), P('dp', 'tp'), P('dp', 'tp'), P(('dp', 'tp'), None), P('dp'))
    return jax.shard_map(device_step, mesh=mesh, in_specs=specs_in, out_specs=specs_out, check_vma=False)
```

```python
import functools
import jax
import jax.numpy as jnp
from jax import lax
from jax.experimental import pallas as pl
from jax.experimental.pallas import tpu as pltpu
from jax.sharding import PartitionSpec as P

HEAD_DIM = 128
SCORE_SCALE = HEAD_DIM ** -0.5
SCALE_LOG2E = SCORE_SCALE * 1.4426950408889634
ROPE_THETA = 1000000.0
NORM_EPS = 1e-05
MASKED = -1e30
Z_SIZE = 4
Y_SIZE = 2
CORE_SIZE = 2
SLOTS = Z_SIZE * CORE_SIZE
EARLY, LATE = (1, 2), (0, 3)
NATURAL = (((1,), (0,)), ((), ()))
COLS_OF_BOTH = (((1,), (1,)), ((), ()))


def dot_f32(lhs, rhs, dims=NATURAL):
    return lax.dot_general(lhs, rhs, dims, preferred_element_type=jnp.float32)


def rope_tables(positions):
    exponents = jnp.arange(0, HEAD_DIM, 2, dtype=jnp.float32) / HEAD_DIM
    angles = jnp.power(ROPE_THETA, -exponents)[:, None] * positions.astype(jnp.float32)[None, :]
    return jnp.cos(angles), jnp.sin(angles)


def rotate_rows(t_f32, cos_t, sin_t):
    lead_half, tail_half = t_f32[:HEAD_DIM // 2], t_f32[HEAD_DIM // 2:]
    return jnp.concatenate([lead_half * cos_t - tail_half * sin_t, tail_half * cos_t + lead_half * sin_t], axis=0).astype(jnp.bfloat16)


def norm_forward(x_f32, norm_gain):
    inv_rms = lax.rsqrt(jnp.mean(x_f32 * x_f32, axis=-1, keepdims=True) + NORM_EPS)
    x_hat = x_f32 * inv_rms
    return (x_hat * norm_gain).astype(jnp.bfloat16), x_hat, inv_rms


def norm_backward(d_hidden, x_hat, inv_rms, norm_gain):
    d_f32 = d_hidden.astype(jnp.float32)
    d_gain = jnp.sum(d_f32 * x_hat, axis=0)
    scaled = d_f32 * norm_gain
    d_input = inv_rms * (scaled - x_hat * jnp.mean(scaled * x_hat, axis=-1, keepdims=True))
    return d_input, d_gain


def slot_of(where_ref, z, c):
    return 2 * lax.rem(where_ref[0] - z + Z_SIZE, Z_SIZE) + (where_ref[2] ^ c)


def slot_of_other(where_ref, z, c):
    return 2 * lax.rem(where_ref[0] - z + Z_SIZE, Z_SIZE) + (1 - (where_ref[2] ^ c))


def block_token(where_ref, b, bq):
    return pl.multiple_of((b // 2) * (4 * bq) + where_ref[1] * (2 * bq) + (b % 2) * bq, bq)


def key_range(pos_ref, start, bq, bk):
    lo_first, lo_last = start - pos_ref[start], start + bq - 1 - pos_ref[start + bq - 1]
    return lo_first // bk, (start + bq - 1) // bk + 1, (lo_last + bk - 1) // bk, (start + 1) // bk


def tile_lanes(row, heads):
    return jnp.concatenate([row] * heads, axis=1)


def row_bounds(lo_ref, start, bq, heads):
    tok = start + lax.broadcasted_iota(jnp.int32, (1, bq), 1)
    return tile_lanes(tok, heads), tile_lanes(lo_ref[:, pl.ds(start, bq)], heads)


def keep_mask(key_start, bk, t_row, lo_row):
    key_idx = key_start + lax.broadcasted_iota(jnp.int32, (bk, t_row.shape[1]), 0)
    return (key_idx <= t_row) & (key_idx >= lo_row)


def head_columns(block, h):
    return block[:, h * HEAD_DIM:(h + 1) * HEAD_DIM]


def rotated_queries(q_blk, cos_ref, sin_ref, start, bq, heads):
    cos_t, sin_t = cos_ref[:, pl.ds(start, bq)], sin_ref[:, pl.ds(start, bq)]
    return [rotate_rows(head_columns(q_blk, h).T.astype(jnp.float32), cos_t, sin_t) for h in range(heads)]


def visit_keys(bounds, step):
    first, end, inner_first, inner_end = bounds

    def visit(j, carry):
        inner = (j >= inner_first) & (j < inner_end)

        @pl.when(inner)
        def _():
            step(j, False)

        @pl.when(jnp.logical_not(inner))
        def _():
            step(j, True)

        return carry

    lax.fori_loop(first, end, visit, 0)


def for_key_blocks(where_ref, mine_ref, theirs_ref, count, bq, store):
    def visit(n, carry):
        z, y, c = n // 4, (n // 2) % 2, n % 2
        block = jnp.where(y == where_ref[1], mine_ref[slot_of(where_ref, z, c)], theirs_ref[slot_of_other(where_ref, z, c)])
        store(pl.ds(pl.multiple_of(n * bq, bq), bq), block)
        return carry

    lax.fori_loop(0, count, visit, 0)


def fwd_kernel(heads, bk, where_ref, pos_ref, q_ref, kv_ref, kv_other_ref, cos_ref, sin_ref, lo_ref, o_ref, lse_ref, k_s, vt_s, qt_s, m_s, l_s, acc_s):
    b = pl.program_id(0)
    bq = q_ref.shape[1]
    seq = k_s.shape[0]

    @pl.when(b == 0)
    def _():
        def store(rows, block):
            k_s[rows, :] = rotate_rows(block[:, :HEAD_DIM].T.astype(jnp.float32), cos_ref[:, rows], sin_ref[:, rows]).T
            vt_s[:, rows] = block[:, HEAD_DIM:].T

        for_key_blocks(where_ref, kv_ref, kv_other_ref, seq // bq, bq, store)

    start = block_token(where_ref, b, bq)
    t_row, lo_row = row_bounds(lo_ref, start, bq, heads)
    q_blk = q_ref[0]
    qt_s[...] = jnp.concatenate(rotated_queries(q_blk, cos_ref, sin_ref, start, bq, heads), axis=1)
    m_s[...] = jnp.full_like(m_s, MASKED)
    l_s[...] = jnp.zeros_like(l_s)
    acc_s[...] = jnp.zeros_like(acc_s)

    def step(j, masked):
        key_start = pl.multiple_of(j * bk, bk)
        keys = pl.ds(key_start, bk)
        scores = dot_f32(k_s[keys, :], qt_s[...])
        if masked:
            scores = jnp.where(keep_mask(key_start, bk, t_row, lo_row), scores, MASKED)
        m_old = m_s[...]
        m_new = jnp.maximum(m_old, jnp.max(scores, axis=0, keepdims=True))
        probs = jnp.exp2(scores * SCALE_LOG2E - m_new * SCALE_LOG2E)
        alpha = jnp.exp2((m_old - m_new) * SCALE_LOG2E)
        m_s[...] = m_new
        l_s[...] = l_s[...] * alpha + jnp.sum(probs, axis=0, keepdims=True)
        acc_s[...] = acc_s[...] * alpha + dot_f32(vt_s[:, keys], probs.astype(jnp.bfloat16))

    visit_keys(key_range(pos_ref, start, bq, bk), step)
    out_t = (acc_s[...] / l_s[...]).astype(jnp.bfloat16)
    for h in range(heads):
        o_ref[0, :, h * HEAD_DIM:(h + 1) * HEAD_DIM] = out_t[:, h * bq:(h + 1) * bq].T
    lse_ref[0] = m_s[...] * SCALE_LOG2E + jnp.log2(l_s[...])


def bwd_block(where_ref, step, rows):
    return rows[0] + (rows[1] - rows[0]) * (step // 2), where_ref[2] ^ (step % 2)


def bwd_kernel(heads, bk, rows_of_z, where_ref, pos_ref, q_ref, do_ref, o_ref, kv_ref, kv_other_ref, cos_ref, sin_ref, lo_ref, lse_ref, *refs):
    first = rows_of_z == EARLY
    if first:
        dq_ref, part_ref, k_s, kt_s, v_s, qt_s, dot_s, dqt_s, acc_s = refs
    else:
        part_ref, dq_ref, mine_ref, send_ref, k_s, kt_s, v_s, qt_s, dot_s, dqt_s, acc_s = refs
    step_idx = pl.program_id(0)
    z_blk, c_blk = bwd_block(where_ref, step_idx, rows_of_z)
    b = 2 * z_blk + c_blk
    bq = q_ref.shape[1]
    seq = k_s.shape[0]

    @pl.when(step_idx == 0)
    def _():
        def store(rows, block):
            acc_s[:, rows] = jnp.zeros((2 * HEAD_DIM, bq), jnp.float32) if first else part_ref[:, rows]
            k_rot_t = rotate_rows(block[:, :HEAD_DIM].T.astype(jnp.float32), cos_ref[:, rows], sin_ref[:, rows])
            kt_s[:, rows] = k_rot_t
            k_s[rows, :] = k_rot_t.T
            v_s[rows, :] = block[:, HEAD_DIM:]

        for_key_blocks(where_ref, kv_ref, kv_other_ref, seq // bq, bq, store)

    start = block_token(where_ref, b, bq)
    t_row, lo_row = row_bounds(lo_ref, start, bq, heads)
    q_blk, do_blk, o_blk = q_ref[0], do_ref[0], o_ref[0]
    deltas = []
    for h, q_rot_t in enumerate(rotated_queries(q_blk, cos_ref, sin_ref, start, bq, heads)):
        lanes = slice(h * bq, (h + 1) * bq)
        qt_s[:, lanes] = q_rot_t
        do_t = head_columns(do_blk, h).T
        dot_s[:, lanes] = do_t
        deltas.append(jnp.sum(do_t.astype(jnp.float32) * head_columns(o_blk, h).T.astype(jnp.float32), axis=0, keepdims=True))
    delta = jnp.concatenate(deltas, axis=1)
    lse = lse_ref[0]
    dqt_s[...] = jnp.zeros_like(dqt_s)

    def step(j, masked):
        key_start = pl.multiple_of(j * bk, bk)
        keys = pl.ds(key_start, bk)
        scores = dot_f32(k_s[keys, :], qt_s[...])
        probs = jnp.exp2(scores * SCALE_LOG2E - lse)
        if masked:
            probs = jnp.where(keep_mask(key_start, bk, t_row, lo_row), probs, 0.0)
        d_probs = dot_f32(v_s[keys, :], dot_s[...])
        d_scores = (probs * (d_probs - delta)).astype(jnp.bfloat16)
        acc_s[HEAD_DIM:, keys] += dot_f32(dot_s[...], probs.astype(jnp.bfloat16), COLS_OF_BOTH)
        acc_s[:HEAD_DIM, keys] += dot_f32(qt_s[...], d_scores, COLS_OF_BOTH) * SCORE_SCALE
        dqt_s[...] += dot_f32(kt_s[:, keys], d_scores)

    visit_keys(key_range(pos_ref, start, bq, bk), step)
    cos_t, sin_t = cos_ref[:, pl.ds(start, bq)], sin_ref[:, pl.ds(start, bq)]
    for h in range(heads):
        dq_rot_t = (dqt_s[:, h * bq:(h + 1) * bq] * SCORE_SCALE).astype(jnp.bfloat16).astype(jnp.float32)
        dq_ref[0, :, h * HEAD_DIM:(h + 1) * HEAD_DIM] = rotate_rows(dq_rot_t, cos_t, -sin_t).T

    @pl.when(step_idx == pl.num_programs(0) - 1)
    def _():
        if first:
            part_ref[...] = acc_s[...]
            return

        def hand_over(y, mine):
            for z in range(Z_SIZE):
                for c in range(CORE_SIZE):
                    rows = ((z * 2 + y) * 2 + c) * bq
                    e = where_ref[2] ^ c
                    if mine:
                        mine_ref[z, e] = acc_s[:, rows:rows + bq].T
                    else:
                        send_ref[z, 1 - e] = acc_s[:, rows:rows + bq].T

        for y in range(Y_SIZE):
            pl.when(where_ref[1] == y)(functools.partial(hand_over, y, True))
            pl.when(where_ref[1] != y)(functools.partial(hand_over, y, False))


def token_grads_kernel(count, *refs):
    blocks, lhs_ref, out_refs, lhs_t = refs[:count], refs[count], refs[count + 1:-1], refs[-1]
    rows = lhs_ref.shape[1]

    @pl.when(pl.program_id(0) == 0)
    def _():
        for n in range(count):
            lhs_t[:, n * rows:(n + 1) * rows] = lhs_ref[n].T

    total = sum(dot_f32(lhs_t[:, n * rows:(n + 1) * rows], blocks[n][...]) for n in range(count))
    start = 0
    for ref in out_refs:
        if ref.shape[0] == blocks[0].shape[1]:
            size = ref.shape[1]
            ref[...] = total[start:start + size, :].T.astype(ref.dtype)
        else:
            size = ref.shape[0]
            ref[...] = total[start:start + size, :].astype(ref.dtype)
        start += size


def token_grads(blocks, lhs, outs, tile=512):
    rows, model = blocks[0].shape
    width = lhs.shape[2]
    specs = [pl.BlockSpec((tile, shape[1]), lambda i: (i, 0)) if shape[0] == model else pl.BlockSpec((shape[0], tile), lambda i: (0, i)) for shape, _ in outs]
    return pl.pallas_call(
        functools.partial(token_grads_kernel, len(blocks)),
        out_shape=[jax.ShapeDtypeStruct(*out) for out in outs], grid=(model // tile,),
        in_specs=[pl.BlockSpec((rows, tile), lambda i: (0, i)) for _ in blocks] + [pl.BlockSpec(lhs.shape, lambda i: (0, 0, 0))], out_specs=specs,
        scratch_shapes=[pltpu.VMEM((width, len(blocks) * rows), jnp.bfloat16)],
        compiler_params=pltpu.CompilerParams(dimension_semantics=('arbitrary',), vmem_limit_bytes=48 << 20),
        cost_estimate=pl.CostEstimate(flops=2 * len(blocks) * rows * model * width, bytes_accessed=2 * len(blocks) * rows * model, transcendentals=0),
    )(*blocks, lhs)


def pick_kernel(count, where_ref, *refs):
    sources, outs, sems = refs[:count * Z_SIZE], refs[count * Z_SIZE:-1], refs[-1]

    def copy(n, k):
        return pltpu.make_async_copy(sources[n * Z_SIZE + k], outs[n], sems.at[n])

    for n in range(count):
        for k in range(Z_SIZE):
            pl.when(where_ref[0] == k)(lambda n=n, k=k: copy(n, k).start())
    for n in range(count):
        copy(n, 0).wait()


def pick(where, *choices):
    shape = choices[0][0].shape
    return pl.pallas_call(
        functools.partial(pick_kernel, len(choices)), out_shape=[jax.ShapeDtypeStruct(shape, jnp.bfloat16)] * len(choices),
        grid_spec=pltpu.PrefetchScalarGridSpec(
            num_scalar_prefetch=1, grid=(1,), in_specs=[pl.BlockSpec(memory_space=pl.ANY)] * (len(choices) * Z_SIZE), out_specs=[full_spec(shape)] * len(choices),
            scratch_shapes=[pltpu.SemaphoreType.DMA((len(choices),))]),
        compiler_params=pltpu.CompilerParams(dimension_semantics=('arbitrary',), vmem_limit_bytes=32 << 20),
        cost_estimate=pl.CostEstimate(flops=1000000, bytes_accessed=8000000, transcendentals=0),
    )(where, *(arr for choice in choices for arr in choice))


def pair_add_kernel(a_ref, b_ref, c_ref, d_ref, ab_ref, cd_ref):
    for left, right, out in ((a_ref, b_ref, ab_ref), (c_ref, d_ref, cd_ref)):
        out[...] = (left[...].astype(jnp.float32) + right[...].astype(jnp.float32)).astype(jnp.bfloat16)


def pair_add(*operands):
    rows, model = operands[0].shape
    tile = model // 4
    spec = pl.BlockSpec((rows, tile), lambda i: (0, i))
    return pl.pallas_call(
        pair_add_kernel, out_shape=[jax.ShapeDtypeStruct((rows, model), jnp.bfloat16)] * 2, grid=(model // tile,), in_specs=[spec] * 4, out_specs=[spec] * 2,
        compiler_params=pltpu.CompilerParams(dimension_semantics=('arbitrary',), vmem_limit_bytes=32 << 20),
        cost_estimate=pl.CostEstimate(flops=4 * rows * model, bytes_accessed=12 * rows * model, transcendentals=0),
    )(*operands)


def finish_kernel(where_ref, mine_ref, other_ref, cos_ref, sin_ref, out_ref):
    for z in range(Z_SIZE):
        slot = lax.rem(where_ref[0] - z + Z_SIZE, Z_SIZE)
        for e in range(CORE_SIZE):
            total = mine_ref[z, e] + other_ref[z, e]
            dk = total[:, :HEAD_DIM].astype(jnp.bfloat16).astype(jnp.float32)
            out_ref[slot, e, :, :HEAD_DIM] = (dk * cos_ref[z, e] + pltpu.roll(dk, HEAD_DIM // 2, 1) * sin_ref[z, e]).astype(jnp.bfloat16)
            out_ref[slot, e, :, HEAD_DIM:] = total[:, HEAD_DIM:].astype(jnp.bfloat16)


def finish_key_grads(where, *operands):
    return pl.pallas_call(
        finish_kernel, out_shape=jax.ShapeDtypeStruct(operands[0].shape, jnp.bfloat16),
        grid_spec=pltpu.PrefetchScalarGridSpec(num_scalar_prefetch=1, grid=(1,), in_specs=[full_spec(arr.shape) for arr in operands], out_specs=full_spec(operands[0].shape)),
        compiler_params=pltpu.CompilerParams(dimension_semantics=('arbitrary',), vmem_limit_bytes=32 << 20),
        cost_estimate=pl.CostEstimate(flops=1000000, bytes_accessed=8000000, transcendentals=0),
    )(where, *operands)


def full_spec(shape):
    return pl.BlockSpec(shape, lambda b, *_: (0,) * len(shape))


def attend(where, positions, q_slots, kv_slots, kv_other, cos_t, sin_t, lo_all, bk):
    slots, bq, width = q_slots.shape
    seq = positions.shape[0]
    heads = width // HEAD_DIM
    lanes = heads * bq
    shared = (kv_slots, kv_other, cos_t, sin_t, lo_all)
    block = pl.BlockSpec((1, bq, width), lambda i, where_ref, _: (slot_of(where_ref, i // 2, i % 2), 0, 0))
    work = slots * bq * heads * seq * HEAD_DIM
    return pl.pallas_call(
        functools.partial(fwd_kernel, heads, bk),
        out_shape=(jax.ShapeDtypeStruct(q_slots.shape, jnp.bfloat16), jax.ShapeDtypeStruct((slots, 1, lanes), jnp.float32)),
        grid_spec=pltpu.PrefetchScalarGridSpec(
            num_scalar_prefetch=2, grid=(slots,), in_specs=[block] + [full_spec(arr.shape) for arr in shared],
            out_specs=(block, pl.BlockSpec((1, 1, lanes), lambda i, *_: (i, 0, 0))),
            scratch_shapes=[pltpu.VMEM((seq, HEAD_DIM), jnp.bfloat16), pltpu.VMEM((HEAD_DIM, seq), jnp.bfloat16), pltpu.VMEM((HEAD_DIM, lanes), jnp.bfloat16),
                            pltpu.VMEM((1, lanes), jnp.float32), pltpu.VMEM((1, lanes), jnp.float32), pltpu.VMEM((HEAD_DIM, lanes), jnp.float32)]),
        compiler_params=pltpu.CompilerParams(dimension_semantics=('arbitrary',), vmem_limit_bytes=48 << 20),
        cost_estimate=pl.CostEstimate(flops=4 * work, bytes_accessed=4 * slots * bq * width + 8 * seq * HEAD_DIM, transcendentals=work // (2 * HEAD_DIM)),
        name='attend_fwd',
    )(where, positions, q_slots, *shared)


def attend_backward(where, positions, q_slots, do_blocks, o_slots, kv_slots, kv_other, cos_t, sin_t, lo_all, lse, bk, rows_of_z, part=None):
    count, bq, width = do_blocks.shape
    seq = positions.shape[0]
    heads = width // HEAD_DIM
    lanes = heads * bq
    shared = (kv_slots, kv_other, cos_t, sin_t, lo_all)

    def slot_index(i, where_ref, _):
        return (slot_of(where_ref, *bwd_block(where_ref, i, rows_of_z)), 0, 0)

    def lse_index(i, where_ref, _):
        z_blk, c_blk = bwd_block(where_ref, i, rows_of_z)
        return (2 * z_blk + c_blk, 0, 0)

    block = pl.BlockSpec((1, bq, width), slot_index)
    local = pl.BlockSpec((1, bq, width), lambda i, *_: (i, 0, 0))
    operands = [q_slots, do_blocks, o_slots, *shared, lse]
    in_specs = [block, local, block] + [full_spec(arr.shape) for arr in shared] + [pl.BlockSpec((1, 1, lanes), lse_index)]
    part_shape, final_shape = (2 * HEAD_DIM, seq), (Z_SIZE, CORE_SIZE, bq, 2 * HEAD_DIM)
    grads = [part_shape] if part is None else [final_shape] * 2
    if part is not None:
        operands.append(part)
        in_specs.append(full_spec(part_shape))
    work = count * bq * heads * seq * HEAD_DIM
    return pl.pallas_call(
        functools.partial(bwd_kernel, heads, bk, rows_of_z),
        out_shape=[jax.ShapeDtypeStruct(do_blocks.shape, jnp.bfloat16)] + [jax.ShapeDtypeStruct(shape, jnp.float32) for shape in grads],
        grid_spec=pltpu.PrefetchScalarGridSpec(
            num_scalar_prefetch=2, grid=(count,), in_specs=in_specs, out_specs=[local] + [full_spec(shape) for shape in grads],
            scratch_shapes=[pltpu.VMEM((seq, HEAD_DIM), jnp.bfloat16), pltpu.VMEM((HEAD_DIM, seq), jnp.bfloat16), pltpu.VMEM((seq, HEAD_DIM), jnp.bfloat16),
                            pltpu.VMEM((HEAD_DIM, lanes), jnp.bfloat16), pltpu.VMEM((HEAD_DIM, lanes), jnp.bfloat16), pltpu.VMEM((HEAD_DIM, lanes), jnp.float32),
                            pltpu.VMEM((2 * HEAD_DIM, seq), jnp.float32)]),
        compiler_params=pltpu.CompilerParams(dimension_semantics=('arbitrary',), vmem_limit_bytes=58 << 20),
        cost_estimate=pl.CostEstimate(flops=10 * work, bytes_accessed=8 * count * bq * width + 24 * seq * HEAD_DIM, transcendentals=work // (2 * HEAD_DIM)),
        name='attend_bwd',
    )(where, positions, *operands)


def solution(mesh):
    def member(z, y, c):
        return (z * Y_SIZE + y) * CORE_SIZE + c

    every = [(z, y, c) for z in range(Z_SIZE) for y in range(Y_SIZE) for c in range(CORE_SIZE)]

    def permuter(target, senders=range(Z_SIZE)):
        pairs = [(member(*src), member(*target(*src))) for src in every if src[0] in senders]
        return lambda val: lax.ppermute(val, 'tp', pairs)

    swap_core = permuter(lambda z, y, c: (z, y, 1 - c))
    swap_y = permuter(lambda z, y, c: (z, 1 - y, c))
    swap_same_head = permuter(lambda z, y, c: (z, 1 - y, 1 - c))
    ring = permuter(lambda z, y, c: ((z + 1) % Z_SIZE, y, c))
    ring_back = {k: permuter(lambda z, y, c, k=k: ((z - k) % Z_SIZE, y, c)) for k in (1, 2)}
    hops = range(1, Z_SIZE)
    gather_right = {k: permuter(lambda z, y, c: (z + 1, y, c), range(k - 1, Z_SIZE - 1)) for k in hops}
    gather_left = {k: permuter(lambda z, y, c: (z - 1, y, c), range(1, Z_SIZE - k + 1)) for k in hops}
    scatter_right = {k: permuter(lambda z, y, c: (z + 1, y, c), range(0, k)) for k in hops}
    scatter_left = {k: permuter(lambda z, y, c: (z - 1, y, c), range(Z_SIZE - k, Z_SIZE)) for k in hops}
    z_swaps = {k: permuter(lambda z, y, c, k=k: (z ^ k, y, c)) for k in hops}

    def after(val, *deps):
        return lax.optimization_barrier((val,) + deps)[0]

    def device_step(x_blk, dy_blk, pos_all, norm_gain, wq_loc, wk_all, wv_all, wo_loc):
        seq_len = pos_all.shape[0]
        bq = seq_len // (Z_SIZE * Y_SIZE * CORE_SIZE)
        bk = 2 * bq
        model = x_blk.shape[1]
        idx = lax.axis_index('tp')
        z_idx, y_idx, c_idx = idx // (Y_SIZE * CORE_SIZE), (idx // CORE_SIZE) % Y_SIZE, idx % CORE_SIZE
        where = jnp.stack([z_idx, y_idx, c_idx])
        on_core0 = c_idx == 0
        pair = wq_loc.shape[1]
        kv_own = Y_SIZE * z_idx + (y_idx ^ c_idx)

        def select(first, second):
            return jnp.where(on_core0, first, second)

        def flip_core(arr):
            return arr[:, ::-1]

        def slots(arrs):
            return jnp.concatenate([arr[None] for arr in arrs], axis=0)

        def interleave(own, partner):
            return [blk for both in zip(own, partner) for blk in both]

        x_f32 = x_blk.astype(jnp.float32)
        hidden, x_hat, inv_rms = norm_forward(x_f32, norm_gain)

        h_own = [hidden]
        for s in hops:
            h_own.append(ring(h_own[-1]))
        h_pair = []
        for blk in h_own:
            h_pair.append(swap_core(blk))

        def slot_order(w_own, w_core, w_y, w_both):
            return [select(w_own, w_y), select(w_core, w_both), select(w_both, w_core), select(w_y, w_own)]

        wq_y = swap_y(wq_loc)
        wq_core = swap_core(wq_loc)
        q_cols = slot_order(wq_loc, wq_core, wq_y, swap_core(wq_y))
        wo_y = swap_y(wo_loc)
        o_rows = (wo_loc, swap_core(wo_loc), wo_y, swap_core(wo_y))

        def kv_columns(head):
            return [lax.dynamic_slice_in_dim(w, head * HEAD_DIM, HEAD_DIM, axis=1) for w in (wk_all, wv_all)]

        w_q = lax.optimization_barrier(jnp.concatenate(q_cols, axis=1))
        w_kv = lax.optimization_barrier(jnp.concatenate(kv_columns(kv_own) + kv_columns(kv_own ^ 1), axis=1))
        kv_heads = [lax.rem(kv_own + k * Y_SIZE, Y_SIZE * Z_SIZE) for k in range(3)]
        w_kv_all = lax.optimization_barrier(jnp.concatenate([cols for head in kv_heads for h in (head, head ^ 1) for cols in kv_columns(h)], axis=1))
        w_own = jnp.concatenate([w_q[:, :2 * pair], w_kv[:, :2 * HEAD_DIM]], axis=1)
        w_mix = jnp.concatenate(slot_order(*o_rows), axis=0)
        lo_all = (lax.iota(jnp.int32, seq_len) - pos_all)[None, :]
        cos_t, sin_t = rope_tables(pos_all)

        def my_tables(lead, tail):
            parts = jnp.concatenate([lead.T, tail.T], axis=1).reshape(Z_SIZE, Y_SIZE, CORE_SIZE, bq, HEAD_DIM)
            parts = lax.dynamic_index_in_dim(parts, y_idx, 1, keepdims=False)
            return select(parts, flip_core(parts))

        cos_my, sin_my = my_tables(cos_t, cos_t), my_tables(sin_t, -sin_t)

        qkv = []
        for s in range(Z_SIZE):
            qkv += [dot_f32(blk, w_own).astype(jnp.bfloat16) for blk in (h_own[s], h_pair[s])]
        kv_blocks = [blk[:, 2 * pair:] for blk in qkv]
        early = SLOTS - CORE_SIZE
        kv_other_early = swap_same_head(slots(kv_blocks[:early]))
        kv_other_late = swap_same_head(slots(kv_blocks[early:]))
        kv_other = jnp.concatenate([kv_other_early, kv_other_late], axis=0)
        q_slots, kv_slots = slots([blk[:, :2 * pair] for blk in qkv]), slots(kv_blocks)

        g_own = []
        for s, blk in enumerate(h_own):
            g_own.append(swap_y(after(blk, kv_other_late) if s else blk))

        right, left = {0: after(dy_blk, h_own[-1])}, {}
        left[0] = right[0]
        for k in hops:
            right[k] = gather_right[k](right[k - 1])
            left[k] = gather_left[k](left[k - 1])
            right[k], left[k] = lax.optimization_barrier((right[k], left[k]))
        dy_one, dy_two = pick(where, (left[1], dy_blk, right[1], right[2]), (left[2], left[1], dy_blk, right[1]))
        dy_zero, dy_three = pick(where, (dy_blk, right[1], right[2], right[3]), (left[3], left[2], left[1], dy_blk))
        dy_own = [dy_zero, dy_one, dy_two, dy_three]
        dy_pair = []
        for blk in dy_own:
            dy_pair.append(swap_core(blk))
        dy_slots = interleave(dy_own, dy_pair)

        def mirrored(lines):
            return jnp.concatenate([lax.dynamic_slice_in_dim(lines, lax.rem(z_idx - s + Z_SIZE, Z_SIZE), 1, axis=0) for s in range(Z_SIZE)], axis=0)

        forward = functools.partial(attend, where, pos_all, q_slots, kv_slots, kv_other, cos_t, sin_t, lo_all, bk)
        o_slots, lse = forward()
        by_line = (Z_SIZE, CORE_SIZE, bq, -1)
        o_lines = o_slots.reshape(by_line)
        o_partner = swap_core(o_slots).reshape(by_line)
        o_mine = jnp.concatenate([o_lines[:, 0], o_partner[:, 1]], axis=-1)

        def pair_sides(own, partner):
            first, last = own[..., :pair], partner[..., pair:2 * pair]
            return select(first, last), select(last, first)

        def by_block(arr):
            return arr.reshape((SLOTS,) + arr.shape[2:])

        o_sides = jnp.concatenate(pair_sides(o_lines, flip_core(o_partner)), axis=-1)
        o_sides = lax.optimization_barrier(by_block(mirrored(o_sides)))
        mix_part = []
        for s in range(Z_SIZE):
            mix_part.append(lax.optimization_barrier(dot_f32(o_mine[s], w_mix).astype(jnp.bfloat16)))

        def plus(*parts):
            return sum(part.astype(jnp.float32) for part in parts)

        sum_right, sum_left = mix_part[1], mix_part[Z_SIZE - 1]
        for k in hops:
            if k > 1:
                sum_right, sum_left = lax.optimization_barrier((sum_right, sum_left))
                sum_right, sum_left = pair_add(mix_part[k], sum_right, mix_part[Z_SIZE - k], sum_left)
            sum_right = scatter_right[k](sum_right)
            sum_left = scatter_left[k](sum_left)
        result = (x_f32 + plus(mix_part[0], sum_right, sum_left)).astype(jnp.bfloat16)

        d_o = []
        for n in range(Z_SIZE):
            d_o.append([dot_f32(blk, w_mix[:2 * pair], COLS_OF_BOTH).astype(jnp.bfloat16) for blk in (dy_own[n], dy_pair[n])])
        shared = (o_slots, kv_slots, kv_other, cos_t, sin_t, lo_all, lse, bk)
        dq_early, dkv_part = attend_backward(where, pos_all, q_slots, slots(d_o[1] + d_o[2]), *shared, EARLY)
        dq_early_partner = swap_core(dq_early)
        early_own, early_partner = lax.optimization_barrier((dq_early, dq_early_partner))
        early_keep, early_send = pair_sides(early_own, early_partner.reshape(2, CORE_SIZE, bq, -1)[:, ::-1].reshape(early_own.shape))
        early_theirs = swap_y(early_send)
        dq_late, dkv_mine, dkv_send = attend_backward(where, pos_all, q_slots, slots(d_o[0] + d_o[3]), *shared, LATE, dkv_part)
        dkv_theirs = swap_same_head(dkv_send)
        dq_late_partner = swap_core(dq_late)

        late_partner = dq_late_partner.reshape(2, CORE_SIZE, bq, -1)[:, ::-1].reshape(dq_late.shape)
        late_keep, late_send = pair_sides(dq_late, late_partner)

        def natural(early, late):
            return jnp.concatenate([late[:2], early, late[2:]], axis=0).reshape((Z_SIZE, CORE_SIZE) + early.shape[1:])

        q_rows = jnp.concatenate([natural(dq_early, dq_late)[:, 0], natural(early_partner, dq_late_partner)[:, 1]], axis=-1)
        dq_rows = [lax.dynamic_index_in_dim(q_rows, lax.rem(z_idx - s + Z_SIZE, Z_SIZE), 0, keepdims=False) for s in range(Z_SIZE)]
        halves = [slice(0, model // 2), slice(model // 2, model)]
        dh_sum = []
        for n, cols in enumerate(halves):
            dh_sum.append(dot_f32(dq_rows[1], w_q[cols], COLS_OF_BOTH).astype(jnp.bfloat16))
            dh_sum[n] = ring(dh_sum[n])

        dkv_lines = finish_key_grads(where, dkv_mine, dkv_theirs, cos_my, sin_my)
        dkv_partner = flip_core(swap_core(dkv_lines))
        dkv_rows = jnp.concatenate([dkv_lines[:, 0], dkv_partner[:, 0]], axis=-1)
        dkv_next = {}
        for k in ring_back:
            dkv_next[k] = ring_back[k](dkv_rows[k])

        def kv_part(rows, weights, cols):
            return dot_f32(rows, weights[cols], COLS_OF_BOTH)

        for s in hops[1:]:
            for n, cols in enumerate(halves):
                part = dot_f32(dq_rows[s], w_q[cols], COLS_OF_BOTH)
                if s == hops[-1]:
                    part = part + kv_part(dkv_rows[s], w_kv, cols)
                dh_sum[n] = (part + dh_sum[n].astype(jnp.float32)).astype(jnp.bfloat16)
                if s == hops[-1] and n == 0:
                    dh_sum[n], result = lax.optimization_barrier((dh_sum[n], result))
                dh_sum[n] = ring(dh_sum[n])
        g_pair = [swap_core(blk) for blk in lax.optimization_barrier((*g_own, dq_late))[:Z_SIZE]]
        kv_keep = select(dkv_lines[..., :HEAD_DIM], dkv_partner[..., HEAD_DIM:])
        kv_send = select(dkv_partner[..., :HEAD_DIM], dkv_lines[..., HEAD_DIM:])
        kv_theirs = swap_y(kv_send)
        late_theirs = swap_y(late_send)

        def rows_of(early, late, kv_lines):
            return by_block(jnp.concatenate([mirrored(natural(early, late)), kv_lines], axis=-1))

        d_keep = rows_of(early_keep, late_keep, kv_keep)
        d_theirs = rows_of(early_theirs, late_theirs, kv_theirs)

        dwo_keep, dwo_send = token_grads(dy_slots, o_sides, [((pair, model), jnp.float32)] * 2)
        theirs_first = swap_y(dwo_send[:, halves[0]])
        theirs_last = swap_y(dwo_send[:, halves[1]])

        d_wq, kv_mine_sum = token_grads([blks[s] for mine, theirs in ((h_own, h_pair), (g_own, g_pair)) for s in range(Z_SIZE) for blks in (mine, theirs)], jnp.concatenate([d_keep, d_theirs], axis=0),
                                        [((model, pair), jnp.bfloat16), ((model, HEAD_DIM), jnp.float32)])
        kv_other_sum = swap_core(kv_mine_sum)
        d_wk = select(kv_mine_sum, kv_other_sum)
        d_wv = select(kv_other_sum, kv_mine_sum)

        dh_own = lax.optimization_barrier([dot_f32(dq_rows[0], w_q[cols], COLS_OF_BOTH) for cols in halves])
        late_rows = after(jnp.concatenate([dkv_next[1], dkv_next[2]], axis=1), kv_mine_sum)
        kv_cols = jnp.concatenate([dkv_rows[0], late_rows], axis=1)
        dh_own = lax.optimization_barrier([own + kv_part(kv_cols, w_kv_all, cols) for own, cols in zip(dh_own, halves)])
        dh_rows = jnp.concatenate([(own + part.astype(jnp.float32)).astype(jnp.bfloat16) for own, part in zip(dh_own, dh_sum)], axis=1)

        d_input, dg_part = norm_backward(dh_rows, x_hat, inv_rms, norm_gain)
        grad_x = (dy_blk.astype(jnp.float32) + d_input).astype(jnp.bfloat16)
        for near, far, both in ((swap_core, swap_y, swap_same_head), (z_swaps[1], z_swaps[2], z_swaps[3])):
            dg_part = (dg_part + near(dg_part)) + (far(dg_part) + both(dg_part))
            if near is swap_core:
                theirs_last = after(theirs_last, dg_part)
        d_wo = (dwo_keep + jnp.concatenate([theirs_first, theirs_last], axis=1)).astype(jnp.bfloat16)
        return result, grad_x, d_wq, d_wk, d_wv, d_wo, dg_part

    specs_in = (P(('dp', 'tp'), None), P(('dp', 'tp'), None), P('dp'), P(), P(None, 'tp'), P(), P(), P('tp', None))
    specs_out = (P(('dp', 'tp'), None), P(('dp', 'tp'), None), P('dp', 'tp'), P('dp', 'tp'), P('dp', 'tp'), P(('dp', 'tp'), None), P('dp'))
    return jax.shard_map(device_step, mesh=mesh, in_specs=specs_in, out_specs=specs_out, check_vma=False)
```

```python
import functools
import jax
import jax.numpy as jnp
from jax import lax
from jax.experimental import pallas as pl
from jax.experimental.pallas import tpu as pltpu
from jax.sharding import PartitionSpec as P

HEAD_DIM = 128
SCORE_SCALE = HEAD_DIM ** -0.5
SCALE_LOG2E = SCORE_SCALE * 1.4426950408889634
ROPE_THETA = 1000000.0
NORM_EPS = 1e-05
MASKED = -1e30
Z_SIZE = 4
Y_SIZE = 2
CORE_SIZE = 2
SLOTS = Z_SIZE * CORE_SIZE
EARLY, LATE = (1, 2), (0, 3)
NATURAL = (((1,), (0,)), ((), ()))
COLS_OF_BOTH = (((1,), (1,)), ((), ()))


def dot_f32(lhs, rhs, dims=NATURAL):
    return lax.dot_general(lhs, rhs, dims, preferred_element_type=jnp.float32)


def rope_tables(positions):
    exponents = jnp.arange(0, HEAD_DIM, 2, dtype=jnp.float32) / HEAD_DIM
    angles = jnp.power(ROPE_THETA, -exponents)[:, None] * positions.astype(jnp.float32)[None, :]
    return jnp.cos(angles), jnp.sin(angles)


def rotate_rows(t_f32, cos_t, sin_t):
    lead_half, tail_half = t_f32[:HEAD_DIM // 2], t_f32[HEAD_DIM // 2:]
    return jnp.concatenate([lead_half * cos_t - tail_half * sin_t, tail_half * cos_t + lead_half * sin_t], axis=0).astype(jnp.bfloat16)


def norm_forward(x_f32, norm_gain):
    inv_rms = lax.rsqrt(jnp.mean(x_f32 * x_f32, axis=-1, keepdims=True) + NORM_EPS)
    x_hat = x_f32 * inv_rms
    return (x_hat * norm_gain).astype(jnp.bfloat16), x_hat, inv_rms


def norm_backward(d_hidden, x_hat, inv_rms, norm_gain):
    d_f32 = d_hidden.astype(jnp.float32)
    d_gain = jnp.sum(d_f32 * x_hat, axis=0)
    scaled = d_f32 * norm_gain
    d_input = inv_rms * (scaled - x_hat * jnp.mean(scaled * x_hat, axis=-1, keepdims=True))
    return d_input, d_gain


def slot_of(where_ref, z, c):
    return 2 * lax.rem(where_ref[0] - z + Z_SIZE, Z_SIZE) + (where_ref[2] ^ c)


def slot_of_other(where_ref, z, c):
    return 2 * lax.rem(where_ref[0] - z + Z_SIZE, Z_SIZE) + (1 - (where_ref[2] ^ c))


def block_token(where_ref, b, bq):
    return pl.multiple_of((b // 2) * (4 * bq) + where_ref[1] * (2 * bq) + (b % 2) * bq, bq)


def key_range(pos_ref, start, bq, bk):
    lo_first, lo_last = start - pos_ref[start], start + bq - 1 - pos_ref[start + bq - 1]
    return lo_first // bk, (start + bq - 1) // bk + 1, (lo_last + bk - 1) // bk, (start + 1) // bk


def tile_lanes(row, heads):
    return jnp.concatenate([row] * heads, axis=1)


def row_bounds(lo_ref, start, bq, heads):
    tok = start + lax.broadcasted_iota(jnp.int32, (1, bq), 1)
    return tile_lanes(tok, heads), tile_lanes(lo_ref[:, pl.ds(start, bq)], heads)


def keep_mask(key_start, bk, t_row, lo_row):
    key_idx = key_start + lax.broadcasted_iota(jnp.int32, (bk, t_row.shape[1]), 0)
    return (key_idx <= t_row) & (key_idx >= lo_row)


def head_columns(block, h):
    return block[:, h * HEAD_DIM:(h + 1) * HEAD_DIM]


def rotated_queries(q_blk, cos_ref, sin_ref, start, bq, heads):
    cos_t, sin_t = cos_ref[:, pl.ds(start, bq)], sin_ref[:, pl.ds(start, bq)]
    return [rotate_rows(head_columns(q_blk, h).T.astype(jnp.float32), cos_t, sin_t) for h in range(heads)]


def visit_keys(bounds, step):
    first, end, inner_first, inner_end = bounds

    def visit(j, carry):
        inner = (j >= inner_first) & (j < inner_end)

        @pl.when(inner)
        def _():
            step(j, False)

        @pl.when(jnp.logical_not(inner))
        def _():
            step(j, True)

        return carry

    lax.fori_loop(first, end, visit, 0)


def for_key_blocks(where_ref, mine_ref, theirs_ref, count, bq, store):
    def visit(n, carry):
        z, y, c = n // 4, (n // 2) % 2, n % 2
        block = jnp.where(y == where_ref[1], mine_ref[slot_of(where_ref, z, c)], theirs_ref[slot_of_other(where_ref, z, c)])
        store(pl.ds(pl.multiple_of(n * bq, bq), bq), block)
        return carry

    lax.fori_loop(0, count, visit, 0)


def fwd_kernel(heads, bk, where_ref, pos_ref, q_ref, kv_ref, kv_other_ref, cos_ref, sin_ref, lo_ref, o_ref, lse_ref, k_s, vt_s, qt_s, m_s, l_s, acc_s):
    b = pl.program_id(0)
    bq = q_ref.shape[1]
    seq = k_s.shape[0]

    @pl.when(b == 0)
    def _():
        def store(rows, block):
            k_s[rows, :] = rotate_rows(block[:, :HEAD_DIM].T.astype(jnp.float32), cos_ref[:, rows], sin_ref[:, rows]).T
            vt_s[:, rows] = block[:, HEAD_DIM:].T

        for_key_blocks(where_ref, kv_ref, kv_other_ref, seq // bq, bq, store)

    start = block_token(where_ref, b, bq)
    t_row, lo_row = row_bounds(lo_ref, start, bq, heads)
    q_blk = q_ref[0]
    qt_s[...] = jnp.concatenate(rotated_queries(q_blk, cos_ref, sin_ref, start, bq, heads), axis=1)
    m_s[...] = jnp.full_like(m_s, MASKED)
    l_s[...] = jnp.zeros_like(l_s)
    acc_s[...] = jnp.zeros_like(acc_s)

    def step(j, masked):
        key_start = pl.multiple_of(j * bk, bk)
        keys = pl.ds(key_start, bk)
        scores = dot_f32(k_s[keys, :], qt_s[...])
        if masked:
            scores = jnp.where(keep_mask(key_start, bk, t_row, lo_row), scores, MASKED)
        m_old = m_s[...]
        m_new = jnp.maximum(m_old, jnp.max(scores, axis=0, keepdims=True))
        probs = jnp.exp2(scores * SCALE_LOG2E - m_new * SCALE_LOG2E)
        alpha = jnp.exp2((m_old - m_new) * SCALE_LOG2E)
        m_s[...] = m_new
        l_s[...] = l_s[...] * alpha + jnp.sum(probs, axis=0, keepdims=True)
        acc_s[...] = acc_s[...] * alpha + dot_f32(vt_s[:, keys], probs.astype(jnp.bfloat16))

    visit_keys(key_range(pos_ref, start, bq, bk), step)
    out_t = (acc_s[...] / l_s[...]).astype(jnp.bfloat16)
    for h in range(heads):
        o_ref[0, :, h * HEAD_DIM:(h + 1) * HEAD_DIM] = out_t[:, h * bq:(h + 1) * bq].T
    lse_ref[0] = m_s[...] * SCALE_LOG2E + jnp.log2(l_s[...])


def bwd_block(where_ref, step, rows):
    return rows[0] + (rows[1] - rows[0]) * (step // 2), where_ref[2] ^ (step % 2)


def bwd_kernel(heads, bk, rows_of_z, where_ref, pos_ref, q_ref, do_ref, o_ref, kv_ref, kv_other_ref, cos_ref, sin_ref, lo_ref, lse_ref, *refs):
    first = rows_of_z == EARLY
    if first:
        dq_ref, part_ref, k_s, kt_s, v_s, qt_s, dot_s, dqt_s, acc_s = refs
    else:
        part_ref, dq_ref, mine_ref, send_ref, k_s, kt_s, v_s, qt_s, dot_s, dqt_s, acc_s = refs
    step_idx = pl.program_id(0)
    z_blk, c_blk = bwd_block(where_ref, step_idx, rows_of_z)
    b = 2 * z_blk + c_blk
    bq = q_ref.shape[1]
    seq = k_s.shape[0]

    @pl.when(step_idx == 0)
    def _():
        def store(rows, block):
            acc_s[:, rows] = jnp.zeros((2 * HEAD_DIM, bq), jnp.float32) if first else part_ref[:, rows]
            k_rot_t = rotate_rows(block[:, :HEAD_DIM].T.astype(jnp.float32), cos_ref[:, rows], sin_ref[:, rows])
            kt_s[:, rows] = k_rot_t
            k_s[rows, :] = k_rot_t.T
            v_s[rows, :] = block[:, HEAD_DIM:]

        for_key_blocks(where_ref, kv_ref, kv_other_ref, seq // bq, bq, store)

    start = block_token(where_ref, b, bq)
    t_row, lo_row = row_bounds(lo_ref, start, bq, heads)
    q_blk, do_blk, o_blk = q_ref[0], do_ref[0], o_ref[0]
    deltas = []
    for h, q_rot_t in enumerate(rotated_queries(q_blk, cos_ref, sin_ref, start, bq, heads)):
        lanes = slice(h * bq, (h + 1) * bq)
        qt_s[:, lanes] = q_rot_t
        do_t = head_columns(do_blk, h).T
        dot_s[:, lanes] = do_t
        deltas.append(jnp.sum(do_t.astype(jnp.float32) * head_columns(o_blk, h).T.astype(jnp.float32), axis=0, keepdims=True))
    delta = jnp.concatenate(deltas, axis=1)
    lse = lse_ref[0]
    dqt_s[...] = jnp.zeros_like(dqt_s)

    def step(j, masked):
        key_start = pl.multiple_of(j * bk, bk)
        keys = pl.ds(key_start, bk)
        scores = dot_f32(k_s[keys, :], qt_s[...])
        probs = jnp.exp2(scores * SCALE_LOG2E - lse)
        if masked:
            probs = jnp.where(keep_mask(key_start, bk, t_row, lo_row), probs, 0.0)
        d_probs = dot_f32(v_s[keys, :], dot_s[...])
        d_scores = (probs * (d_probs - delta)).astype(jnp.bfloat16)
        acc_s[HEAD_DIM:, keys] += dot_f32(dot_s[...], probs.astype(jnp.bfloat16), COLS_OF_BOTH)
        acc_s[:HEAD_DIM, keys] += dot_f32(qt_s[...], d_scores, COLS_OF_BOTH) * SCORE_SCALE
        dqt_s[...] += dot_f32(kt_s[:, keys], d_scores)

    visit_keys(key_range(pos_ref, start, bq, bk), step)
    cos_t, sin_t = cos_ref[:, pl.ds(start, bq)], sin_ref[:, pl.ds(start, bq)]
    for h in range(heads):
        dq_rot_t = (dqt_s[:, h * bq:(h + 1) * bq] * SCORE_SCALE).astype(jnp.bfloat16).astype(jnp.float32)
        dq_ref[0, :, h * HEAD_DIM:(h + 1) * HEAD_DIM] = rotate_rows(dq_rot_t, cos_t, -sin_t).T

    @pl.when(step_idx == pl.num_programs(0) - 1)
    def _():
        if first:
            part_ref[...] = acc_s[...]
            return

        def hand_over(y, mine):
            for z in range(Z_SIZE):
                for c in range(CORE_SIZE):
                    rows = ((z * 2 + y) * 2 + c) * bq
                    e = where_ref[2] ^ c
                    if mine:
                        mine_ref[z, e] = acc_s[:, rows:rows + bq].T
                    else:
                        send_ref[z, 1 - e] = acc_s[:, rows:rows + bq].T

        for y in range(Y_SIZE):
            pl.when(where_ref[1] == y)(functools.partial(hand_over, y, True))
            pl.when(where_ref[1] != y)(functools.partial(hand_over, y, False))


def token_grads_kernel(count, *refs):
    blocks, lhs_ref, out_refs, lhs_t = refs[:count], refs[count], refs[count + 1:-1], refs[-1]
    rows = lhs_ref.shape[1]

    @pl.when(pl.program_id(0) == 0)
    def _():
        for n in range(count):
            lhs_t[:, n * rows:(n + 1) * rows] = lhs_ref[n].T

    total = sum(dot_f32(lhs_t[:, n * rows:(n + 1) * rows], blocks[n][...]) for n in range(count))
    start = 0
    for ref in out_refs:
        if ref.shape[0] == blocks[0].shape[1]:
            size = ref.shape[1]
            ref[...] = total[start:start + size, :].T.astype(ref.dtype)
        else:
            size = ref.shape[0]
            ref[...] = total[start:start + size, :].astype(ref.dtype)
        start += size


def token_grads(blocks, lhs, outs, tile=512):
    rows, model = blocks[0].shape
    width = lhs.shape[2]
    specs = [pl.BlockSpec((tile, shape[1]), lambda i: (i, 0)) if shape[0] == model else pl.BlockSpec((shape[0], tile), lambda i: (0, i)) for shape, _ in outs]
    return pl.pallas_call(
        functools.partial(token_grads_kernel, len(blocks)),
        out_shape=[jax.ShapeDtypeStruct(*out) for out in outs], grid=(model // tile,),
        in_specs=[pl.BlockSpec((rows, tile), lambda i: (0, i)) for _ in blocks] + [pl.BlockSpec(lhs.shape, lambda i: (0, 0, 0))], out_specs=specs,
        scratch_shapes=[pltpu.VMEM((width, len(blocks) * rows), jnp.bfloat16)],
        compiler_params=pltpu.CompilerParams(dimension_semantics=('arbitrary',), vmem_limit_bytes=48 << 20),
        cost_estimate=pl.CostEstimate(flops=2 * len(blocks) * rows * model * width, bytes_accessed=2 * len(blocks) * rows * model, transcendentals=0),
    )(*blocks, lhs)


def rows_product_kernel(count, *refs):
    blocks, w_ref, out_ref, acc_ref = refs[:count], refs[count], refs[count + 1], refs[count + 2]
    step, rows = pl.program_id(0), blocks[0].shape[0]
    lhs = jnp.concatenate([blk[...] for blk in blocks], axis=0)
    part = dot_f32(lhs, w_ref[...], COLS_OF_BOTH)

    @pl.when(step == 0)
    def _():
        acc_ref[...] = part

    @pl.when(step > 0)
    def _():
        acc_ref[...] += part

    @pl.when(step == pl.num_programs(0) - 1)
    def _():
        for n in range(count):
            out_ref[n] = acc_ref[n * rows:(n + 1) * rows, :].astype(jnp.bfloat16)


def rows_product(blocks, weights, width):
    rows, model = blocks[0].shape
    tile = model // 4
    out_shape = (len(blocks), rows, width)
    return pl.pallas_call(
        functools.partial(rows_product_kernel, len(blocks)), out_shape=jax.ShapeDtypeStruct(out_shape, jnp.bfloat16), grid=(model // tile,),
        in_specs=[pl.BlockSpec((rows, tile), lambda i: (0, i))] * len(blocks) + [pl.BlockSpec((width, tile), lambda i: (0, i))],
        out_specs=pl.BlockSpec(out_shape, lambda i: (0, 0, 0)), scratch_shapes=[pltpu.VMEM((len(blocks) * rows, width), jnp.float32)],
        compiler_params=pltpu.CompilerParams(dimension_semantics=('arbitrary',), vmem_limit_bytes=40 << 20),
        cost_estimate=pl.CostEstimate(flops=2 * len(blocks) * rows * model * width, bytes_accessed=2 * (len(blocks) * rows + width) * model, transcendentals=0),
    )(*blocks, weights)


def pick_kernel(count, where_ref, *refs):
    sources, outs, sems = refs[:count * Z_SIZE], refs[count * Z_SIZE:-1], refs[-1]

    def copy(n, k):
        return pltpu.make_async_copy(sources[n * Z_SIZE + k], outs[n], sems.at[n])

    for n in range(count):
        for k in range(Z_SIZE):
            pl.when(where_ref[0] == k)(lambda n=n, k=k: copy(n, k).start())
    for n in range(count):
        copy(n, 0).wait()


def pick(where, *choices):
    shape = choices[0][0].shape
    return pl.pallas_call(
        functools.partial(pick_kernel, len(choices)), out_shape=[jax.ShapeDtypeStruct(shape, jnp.bfloat16)] * len(choices),
        grid_spec=pltpu.PrefetchScalarGridSpec(
            num_scalar_prefetch=1, grid=(1,), in_specs=[pl.BlockSpec(memory_space=pl.ANY)] * (len(choices) * Z_SIZE), out_specs=[full_spec(shape)] * len(choices),
            scratch_shapes=[pltpu.SemaphoreType.DMA((len(choices),))]),
        compiler_params=pltpu.CompilerParams(dimension_semantics=('arbitrary',), vmem_limit_bytes=32 << 20),
        cost_estimate=pl.CostEstimate(flops=1000000, bytes_accessed=8000000, transcendentals=0),
    )(where, *(arr for choice in choices for arr in choice))


def pair_add_kernel(a_ref, b_ref, c_ref, d_ref, ab_ref, cd_ref):
    for left, right, out in ((a_ref, b_ref, ab_ref), (c_ref, d_ref, cd_ref)):
        out[...] = (left[...].astype(jnp.float32) + right[...].astype(jnp.float32)).astype(jnp.bfloat16)


def pair_add(*operands):
    rows, model = operands[0].shape
    tile = model // 4
    spec = pl.BlockSpec((rows, tile), lambda i: (0, i))
    return pl.pallas_call(
        pair_add_kernel, out_shape=[jax.ShapeDtypeStruct((rows, model), jnp.bfloat16)] * 2, grid=(model // tile,), in_specs=[spec] * 4, out_specs=[spec] * 2,
        compiler_params=pltpu.CompilerParams(dimension_semantics=('arbitrary',), vmem_limit_bytes=32 << 20),
        cost_estimate=pl.CostEstimate(flops=4 * rows * model, bytes_accessed=12 * rows * model, transcendentals=0),
    )(*operands)


def finish_kernel(where_ref, mine_ref, other_ref, cos_ref, sin_ref, out_ref):
    for z in range(Z_SIZE):
        slot = lax.rem(where_ref[0] - z + Z_SIZE, Z_SIZE)
        for e in range(CORE_SIZE):
            total = mine_ref[z, e] + other_ref[z, e]
            dk = total[:, :HEAD_DIM].astype(jnp.bfloat16).astype(jnp.float32)
            out_ref[slot, e, :, :HEAD_DIM] = (dk * cos_ref[z, e] + pltpu.roll(dk, HEAD_DIM // 2, 1) * sin_ref[z, e]).astype(jnp.bfloat16)
            out_ref[slot, e, :, HEAD_DIM:] = total[:, HEAD_DIM:].astype(jnp.bfloat16)


def finish_key_grads(where, *operands):
    return pl.pallas_call(
        finish_kernel, out_shape=jax.ShapeDtypeStruct(operands[0].shape, jnp.bfloat16),
        grid_spec=pltpu.PrefetchScalarGridSpec(num_scalar_prefetch=1, grid=(1,), in_specs=[full_spec(arr.shape) for arr in operands], out_specs=full_spec(operands[0].shape)),
        compiler_params=pltpu.CompilerParams(dimension_semantics=('arbitrary',), vmem_limit_bytes=32 << 20),
        cost_estimate=pl.CostEstimate(flops=1000000, bytes_accessed=8000000, transcendentals=0),
    )(where, *operands)


def full_spec(shape):
    return pl.BlockSpec(shape, lambda b, *_: (0,) * len(shape))


def attend(where, positions, q_slots, kv_slots, kv_other, cos_t, sin_t, lo_all, bk):
    slots, bq, width = q_slots.shape
    seq = positions.shape[0]
    heads = width // HEAD_DIM
    lanes = heads * bq
    shared = (kv_slots, kv_other, cos_t, sin_t, lo_all)
    block = pl.BlockSpec((1, bq, width), lambda i, where_ref, _: (slot_of(where_ref, i // 2, i % 2), 0, 0))
    work = slots * bq * heads * seq * HEAD_DIM
    return pl.pallas_call(
        functools.partial(fwd_kernel, heads, bk),
        out_shape=(jax.ShapeDtypeStruct(q_slots.shape, jnp.bfloat16), jax.ShapeDtypeStruct((slots, 1, lanes), jnp.float32)),
        grid_spec=pltpu.PrefetchScalarGridSpec(
            num_scalar_prefetch=2, grid=(slots,), in_specs=[block] + [full_spec(arr.shape) for arr in shared],
            out_specs=(block, pl.BlockSpec((1, 1, lanes), lambda i, *_: (i, 0, 0))),
            scratch_shapes=[pltpu.VMEM((seq, HEAD_DIM), jnp.bfloat16), pltpu.VMEM((HEAD_DIM, seq), jnp.bfloat16), pltpu.VMEM((HEAD_DIM, lanes), jnp.bfloat16),
                            pltpu.VMEM((1, lanes), jnp.float32), pltpu.VMEM((1, lanes), jnp.float32), pltpu.VMEM((HEAD_DIM, lanes), jnp.float32)]),
        compiler_params=pltpu.CompilerParams(dimension_semantics=('arbitrary',), vmem_limit_bytes=48 << 20),
        cost_estimate=pl.CostEstimate(flops=4 * work, bytes_accessed=4 * slots * bq * width + 8 * seq * HEAD_DIM, transcendentals=work // (2 * HEAD_DIM)),
        name='attend_fwd',
    )(where, positions, q_slots, *shared)


def attend_backward(where, positions, q_slots, do_blocks, o_slots, kv_slots, kv_other, cos_t, sin_t, lo_all, lse, bk, rows_of_z, part=None):
    count, bq, width = do_blocks.shape
    seq = positions.shape[0]
    heads = width // HEAD_DIM
    lanes = heads * bq
    shared = (kv_slots, kv_other, cos_t, sin_t, lo_all)

    def slot_index(i, where_ref, _):
        return (slot_of(where_ref, *bwd_block(where_ref, i, rows_of_z)), 0, 0)

    def lse_index(i, where_ref, _):
        z_blk, c_blk = bwd_block(where_ref, i, rows_of_z)
        return (2 * z_blk + c_blk, 0, 0)

    block = pl.BlockSpec((1, bq, width), slot_index)
    local = pl.BlockSpec((1, bq, width), lambda i, *_: (i, 0, 0))
    operands = [q_slots, do_blocks, o_slots, *shared, lse]
    in_specs = [block, local, block] + [full_spec(arr.shape) for arr in shared] + [pl.BlockSpec((1, 1, lanes), lse_index)]
    part_shape, final_shape = (2 * HEAD_DIM, seq), (Z_SIZE, CORE_SIZE, bq, 2 * HEAD_DIM)
    grads = [part_shape] if part is None else [final_shape] * 2
    if part is not None:
        operands.append(part)
        in_specs.append(full_spec(part_shape))
    work = count * bq * heads * seq * HEAD_DIM
    return pl.pallas_call(
        functools.partial(bwd_kernel, heads, bk, rows_of_z),
        out_shape=[jax.ShapeDtypeStruct(do_blocks.shape, jnp.bfloat16)] + [jax.ShapeDtypeStruct(shape, jnp.float32) for shape in grads],
        grid_spec=pltpu.PrefetchScalarGridSpec(
            num_scalar_prefetch=2, grid=(count,), in_specs=in_specs, out_specs=[local] + [full_spec(shape) for shape in grads],
            scratch_shapes=[pltpu.VMEM((seq, HEAD_DIM), jnp.bfloat16), pltpu.VMEM((HEAD_DIM, seq), jnp.bfloat16), pltpu.VMEM((seq, HEAD_DIM), jnp.bfloat16),
                            pltpu.VMEM((HEAD_DIM, lanes), jnp.bfloat16), pltpu.VMEM((HEAD_DIM, lanes), jnp.bfloat16), pltpu.VMEM((HEAD_DIM, lanes), jnp.float32),
                            pltpu.VMEM((2 * HEAD_DIM, seq), jnp.float32)]),
        compiler_params=pltpu.CompilerParams(dimension_semantics=('arbitrary',), vmem_limit_bytes=58 << 20),
        cost_estimate=pl.CostEstimate(flops=10 * work, bytes_accessed=8 * count * bq * width + 24 * seq * HEAD_DIM, transcendentals=work // (2 * HEAD_DIM)),
        name='attend_bwd',
    )(where, positions, *operands)


def solution(mesh):
    def member(z, y, c):
        return (z * Y_SIZE + y) * CORE_SIZE + c

    every = [(z, y, c) for z in range(Z_SIZE) for y in range(Y_SIZE) for c in range(CORE_SIZE)]

    def permuter(target, senders=range(Z_SIZE)):
        pairs = [(member(*src), member(*target(*src))) for src in every if src[0] in senders]
        return lambda val: lax.ppermute(val, 'tp', pairs)

    swap_core = permuter(lambda z, y, c: (z, y, 1 - c))
    swap_y = permuter(lambda z, y, c: (z, 1 - y, c))
    swap_same_head = permuter(lambda z, y, c: (z, 1 - y, 1 - c))
    ring = permuter(lambda z, y, c: ((z + 1) % Z_SIZE, y, c))
    ring_back = permuter(lambda z, y, c: ((z - 1) % Z_SIZE, y, c))
    hops = range(1, Z_SIZE)
    gather_right = {k: permuter(lambda z, y, c: (z + 1, y, c), range(k - 1, Z_SIZE - 1)) for k in hops}
    gather_left = {k: permuter(lambda z, y, c: (z - 1, y, c), range(1, Z_SIZE - k + 1)) for k in hops}
    scatter_right = {k: permuter(lambda z, y, c: (z + 1, y, c), range(0, k)) for k in hops}
    scatter_left = {k: permuter(lambda z, y, c: (z - 1, y, c), range(Z_SIZE - k, Z_SIZE)) for k in hops}
    z_swaps = {k: permuter(lambda z, y, c, k=k: (z ^ k, y, c)) for k in hops}

    def after(val, *deps):
        return lax.optimization_barrier((val,) + deps)[0]

    def device_step(x_blk, dy_blk, pos_all, norm_gain, wq_loc, wk_all, wv_all, wo_loc):
        seq_len = pos_all.shape[0]
        bq = seq_len // (Z_SIZE * Y_SIZE * CORE_SIZE)
        bk = 2 * bq
        model = x_blk.shape[1]
        idx = lax.axis_index('tp')
        z_idx, y_idx, c_idx = idx // (Y_SIZE * CORE_SIZE), (idx // CORE_SIZE) % Y_SIZE, idx % CORE_SIZE
        where = jnp.stack([z_idx, y_idx, c_idx])
        on_core0 = c_idx == 0
        pair = wq_loc.shape[1]
        kv_own = Y_SIZE * z_idx + (y_idx ^ c_idx)

        def select(first, second):
            return jnp.where(on_core0, first, second)

        def flip_core(arr):
            return arr[:, ::-1]

        def slots(arrs):
            return jnp.concatenate([arr[None] for arr in arrs], axis=0)

        def interleave(own, partner):
            return [blk for both in zip(own, partner) for blk in both]

        x_f32 = x_blk.astype(jnp.float32)
        hidden, x_hat, inv_rms = norm_forward(x_f32, norm_gain)

        h_own = [hidden]
        for s in hops:
            h_own.append(ring(h_own[-1]))
        h_pair = []
        for blk in h_own:
            h_pair.append(swap_core(blk))

        def slot_order(w_own, w_core, w_y, w_both):
            return [select(w_own, w_y), select(w_core, w_both), select(w_both, w_core), select(w_y, w_own)]

        wq_y = swap_y(wq_loc)
        wq_core = swap_core(wq_loc)
        q_cols = slot_order(wq_loc, wq_core, wq_y, swap_core(wq_y))
        wo_y = swap_y(wo_loc)
        o_rows = (wo_loc, swap_core(wo_loc), wo_y, swap_core(wo_y))

        def kv_columns(head):
            return [lax.dynamic_slice_in_dim(w, head * HEAD_DIM, HEAD_DIM, axis=1) for w in (wk_all, wv_all)]

        w_q = lax.optimization_barrier(jnp.concatenate(q_cols, axis=1))
        w_kv = lax.optimization_barrier(jnp.concatenate(kv_columns(kv_own) + kv_columns(kv_own ^ 1), axis=1))
        kv_heads = [lax.rem(kv_own + k * Y_SIZE, Y_SIZE * Z_SIZE) for k in range(2)]
        w_kv_all = lax.optimization_barrier(jnp.concatenate([cols for head in kv_heads for h in (head, head ^ 1) for cols in kv_columns(h)], axis=1))
        w_own = jnp.concatenate([w_q[:, :2 * pair], w_kv[:, :2 * HEAD_DIM]], axis=1)
        w_mix = jnp.concatenate(slot_order(*o_rows), axis=0)
        lo_all = (lax.iota(jnp.int32, seq_len) - pos_all)[None, :]
        cos_t, sin_t = rope_tables(pos_all)

        def my_tables(lead, tail):
            parts = jnp.concatenate([lead.T, tail.T], axis=1).reshape(Z_SIZE, Y_SIZE, CORE_SIZE, bq, HEAD_DIM)
            parts = lax.dynamic_index_in_dim(parts, y_idx, 1, keepdims=False)
            return select(parts, flip_core(parts))

        cos_my, sin_my = my_tables(cos_t, cos_t), my_tables(sin_t, -sin_t)

        qkv = []
        for s in range(Z_SIZE):
            qkv += [dot_f32(blk, w_own).astype(jnp.bfloat16) for blk in (h_own[s], h_pair[s])]
        kv_blocks = [blk[:, 2 * pair:] for blk in qkv]
        early = SLOTS - CORE_SIZE
        kv_other_early = swap_same_head(slots(kv_blocks[:early]))
        kv_other_late = swap_same_head(slots(kv_blocks[early:]))
        kv_other = jnp.concatenate([kv_other_early, kv_other_late], axis=0)
        q_slots, kv_slots = slots([blk[:, :2 * pair] for blk in qkv]), slots(kv_blocks)

        g_own = []
        for s, blk in enumerate(h_own):
            g_own.append(swap_y(after(blk, kv_other_late) if s else blk))

        right, left = {0: after(dy_blk, h_own[-1])}, {}
        left[0] = right[0]
        for k in hops:
            right[k] = gather_right[k](right[k - 1])
            left[k] = gather_left[k](left[k - 1])
            right[k], left[k] = lax.optimization_barrier((right[k], left[k]))
        dy_one, dy_two = pick(where, (left[1], dy_blk, right[1], right[2]), (left[2], left[1], dy_blk, right[1]))
        dy_zero, dy_three = pick(where, (dy_blk, right[1], right[2], right[3]), (left[3], left[2], left[1], dy_blk))
        dy_own = [dy_zero, dy_one, dy_two, dy_three]
        dy_pair = []
        for blk in dy_own:
            dy_pair.append(swap_core(blk))
        dy_slots = interleave(dy_own, dy_pair)

        def mirrored(lines):
            return jnp.concatenate([lax.dynamic_slice_in_dim(lines, lax.rem(z_idx - s + Z_SIZE, Z_SIZE), 1, axis=0) for s in range(Z_SIZE)], axis=0)

        forward = functools.partial(attend, where, pos_all, q_slots, kv_slots, kv_other, cos_t, sin_t, lo_all, bk)
        o_slots, lse = forward()
        by_line = (Z_SIZE, CORE_SIZE, bq, -1)
        o_lines = o_slots.reshape(by_line)
        o_partner = swap_core(o_slots).reshape(by_line)
        o_mine = jnp.concatenate([o_lines[:, 0], o_partner[:, 1]], axis=-1)

        def pair_sides(own, partner):
            first, last = own[..., :pair], partner[..., pair:2 * pair]
            return select(first, last), select(last, first)

        def by_block(arr):
            return arr.reshape((SLOTS,) + arr.shape[2:])

        o_sides = jnp.concatenate(pair_sides(o_lines, flip_core(o_partner)), axis=-1)
        o_sides = lax.optimization_barrier(by_block(mirrored(o_sides)))
        mix_part = []
        for s in range(Z_SIZE):
            mix_part.append(lax.optimization_barrier(dot_f32(o_mine[s], w_mix).astype(jnp.bfloat16)))

        def plus(*parts):
            return sum(part.astype(jnp.float32) for part in parts)

        sum_right, sum_left = mix_part[1], mix_part[Z_SIZE - 1]
        for k in hops:
            if k > 1:
                sum_right, sum_left = lax.optimization_barrier((sum_right, sum_left))
                sum_right, sum_left = pair_add(mix_part[k], sum_right, mix_part[Z_SIZE - k], sum_left)
            sum_right = scatter_right[k](sum_right)
            sum_left = scatter_left[k](sum_left)
        result = (x_f32 + plus(mix_part[0], sum_right, sum_left)).astype(jnp.bfloat16)

        def output_grads(rows_of_z):
            return rows_product([blks[n] for n in rows_of_z for blks in (dy_own, dy_pair)], w_mix, 2 * pair)

        do_early = output_grads(EARLY)
        do_late = output_grads(LATE)
        shared = (o_slots, kv_slots, kv_other, cos_t, sin_t, lo_all, lse, bk)
        dq_early, dkv_part = attend_backward(where, pos_all, q_slots, do_early, *shared, EARLY)

        def other_order(arr):
            lines = arr.reshape((2, CORE_SIZE) + arr.shape[1:])
            return jnp.concatenate([lines[:, 1:], lines[:, :1]], axis=1).reshape(arr.shape)

        dq_early_partner = swap_core(dq_early)
        early_own, early_partner = lax.optimization_barrier((dq_early, dq_early_partner))
        early_keep, early_send = pair_sides(early_own, other_order(early_partner))
        early_theirs = swap_y(early_send)
        dq_late, dkv_mine, dkv_send = attend_backward(where, pos_all, q_slots, do_late, *shared, LATE, dkv_part)
        dkv_theirs = swap_same_head(dkv_send)
        dq_late_partner = swap_core(dq_late)

        late_keep, late_send = pair_sides(dq_late, other_order(dq_late_partner))

        def natural(early, late):
            return jnp.concatenate([late[:2], early, late[2:]], axis=0).reshape((Z_SIZE, CORE_SIZE) + early.shape[1:])

        q_rows = jnp.concatenate([natural(dq_early, dq_late)[:, 0], natural(early_partner, dq_late_partner)[:, 1]], axis=-1)
        dq_rows = [lax.dynamic_index_in_dim(q_rows, lax.rem(z_idx - s + Z_SIZE, Z_SIZE), 0, keepdims=False) for s in range(Z_SIZE)]
        halves = [slice(0, model // 2), slice(model // 2, model)]
        dh_sum = []
        for n, cols in enumerate(halves):
            dh_sum.append(dot_f32(dq_rows[1], w_q[cols], COLS_OF_BOTH).astype(jnp.bfloat16))
            dh_sum[n] = ring(dh_sum[n])

        dkv_lines = finish_key_grads(where, dkv_mine, dkv_theirs, cos_my, sin_my)
        dkv_partner = flip_core(swap_core(dkv_lines))
        dkv_rows = jnp.concatenate([dkv_lines[:, 0], dkv_partner[:, 0]], axis=-1)
        dkv_next = ring_back(dkv_rows[1])

        def kv_part(rows, weights, cols):
            return dot_f32(rows, weights[cols], COLS_OF_BOTH)

        for s in hops[1:]:
            for n, cols in enumerate(halves):
                part = dot_f32(dq_rows[s], w_q[cols], COLS_OF_BOTH) + kv_part(dkv_rows[s], w_kv, cols)
                dh_sum[n] = (part + dh_sum[n].astype(jnp.float32)).astype(jnp.bfloat16)
                if s == hops[-1] and n == 0:
                    dh_sum[n], result = lax.optimization_barrier((dh_sum[n], result))
                dh_sum[n] = ring(dh_sum[n])
        g_pair = [swap_core(blk) for blk in lax.optimization_barrier((*g_own, dq_late))[:Z_SIZE]]
        kv_keep = select(dkv_lines[..., :HEAD_DIM], dkv_partner[..., HEAD_DIM:])
        kv_send = select(dkv_partner[..., :HEAD_DIM], dkv_lines[..., HEAD_DIM:])
        kv_theirs = swap_y(kv_send)
        late_theirs = swap_y(late_send)

        def rows_of(early, late, kv_lines):
            return by_block(jnp.concatenate([mirrored(natural(early, late)), kv_lines], axis=-1))

        d_keep = rows_of(early_keep, late_keep, kv_keep)
        d_theirs = rows_of(early_theirs, late_theirs, kv_theirs)

        dwo_keep, dwo_send = token_grads(dy_slots, o_sides, [((pair, model), jnp.float32)] * 2)
        theirs_first = swap_y(dwo_send[:, halves[0]])
        theirs_last = swap_y(dwo_send[:, halves[1]])

        d_wq, kv_mine_sum = token_grads([blks[s] for mine, theirs in ((h_own, h_pair), (g_own, g_pair)) for s in range(Z_SIZE) for blks in (mine, theirs)], jnp.concatenate([d_keep, d_theirs], axis=0),
                                        [((model, pair), jnp.bfloat16), ((model, HEAD_DIM), jnp.float32)])
        kv_other_sum = swap_core(kv_mine_sum)
        d_wk = select(kv_mine_sum, kv_other_sum)
        d_wv = select(kv_other_sum, kv_mine_sum)

        dh_own = lax.optimization_barrier([dot_f32(dq_rows[0], w_q[cols], COLS_OF_BOTH) for cols in halves])
        kv_cols = jnp.concatenate([dkv_rows[0], after(dkv_next, kv_mine_sum)], axis=1)
        dh_own = lax.optimization_barrier([own + kv_part(kv_cols, w_kv_all, cols) for own, cols in zip(dh_own, halves)])
        dh_rows = jnp.concatenate([(own + part.astype(jnp.float32)).astype(jnp.bfloat16) for own, part in zip(dh_own, dh_sum)], axis=1)

        d_input, dg_part = norm_backward(dh_rows, x_hat, inv_rms, norm_gain)
        grad_x = (dy_blk.astype(jnp.float32) + d_input).astype(jnp.bfloat16)
        for near, far, both in ((swap_core, swap_y, swap_same_head), (z_swaps[1], z_swaps[2], z_swaps[3])):
            dg_part = (dg_part + near(dg_part)) + (far(dg_part) + both(dg_part))
            if near is swap_core:
                theirs_last = after(theirs_last, dg_part)
        d_wo = (dwo_keep + jnp.concatenate([theirs_first, theirs_last], axis=1)).astype(jnp.bfloat16)
        return result, grad_x, d_wq, d_wk, d_wv, d_wo, dg_part

    specs_in = (P(('dp', 'tp'), None), P(('dp', 'tp'), None), P('dp'), P(), P(None, 'tp'), P(), P(), P('tp', None))
    specs_out = (P(('dp', 'tp'), None), P(('dp', 'tp'), None), P('dp', 'tp'), P('dp', 'tp'), P('dp', 'tp'), P(('dp', 'tp'), None), P('dp'))
    return jax.shard_map(device_step, mesh=mesh, in_specs=specs_in, out_specs=specs_out, check_vma=False)
```

```python
import functools
import jax
import jax.numpy as jnp
from jax import lax
from jax.experimental import pallas as pl
from jax.experimental.pallas import tpu as pltpu
from jax.sharding import PartitionSpec as P

HEAD_DIM = 128
SCORE_SCALE = HEAD_DIM ** -0.5
SCALE_LOG2E = SCORE_SCALE * 1.4426950408889634
ROPE_THETA = 1000000.0
NORM_EPS = 1e-05
MASKED = -1e30
Z_SIZE = 4
Y_SIZE = 2
CORE_SIZE = 2
SLOTS = Z_SIZE * CORE_SIZE
EARLY, LATE = (1, 2), (0, 3)
NATURAL = (((1,), (0,)), ((), ()))
COLS_OF_BOTH = (((1,), (1,)), ((), ()))


def dot_f32(lhs, rhs, dims=NATURAL):
    return lax.dot_general(lhs, rhs, dims, preferred_element_type=jnp.float32)


def rope_tables(positions):
    exponents = jnp.arange(0, HEAD_DIM, 2, dtype=jnp.float32) / HEAD_DIM
    angles = jnp.power(ROPE_THETA, -exponents)[:, None] * positions.astype(jnp.float32)[None, :]
    return jnp.cos(angles), jnp.sin(angles)


def rotate_rows(t_f32, cos_t, sin_t):
    lead_half, tail_half = t_f32[:HEAD_DIM // 2], t_f32[HEAD_DIM // 2:]
    return jnp.concatenate([lead_half * cos_t - tail_half * sin_t, tail_half * cos_t + lead_half * sin_t], axis=0).astype(jnp.bfloat16)


def norm_forward(x_f32, norm_gain):
    inv_rms = lax.rsqrt(jnp.mean(x_f32 * x_f32, axis=-1, keepdims=True) + NORM_EPS)
    x_hat = x_f32 * inv_rms
    return (x_hat * norm_gain).astype(jnp.bfloat16), x_hat, inv_rms


def norm_backward(d_hidden, x_hat, inv_rms, norm_gain):
    d_f32 = d_hidden.astype(jnp.float32)
    d_gain = jnp.sum(d_f32 * x_hat, axis=0)
    scaled = d_f32 * norm_gain
    d_input = inv_rms * (scaled - x_hat * jnp.mean(scaled * x_hat, axis=-1, keepdims=True))
    return d_input, d_gain


def slot_of(where_ref, z, c):
    return 2 * lax.rem(where_ref[0] - z + Z_SIZE, Z_SIZE) + (where_ref[2] ^ c)


def slot_of_other(where_ref, z, c):
    return 2 * lax.rem(where_ref[0] - z + Z_SIZE, Z_SIZE) + (1 - (where_ref[2] ^ c))


def block_token(where_ref, b, bq):
    return pl.multiple_of((b // 2) * (4 * bq) + where_ref[1] * (2 * bq) + (b % 2) * bq, bq)


def key_range(pos_ref, start, bq, bk):
    lo_first, lo_last = start - pos_ref[start], start + bq - 1 - pos_ref[start + bq - 1]
    return lo_first // bk, (start + bq - 1) // bk + 1, (lo_last + bk - 1) // bk, (start + 1) // bk


def tile_lanes(row, heads):
    return jnp.concatenate([row] * heads, axis=1)


def row_bounds(lo_ref, start, bq, heads):
    tok = start + lax.broadcasted_iota(jnp.int32, (1, bq), 1)
    return tile_lanes(tok, heads), tile_lanes(lo_ref[:, pl.ds(start, bq)], heads)


def keep_mask(key_start, bk, t_row, lo_row):
    key_idx = key_start + lax.broadcasted_iota(jnp.int32, (bk, t_row.shape[1]), 0)
    return (key_idx <= t_row) & (key_idx >= lo_row)


def head_columns(block, h):
    return block[:, h * HEAD_DIM:(h + 1) * HEAD_DIM]


def rotated_queries(q_blk, cos_ref, sin_ref, start, bq, heads):
    cos_t, sin_t = cos_ref[:, pl.ds(start, bq)], sin_ref[:, pl.ds(start, bq)]
    return [rotate_rows(head_columns(q_blk, h).T.astype(jnp.float32), cos_t, sin_t) for h in range(heads)]


def visit_keys(bounds, step):
    first, end, inner_first, inner_end = bounds

    def visit(j, carry):
        inner = (j >= inner_first) & (j < inner_end)

        @pl.when(inner)
        def _():
            step(j, False)

        @pl.when(jnp.logical_not(inner))
        def _():
            step(j, True)

        return carry

    lax.fori_loop(first, end, visit, 0)


def for_key_blocks(where_ref, mine_ref, theirs_ref, count, bq, store):
    def visit(n, carry):
        z, y, c = n // 4, (n // 2) % 2, n % 2
        block = jnp.where(y == where_ref[1], mine_ref[slot_of(where_ref, z, c)], theirs_ref[slot_of_other(where_ref, z, c)])
        store(pl.ds(pl.multiple_of(n * bq, bq), bq), block)
        return carry

    lax.fori_loop(0, count, visit, 0)


def fwd_kernel(heads, bk, where_ref, pos_ref, q_ref, kv_ref, kv_other_ref, cos_ref, sin_ref, lo_ref, o_ref, lse_ref, k_s, vt_s, qt_s, m_s, l_s, acc_s):
    b = pl.program_id(0)
    bq = q_ref.shape[1]
    seq = k_s.shape[0]

    @pl.when(b == 0)
    def _():
        def store(rows, block):
            k_s[rows, :] = rotate_rows(block[:, :HEAD_DIM].T.astype(jnp.float32), cos_ref[:, rows], sin_ref[:, rows]).T
            vt_s[:, rows] = block[:, HEAD_DIM:].T

        for_key_blocks(where_ref, kv_ref, kv_other_ref, seq // bq, bq, store)

    start = block_token(where_ref, b, bq)
    t_row, lo_row = row_bounds(lo_ref, start, bq, heads)
    q_blk = q_ref[0]
    qt_s[...] = jnp.concatenate(rotated_queries(q_blk, cos_ref, sin_ref, start, bq, heads), axis=1)
    m_s[...] = jnp.full_like(m_s, MASKED)
    l_s[...] = jnp.zeros_like(l_s)
    acc_s[...] = jnp.zeros_like(acc_s)

    def step(j, masked):
        key_start = pl.multiple_of(j * bk, bk)
        keys = pl.ds(key_start, bk)
        scores = dot_f32(k_s[keys, :], qt_s[...])
        if masked:
            scores = jnp.where(keep_mask(key_start, bk, t_row, lo_row), scores, MASKED)
        m_old = m_s[...]
        m_new = jnp.maximum(m_old, jnp.max(scores, axis=0, keepdims=True))
        probs = jnp.exp2(scores * SCALE_LOG2E - m_new * SCALE_LOG2E)
        alpha = jnp.exp2((m_old - m_new) * SCALE_LOG2E)
        m_s[...] = m_new
        l_s[...] = l_s[...] * alpha + jnp.sum(probs, axis=0, keepdims=True)
        acc_s[...] = acc_s[...] * alpha + dot_f32(vt_s[:, keys], probs.astype(jnp.bfloat16))

    visit_keys(key_range(pos_ref, start, bq, bk), step)
    out_t = (acc_s[...] / l_s[...]).astype(jnp.bfloat16)
    for h in range(heads):
        o_ref[0, :, h * HEAD_DIM:(h + 1) * HEAD_DIM] = out_t[:, h * bq:(h + 1) * bq].T
    lse_ref[0] = m_s[...] * SCALE_LOG2E + jnp.log2(l_s[...])


def bwd_block(where_ref, step, rows):
    return rows[0] + (rows[1] - rows[0]) * (step // 2), where_ref[2] ^ (step % 2)


def bwd_kernel(heads, bk, rows_of_z, where_ref, pos_ref, q_ref, do_ref, o_ref, kv_ref, kv_other_ref, cos_ref, sin_ref, lo_ref, lse_ref, *refs):
    first = rows_of_z == EARLY
    if first:
        dq_ref, part_ref, k_s, kt_s, v_s, qt_s, dot_s, dqt_s, acc_s = refs
    else:
        part_ref, dq_ref, mine_ref, send_ref, k_s, kt_s, v_s, qt_s, dot_s, dqt_s, acc_s = refs
    step_idx = pl.program_id(0)
    z_blk, c_blk = bwd_block(where_ref, step_idx, rows_of_z)
    b = 2 * z_blk + c_blk
    bq = q_ref.shape[1]
    seq = k_s.shape[0]

    @pl.when(step_idx == 0)
    def _():
        def store(rows, block):
            acc_s[:, rows] = jnp.zeros((2 * HEAD_DIM, bq), jnp.float32) if first else part_ref[:, rows]
            k_rot_t = rotate_rows(block[:, :HEAD_DIM].T.astype(jnp.float32), cos_ref[:, rows], sin_ref[:, rows])
            kt_s[:, rows] = k_rot_t
            k_s[rows, :] = k_rot_t.T
            v_s[rows, :] = block[:, HEAD_DIM:]

        for_key_blocks(where_ref, kv_ref, kv_other_ref, seq // bq, bq, store)

    start = block_token(where_ref, b, bq)
    t_row, lo_row = row_bounds(lo_ref, start, bq, heads)
    q_blk, do_blk, o_blk = q_ref[0], do_ref[0], o_ref[0]
    deltas = []
    for h, q_rot_t in enumerate(rotated_queries(q_blk, cos_ref, sin_ref, start, bq, heads)):
        lanes = slice(h * bq, (h + 1) * bq)
        qt_s[:, lanes] = q_rot_t
        do_t = head_columns(do_blk, h).T
        dot_s[:, lanes] = do_t
        deltas.append(jnp.sum(do_t.astype(jnp.float32) * head_columns(o_blk, h).T.astype(jnp.float32), axis=0, keepdims=True))
    delta = jnp.concatenate(deltas, axis=1)
    lse = lse_ref[0]
    dqt_s[...] = jnp.zeros_like(dqt_s)

    def step(j, masked):
        key_start = pl.multiple_of(j * bk, bk)
        keys = pl.ds(key_start, bk)
        scores = dot_f32(k_s[keys, :], qt_s[...])
        probs = jnp.exp2(scores * SCALE_LOG2E - lse)
        if masked:
            probs = jnp.where(keep_mask(key_start, bk, t_row, lo_row), probs, 0.0)
        d_probs = dot_f32(v_s[keys, :], dot_s[...])
        d_scores = (probs * (d_probs - delta)).astype(jnp.bfloat16)
        acc_s[HEAD_DIM:, keys] += dot_f32(dot_s[...], probs.astype(jnp.bfloat16), COLS_OF_BOTH)
        acc_s[:HEAD_DIM, keys] += dot_f32(qt_s[...], d_scores, COLS_OF_BOTH) * SCORE_SCALE
        dqt_s[...] += dot_f32(kt_s[:, keys], d_scores)

    visit_keys(key_range(pos_ref, start, bq, bk), step)
    cos_t, sin_t = cos_ref[:, pl.ds(start, bq)], sin_ref[:, pl.ds(start, bq)]
    for h in range(heads):
        dq_rot_t = (dqt_s[:, h * bq:(h + 1) * bq] * SCORE_SCALE).astype(jnp.bfloat16).astype(jnp.float32)
        dq_ref[0, :, h * HEAD_DIM:(h + 1) * HEAD_DIM] = rotate_rows(dq_rot_t, cos_t, -sin_t).T

    @pl.when(step_idx == pl.num_programs(0) - 1)
    def _():
        if first:
            part_ref[...] = acc_s[...]
            return

        def hand_over(y, mine):
            for z in range(Z_SIZE):
                for c in range(CORE_SIZE):
                    rows = ((z * 2 + y) * 2 + c) * bq
                    e = where_ref[2] ^ c
                    if mine:
                        mine_ref[z, e] = acc_s[:, rows:rows + bq].T
                    else:
                        send_ref[z, 1 - e] = acc_s[:, rows:rows + bq].T

        for y in range(Y_SIZE):
            pl.when(where_ref[1] == y)(functools.partial(hand_over, y, True))
            pl.when(where_ref[1] != y)(functools.partial(hand_over, y, False))


def token_grads_kernel(count, *refs):
    blocks, lhs_ref, out_refs, lhs_t = refs[:count], refs[count], refs[count + 1:-1], refs[-1]
    rows = lhs_ref.shape[1]

    @pl.when(pl.program_id(0) == 0)
    def _():
        for n in range(count):
            lhs_t[:, n * rows:(n + 1) * rows] = lhs_ref[n].T

    total = sum(dot_f32(lhs_t[:, n * rows:(n + 1) * rows], blocks[n][...]) for n in range(count))
    start = 0
    for ref in out_refs:
        if ref.shape[0] == blocks[0].shape[1]:
            size = ref.shape[1]
            ref[...] = total[start:start + size, :].T.astype(ref.dtype)
        else:
            size = ref.shape[0]
            ref[...] = total[start:start + size, :].astype(ref.dtype)
        start += size


def token_grads(blocks, lhs, outs, tile=512):
    rows, model = blocks[0].shape
    width = lhs.shape[2]
    specs = [pl.BlockSpec((tile, shape[1]), lambda i: (i, 0)) if shape[0] == model else pl.BlockSpec((shape[0], tile), lambda i: (0, i)) for shape, _ in outs]
    return pl.pallas_call(
        functools.partial(token_grads_kernel, len(blocks)),
        out_shape=[jax.ShapeDtypeStruct(*out) for out in outs], grid=(model // tile,),
        in_specs=[pl.BlockSpec((rows, tile), lambda i: (0, i)) for _ in blocks] + [pl.BlockSpec(lhs.shape, lambda i: (0, 0, 0))], out_specs=specs,
        scratch_shapes=[pltpu.VMEM((width, len(blocks) * rows), jnp.bfloat16)],
        compiler_params=pltpu.CompilerParams(dimension_semantics=('arbitrary',), vmem_limit_bytes=48 << 20),
        cost_estimate=pl.CostEstimate(flops=2 * len(blocks) * rows * model * width, bytes_accessed=2 * len(blocks) * rows * model, transcendentals=0),
    )(*blocks, lhs)


def rows_product_kernel(count, *refs):
    blocks, w_ref, out_ref, acc_ref = refs[:count], refs[count], refs[count + 1], refs[count + 2]
    step, rows = pl.program_id(0), blocks[0].shape[0]
    lhs = jnp.concatenate([blk[...] for blk in blocks], axis=0)
    part = dot_f32(lhs, w_ref[...], COLS_OF_BOTH)

    @pl.when(step == 0)
    def _():
        acc_ref[...] = part

    @pl.when(step > 0)
    def _():
        acc_ref[...] += part

    @pl.when(step == pl.num_programs(0) - 1)
    def _():
        for n in range(count):
            out_ref[n] = acc_ref[n * rows:(n + 1) * rows, :].astype(jnp.bfloat16)


def rows_product(blocks, weights, width):
    rows, model = blocks[0].shape
    tile = model // 4
    out_shape = (len(blocks), rows, width)
    return pl.pallas_call(
        functools.partial(rows_product_kernel, len(blocks)), out_shape=jax.ShapeDtypeStruct(out_shape, jnp.bfloat16), grid=(model // tile,),
        in_specs=[pl.BlockSpec((rows, tile), lambda i: (0, i))] * len(blocks) + [pl.BlockSpec((width, tile), lambda i: (0, i))],
        out_specs=pl.BlockSpec(out_shape, lambda i: (0, 0, 0)), scratch_shapes=[pltpu.VMEM((len(blocks) * rows, width), jnp.float32)],
        compiler_params=pltpu.CompilerParams(dimension_semantics=('arbitrary',), vmem_limit_bytes=40 << 20),
        cost_estimate=pl.CostEstimate(flops=2 * len(blocks) * rows * model * width, bytes_accessed=2 * (len(blocks) * rows + width) * model, transcendentals=0),
    )(*blocks, weights)


def pick_kernel(count, where_ref, *refs):
    sources, outs, sems = refs[:count * Z_SIZE], refs[count * Z_SIZE:-1], refs[-1]

    def copy(n, k):
        return pltpu.make_async_copy(sources[n * Z_SIZE + k], outs[n], sems.at[n])

    for n in range(count):
        for k in range(Z_SIZE):
            pl.when(where_ref[0] == k)(lambda n=n, k=k: copy(n, k).start())
    for n in range(count):
        copy(n, 0).wait()


def pick(where, *choices):
    shape = choices[0][0].shape
    return pl.pallas_call(
        functools.partial(pick_kernel, len(choices)), out_shape=[jax.ShapeDtypeStruct(shape, jnp.bfloat16)] * len(choices),
        grid_spec=pltpu.PrefetchScalarGridSpec(
            num_scalar_prefetch=1, grid=(1,), in_specs=[pl.BlockSpec(memory_space=pl.ANY)] * (len(choices) * Z_SIZE), out_specs=[full_spec(shape)] * len(choices),
            scratch_shapes=[pltpu.SemaphoreType.DMA((len(choices),))]),
        compiler_params=pltpu.CompilerParams(dimension_semantics=('arbitrary',), vmem_limit_bytes=32 << 20),
        cost_estimate=pl.CostEstimate(flops=1000000, bytes_accessed=8000000, transcendentals=0),
    )(where, *(arr for choice in choices for arr in choice))


def pair_add_kernel(a_ref, b_ref, c_ref, d_ref, ab_ref, cd_ref):
    for left, right, out in ((a_ref, b_ref, ab_ref), (c_ref, d_ref, cd_ref)):
        out[...] = (left[...].astype(jnp.float32) + right[...].astype(jnp.float32)).astype(jnp.bfloat16)


def pair_add(*operands):
    rows, model = operands[0].shape
    tile = model // 4
    spec = pl.BlockSpec((rows, tile), lambda i: (0, i))
    return pl.pallas_call(
        pair_add_kernel, out_shape=[jax.ShapeDtypeStruct((rows, model), jnp.bfloat16)] * 2, grid=(model // tile,), in_specs=[spec] * 4, out_specs=[spec] * 2,
        compiler_params=pltpu.CompilerParams(dimension_semantics=('arbitrary',), vmem_limit_bytes=32 << 20),
        cost_estimate=pl.CostEstimate(flops=4 * rows * model, bytes_accessed=12 * rows * model, transcendentals=0),
    )(*operands)


def finish_kernel(where_ref, mine_ref, other_ref, cos_ref, sin_ref, out_ref):
    for z in range(Z_SIZE):
        slot = lax.rem(where_ref[0] - z + Z_SIZE, Z_SIZE)
        for e in range(CORE_SIZE):
            total = mine_ref[z, e] + other_ref[z, e]
            dk = total[:, :HEAD_DIM].astype(jnp.bfloat16).astype(jnp.float32)
            out_ref[slot, e, :, :HEAD_DIM] = (dk * cos_ref[z, e] + pltpu.roll(dk, HEAD_DIM // 2, 1) * sin_ref[z, e]).astype(jnp.bfloat16)
            out_ref[slot, e, :, HEAD_DIM:] = total[:, HEAD_DIM:].astype(jnp.bfloat16)


def finish_key_grads(where, *operands):
    return pl.pallas_call(
        finish_kernel, out_shape=jax.ShapeDtypeStruct(operands[0].shape, jnp.bfloat16),
        grid_spec=pltpu.PrefetchScalarGridSpec(num_scalar_prefetch=1, grid=(1,), in_specs=[full_spec(arr.shape) for arr in operands], out_specs=full_spec(operands[0].shape)),
        compiler_params=pltpu.CompilerParams(dimension_semantics=('arbitrary',), vmem_limit_bytes=32 << 20),
        cost_estimate=pl.CostEstimate(flops=1000000, bytes_accessed=8000000, transcendentals=0),
    )(where, *operands)


def full_spec(shape):
    return pl.BlockSpec(shape, lambda b, *_: (0,) * len(shape))


def attend(where, positions, q_slots, kv_slots, kv_other, cos_t, sin_t, lo_all, bk):
    slots, bq, width = q_slots.shape
    seq = positions.shape[0]
    heads = width // HEAD_DIM
    lanes = heads * bq
    shared = (kv_slots, kv_other, cos_t, sin_t, lo_all)
    block = pl.BlockSpec((1, bq, width), lambda i, where_ref, _: (slot_of(where_ref, i // 2, i % 2), 0, 0))
    work = slots * bq * heads * seq * HEAD_DIM
    return pl.pallas_call(
        functools.partial(fwd_kernel, heads, bk),
        out_shape=(jax.ShapeDtypeStruct(q_slots.shape, jnp.bfloat16), jax.ShapeDtypeStruct((slots, 1, lanes), jnp.float32)),
        grid_spec=pltpu.PrefetchScalarGridSpec(
            num_scalar_prefetch=2, grid=(slots,), in_specs=[block] + [full_spec(arr.shape) for arr in shared],
            out_specs=(block, pl.BlockSpec((1, 1, lanes), lambda i, *_: (i, 0, 0))),
            scratch_shapes=[pltpu.VMEM((seq, HEAD_DIM), jnp.bfloat16), pltpu.VMEM((HEAD_DIM, seq), jnp.bfloat16), pltpu.VMEM((HEAD_DIM, lanes), jnp.bfloat16),
                            pltpu.VMEM((1, lanes), jnp.float32), pltpu.VMEM((1, lanes), jnp.float32), pltpu.VMEM((HEAD_DIM, lanes), jnp.float32)]),
        compiler_params=pltpu.CompilerParams(dimension_semantics=('arbitrary',), vmem_limit_bytes=48 << 20),
        cost_estimate=pl.CostEstimate(flops=4 * work, bytes_accessed=4 * slots * bq * width + 8 * seq * HEAD_DIM, transcendentals=work // (2 * HEAD_DIM)),
        name='attend_fwd',
    )(where, positions, q_slots, *shared)


def attend_backward(where, positions, q_slots, do_blocks, o_slots, kv_slots, kv_other, cos_t, sin_t, lo_all, lse, bk, rows_of_z, part=None):
    count, bq, width = do_blocks.shape
    seq = positions.shape[0]
    heads = width // HEAD_DIM
    lanes = heads * bq
    shared = (kv_slots, kv_other, cos_t, sin_t, lo_all)

    def slot_index(i, where_ref, _):
        return (slot_of(where_ref, *bwd_block(where_ref, i, rows_of_z)), 0, 0)

    def lse_index(i, where_ref, _):
        z_blk, c_blk = bwd_block(where_ref, i, rows_of_z)
        return (2 * z_blk + c_blk, 0, 0)

    block = pl.BlockSpec((1, bq, width), slot_index)
    local = pl.BlockSpec((1, bq, width), lambda i, *_: (i, 0, 0))
    operands = [q_slots, do_blocks, o_slots, *shared, lse]
    in_specs = [block, local, block] + [full_spec(arr.shape) for arr in shared] + [pl.BlockSpec((1, 1, lanes), lse_index)]
    part_shape, final_shape = (2 * HEAD_DIM, seq), (Z_SIZE, CORE_SIZE, bq, 2 * HEAD_DIM)
    grads = [part_shape] if part is None else [final_shape] * 2
    if part is not None:
        operands.append(part)
        in_specs.append(full_spec(part_shape))
    work = count * bq * heads * seq * HEAD_DIM
    return pl.pallas_call(
        functools.partial(bwd_kernel, heads, bk, rows_of_z),
        out_shape=[jax.ShapeDtypeStruct(do_blocks.shape, jnp.bfloat16)] + [jax.ShapeDtypeStruct(shape, jnp.float32) for shape in grads],
        grid_spec=pltpu.PrefetchScalarGridSpec(
            num_scalar_prefetch=2, grid=(count,), in_specs=in_specs, out_specs=[local] + [full_spec(shape) for shape in grads],
            scratch_shapes=[pltpu.VMEM((seq, HEAD_DIM), jnp.bfloat16), pltpu.VMEM((HEAD_DIM, seq), jnp.bfloat16), pltpu.VMEM((seq, HEAD_DIM), jnp.bfloat16),
                            pltpu.VMEM((HEAD_DIM, lanes), jnp.bfloat16), pltpu.VMEM((HEAD_DIM, lanes), jnp.bfloat16), pltpu.VMEM((HEAD_DIM, lanes), jnp.float32),
                            pltpu.VMEM((2 * HEAD_DIM, seq), jnp.float32)]),
        compiler_params=pltpu.CompilerParams(dimension_semantics=('arbitrary',), vmem_limit_bytes=58 << 20),
        cost_estimate=pl.CostEstimate(flops=10 * work, bytes_accessed=8 * count * bq * width + 24 * seq * HEAD_DIM, transcendentals=work // (2 * HEAD_DIM)),
        name='attend_bwd',
    )(where, positions, *operands)


def solution(mesh):
    def member(z, y, c):
        return (z * Y_SIZE + y) * CORE_SIZE + c

    every = [(z, y, c) for z in range(Z_SIZE) for y in range(Y_SIZE) for c in range(CORE_SIZE)]

    def permuter(target, senders=range(Z_SIZE)):
        pairs = [(member(*src), member(*target(*src))) for src in every if src[0] in senders]
        return lambda val: lax.ppermute(val, 'tp', pairs)

    swap_core = permuter(lambda z, y, c: (z, y, 1 - c))
    swap_y = permuter(lambda z, y, c: (z, 1 - y, c))
    swap_same_head = permuter(lambda z, y, c: (z, 1 - y, 1 - c))
    ring = permuter(lambda z, y, c: ((z + 1) % Z_SIZE, y, c))
    ring_back = permuter(lambda z, y, c: ((z - 1) % Z_SIZE, y, c))
    hops = range(1, Z_SIZE)
    gather_right = {k: permuter(lambda z, y, c: (z + 1, y, c), range(k - 1, Z_SIZE - 1)) for k in hops}
    gather_left = {k: permuter(lambda z, y, c: (z - 1, y, c), range(1, Z_SIZE - k + 1)) for k in hops}
    scatter_right = {k: permuter(lambda z, y, c: (z + 1, y, c), range(0, k)) for k in hops}
    scatter_left = {k: permuter(lambda z, y, c: (z - 1, y, c), range(Z_SIZE - k, Z_SIZE)) for k in hops}
    z_swaps = {k: permuter(lambda z, y, c, k=k: (z ^ k, y, c)) for k in hops}

    def after(val, *deps):
        return lax.optimization_barrier((val,) + deps)[0]

    def device_step(x_blk, dy_blk, pos_all, norm_gain, wq_loc, wk_all, wv_all, wo_loc):
        seq_len = pos_all.shape[0]
        bq = seq_len // (Z_SIZE * Y_SIZE * CORE_SIZE)
        bk = 2 * bq
        model = x_blk.shape[1]
        idx = lax.axis_index('tp')
        z_idx, y_idx, c_idx = idx // (Y_SIZE * CORE_SIZE), (idx // CORE_SIZE) % Y_SIZE, idx % CORE_SIZE
        where = jnp.stack([z_idx, y_idx, c_idx])
        on_core0 = c_idx == 0
        pair = wq_loc.shape[1]
        kv_own = Y_SIZE * z_idx + (y_idx ^ c_idx)

        def select(first, second):
            return jnp.where(on_core0, first, second)

        def flip_core(arr):
            return arr[:, ::-1]

        def slots(arrs):
            return jnp.concatenate([arr[None] for arr in arrs], axis=0)

        def interleave(own, partner):
            return [blk for both in zip(own, partner) for blk in both]

        x_f32 = x_blk.astype(jnp.float32)
        hidden, x_hat, inv_rms = norm_forward(x_f32, norm_gain)

        h_own = [hidden]
        for s in hops:
            h_own.append(ring(h_own[-1]))
        h_pair = []
        for blk in h_own:
            h_pair.append(swap_core(blk))

        def slot_order(w_own, w_core, w_y, w_both):
            return [select(w_own, w_y), select(w_core, w_both), select(w_both, w_core), select(w_y, w_own)]

        wq_y = swap_y(wq_loc)
        wq_core = swap_core(wq_loc)
        q_cols = slot_order(wq_loc, wq_core, wq_y, swap_core(wq_y))
        wo_y = swap_y(wo_loc)
        o_rows = (wo_loc, swap_core(wo_loc), wo_y, swap_core(wo_y))

        def kv_columns(head):
            return [lax.dynamic_slice_in_dim(w, head * HEAD_DIM, HEAD_DIM, axis=1) for w in (wk_all, wv_all)]

        w_q = lax.optimization_barrier(jnp.concatenate(q_cols, axis=1))
        w_kv = lax.optimization_barrier(jnp.concatenate(kv_columns(kv_own) + kv_columns(kv_own ^ 1), axis=1))
        kv_heads = [lax.rem(kv_own + k * Y_SIZE, Y_SIZE * Z_SIZE) for k in range(2)]
        w_kv_all = lax.optimization_barrier(jnp.concatenate([cols for head in kv_heads for h in (head, head ^ 1) for cols in kv_columns(h)], axis=1))
        w_own = jnp.concatenate([w_q[:, :2 * pair], w_kv[:, :2 * HEAD_DIM]], axis=1)
        w_mix = jnp.concatenate(slot_order(*o_rows), axis=0)
        lo_all = (lax.iota(jnp.int32, seq_len) - pos_all)[None, :]
        cos_t, sin_t = rope_tables(pos_all)

        def my_tables(lead, tail):
            parts = jnp.concatenate([lead.T, tail.T], axis=1).reshape(Z_SIZE, Y_SIZE, CORE_SIZE, bq, HEAD_DIM)
            parts = lax.dynamic_index_in_dim(parts, y_idx, 1, keepdims=False)
            return select(parts, flip_core(parts))

        cos_my, sin_my = my_tables(cos_t, cos_t), my_tables(sin_t, -sin_t)

        qkv = []
        for s in range(Z_SIZE):
            qkv += [dot_f32(blk, w_own).astype(jnp.bfloat16) for blk in (h_own[s], h_pair[s])]
        kv_blocks = [blk[:, 2 * pair:] for blk in qkv]
        early = SLOTS - CORE_SIZE
        kv_other_early = swap_same_head(slots(kv_blocks[:early]))
        kv_other_late = swap_same_head(slots(kv_blocks[early:]))
        kv_other = jnp.concatenate([kv_other_early, kv_other_late], axis=0)
        q_slots, kv_slots = slots([blk[:, :2 * pair] for blk in qkv]), slots(kv_blocks)

        g_own = []
        for s, blk in enumerate(h_own):
            g_own.append(swap_y(after(blk, kv_other_late) if s else blk))

        right, left = {0: after(dy_blk, h_own[-1])}, {}
        left[0] = right[0]
        for k in hops:
            right[k] = gather_right[k](right[k - 1])
            left[k] = gather_left[k](left[k - 1])
            right[k], left[k] = lax.optimization_barrier((right[k], left[k]))
        dy_one, dy_two = pick(where, (left[1], dy_blk, right[1], right[2]), (left[2], left[1], dy_blk, right[1]))
        dy_zero, dy_three = pick(where, (dy_blk, right[1], right[2], right[3]), (left[3], left[2], left[1], dy_blk))
        dy_own = [dy_zero, dy_one, dy_two, dy_three]
        dy_pair = []
        for blk in dy_own:
            dy_pair.append(swap_core(blk))
        dy_slots = interleave(dy_own, dy_pair)

        def mirrored(lines):
            return jnp.concatenate([lax.dynamic_slice_in_dim(lines, lax.rem(z_idx - s + Z_SIZE, Z_SIZE), 1, axis=0) for s in range(Z_SIZE)], axis=0)

        forward = functools.partial(attend, where, pos_all, q_slots, kv_slots, kv_other, cos_t, sin_t, lo_all, bk)
        o_slots, lse = forward()
        by_line = (Z_SIZE, CORE_SIZE, bq, -1)
        o_lines = o_slots.reshape(by_line)
        o_partner = swap_core(o_slots).reshape(by_line)
        o_mine = jnp.concatenate([o_lines[:, 0], o_partner[:, 1]], axis=-1)

        def pair_sides(own, partner):
            first, last = own[..., :pair], partner[..., pair:2 * pair]
            return select(first, last), select(last, first)

        def by_block(arr):
            return arr.reshape((SLOTS,) + arr.shape[2:])

        o_sides = jnp.concatenate(pair_sides(o_lines, flip_core(o_partner)), axis=-1)
        o_sides = lax.optimization_barrier(by_block(mirrored(o_sides)))
        mix_part = []
        for s in range(Z_SIZE):
            mix_part.append(lax.optimization_barrier(dot_f32(o_mine[s], w_mix).astype(jnp.bfloat16)))

        def plus(*parts):
            return sum(part.astype(jnp.float32) for part in parts)

        sum_right, sum_left = mix_part[1], mix_part[Z_SIZE - 1]
        for k in hops:
            if k > 1:
                sum_right, sum_left = lax.optimization_barrier((sum_right, sum_left))
                sum_right, sum_left = pair_add(mix_part[k], sum_right, mix_part[Z_SIZE - k], sum_left)
            sum_right = scatter_right[k](sum_right)
            sum_left = scatter_left[k](sum_left)
        result = (x_f32 + plus(mix_part[0], sum_right, sum_left)).astype(jnp.bfloat16)

        def output_grads(rows_of_z):
            return rows_product([blks[n] for n in rows_of_z for blks in (dy_own, dy_pair)], w_mix, 2 * pair)

        do_early = output_grads(EARLY)
        do_late = output_grads(LATE)
        shared = (o_slots, kv_slots, kv_other, cos_t, sin_t, lo_all, lse, bk)
        dq_early, dkv_part = attend_backward(where, pos_all, q_slots, do_early, *shared, EARLY)

        def other_order(arr):
            lines = arr.reshape((2, CORE_SIZE) + arr.shape[1:])
            return jnp.concatenate([lines[:, 1:], lines[:, :1]], axis=1).reshape(arr.shape)

        dq_early_partner = swap_core(dq_early)
        early_own, early_partner = lax.optimization_barrier((dq_early, dq_early_partner))
        early_keep, early_send = pair_sides(early_own, other_order(early_partner))
        early_theirs = swap_y(early_send)
        dq_late, dkv_mine, dkv_send = attend_backward(where, pos_all, q_slots, do_late, *shared, LATE, dkv_part)
        dkv_theirs = swap_same_head(dkv_send)
        dq_late_partner = swap_core(dq_late)

        late_keep, late_send = pair_sides(dq_late, other_order(dq_late_partner))

        def natural(early, late):
            return jnp.concatenate([late[:2], early, late[2:]], axis=0).reshape((Z_SIZE, CORE_SIZE) + early.shape[1:])

        q_rows = lax.optimization_barrier(jnp.concatenate([natural(dq_early, dq_late)[:, 0], natural(early_partner, dq_late_partner)[:, 1]], axis=-1))
        dq_rows = [lax.dynamic_index_in_dim(q_rows, lax.rem(z_idx - s + Z_SIZE, Z_SIZE), 0, keepdims=False) for s in range(Z_SIZE)]
        halves = [slice(0, model // 2), slice(model // 2, model)]

        def first_rows(early, late, e):
            pick_row = functools.partial(lax.dynamic_index_in_dim, axis=0, keepdims=False)
            return jnp.where(z_idx < 2, pick_row(late, jnp.clip(2 - 2 * z_idx, 0, 2) + e), pick_row(early, jnp.clip(2 * z_idx - 4, 0, 2) + e))

        first = jnp.concatenate([first_rows(dq_early, dq_late, 0), first_rows(early_partner, dq_late_partner, 1)], axis=-1)
        dh_sum = []
        for n, cols in enumerate(halves):
            dh_sum.append(dot_f32(first, w_q[cols], COLS_OF_BOTH).astype(jnp.bfloat16))
            dh_sum[n] = ring(dh_sum[n])

        dkv_lines = finish_key_grads(where, dkv_mine, dkv_theirs, cos_my, sin_my)
        dkv_partner = flip_core(swap_core(dkv_lines))
        dkv_rows = jnp.concatenate([dkv_lines[:, 0], dkv_partner[:, 0]], axis=-1)
        dkv_next = ring_back(dkv_rows[1])

        def kv_part(rows, weights, cols):
            return dot_f32(rows, weights[cols], COLS_OF_BOTH)

        for s in hops[1:]:
            for n, cols in enumerate(halves):
                part = dot_f32(dq_rows[s], w_q[cols], COLS_OF_BOTH) + kv_part(dkv_rows[s], w_kv, cols)
                dh_sum[n] = (part + dh_sum[n].astype(jnp.float32)).astype(jnp.bfloat16)
                if s == hops[-1] and n == 0:
                    dh_sum[n], result = lax.optimization_barrier((dh_sum[n], result))
                dh_sum[n] = ring(dh_sum[n])
        g_pair = [swap_core(blk) for blk in lax.optimization_barrier((*g_own, dq_late))[:Z_SIZE]]
        kv_keep = select(dkv_lines[..., :HEAD_DIM], dkv_partner[..., HEAD_DIM:])
        kv_send = select(dkv_partner[..., :HEAD_DIM], dkv_lines[..., HEAD_DIM:])
        kv_theirs = swap_y(kv_send)
        late_theirs = swap_y(late_send)

        def rows_of(early, late, kv_lines):
            return by_block(jnp.concatenate([mirrored(natural(early, late)), kv_lines], axis=-1))

        d_keep = rows_of(early_keep, late_keep, kv_keep)
        d_theirs = rows_of(early_theirs, late_theirs, kv_theirs)

        dwo_keep, dwo_send = token_grads(dy_slots, o_sides, [((pair, model), jnp.float32)] * 2)
        theirs_first = swap_y(dwo_send[:, halves[0]])
        theirs_last = swap_y(dwo_send[:, halves[1]])

        d_wq, kv_mine_sum = token_grads([blks[s] for mine, theirs in ((h_own, h_pair), (g_own, g_pair)) for s in range(Z_SIZE) for blks in (mine, theirs)], jnp.concatenate([d_keep, d_theirs], axis=0),
                                        [((model, pair), jnp.bfloat16), ((model, HEAD_DIM), jnp.float32)])
        kv_other_sum = swap_core(kv_mine_sum)
        d_wk = select(kv_mine_sum, kv_other_sum)
        d_wv = select(kv_other_sum, kv_mine_sum)

        dh_own = lax.optimization_barrier([dot_f32(dq_rows[0], w_q[cols], COLS_OF_BOTH) for cols in halves])
        kv_cols = jnp.concatenate([dkv_rows[0], after(dkv_next, kv_mine_sum)], axis=1)
        dh_own = lax.optimization_barrier([own + kv_part(kv_cols, w_kv_all, cols) for own, cols in zip(dh_own, halves)])
        dh_rows = jnp.concatenate([(own + part.astype(jnp.float32)).astype(jnp.bfloat16) for own, part in zip(dh_own, dh_sum)], axis=1)

        d_input, dg_part = norm_backward(dh_rows, x_hat, inv_rms, norm_gain)
        grad_x = (dy_blk.astype(jnp.float32) + d_input).astype(jnp.bfloat16)
        for near, far, both in ((swap_core, swap_y, swap_same_head), (z_swaps[1], z_swaps[2], z_swaps[3])):
            dg_part = (dg_part + near(dg_part)) + (far(dg_part) + both(dg_part))
            if near is swap_core:
                theirs_last = after(theirs_last, dg_part)
        d_wo = (dwo_keep + jnp.concatenate([theirs_first, theirs_last], axis=1)).astype(jnp.bfloat16)
        return result, grad_x, d_wq, d_wk, d_wv, d_wo, dg_part

    specs_in = (P(('dp', 'tp'), None), P(('dp', 'tp'), None), P('dp'), P(), P(None, 'tp'), P(), P(), P('tp', None))
    specs_out = (P(('dp', 'tp'), None), P(('dp', 'tp'), None), P('dp', 'tp'), P('dp', 'tp'), P('dp', 'tp'), P(('dp', 'tp'), None), P('dp'))
    return jax.shard_map(device_step, mesh=mesh, in_specs=specs_in, out_specs=specs_out, check_vma=False)
```

```python
import functools
import jax
import jax.numpy as jnp
from jax import lax
from jax.experimental import pallas as pl
from jax.experimental.pallas import tpu as pltpu
from jax.sharding import PartitionSpec as P

HEAD_DIM = 128
SCORE_SCALE = HEAD_DIM ** -0.5
SCALE_LOG2E = SCORE_SCALE * 1.4426950408889634
ROPE_THETA = 1000000.0
NORM_EPS = 1e-05
MASKED = -1e30
Z_SIZE = 4
Y_SIZE = 2
CORE_SIZE = 2
SLOTS = Z_SIZE * CORE_SIZE
EARLY, LATE = (1, 2), (0, 3)
TOKENS, WHOLE, FIRST_HALF, LAST_HALF = range(4)
NATURAL = (((1,), (0,)), ((), ()))
COLS_OF_BOTH = (((1,), (1,)), ((), ()))


def dot_f32(lhs, rhs, dims=NATURAL):
    return lax.dot_general(lhs, rhs, dims, preferred_element_type=jnp.float32)


def rope_tables(positions):
    exponents = jnp.arange(0, HEAD_DIM, 2, dtype=jnp.float32) / HEAD_DIM
    angles = jnp.power(ROPE_THETA, -exponents)[:, None] * positions.astype(jnp.float32)[None, :]
    return jnp.cos(angles), jnp.sin(angles)


def rotate_rows(t_f32, cos_t, sin_t):
    lead_half, tail_half = t_f32[:HEAD_DIM // 2], t_f32[HEAD_DIM // 2:]
    return jnp.concatenate([lead_half * cos_t - tail_half * sin_t, tail_half * cos_t + lead_half * sin_t], axis=0).astype(jnp.bfloat16)


def norm_forward(x_f32, norm_gain):
    inv_rms = lax.rsqrt(jnp.mean(x_f32 * x_f32, axis=-1, keepdims=True) + NORM_EPS)
    x_hat = x_f32 * inv_rms
    return (x_hat * norm_gain).astype(jnp.bfloat16), x_hat, inv_rms


def norm_backward(d_hidden, x_hat, inv_rms, norm_gain):
    d_f32 = d_hidden.astype(jnp.float32)
    d_gain = jnp.sum(d_f32 * x_hat, axis=0)
    scaled = d_f32 * norm_gain
    d_input = inv_rms * (scaled - x_hat * jnp.mean(scaled * x_hat, axis=-1, keepdims=True))
    return d_input, d_gain


def slot_of(where_ref, z, c):
    return 2 * lax.rem(where_ref[0] - z + Z_SIZE, Z_SIZE) + (where_ref[2] ^ c)


def slot_of_other(where_ref, z, c):
    return 2 * lax.rem(where_ref[0] - z + Z_SIZE, Z_SIZE) + (1 - (where_ref[2] ^ c))


def block_token(where_ref, b, bq):
    return pl.multiple_of((b // 2) * (4 * bq) + where_ref[1] * (2 * bq) + (b % 2) * bq, bq)


def key_range(pos_ref, start, bq, bk):
    lo_first, lo_last = start - pos_ref[start], start + bq - 1 - pos_ref[start + bq - 1]
    return lo_first // bk, (start + bq - 1) // bk + 1, (lo_last + bk - 1) // bk, (start + 1) // bk


def tile_lanes(row, heads):
    return jnp.concatenate([row] * heads, axis=1)


def row_bounds(lo_ref, start, bq, heads):
    tok = start + lax.broadcasted_iota(jnp.int32, (1, bq), 1)
    return tile_lanes(tok, heads), tile_lanes(lo_ref[:, pl.ds(start, bq)], heads)


def keep_mask(key_start, bk, t_row, lo_row):
    key_idx = key_start + lax.broadcasted_iota(jnp.int32, (bk, t_row.shape[1]), 0)
    return (key_idx <= t_row) & (key_idx >= lo_row)


def head_columns(block, h):
    return block[:, h * HEAD_DIM:(h + 1) * HEAD_DIM]


def rotated_queries(q_blk, cos_ref, sin_ref, start, bq, heads):
    cos_t, sin_t = cos_ref[:, pl.ds(start, bq)], sin_ref[:, pl.ds(start, bq)]
    return [rotate_rows(head_columns(q_blk, h).T.astype(jnp.float32), cos_t, sin_t) for h in range(heads)]


def visit_keys(bounds, step):
    first, end, inner_first, inner_end = bounds

    def visit(j, carry):
        inner = (j >= inner_first) & (j < inner_end)

        @pl.when(inner)
        def _():
            step(j, False)

        @pl.when(jnp.logical_not(inner))
        def _():
            step(j, True)

        return carry

    lax.fori_loop(first, end, visit, 0)


def for_key_blocks(where_ref, mine_ref, theirs_ref, count, bq, store):
    def visit(n, carry):
        z, y, c = n // 4, (n // 2) % 2, n % 2
        block = jnp.where(y == where_ref[1], mine_ref[slot_of(where_ref, z, c)], theirs_ref[slot_of_other(where_ref, z, c)])
        store(pl.ds(pl.multiple_of(n * bq, bq), bq), block)
        return carry

    lax.fori_loop(0, count, visit, 0)


def fwd_kernel(heads, bk, where_ref, pos_ref, q_ref, kv_ref, kv_other_ref, cos_ref, sin_ref, lo_ref, o_ref, lse_ref, k_s, vt_s, qt_s, m_s, l_s, acc_s):
    b = pl.program_id(0)
    bq = q_ref.shape[1]
    seq = k_s.shape[0]

    @pl.when(b == 0)
    def _():
        def store(rows, block):
            k_s[rows, :] = rotate_rows(block[:, :HEAD_DIM].T.astype(jnp.float32), cos_ref[:, rows], sin_ref[:, rows]).T
            vt_s[:, rows] = block[:, HEAD_DIM:].T

        for_key_blocks(where_ref, kv_ref, kv_other_ref, seq // bq, bq, store)

    start = block_token(where_ref, b, bq)
    t_row, lo_row = row_bounds(lo_ref, start, bq, heads)
    q_blk = q_ref[0]
    qt_s[...] = jnp.concatenate(rotated_queries(q_blk, cos_ref, sin_ref, start, bq, heads), axis=1)
    m_s[...] = jnp.full_like(m_s, MASKED)
    l_s[...] = jnp.zeros_like(l_s)
    acc_s[...] = jnp.zeros_like(acc_s)

    def step(j, masked):
        key_start = pl.multiple_of(j * bk, bk)
        keys = pl.ds(key_start, bk)
        scores = dot_f32(k_s[keys, :], qt_s[...])
        if masked:
            scores = jnp.where(keep_mask(key_start, bk, t_row, lo_row), scores, MASKED)
        m_old = m_s[...]
        m_new = jnp.maximum(m_old, jnp.max(scores, axis=0, keepdims=True))
        probs = jnp.exp2(scores * SCALE_LOG2E - m_new * SCALE_LOG2E)
        alpha = jnp.exp2((m_old - m_new) * SCALE_LOG2E)
        m_s[...] = m_new
        l_s[...] = l_s[...] * alpha + jnp.sum(probs, axis=0, keepdims=True)
        acc_s[...] = acc_s[...] * alpha + dot_f32(vt_s[:, keys], probs.astype(jnp.bfloat16))

    visit_keys(key_range(pos_ref, start, bq, bk), step)
    out_t = (acc_s[...] / l_s[...]).astype(jnp.bfloat16)
    for h in range(heads):
        o_ref[0, :, h * HEAD_DIM:(h + 1) * HEAD_DIM] = out_t[:, h * bq:(h + 1) * bq].T
    lse_ref[0] = m_s[...] * SCALE_LOG2E + jnp.log2(l_s[...])


def bwd_block(where_ref, step, rows):
    return rows[0] + (rows[1] - rows[0]) * (step // 2), where_ref[2] ^ (step % 2)


def bwd_kernel(heads, bk, rows_of_z, where_ref, pos_ref, q_ref, do_ref, o_ref, kv_ref, kv_other_ref, cos_ref, sin_ref, lo_ref, lse_ref, *refs):
    first = rows_of_z == EARLY
    if first:
        dq_ref, part_ref, k_s, kt_s, v_s, qt_s, dot_s, dqt_s, acc_s = refs
    else:
        part_ref, dq_ref, mine_ref, send_ref, k_s, kt_s, v_s, qt_s, dot_s, dqt_s, acc_s = refs
    step_idx = pl.program_id(0)
    z_blk, c_blk = bwd_block(where_ref, step_idx, rows_of_z)
    b = 2 * z_blk + c_blk
    bq = q_ref.shape[1]
    seq = k_s.shape[0]

    @pl.when(step_idx == 0)
    def _():
        def store(rows, block):
            acc_s[:, rows] = jnp.zeros((2 * HEAD_DIM, bq), jnp.float32) if first else part_ref[:, rows]
            k_rot_t = rotate_rows(block[:, :HEAD_DIM].T.astype(jnp.float32), cos_ref[:, rows], sin_ref[:, rows])
            kt_s[:, rows] = k_rot_t
            k_s[rows, :] = k_rot_t.T
            v_s[rows, :] = block[:, HEAD_DIM:]

        for_key_blocks(where_ref, kv_ref, kv_other_ref, seq // bq, bq, store)

    start = block_token(where_ref, b, bq)
    t_row, lo_row = row_bounds(lo_ref, start, bq, heads)
    q_blk, do_blk, o_blk = q_ref[0], do_ref[0], o_ref[0]
    deltas = []
    for h, q_rot_t in enumerate(rotated_queries(q_blk, cos_ref, sin_ref, start, bq, heads)):
        lanes = slice(h * bq, (h + 1) * bq)
        qt_s[:, lanes] = q_rot_t
        do_t = head_columns(do_blk, h).T
        dot_s[:, lanes] = do_t
        deltas.append(jnp.sum(do_t.astype(jnp.float32) * head_columns(o_blk, h).T.astype(jnp.float32), axis=0, keepdims=True))
    delta = jnp.concatenate(deltas, axis=1)
    lse = lse_ref[0]
    dqt_s[...] = jnp.zeros_like(dqt_s)

    def step(j, masked):
        key_start = pl.multiple_of(j * bk, bk)
        keys = pl.ds(key_start, bk)
        scores = dot_f32(k_s[keys, :], qt_s[...])
        probs = jnp.exp2(scores * SCALE_LOG2E - lse)
        if masked:
            probs = jnp.where(keep_mask(key_start, bk, t_row, lo_row), probs, 0.0)
        d_probs = dot_f32(v_s[keys, :], dot_s[...])
        d_scores = (probs * (d_probs - delta)).astype(jnp.bfloat16)
        acc_s[HEAD_DIM:, keys] += dot_f32(dot_s[...], probs.astype(jnp.bfloat16), COLS_OF_BOTH)
        acc_s[:HEAD_DIM, keys] += dot_f32(qt_s[...], d_scores, COLS_OF_BOTH) * SCORE_SCALE
        dqt_s[...] += dot_f32(kt_s[:, keys], d_scores)

    visit_keys(key_range(pos_ref, start, bq, bk), step)
    cos_t, sin_t = cos_ref[:, pl.ds(start, bq)], sin_ref[:, pl.ds(start, bq)]
    for h in range(heads):
        dq_rot_t = (dqt_s[:, h * bq:(h + 1) * bq] * SCORE_SCALE).astype(jnp.bfloat16).astype(jnp.float32)
        dq_ref[0, :, h * HEAD_DIM:(h + 1) * HEAD_DIM] = rotate_rows(dq_rot_t, cos_t, -sin_t).T

    @pl.when(step_idx == pl.num_programs(0) - 1)
    def _():
        if first:
            part_ref[...] = acc_s[...]
            return

        def hand_over(y, mine):
            for z in range(Z_SIZE):
                for c in range(CORE_SIZE):
                    rows = ((z * 2 + y) * 2 + c) * bq
                    e = where_ref[2] ^ c
                    if mine:
                        mine_ref[z, e] = acc_s[:, rows:rows + bq].T
                    else:
                        send_ref[z, 1 - e] = acc_s[:, rows:rows + bq].T

        for y in range(Y_SIZE):
            pl.when(where_ref[1] == y)(functools.partial(hand_over, y, True))
            pl.when(where_ref[1] != y)(functools.partial(hand_over, y, False))


def token_grads_kernel(count, parts, *refs):
    blocks, lhs_ref, out_refs, lhs_t = refs[:count], refs[count], refs[count + 1:-1], refs[-1]
    rows = lhs_ref.shape[1]
    step, steps = pl.program_id(0), pl.num_programs(0)

    @pl.when(step == 0)
    def _():
        for n in range(count):
            lhs_t[:, n * rows:(n + 1) * rows] = lhs_ref[n].T

    total = sum(dot_f32(lhs_t[:, n * rows:(n + 1) * rows], blocks[n][...]) for n in range(count))
    for ref, (start, size, kind) in zip(out_refs, parts):
        if kind == TOKENS:
            ref[...] = total[start:start + size, :].T.astype(ref.dtype)
            continue

        def store(ref=ref, start=start, size=size):
            ref[...] = total[start:start + size, :].astype(ref.dtype)

        if kind == WHOLE:
            store()
        else:
            pl.when((step < steps // 2) == (kind == FIRST_HALF))(store)


def token_grads(blocks, lhs, outs, tile=512):
    rows, model = blocks[0].shape
    width, steps = lhs.shape[2], model // tile
    columns = {WHOLE: lambda i: (0, i), FIRST_HALF: lambda i: (0, jnp.minimum(i, steps // 2 - 1)), LAST_HALF: lambda i: (0, jnp.maximum(i - steps // 2, 0))}
    parts, shapes, specs = [], [], []
    for start, size, kind, dtype in outs:
        parts.append((start, size, kind))
        if kind == TOKENS:
            shapes.append(jax.ShapeDtypeStruct((model, size), dtype))
            specs.append(pl.BlockSpec((tile, size), lambda i: (i, 0)))
        else:
            shapes.append(jax.ShapeDtypeStruct((size, model if kind == WHOLE else model // 2), dtype))
            specs.append(pl.BlockSpec((size, tile), columns[kind]))
    return pl.pallas_call(
        functools.partial(token_grads_kernel, len(blocks), parts), out_shape=shapes, grid=(steps,),
        in_specs=[pl.BlockSpec((rows, tile), lambda i: (0, i)) for _ in blocks] + [pl.BlockSpec(lhs.shape, lambda i: (0, 0, 0))], out_specs=specs,
        scratch_shapes=[pltpu.VMEM((width, len(blocks) * rows), jnp.bfloat16)],
        compiler_params=pltpu.CompilerParams(dimension_semantics=('arbitrary',), vmem_limit_bytes=48 << 20),
        cost_estimate=pl.CostEstimate(flops=2 * len(blocks) * rows * model * width, bytes_accessed=2 * len(blocks) * rows * model, transcendentals=0),
    )(*blocks, lhs)


def rows_product_kernel(count, *refs):
    blocks, w_ref, out_ref, acc_ref = refs[:count], refs[count], refs[count + 1], refs[count + 2]
    step, rows = pl.program_id(0), blocks[0].shape[0]
    lhs = jnp.concatenate([blk[...] for blk in blocks], axis=0)
    part = dot_f32(lhs, w_ref[...], COLS_OF_BOTH)

    @pl.when(step == 0)
    def _():
        acc_ref[...] = part

    @pl.when(step > 0)
    def _():
        acc_ref[...] += part

    @pl.when(step == pl.num_programs(0) - 1)
    def _():
        for n in range(count):
            out_ref[n] = acc_ref[n * rows:(n + 1) * rows, :].astype(jnp.bfloat16)


def rows_product(blocks, weights, width):
    rows, model = blocks[0].shape
    tile = model // 4
    out_shape = (len(blocks), rows, width)
    return pl.pallas_call(
        functools.partial(rows_product_kernel, len(blocks)), out_shape=jax.ShapeDtypeStruct(out_shape, jnp.bfloat16), grid=(model // tile,),
        in_specs=[pl.BlockSpec((rows, tile), lambda i: (0, i))] * len(blocks) + [pl.BlockSpec((width, tile), lambda i: (0, i))],
        out_specs=pl.BlockSpec(out_shape, lambda i: (0, 0, 0)), scratch_shapes=[pltpu.VMEM((len(blocks) * rows, width), jnp.float32)],
        compiler_params=pltpu.CompilerParams(dimension_semantics=('arbitrary',), vmem_limit_bytes=40 << 20),
        cost_estimate=pl.CostEstimate(flops=2 * len(blocks) * rows * model * width, bytes_accessed=2 * (len(blocks) * rows + width) * model, transcendentals=0),
    )(*blocks, weights)


def pick_kernel(count, where_ref, *refs):
    sources, outs, sems = refs[:count * Z_SIZE], refs[count * Z_SIZE:-1], refs[-1]

    def copy(n, k):
        return pltpu.make_async_copy(sources[n * Z_SIZE + k], outs[n], sems.at[n])

    for n in range(count):
        for k in range(Z_SIZE):
            pl.when(where_ref[0] == k)(lambda n=n, k=k: copy(n, k).start())
    for n in range(count):
        copy(n, 0).wait()


def pick(where, *choices):
    shape = choices[0][0].shape
    return pl.pallas_call(
        functools.partial(pick_kernel, len(choices)), out_shape=[jax.ShapeDtypeStruct(shape, jnp.bfloat16)] * len(choices),
        grid_spec=pltpu.PrefetchScalarGridSpec(
            num_scalar_prefetch=1, grid=(1,), in_specs=[pl.BlockSpec(memory_space=pl.ANY)] * (len(choices) * Z_SIZE), out_specs=[full_spec(shape)] * len(choices),
            scratch_shapes=[pltpu.SemaphoreType.DMA((len(choices),))]),
        compiler_params=pltpu.CompilerParams(dimension_semantics=('arbitrary',), vmem_limit_bytes=32 << 20),
        cost_estimate=pl.CostEstimate(flops=1000000, bytes_accessed=8000000, transcendentals=0),
    )(where, *(arr for choice in choices for arr in choice))


def pair_add_kernel(a_ref, b_ref, c_ref, d_ref, ab_ref, cd_ref):
    for left, right, out in ((a_ref, b_ref, ab_ref), (c_ref, d_ref, cd_ref)):
        out[...] = (left[...].astype(jnp.float32) + right[...].astype(jnp.float32)).astype(jnp.bfloat16)


def pair_add(*operands):
    rows, model = operands[0].shape
    tile = model // 4
    spec = pl.BlockSpec((rows, tile), lambda i: (0, i))
    return pl.pallas_call(
        pair_add_kernel, out_shape=[jax.ShapeDtypeStruct((rows, model), jnp.bfloat16)] * 2, grid=(model // tile,), in_specs=[spec] * 4, out_specs=[spec] * 2,
        compiler_params=pltpu.CompilerParams(dimension_semantics=('arbitrary',), vmem_limit_bytes=32 << 20),
        cost_estimate=pl.CostEstimate(flops=4 * rows * model, bytes_accessed=12 * rows * model, transcendentals=0),
    )(*operands)


def finish_kernel(where_ref, mine_ref, other_ref, cos_ref, sin_ref, out_ref):
    for z in range(Z_SIZE):
        slot = lax.rem(where_ref[0] - z + Z_SIZE, Z_SIZE)
        for e in range(CORE_SIZE):
            total = mine_ref[z, e] + other_ref[z, e]
            dk = total[:, :HEAD_DIM].astype(jnp.bfloat16).astype(jnp.float32)
            out_ref[slot, e, :, :HEAD_DIM] = (dk * cos_ref[z, e] + pltpu.roll(dk, HEAD_DIM // 2, 1) * sin_ref[z, e]).astype(jnp.bfloat16)
            out_ref[slot, e, :, HEAD_DIM:] = total[:, HEAD_DIM:].astype(jnp.bfloat16)


def finish_key_grads(where, *operands):
    return pl.pallas_call(
        finish_kernel, out_shape=jax.ShapeDtypeStruct(operands[0].shape, jnp.bfloat16),
        grid_spec=pltpu.PrefetchScalarGridSpec(num_scalar_prefetch=1, grid=(1,), in_specs=[full_spec(arr.shape) for arr in operands], out_specs=full_spec(operands[0].shape)),
        compiler_params=pltpu.CompilerParams(dimension_semantics=('arbitrary',), vmem_limit_bytes=32 << 20),
        cost_estimate=pl.CostEstimate(flops=1000000, bytes_accessed=8000000, transcendentals=0),
    )(where, *operands)


def full_spec(shape):
    return pl.BlockSpec(shape, lambda b, *_: (0,) * len(shape))


def attend(where, positions, q_slots, kv_slots, kv_other, cos_t, sin_t, lo_all, bk):
    slots, bq, width = q_slots.shape
    seq = positions.shape[0]
    heads = width // HEAD_DIM
    lanes = heads * bq
    shared = (kv_slots, kv_other, cos_t, sin_t, lo_all)
    block = pl.BlockSpec((1, bq, width), lambda i, where_ref, _: (slot_of(where_ref, i // 2, i % 2), 0, 0))
    work = slots * bq * heads * seq * HEAD_DIM
    return pl.pallas_call(
        functools.partial(fwd_kernel, heads, bk),
        out_shape=(jax.ShapeDtypeStruct(q_slots.shape, jnp.bfloat16), jax.ShapeDtypeStruct((slots, 1, lanes), jnp.float32)),
        grid_spec=pltpu.PrefetchScalarGridSpec(
            num_scalar_prefetch=2, grid=(slots,), in_specs=[block] + [full_spec(arr.shape) for arr in shared],
            out_specs=(block, pl.BlockSpec((1, 1, lanes), lambda i, *_: (i, 0, 0))),
            scratch_shapes=[pltpu.VMEM((seq, HEAD_DIM), jnp.bfloat16), pltpu.VMEM((HEAD_DIM, seq), jnp.bfloat16), pltpu.VMEM((HEAD_DIM, lanes), jnp.bfloat16),
                            pltpu.VMEM((1, lanes), jnp.float32), pltpu.VMEM((1, lanes), jnp.float32), pltpu.VMEM((HEAD_DIM, lanes), jnp.float32)]),
        compiler_params=pltpu.CompilerParams(dimension_semantics=('arbitrary',), vmem_limit_bytes=48 << 20),
        cost_estimate=pl.CostEstimate(flops=4 * work, bytes_accessed=4 * slots * bq * width + 8 * seq * HEAD_DIM, transcendentals=work // (2 * HEAD_DIM)),
        name='attend_fwd',
    )(where, positions, q_slots, *shared)


def attend_backward(where, positions, q_slots, do_blocks, o_slots, kv_slots, kv_other, cos_t, sin_t, lo_all, lse, bk, rows_of_z, part=None):
    count, bq, width = do_blocks.shape
    seq = positions.shape[0]
    heads = width // HEAD_DIM
    lanes = heads * bq
    shared = (kv_slots, kv_other, cos_t, sin_t, lo_all)

    def slot_index(i, where_ref, _):
        return (slot_of(where_ref, *bwd_block(where_ref, i, rows_of_z)), 0, 0)

    def lse_index(i, where_ref, _):
        z_blk, c_blk = bwd_block(where_ref, i, rows_of_z)
        return (2 * z_blk + c_blk, 0, 0)

    block = pl.BlockSpec((1, bq, width), slot_index)
    local = pl.BlockSpec((1, bq, width), lambda i, *_: (i, 0, 0))
    operands = [q_slots, do_blocks, o_slots, *shared, lse]
    in_specs = [block, local, block] + [full_spec(arr.shape) for arr in shared] + [pl.BlockSpec((1, 1, lanes), lse_index)]
    part_shape, final_shape = (2 * HEAD_DIM, seq), (Z_SIZE, CORE_SIZE, bq, 2 * HEAD_DIM)
    grads = [part_shape] if part is None else [final_shape] * 2
    if part is not None:
        operands.append(part)
        in_specs.append(full_spec(part_shape))
    work = count * bq * heads * seq * HEAD_DIM
    return pl.pallas_call(
        functools.partial(bwd_kernel, heads, bk, rows_of_z),
        out_shape=[jax.ShapeDtypeStruct(do_blocks.shape, jnp.bfloat16)] + [jax.ShapeDtypeStruct(shape, jnp.float32) for shape in grads],
        grid_spec=pltpu.PrefetchScalarGridSpec(
            num_scalar_prefetch=2, grid=(count,), in_specs=in_specs, out_specs=[local] + [full_spec(shape) for shape in grads],
            scratch_shapes=[pltpu.VMEM((seq, HEAD_DIM), jnp.bfloat16), pltpu.VMEM((HEAD_DIM, seq), jnp.bfloat16), pltpu.VMEM((seq, HEAD_DIM), jnp.bfloat16),
                            pltpu.VMEM((HEAD_DIM, lanes), jnp.bfloat16), pltpu.VMEM((HEAD_DIM, lanes), jnp.bfloat16), pltpu.VMEM((HEAD_DIM, lanes), jnp.float32),
                            pltpu.VMEM((2 * HEAD_DIM, seq), jnp.float32)]),
        compiler_params=pltpu.CompilerParams(dimension_semantics=('arbitrary',), vmem_limit_bytes=58 << 20),
        cost_estimate=pl.CostEstimate(flops=10 * work, bytes_accessed=8 * count * bq * width + 24 * seq * HEAD_DIM, transcendentals=work // (2 * HEAD_DIM)),
        name='attend_bwd',
    )(where, positions, *operands)


def solution(mesh):
    def member(z, y, c):
        return (z * Y_SIZE + y) * CORE_SIZE + c

    every = [(z, y, c) for z in range(Z_SIZE) for y in range(Y_SIZE) for c in range(CORE_SIZE)]

    def permuter(target, senders=range(Z_SIZE)):
        pairs = [(member(*src), member(*target(*src))) for src in every if src[0] in senders]
        return lambda val: lax.ppermute(val, 'tp', pairs)

    swap_core = permuter(lambda z, y, c: (z, y, 1 - c))
    swap_y = permuter(lambda z, y, c: (z, 1 - y, c))
    swap_same_head = permuter(lambda z, y, c: (z, 1 - y, 1 - c))
    ring = permuter(lambda z, y, c: ((z + 1) % Z_SIZE, y, c))
    ring_back = permuter(lambda z, y, c: ((z - 1) % Z_SIZE, y, c))
    hops = range(1, Z_SIZE)
    gather_right = {k: permuter(lambda z, y, c: (z + 1, y, c), range(k - 1, Z_SIZE - 1)) for k in hops}
    gather_left = {k: permuter(lambda z, y, c: (z - 1, y, c), range(1, Z_SIZE - k + 1)) for k in hops}
    scatter_right = {k: permuter(lambda z, y, c: (z + 1, y, c), range(0, k)) for k in hops}
    scatter_left = {k: permuter(lambda z, y, c: (z - 1, y, c), range(Z_SIZE - k, Z_SIZE)) for k in hops}
    z_swaps = {k: permuter(lambda z, y, c, k=k: (z ^ k, y, c)) for k in hops}

    def after(val, *deps):
        return lax.optimization_barrier((val,) + deps)[0]

    def device_step(x_blk, dy_blk, pos_all, norm_gain, wq_loc, wk_all, wv_all, wo_loc):
        seq_len = pos_all.shape[0]
        bq = seq_len // (Z_SIZE * Y_SIZE * CORE_SIZE)
        bk = 2 * bq
        model = x_blk.shape[1]
        idx = lax.axis_index('tp')
        z_idx, y_idx, c_idx = idx // (Y_SIZE * CORE_SIZE), (idx // CORE_SIZE) % Y_SIZE, idx % CORE_SIZE
        where = jnp.stack([z_idx, y_idx, c_idx])
        on_core0 = c_idx == 0
        pair = wq_loc.shape[1]
        kv_own = Y_SIZE * z_idx + (y_idx ^ c_idx)

        def select(first, second):
            return jnp.where(on_core0, first, second)

        def flip_core(arr):
            return arr[:, ::-1]

        def slots(arrs):
            return jnp.concatenate([arr[None] for arr in arrs], axis=0)

        def interleave(own, partner):
            return [blk for both in zip(own, partner) for blk in both]

        x_f32 = x_blk.astype(jnp.float32)
        hidden, x_hat, inv_rms = norm_forward(x_f32, norm_gain)

        h_own = [hidden]
        for s in hops:
            h_own.append(ring(h_own[-1]))
        h_pair = []
        for blk in h_own:
            h_pair.append(swap_core(blk))

        def slot_order(w_own, w_core, w_y, w_both):
            return [select(w_own, w_y), select(w_core, w_both), select(w_both, w_core), select(w_y, w_own)]

        wq_y = swap_y(wq_loc)
        wq_core = swap_core(wq_loc)
        q_cols = slot_order(wq_loc, wq_core, wq_y, swap_core(wq_y))
        wo_y = swap_y(wo_loc)
        o_rows = (wo_loc, swap_core(wo_loc), wo_y, swap_core(wo_y))

        def kv_columns(head):
            return [lax.dynamic_slice_in_dim(w, head * HEAD_DIM, HEAD_DIM, axis=1) for w in (wk_all, wv_all)]

        w_q = lax.optimization_barrier(jnp.concatenate(q_cols, axis=1))
        w_kv = lax.optimization_barrier(jnp.concatenate(kv_columns(kv_own) + kv_columns(kv_own ^ 1), axis=1))
        kv_heads = [lax.rem(kv_own + k * Y_SIZE, Y_SIZE * Z_SIZE) for k in range(2)]
        w_kv_all = lax.optimization_barrier(jnp.concatenate([cols for head in kv_heads for h in (head, head ^ 1) for cols in kv_columns(h)], axis=1))
        w_own = jnp.concatenate([w_q[:, :2 * pair], w_kv[:, :2 * HEAD_DIM]], axis=1)
        w_mix = jnp.concatenate(slot_order(*o_rows), axis=0)
        lo_all = (lax.iota(jnp.int32, seq_len) - pos_all)[None, :]
        cos_t, sin_t = rope_tables(pos_all)

        def my_tables(lead, tail):
            parts = jnp.concatenate([lead.T, tail.T], axis=1).reshape(Z_SIZE, Y_SIZE, CORE_SIZE, bq, HEAD_DIM)
            parts = lax.dynamic_index_in_dim(parts, y_idx, 1, keepdims=False)
            return select(parts, flip_core(parts))

        cos_my, sin_my = my_tables(cos_t, cos_t), my_tables(sin_t, -sin_t)

        qkv = []
        for s in range(Z_SIZE):
            qkv += [dot_f32(blk, w_own).astype(jnp.bfloat16) for blk in (h_own[s], h_pair[s])]
        kv_blocks = [blk[:, 2 * pair:] for blk in qkv]
        early = SLOTS - CORE_SIZE
        kv_other_early = swap_same_head(slots(kv_blocks[:early]))
        kv_other_late = swap_same_head(slots(kv_blocks[early:]))
        kv_other = jnp.concatenate([kv_other_early, kv_other_late], axis=0)
        q_slots, kv_slots = slots([blk[:, :2 * pair] for blk in qkv]), slots(kv_blocks)

        g_own = []
        for s, blk in enumerate(h_own):
            g_own.append(swap_y(after(blk, kv_other_late) if s else blk))

        right, left = {0: after(dy_blk, h_own[-1])}, {}
        left[0] = right[0]
        for k in hops:
            right[k] = gather_right[k](right[k - 1])
            left[k] = gather_left[k](left[k - 1])
            right[k], left[k] = lax.optimization_barrier((right[k], left[k]))
        dy_one, dy_two = pick(where, (left[1], dy_blk, right[1], right[2]), (left[2], left[1], dy_blk, right[1]))
        dy_zero, dy_three = pick(where, (dy_blk, right[1], right[2], right[3]), (left[3], left[2], left[1], dy_blk))
        dy_own = [dy_zero, dy_one, dy_two, dy_three]
        dy_pair = []
        for blk in dy_own:
            dy_pair.append(swap_core(blk))
        dy_slots = interleave(dy_own, dy_pair)

        def mirrored(lines):
            return jnp.concatenate([lax.dynamic_slice_in_dim(lines, lax.rem(z_idx - s + Z_SIZE, Z_SIZE), 1, axis=0) for s in range(Z_SIZE)], axis=0)

        forward = functools.partial(attend, where, pos_all, q_slots, kv_slots, kv_other, cos_t, sin_t, lo_all, bk)
        o_slots, lse = forward()
        by_line = (Z_SIZE, CORE_SIZE, bq, -1)
        o_lines = o_slots.reshape(by_line)
        o_partner = swap_core(o_slots).reshape(by_line)
        o_mine = jnp.concatenate([o_lines[:, 0], o_partner[:, 1]], axis=-1)

        def pair_sides(own, partner):
            first, last = own[..., :pair], partner[..., pair:2 * pair]
            return select(first, last), select(last, first)

        def by_block(arr):
            return arr.reshape((SLOTS,) + arr.shape[2:])

        o_sides = jnp.concatenate(pair_sides(o_lines, flip_core(o_partner)), axis=-1)
        o_sides = lax.optimization_barrier(by_block(mirrored(o_sides)))
        mix_part = []
        for s in range(Z_SIZE):
            mix_part.append(lax.optimization_barrier(dot_f32(o_mine[s], w_mix).astype(jnp.bfloat16)))

        def plus(*parts):
            return sum(part.astype(jnp.float32) for part in parts)

        sum_right, sum_left = mix_part[1], mix_part[Z_SIZE - 1]
        for k in hops:
            if k > 1:
                sum_right, sum_left = lax.optimization_barrier((sum_right, sum_left))
                sum_right, sum_left = pair_add(mix_part[k], sum_right, mix_part[Z_SIZE - k], sum_left)
            sum_right = scatter_right[k](sum_right)
            sum_left = scatter_left[k](sum_left)
        result = (x_f32 + plus(mix_part[0], sum_right, sum_left)).astype(jnp.bfloat16)

        def output_grads(rows_of_z):
            return rows_product([blks[n] for n in rows_of_z for blks in (dy_own, dy_pair)], w_mix, 2 * pair)

        do_early = output_grads(EARLY)
        do_late = output_grads(LATE)
        shared = (o_slots, kv_slots, kv_other, cos_t, sin_t, lo_all, lse, bk)
        dq_early, dkv_part = attend_backward(where, pos_all, q_slots, do_early, *shared, EARLY)

        def other_order(arr):
            lines = arr.reshape((2, CORE_SIZE) + arr.shape[1:])
            return jnp.concatenate([lines[:, 1:], lines[:, :1]], axis=1).reshape(arr.shape)

        dq_early_partner = swap_core(dq_early)
        early_own, early_partner = lax.optimization_barrier((dq_early, dq_early_partner))
        early_keep, early_send = pair_sides(early_own, other_order(early_partner))
        early_theirs = swap_y(early_send)
        dq_late, dkv_mine, dkv_send = attend_backward(where, pos_all, q_slots, do_late, *shared, LATE, dkv_part)
        dkv_theirs = swap_same_head(dkv_send)
        dq_late_partner = swap_core(dq_late)

        late_keep, late_send = pair_sides(dq_late, other_order(dq_late_partner))

        def natural(early, late):
            return jnp.concatenate([late[:2], early, late[2:]], axis=0).reshape((Z_SIZE, CORE_SIZE) + early.shape[1:])

        q_rows = lax.optimization_barrier(jnp.concatenate([natural(dq_early, dq_late)[:, 0], natural(early_partner, dq_late_partner)[:, 1]], axis=-1))
        dq_rows = [lax.dynamic_index_in_dim(q_rows, lax.rem(z_idx - s + Z_SIZE, Z_SIZE), 0, keepdims=False) for s in range(Z_SIZE)]
        halves = [slice(0, model // 2), slice(model // 2, model)]

        def first_rows(early, late, e):
            pick_row = functools.partial(lax.dynamic_index_in_dim, axis=0, keepdims=False)
            return jnp.where(z_idx < 2, pick_row(late, jnp.clip(2 - 2 * z_idx, 0, 2) + e), pick_row(early, jnp.clip(2 * z_idx - 4, 0, 2) + e))

        first = jnp.concatenate([first_rows(dq_early, dq_late, 0), first_rows(early_partner, dq_late_partner, 1)], axis=-1)
        dh_sum = []
        for n, cols in enumerate(halves):
            dh_sum.append(dot_f32(first, w_q[cols], COLS_OF_BOTH).astype(jnp.bfloat16))
            dh_sum[n] = ring(dh_sum[n])

        dkv_lines = finish_key_grads(where, dkv_mine, dkv_theirs, cos_my, sin_my)
        dkv_partner = flip_core(swap_core(dkv_lines))
        dkv_rows = jnp.concatenate([dkv_lines[:, 0], dkv_partner[:, 0]], axis=-1)
        dkv_next = ring_back(dkv_rows[1])

        def kv_part(rows, weights, cols):
            return dot_f32(rows, weights[cols], COLS_OF_BOTH)

        for s in hops[1:]:
            for n, cols in enumerate(halves):
                part = dot_f32(dq_rows[s], w_q[cols], COLS_OF_BOTH) + kv_part(dkv_rows[s], w_kv, cols)
                dh_sum[n] = (part + dh_sum[n].astype(jnp.float32)).astype(jnp.bfloat16)
                if s == hops[-1] and n == 0:
                    dh_sum[n], result = lax.optimization_barrier((dh_sum[n], result))
                dh_sum[n] = ring(dh_sum[n])
        g_pair = [swap_core(blk) for blk in lax.optimization_barrier((*g_own, dq_late))[:Z_SIZE]]
        kv_keep = select(dkv_lines[..., :HEAD_DIM], dkv_partner[..., HEAD_DIM:])
        kv_send = select(dkv_partner[..., :HEAD_DIM], dkv_lines[..., HEAD_DIM:])
        kv_theirs = swap_y(kv_send)
        late_theirs = swap_y(late_send)

        def rows_of(early, late, kv_lines):
            return by_block(jnp.concatenate([mirrored(natural(early, late)), kv_lines], axis=-1))

        d_keep = rows_of(early_keep, late_keep, kv_keep)
        d_theirs = rows_of(early_theirs, late_theirs, kv_theirs)

        f32, tile = jnp.float32, min(512, model // 2)
        dwo_keep, send_first, send_last = token_grads(dy_slots, o_sides, [(0, pair, WHOLE, f32), (pair, pair, FIRST_HALF, f32), (pair, pair, LAST_HALF, f32)], tile)
        theirs_first = swap_y(send_first)
        theirs_last = swap_y(send_last)

        d_wq, kv_mine_sum = token_grads([blks[s] for mine, theirs in ((h_own, h_pair), (g_own, g_pair)) for s in range(Z_SIZE) for blks in (mine, theirs)], jnp.concatenate([d_keep, d_theirs], axis=0),
                                        [(0, pair, TOKENS, jnp.bfloat16), (pair, HEAD_DIM, TOKENS, f32)], tile)
        kv_other_sum = swap_core(kv_mine_sum)
        d_wk = select(kv_mine_sum, kv_other_sum)
        d_wv = select(kv_other_sum, kv_mine_sum)

        dh_own = lax.optimization_barrier([dot_f32(dq_rows[0], w_q[cols], COLS_OF_BOTH) for cols in halves])
        kv_cols = jnp.concatenate([dkv_rows[0], after(dkv_next, kv_mine_sum)], axis=1)
        dh_own = lax.optimization_barrier([own + kv_part(kv_cols, w_kv_all, cols) for own, cols in zip(dh_own, halves)])
        dh_rows = jnp.concatenate([(own + part.astype(jnp.float32)).astype(jnp.bfloat16) for own, part in zip(dh_own, dh_sum)], axis=1)

        d_input, dg_part = norm_backward(dh_rows, x_hat, inv_rms, norm_gain)
        grad_x = (dy_blk.astype(jnp.float32) + d_input).astype(jnp.bfloat16)
        for near, far, both in ((swap_core, swap_y, swap_same_head), (z_swaps[1], z_swaps[2], z_swaps[3])):
            dg_part = (dg_part + near(dg_part)) + (far(dg_part) + both(dg_part))
            if near is swap_core:
                theirs_last = after(theirs_last, dg_part)
        d_wo = (dwo_keep + jnp.concatenate([theirs_first, theirs_last], axis=1)).astype(jnp.bfloat16)
        return result, grad_x, d_wq, d_wk, d_wv, d_wo, dg_part

    specs_in = (P(('dp', 'tp'), None), P(('dp', 'tp'), None), P('dp'), P(), P(None, 'tp'), P(), P(), P('tp', None))
    specs_out = (P(('dp', 'tp'), None), P(('dp', 'tp'), None), P('dp', 'tp'), P('dp', 'tp'), P('dp', 'tp'), P(('dp', 'tp'), None), P('dp'))
    return jax.shard_map(device_step, mesh=mesh, in_specs=specs_in, out_specs=specs_out, check_vma=False)
```
